32 devices in a mesh: fsdp: 8 (over y, x, core), tp: 4 (over z).
Axes of the slice: x: 2, y: 2, z: 4, core: 2. Of those that a mesh axis runs over, the one named last changes fastest.
Arguments:
- emb: bfloat16 [8192, 1536], P(('fsdp', 'tp')), may hold values from -0.5 to 0.5
- segment_ids: int32 [16, 512], P('fsdp'), may hold values from 0 to 3, never falling along the last dimension, each value on 1 to 256 neighbouring positions
- routes: int32 [8192, 8], P('fsdp'), may hold values from 0 to 39, all different within a row; in each aligned block of 1024 rows (0 to 1023, 1024 to 2047, ...) at most 408 rows name the same one
- norm1_gain: bfloat16 [1536], replicated, may hold values from 0.5 to 1.5
- w_query: bfloat16 [1536, 1536], P('fsdp', 'tp'), may hold values from -0.625 to 0.625
- w_key: bfloat16 [1536, 512], P('fsdp', 'tp'), may hold values from -0.625 to 0.625
- w_value: bfloat16 [1536, 512], P('fsdp', 'tp'), may hold values from -0.15625 to 0.15625
- w_out: bfloat16 [1536, 1536], P('fsdp', 'tp'), may hold values from -1.25 to 1.25
- norm2_gain: bfloat16 [1536], replicated, may hold values from 0.5 to 1.5
- w_router: bfloat16 [1536, 40], P('fsdp'), may hold values from -0.15625 to 0.15625
- w_gate: bfloat16 [40, 1536, 512], P('tp', 'fsdp'), may hold values from -0.15625 to 0.15625
- w_up: bfloat16 [40, 1536, 512], P('tp', 'fsdp'), may hold values from -0.15625 to 0.15625
- w_down: bfloat16 [40, 1536, 512], P('tp', 'fsdp'), may hold values from -3 to 3
- cotangent: bfloat16 [8192, 1536], P(('fsdp', 'tp')), may hold values from -6 to 6
Outputs:
- out: bfloat16 [8192, 1536], P(('fsdp', 'tp'))
- grad_emb: float32 [8192, 1536], P(('fsdp', 'tp'))
- grad_norm1_gain: float32 [1536], replicated
- grad_w_query: float32 [1536, 1536], P('fsdp', 'tp')
- grad_w_key: float32 [1536, 512], P('fsdp', 'tp')
- grad_w_value: float32 [1536, 512], P('fsdp', 'tp')
- grad_w_out: float32 [1536, 1536], P('fsdp', 'tp')
- grad_norm2_gain: float32 [1536], replicated
- grad_w_router: float32 [1536, 40], P('fsdp')
- grad_w_gate: float32 [40, 1536, 512], P('tp', 'fsdp')
- grad_w_up: float32 [40, 1536, 512], P('tp', 'fsdp')
- grad_w_down: float32 [40, 1536, 512], P('tp', 'fsdp')
The draws below stay inside these ranges and needn't reach their ends.
Inputs may be any that keep to these rules, and one draw needn't show every extreme that they name: `routes`: in each aligned block of 1024 rows no expert is named by more than 408 rows, a bound that some block reaches. `segment_ids`: along a sequence the numbers never fall; a document spans at most 256 tokens, and one spans exactly 256.
All inputs are finite; a program needn't handle non-finite values.
Results may differ from the reference program's by a relative error of at most 0.015.
Values may be sent and summed in bfloat16 or wider, within the bound.
A program may use at most 384 MiB of HBM per device.

```python
import math
from functools import partial
import jax
import jax.numpy as jnp
import numpy as np
from jax import lax

D = 1536
HEADS = 24
KV_HEADS = 8
HEAD_DIM = 64
EXPERTS = 40
FF = 512
TOP = 8
SEQ = 512
SEGS = 4
SEG_MOST = 256
GROUP = 1024
TOKENS = 8192
SEQS = 16
CAP = 408


def spiked(values, key, source, target, shards_of, factor):
    owner, partner = [(jnp.arange(values.shape[axis_at]) // (values.shape[axis_at] // shards_of)).reshape([-1 if axis == axis_at else 1 for axis in range(values.ndim)]) for axis_at in (source, target)]
    chosen = jax.random.permutation(key, shards_of)[partner]
    strong = (owner == chosen) | (owner == (partner + shards_of // 2) % shards_of)
    return jnp.where(strong, factor * values, values)


def levels(key, dims, shards, least, largest):
    gain = 1.0
    for position, shards_of in shards:
        heights = jax.random.uniform(jax.random.fold_in(jax.random.fold_in(key, 6), position), (shards_of,), jnp.float32, least / len(shards), largest / len(shards))
        gain = gain * jnp.repeat(jnp.exp(heights), dims[position] // shards_of).reshape((-1,) + (1,) * (len(dims) - 1 - position))
    return gain


def split_up(number_of, total, limit, lean):
    weights = [(1 << 20) // math.isqrt(grade ** lean) + 1 for grade in range(2, number_of + 1)]
    spare, holding = total - limit - (number_of - 1), [1] * (number_of - 1)
    while spare > 0:
        free = [i for i in range(number_of - 1) if holding[i] < limit]
        whole, left = sum([weights[i] for i in free]), spare
        for i in free:
            addition = min(limit - holding[i], max(1, left * weights[i] // whole), spare)
            holding[i] = holding[i] + addition
            spare = spare - addition
    return np.array([limit] + holding)


def ragged(own_key, count, total, limit, slope):
    if count == 2:
        one = jax.random.randint(own_key, (), max(1, total - limit), min(limit, total - 1) + 1)
        return jnp.stack([one, total - one])
    tallies = jnp.asarray(split_up(count, total, limit, slope), jnp.int32)
    twos = (count - 1) // 2
    source_of, taker = tallies[1:1 + 2 * twos:2], tallies[2:2 + 2 * twos:2]
    slack = jnp.minimum(source_of - 1, limit - taker)
    passed = jax.random.randint(jax.random.fold_in(own_key, 1), (twos,), 0, 1 << 20) % (slack + 1)
    tallies = tallies.at[1:1 + 2 * twos:2].set(source_of - passed).at[2:2 + 2 * twos:2].set(taker + passed)
    return tallies[jax.random.permutation(jax.random.fold_in(own_key, 2), count)]


def deal_out(rng, own, number, rows, amount, top, most, skew):
    sequence = jax.random.permutation(rng, amount)
    crowded, common = load_shares(amount, rows * top, most, skew, True), load_shares(amount, rows * top, most, skew, False)
    places = jnp.arange(amount)

    def named(tallies, offset_by):
        used = int((tallies > 0).sum())
        fixed = max(1, used // 4)
        moved = fixed + (places - fixed + offset_by * (used - fixed)) % max(1, amount - fixed)
        return jnp.zeros((amount,), jnp.int32).at[sequence[jnp.where(places < fixed, places, moved)]].set(jnp.asarray(tallies, jnp.int32))

    tallies = jnp.where(number % 4 == 0, named(crowded, number // 4), named(common, number - number // 4 - 1))
    mixed = jax.random.permutation(jax.random.fold_in(own, 3), amount)
    donor, sink = mixed[0:amount // 2 * 2:2], mixed[1:amount // 2 * 2:2]
    margin = jnp.minimum(tallies[donor] - 1, most - tallies[sink]) // 2
    margin = jnp.where((donor == sequence[0]) | (sink == sequence[0]) | (tallies[sink] == 0), 0, jnp.maximum(margin, 0))
    moved = jax.random.randint(jax.random.fold_in(own, 4), (amount // 2,), 0, 1 << 20) % (margin + 1)
    tallies = tallies.at[donor].add(-moved).at[sink].add(moved)
    labels = jnp.searchsorted(jnp.cumsum(tallies), jnp.arange(rows * top), side="right").astype(jnp.int32)
    table = labels.reshape(top, rows).T
    table = table[jax.random.permutation(jax.random.fold_in(own, 1), rows)]
    offset_by = jax.random.randint(jax.random.fold_in(own, 2), (rows, 1), 0, top)
    return jnp.take_along_axis(table, (jnp.arange(top)[None, :] + offset_by) % top, axis=1)


def load_shares(amount, total, bound, skew, full):
    weights = [(1 << 20) // math.isqrt(standing ** skew) + 1 for standing in range(1, amount + 1)]
    largest = bound if full else min(bound, max(-(-total // amount), total * weights[0] // sum(weights)))
    least = 1 if total - largest >= amount - 1 else 0
    given, surplus = [largest] + [least] * (amount - 1), total - largest - least * (amount - 1)
    while surplus > 0:
        movable = [i for i in range(1, amount) if given[i] < largest] or [i for i in range(1, amount) if given[i] < bound]
        mass, left = sum([weights[i] for i in movable]), surplus
        for i in movable:
            more = min(bound - given[i], max(1, left * weights[i] // mass), surplus)
            given[i] = given[i] + more
            surplus = surplus - more
    return np.array(given)


def scatter_about(rng, extent, deviation, limit, cuts=(), kind=jnp.bfloat16):
    loudness = levels(rng, extent, cuts, -0.22, 0.18) if cuts else 1.0
    drawn = jax.random.normal(rng, extent, jnp.float32) * deviation * loudness
    return jnp.minimum(jnp.maximum(drawn, -limit), limit).astype(kind)


def noise_with(key, dims, scale, bound, cuts, heavy, dtype=jnp.bfloat16):
    values = scale * jax.random.normal(key, dims, jnp.float32)
    if cuts:
        values = values * levels(key, dims, cuts, -0.22, 0.18)
    return jnp.clip(spiked(values, jax.random.fold_in(key, 3), *heavy), -bound, bound).astype(dtype)


def setup_inputs(seed: int = 0) -> dict:
    streams_of = jax.random.split(jax.random.key(seed), 15)
    emb = noise_with(streams_of[0], (TOKENS, D), 0.083, 0.5, ((0, 32),), (0, 1, 32, 2.75))
    segment_ids = jax.vmap(lambda own: jnp.searchsorted(jnp.cumsum(ragged(own, SEGS, SEQ, SEG_MOST, 1)), jnp.arange(SEQ), side="right"))(jax.random.split(streams_of[1], SEQS)).reshape((SEQS, SEQ)).astype(jnp.int32)
    routes_keys = jax.random.split(jax.random.fold_in(streams_of[2], 1), TOKENS // GROUP)
    routes_turns = jax.random.permutation(jax.random.fold_in(streams_of[2], 3), TOKENS // GROUP)
    routes = jax.vmap(lambda own, number: deal_out(jax.random.fold_in(streams_of[2], 2), own, number, GROUP, EXPERTS, TOP, CAP, 1))(routes_keys, routes_turns).reshape((TOKENS, TOP))
    norm1_gain = jnp.clip(1.0 + 0.1 * jax.random.normal(streams_of[3], (D,), jnp.float32), 0.5, 1.5).astype(jnp.bfloat16)
    w_query = scatter_about(streams_of[4], (D, HEADS * HEAD_DIM), (D // 16) ** -0.5, 0.625, ((0, 8), (1, 4)))
    w_key = scatter_about(streams_of[5], (D, KV_HEADS * HEAD_DIM), (D // 16) ** -0.5, 0.625, ((0, 8), (1, 4)))
    w_value = scatter_about(streams_of[6], (D, KV_HEADS * HEAD_DIM), D ** -0.5, 0.15625, ((0, 8), (1, 4)))
    w_out = scatter_about(streams_of[7], (D, HEADS * HEAD_DIM), (HEADS * HEAD_DIM // 64) ** -0.5, 1.25, ((0, 8), (1, 4)))
    norm2_gain = jnp.clip(1.0 + 0.1 * jax.random.normal(streams_of[8], (D,), jnp.float32), 0.5, 1.5).astype(jnp.bfloat16)
    w_router = scatter_about(streams_of[9], (D, EXPERTS), D ** -0.5, 0.15625, ((0, 8),))
    w_gate = scatter_about(streams_of[10], (EXPERTS, D, FF), D ** -0.5, 0.15625, ((0, 4), (1, 8)))
    w_up = scatter_about(streams_of[11], (EXPERTS, D, FF), D ** -0.5, 0.15625, ((0, 4), (1, 8)))
    w_down = scatter_about(streams_of[12], (EXPERTS, D, FF), (max(FF // 128, 1)) ** -0.5, 3.0, ((0, 4), (1, 8)))
    cotangent = scatter_about(streams_of[13], (TOKENS, D), 1.0, 6.0, ((0, 32),))
    return dict(emb=emb, segment_ids=segment_ids, routes=routes, norm1_gain=norm1_gain, w_query=w_query, w_key=w_key, w_value=w_value, w_out=w_out, norm2_gain=norm2_gain, w_router=w_router, w_gate=w_gate, w_up=w_up, w_down=w_down, cotangent=cotangent)


emb_scale = 12.0
resid_scale = 0.22
attn_scale = 0.015625
norm_eps = 1e-06
rope_base = 10000.0
masked_value = -1e+30

@jax.custom_vjp
def low(v):
    return lax.optimization_barrier(v.astype(jnp.bfloat16)).astype(jnp.float32)

@jax.custom_vjp
def low_back(v):
    return v

def low_keep(v):
    return (low(v), None)

def low_pass(kept, grad):
    return (grad,)

def back_keep(v):
    return (v, None)

def back_low(kept, grad):
    return (low(grad),)
low.defvjp(low_keep, low_pass)
low_back.defvjp(back_keep, back_low)

def matmul(left_op, right_op):
    return jnp.dot(left_op, right_op, precision=lax.Precision.HIGHEST, preferred_element_type=jnp.float32)

def rms_norm(values, gain_vec):
    return values * lax.rsqrt(lax.optimization_barrier(jnp.mean(values * values, axis=-1, keepdims=True)) + norm_eps) * gain_vec

def rotary_tables(row_count, head_width):
    half_width = head_width // 2
    positions = (jnp.arange(row_count) % SEQ).astype(jnp.float32)
    frequency = rope_base ** (-jnp.arange(half_width).astype(jnp.float32) * 2.0 / head_width)
    angles = positions[:, None] * frequency[None, :]
    return (jnp.cos(angles)[:, None, :], jnp.sin(angles)[:, None, :])

def rotate(values, cosine_table, sine_table):
    half_width = values.shape[-1] // 2
    lead_half = values[..., :half_width]
    tail_half = values[..., half_width:]
    return jnp.concatenate([lead_half * cosine_table - tail_half * sine_table, tail_half * cosine_table + lead_half * sine_table], axis=-1)

def softmax_rows(scores):
    row_top = lax.optimization_barrier(jnp.max(scores, axis=-1, keepdims=True))
    raised = jnp.exp(scores - row_top)
    return raised / lax.optimization_barrier(jnp.sum(raised, axis=-1, keepdims=True))

def attend_group(pieces):
    queries, key_rows, value_rows, segments = pieces
    seq_count = queries.shape[0]
    grouped = queries.reshape(seq_count, SEQ, KV_HEADS, HEADS // KV_HEADS, HEAD_DIM)
    scores = jnp.einsum('nqkgd,ntkd->nkgqt', grouped, key_rows, precision=lax.Precision.HIGHEST) * attn_scale
    scores = low_back(scores)
    places = jnp.arange(SEQ)
    causal = places[:, None] >= places[None, :]
    allowed = causal[None, :, :] & (segments[:, :, None] == segments[:, None, :])
    scores = jnp.where(allowed[:, None, None, :, :], scores, masked_value)
    attn_probs = low(softmax_rows(scores))
    mixed_out = jnp.einsum('nkgqt,ntkd->nqkgd', attn_probs, value_rows, precision=lax.Precision.HIGHEST)
    return mixed_out.reshape(seq_count, SEQ, HEADS * HEAD_DIM)

def experts_group(pieces, gate_w, up_w, down_w):
    normed_rows, combine = pieces
    gate_pre = low_back(jnp.einsum('td,edf->etf', normed_rows, gate_w, precision=lax.Precision.HIGHEST))
    up_pre = low_back(jnp.einsum('td,edf->etf', normed_rows, up_w, precision=lax.Precision.HIGHEST))
    activated = low(gate_pre * jax.nn.sigmoid(gate_pre) * up_pre)
    expert_out = low_back(jnp.einsum('etf,edf->etd', activated, down_w, precision=lax.Precision.HIGHEST))
    return jnp.einsum('etd,te->td', expert_out, combine, precision=lax.Precision.HIGHEST)

def reference(emb, segment_ids, routes, norm1_gain, w_query, w_key, w_value, w_out, norm2_gain, w_router, w_gate, w_up, w_down, cotangent):
    group_count = TOKENS // GROUP
    per_group = GROUP // SEQ

    def forward(emb_in, gain_one, query_w, key_w, value_w, out_w, gain_two, router_w, gate_w, up_w, down_w):
        start_x = emb_scale * emb_in
        normed_one = low(rms_norm(start_x, gain_one))
        query_proj = low_back(matmul(normed_one, query_w))
        key_proj = low_back(matmul(normed_one, key_w))
        value_proj = low(low_back(matmul(normed_one, value_w)))
        cosine_table, sine_table = rotary_tables(TOKENS, HEAD_DIM)
        queries = low(rotate(query_proj.reshape(TOKENS, HEADS, HEAD_DIM), cosine_table, sine_table))
        key_rows = low(rotate(key_proj.reshape(TOKENS, KV_HEADS, HEAD_DIM), cosine_table, sine_table))
        mixed_out = lax.map(jax.checkpoint(attend_group), (queries.reshape(group_count, per_group, SEQ, HEADS, HEAD_DIM), key_rows.reshape(group_count, per_group, SEQ, KV_HEADS, HEAD_DIM), value_proj.reshape(group_count, per_group, SEQ, KV_HEADS, HEAD_DIM), segment_ids.reshape(group_count, per_group, SEQ)))
        mixed_rows = low(low_back(mixed_out.reshape(TOKENS, HEADS * HEAD_DIM)))
        attn_branch = low_back(matmul(mixed_rows, out_w.T))
        mid_x = start_x + resid_scale * attn_branch
        normed_two = low(rms_norm(mid_x, gain_two))
        logits = low_back(matmul(normed_two, router_w))
        chosen = (routes[:, :, None] == jnp.arange(EXPERTS)[None, None, :]).astype(jnp.float32)
        selected = lax.optimization_barrier(jnp.sum(chosen * logits[:, None, :], axis=-1))
        gates = low(softmax_rows(selected))
        combine = lax.optimization_barrier(jnp.sum(chosen * gates[:, :, None], axis=1))
        moe_out = lax.map(jax.checkpoint(partial(experts_group, gate_w=gate_w, up_w=up_w, down_w=down_w)), (normed_two.reshape(group_count, GROUP, D), combine.reshape(group_count, GROUP, EXPERTS)))
        moe_out = low_back(moe_out.reshape(TOKENS, D))
        return mid_x + resid_scale * moe_out
    floats = tuple((operand.astype(jnp.float32) for operand in (emb, norm1_gain, w_query, w_key, w_value, w_out, norm2_gain, w_router, w_gate, w_up, w_down)))
    result, pullback = jax.vjp(forward, *floats)
    grads = pullback(cotangent.astype(jnp.float32))
    return (result.astype(jnp.bfloat16), grads[0], grads[1], grads[2], grads[3], grads[4], grads[5], grads[6], grads[7], grads[8], grads[9], grads[10])
```

```python
import functools

import jax
import jax.numpy as jnp
from jax import lax
from jax.experimental import pallas as pl
from jax.experimental.pallas import tpu as pltpu
from jax.sharding import PartitionSpec as P

HEAD_DIM = 64
SEQ = 512


emb_scale = 12.0
resid_scale = 0.22
attn_scale = 0.015625
norm_eps = 1e-06
rope_base = 10000.0
masked_value = -1e30


def contract_last(left_op, right_op):
    return lax.dot_general(
        left_op, right_op, (((1,), (1,)), ((), ())), preferred_element_type=jnp.float32
    )


def contract_first(left_op, right_op):
    return lax.dot_general(
        left_op, right_op, (((0,), (0,)), ((), ())), preferred_element_type=jnp.float32
    )


def rms_forward(values, gain_vec):
    inverse = lax.rsqrt(jnp.mean(values * values, axis=-1, keepdims=True) + norm_eps)
    return (values * inverse * gain_vec, inverse)


def rms_backward(incoming, values, inverse, gain_vec):
    scaled = values * inverse
    gain_grad = jnp.sum(incoming * scaled, axis=0)
    weighted = incoming * gain_vec
    row_inner = jnp.mean(weighted * scaled, axis=-1, keepdims=True)
    return (inverse * (weighted - scaled * row_inner), gain_grad)


def rotary_tables(row_count, head_width):
    half_width = head_width // 2
    positions = (jnp.arange(row_count) % SEQ).astype(jnp.float32)
    frequency = rope_base ** (-jnp.arange(half_width).astype(jnp.float32) * 2.0 / head_width)
    angles = positions[:, None] * frequency[None, :]
    return (jnp.cos(angles)[:, None, :], jnp.sin(angles)[:, None, :])


def rotate(values, cosine_table, sine_table):
    half_width = values.shape[-1] // 2
    lead_half = values[..., :half_width]
    tail_half = values[..., half_width:]
    return jnp.concatenate(
        [
            lead_half * cosine_table - tail_half * sine_table,
            tail_half * cosine_table + lead_half * sine_table,
        ],
        axis=-1,
    )


def attention_scores(queries, key_rows, segments):
    length, heads_here, head_width = queries.shape
    kv_here = key_rows.shape[1]
    grouped = queries.reshape(length, kv_here, heads_here // kv_here, head_width)
    scores = (
        jnp.einsum("qkgd,tkd->kgqt", grouped, key_rows, preferred_element_type=jnp.float32)
        * attn_scale
    )
    places = jnp.arange(length)
    allowed = (places[:, None] >= places[None, :]) & (segments[:, None] == segments[None, :])
    return (jnp.where(allowed, scores, masked_value), grouped)


def attend_forward(pieces):
    queries, key_rows, value_rows, segments = pieces
    scores, grouped = attention_scores(queries, key_rows, segments)
    row_top = jnp.max(scores, axis=-1, keepdims=True)
    raised = jnp.exp(scores - row_top)
    row_total = jnp.sum(raised, axis=-1, keepdims=True)
    probs_low = (raised / row_total).astype(jnp.bfloat16)
    mixed_out = jnp.einsum(
        "kgqt,tkd->qkgd", probs_low, value_rows, preferred_element_type=jnp.float32
    )
    return (
        mixed_out.astype(jnp.bfloat16).reshape(queries.shape[0], -1),
        (row_top + jnp.log(row_total))[..., 0],
    )


def attend_backward(pieces):
    queries, key_rows, value_rows, segments, logsum, mixed_grad = pieces
    scores, grouped = attention_scores(queries, key_rows, segments)
    attn_probs = jnp.exp(scores - logsum[..., None])
    grad_grouped = mixed_grad.reshape(grouped.shape)
    probs_grad = jnp.einsum(
        "qkgd,tkd->kgqt", grad_grouped, value_rows, preferred_element_type=jnp.float32
    )
    row_inner = jnp.sum(attn_probs * probs_grad, axis=-1, keepdims=True)
    score_grad = (attn_probs * (probs_grad - row_inner)).astype(jnp.bfloat16)
    query_grad = (
        jnp.einsum("kgqt,tkd->qkgd", score_grad, key_rows, preferred_element_type=jnp.float32)
        * attn_scale
    )
    key_grad = (
        jnp.einsum("kgqt,qkgd->tkd", score_grad, grouped, preferred_element_type=jnp.float32)
        * attn_scale
    )
    value_grad = jnp.einsum(
        "kgqt,qkgd->tkd",
        attn_probs.astype(jnp.bfloat16),
        grad_grouped,
        preferred_element_type=jnp.float32,
    )
    return (query_grad.reshape(queries.shape), key_grad, value_grad)


def line_barrier(me, count):
    barrier = pltpu.get_barrier_semaphore()

    @pl.when(me > 0)
    def _():
        pl.semaphore_signal(barrier, inc=1, device_id={"tp": me - 1})

    @pl.when(me < count - 1)
    def _():
        pl.semaphore_signal(barrier, inc=1, device_id={"tp": me + 1})

    pl.semaphore_wait(barrier, jnp.where((me > 0) & (me < count - 1), 2, 1))


def line_gather_kernel(count, x_ref, o_ref, send_sem, recv_sem, own_sem):
    rows = x_ref.shape[0]
    me = lax.axis_index("tp")
    line_barrier(me, count)

    def part(chunk):
        return o_ref.at[pl.ds(pl.multiple_of(chunk * rows, rows), rows)]

    def hop(way, step, chunk):
        return pltpu.make_async_remote_copy(
            src_ref=x_ref if step == 0 else part(chunk),
            dst_ref=part(chunk),
            send_sem=send_sem.at[way, step],
            recv_sem=recv_sem.at[way, step],
            device_id={"tp": me + 1 if way == 0 else me - 1},
        )

    own = pltpu.make_async_copy(x_ref, part(me), own_sem)
    sends = [[(me >= step) & (me < count - 1) for step in range(count - 1)],
             [(me + step < count) & (me > 0) for step in range(count - 1)]]
    gets = [[me - 1 - step >= 0 for step in range(count - 1)],
            [me + 1 + step < count for step in range(count - 1)]]
    for step in range(count - 1):

        @pl.when(sends[0][step])
        def _():
            hop(0, step, me - step).start()

        @pl.when(sends[1][step])
        def _():
            hop(1, step, me + step).start()

        if step == 0:
            own.start()

        @pl.when(gets[0][step])
        def _():
            hop(0, step, me - 1 - step).wait_recv()

        @pl.when(gets[1][step])
        def _():
            hop(1, step, me + 1 + step).wait_recv()

    own.wait()
    for step in range(count - 1):

        @pl.when(sends[0][step])
        def _():
            hop(0, step, me - step).wait_send()

        @pl.when(sends[1][step])
        def _():
            hop(1, step, me + step).wait_send()


def line_gather(rows_in, count, ident):
    rows, width = rows_in.shape
    return pl.pallas_call(
        functools.partial(line_gather_kernel, count),
        out_shape=jax.ShapeDtypeStruct((rows * count, width), rows_in.dtype),
        in_specs=[pl.BlockSpec(memory_space=pltpu.VMEM)],
        out_specs=pl.BlockSpec(memory_space=pl.ANY),
        scratch_shapes=[
            pltpu.SemaphoreType.DMA((2, count - 1)),
            pltpu.SemaphoreType.DMA((2, count - 1)),
            pltpu.SemaphoreType.DMA,
        ],
        compiler_params=pltpu.CompilerParams(collective_id=ident, has_side_effects=True),
        cost_estimate=pl.CostEstimate(flops=0, transcendentals=0, bytes_accessed=150_000_000),
    )(rows_in)


def line_scatter_kernel(count, x_ref, o_ref, recv, send, send_sem, recv_sem):
    rows = o_ref.shape[0]
    me = lax.axis_index("tp")
    line_barrier(me, count)

    def block(dest):
        return x_ref[pl.ds(pl.multiple_of(dest * rows, rows), rows), :].astype(jnp.float32)

    def hop(way, step):
        return pltpu.make_async_remote_copy(
            src_ref=send.at[way, step],
            dst_ref=recv.at[way, step],
            send_sem=send_sem.at[way, step],
            recv_sem=recv_sem.at[way, step],
            device_id={"tp": me + 1 if way == 0 else me - 1},
        )

    behind = (me, count - 1 - me)
    has_next = (me < count - 1, me > 0)
    has_prev = (me > 0, me < count - 1)
    for step in range(count - 1):
        for way in range(2):
            dest = count - 1 - step + me if way == 0 else step - (count - 1 - me)

            @pl.when(has_next[way] & (step >= behind[way]) & (behind[way] == 0))
            def _():
                send[way, step] = block(dest).astype(send.dtype)
                hop(way, step).start()

            if step > 0:

                @pl.when(has_next[way] & (step >= behind[way]) & (behind[way] > 0))
                def _():
                    total = block(dest) + recv[way, step - 1].astype(jnp.float32)
                    send[way, step] = total.astype(send.dtype)
                    hop(way, step).start()

        for way in range(2):

            @pl.when(has_prev[way] & (step >= behind[way] - 1))
            def _():
                hop(way, step).wait_recv()

    o_ref[...] = block(me)
    for way in range(2):

        @pl.when(has_prev[way])
        def _():
            o_ref[...] += recv[way, count - 2].astype(jnp.float32)

    for step in range(count - 1):
        for way in range(2):

            @pl.when(has_next[way] & (step >= behind[way]))
            def _():
                hop(way, step).wait_send()


def line_scatter(partial_rows, count, ident):
    rows, width = partial_rows.shape[0] // count, partial_rows.shape[1]
    return pl.pallas_call(
        functools.partial(line_scatter_kernel, count),
        out_shape=jax.ShapeDtypeStruct((rows, width), jnp.float32),
        in_specs=[pl.BlockSpec(memory_space=pltpu.VMEM)],
        out_specs=pl.BlockSpec(memory_space=pltpu.VMEM),
        scratch_shapes=[
            pltpu.VMEM((2, count - 1, rows, width), jnp.bfloat16),
            pltpu.VMEM((2, count - 1, rows, width), jnp.bfloat16),
            pltpu.SemaphoreType.DMA((2, count - 1)),
            pltpu.SemaphoreType.DMA((2, count - 1)),
        ],
        compiler_params=pltpu.CompilerParams(
            collective_id=ident, has_side_effects=True, vmem_limit_bytes=56 << 20
        ),
        cost_estimate=pl.CostEstimate(flops=0, transcendentals=0, bytes_accessed=150_000_000),
    )(partial_rows)


SLOTS = 256


def experts_kernel(
    first_expert,
    capacity,
    meta,
    place_row,
    place_cols,
    gate_row,
    x_ref,
    g_ref,
    weights,
    y_ref,
    dx_ref,
    grads,
):
    step = pl.program_id(0)
    expert = step + first_expert
    group, width = x_ref.shape
    tail = dx_ref.shape[1] - width

    @pl.when(step == 0)
    def _():
        y_ref[...] = jnp.zeros_like(y_ref)
        dx_ref[...] = jnp.zeros_like(dx_ref)

    lanes = lax.broadcasted_iota(jnp.int32, place_cols.shape, 1)
    place_col = jnp.sum(jnp.where(lanes == expert, place_cols[...], 0), axis=1, keepdims=True)
    column = expert + meta[meta.shape[0] - 1]
    mark = jnp.where(lax.broadcasted_iota(jnp.int32, (1, tail), 1) == column, 1.0, 0.0)

    def run(base, span):
        slots = lax.broadcasted_iota(jnp.int32, (span, group), 0) + base
        hit = slots == place_row[0]
        pick = jnp.where(hit, 1.0, 0.0).astype(jnp.bfloat16)
        scale = jnp.sum(jnp.where(hit, gate_row[0], 0.0), axis=1, keepdims=True)
        x_taken = jnp.dot(pick, x_ref[...], preferred_element_type=jnp.float32).astype(jnp.bfloat16)
        g_taken = jnp.dot(pick, g_ref[...], preferred_element_type=jnp.float32).astype(jnp.bfloat16)
        gate_pre = jnp.dot(x_taken, weights[0, 0], preferred_element_type=jnp.float32)
        up_pre = jnp.dot(x_taken, weights[0, 1], preferred_element_type=jnp.float32)
        raw = jnp.dot(g_taken, weights[0, 2], preferred_element_type=jnp.float32)
        sig = jax.nn.sigmoid(gate_pre)
        silu = gate_pre * sig
        act = (silu * up_pre).astype(jnp.bfloat16).astype(jnp.float32)
        slot_grad = jnp.sum(act * raw, axis=1, keepdims=True)
        act_grad = raw * scale
        act_scaled = (act * scale).astype(jnp.bfloat16)
        gate_grad = (act_grad * up_pre * sig * (1.0 + gate_pre * (1.0 - sig))).astype(jnp.bfloat16)
        up_grad = (act_grad * silu).astype(jnp.bfloat16)
        extra = (slot_grad * mark).astype(jnp.bfloat16)
        rows_out = contract_last(act_scaled, weights[0, 2]).astype(jnp.bfloat16)
        rows_in = (
            contract_last(gate_grad, weights[0, 0]) + contract_last(up_grad, weights[0, 1])
        ).astype(jnp.bfloat16)
        for slot, left_op, right_op in (
            (0, x_taken, gate_grad),
            (1, x_taken, up_grad),
            (2, g_taken, act_scaled),
        ):
            grad = contract_first(left_op, right_op)
            if base > 0:
                grad = grad + grads[0, slot].astype(jnp.float32)
            grads[0, slot] = grad.astype(jnp.bfloat16)
        block = min(256, group)
        for start in range(0, group, block):
            back = jnp.where(
                lax.broadcasted_iota(jnp.int32, (block, span), 1) + base
                == place_col[start : start + block],
                1.0,
                0.0,
            ).astype(jnp.bfloat16)
            for target, low_col, addend in (
                (y_ref, 0, rows_out),
                (dx_ref, 0, rows_in),
                (dx_ref, width, extra),
            ):
                area = (slice(start, start + block), slice(low_col, low_col + addend.shape[1]))
                target[area] = (
                    target[area].astype(jnp.float32)
                    + jnp.dot(back, addend, preferred_element_type=jnp.float32)
                ).astype(target.dtype)

    run(0, min(SLOTS, capacity))
    for base in range(SLOTS, capacity, SLOTS):
        span = min(SLOTS, -(-(capacity - base) // 16) * 16)

        @pl.when(meta[expert] > base)
        def _():
            run(base, span)


def experts_step(meta, place_rows, place_cols, gate_rows, x_rows, g_rows, weights, first, capacity):
    group, width = x_rows.shape
    count, _, _, hidden = weights.shape
    keep = jnp.float32 if group <= 1024 else jnp.bfloat16
    tail = 128

    def whole(shape):
        return pl.BlockSpec(
            shape, lambda step, meta: (0,) * len(shape), pipeline_mode=pl.Buffered(1)
        )

    def row(shape):
        return pl.BlockSpec(shape, lambda step, meta: (step + first, 0, 0))

    def big():
        return pl.BlockSpec((1, 3, width, hidden), lambda step, meta: (step, 0, 0, 0))

    return pl.pallas_call(
        functools.partial(experts_kernel, first, capacity),
        grid_spec=pltpu.PrefetchScalarGridSpec(
            num_scalar_prefetch=1,
            grid=(count,),
            in_specs=[
                row((1, 1, group)),
                whole(place_cols.shape),
                row((1, 1, group)),
                whole(x_rows.shape),
                whole(g_rows.shape),
                big(),
            ],
            out_specs=[
                whole((group, width)),
                whole((group, width + tail)),
                big(),
            ],
        ),
        out_shape=[
            jax.ShapeDtypeStruct((group, width), keep),
            jax.ShapeDtypeStruct((group, width + tail), keep),
            jax.ShapeDtypeStruct(weights.shape, jnp.bfloat16),
        ],
        compiler_params=pltpu.CompilerParams(
            dimension_semantics=("arbitrary",), vmem_limit_bytes=63 << 20
        ),
        cost_estimate=pl.CostEstimate(
            flops=count * 17 * 2 * 408 * width * hidden,
            transcendentals=count * 408 * hidden,
            bytes_accessed=count * 12 * width * hidden,
        ),
    )(meta, place_rows, place_cols, gate_rows, x_rows, g_rows, weights)


CHUNKS = 2


def local(
    emb,
    segment_ids,
    routes,
    norm1_gain,
    w_query,
    w_key,
    w_value,
    w_out,
    norm2_gain,
    w_router,
    w_gate,
    w_up,
    w_down,
    cotangent,
):
    local_rows = emb.shape[0]
    tp_count = lax.axis_size("tp")
    tp_index = lax.axis_index("tp")
    experts_here = w_gate.shape[0]
    attn_w = lax.all_gather(
        jnp.concatenate([w_query, w_key, w_value, w_out, jnp.pad(w_router, ((0, 0), (0, 128 - w_router.shape[1])))], axis=1),
        "fsdp", axis=0, tiled=True)
    q_width, kv_width = w_query.shape[1], w_key.shape[1]
    query_w = attn_w[:, :q_width]
    key_w = attn_w[:, q_width : q_width + kv_width]
    value_w = attn_w[:, q_width + kv_width : q_width + 2 * kv_width]
    out_w = attn_w[:, q_width + 2 * kv_width : 2 * q_width + 2 * kv_width]
    expert_count = w_router.shape[1]
    router_w = attn_w[:, 2 * q_width + 2 * kv_width :]
    stacked = jnp.stack([w_gate, w_up, w_down], axis=1)
    edges = [experts_here * part // CHUNKS for part in range(CHUNKS + 1)]
    pieces = []
    for low, high in zip(edges[:-1], edges[1:]):
        pieces.append(lax.all_gather(stacked[low:high], "fsdp", axis=2, tiled=True))

    gain_one = norm1_gain.astype(jnp.float32)
    gain_two = norm2_gain.astype(jnp.float32)
    start_x = emb.astype(jnp.float32) * emb_scale
    normed_one, inverse_one = rms_forward(start_x, gain_one)
    group_rows = line_gather(normed_one.astype(jnp.bfloat16), tp_count, 0)
    out_grad = cotangent.astype(jnp.float32)
    moe_grad_rows = line_gather((resid_scale * out_grad).astype(jnp.bfloat16), tp_count, 1)
    group_size = group_rows.shape[0]
    seq_count = group_size // SEQ
    heads_here = query_w.shape[1] // HEAD_DIM
    kv_here = key_w.shape[1] // HEAD_DIM

    capacity = group_size * routes.shape[1] // expert_count * 2
    all_experts = jnp.arange(expert_count, dtype=jnp.int32)
    member_all = jnp.any(routes[:, :, None] == all_experts[None, None, :], axis=1)
    own_member = lax.dynamic_slice_in_dim(member_all, tp_index * local_rows, local_rows, 0)
    member = lax.dynamic_slice_in_dim(member_all, tp_index * experts_here, experts_here, 1)
    ids = jnp.arange(group_size)
    earlier = (ids[:, None] > ids[None, :]).astype(jnp.bfloat16)
    ranks = jnp.dot(earlier, member.astype(jnp.bfloat16), preferred_element_type=jnp.float32)
    places = jnp.where(member, ranks.astype(jnp.int32), -1)
    meta = jnp.concatenate(
        [jnp.sum(member.astype(jnp.int32), axis=0), (tp_index * experts_here)[None]]
    )

    cosine_table, sine_table = rotary_tables(group_size, HEAD_DIM)
    query_proj = jnp.dot(group_rows, query_w, preferred_element_type=jnp.float32).reshape(
        group_size, heads_here, HEAD_DIM
    )
    key_proj = jnp.dot(group_rows, key_w, preferred_element_type=jnp.float32).reshape(
        group_size, kv_here, HEAD_DIM
    )
    queries = rotate(query_proj, cosine_table, sine_table).astype(jnp.bfloat16)
    key_rows = rotate(key_proj, cosine_table, sine_table).astype(jnp.bfloat16)
    value_rows = jnp.dot(group_rows, value_w, preferred_element_type=jnp.float32).astype(
        jnp.bfloat16
    )
    seq_queries = queries.reshape(seq_count, SEQ, heads_here, HEAD_DIM)
    seq_keys = key_rows.reshape(seq_count, SEQ, kv_here, HEAD_DIM)
    seq_values = value_rows.reshape(seq_count, SEQ, kv_here, HEAD_DIM)
    mixed_out, logsum = lax.map(attend_forward, (seq_queries, seq_keys, seq_values, segment_ids))
    mixed_rows = mixed_out.reshape(group_size, heads_here * HEAD_DIM)
    attn_branch = line_scatter(contract_last(mixed_rows, out_w), tp_count, 2)
    mid_x = start_x + resid_scale * attn_branch
    normed_two, inverse_two = rms_forward(mid_x, gain_two)
    normed_low = normed_two.astype(jnp.bfloat16)
    moe_rows = line_gather(normed_low, tp_count, 3)

    def gates_of(rows, inside):
        logits = jnp.dot(rows, router_w, preferred_element_type=jnp.float32)[:, :expert_count]
        top = jnp.max(jnp.where(inside, logits, masked_value), axis=-1, keepdims=True)
        raised = jnp.where(inside, jnp.exp(jnp.where(inside, logits - top, 0.0)), 0.0)
        return raised / jnp.sum(raised, axis=-1, keepdims=True)

    gates = gates_of(normed_low, own_member)
    gates_here = lax.dynamic_slice_in_dim(
        gates_of(moe_rows, member_all).astype(jnp.bfloat16).astype(jnp.float32),
        tp_index * experts_here, experts_here, 1)
    place_rows = places.T[:, None, :]
    gate_rows = gates_here.T[:, None, :]

    outs = []
    for first, piece in zip(edges[:-1], pieces):
        outs.append(experts_step(
            meta, place_rows, places, gate_rows, moe_rows, moe_grad_rows, piece, first, capacity))
    grad_sums = []
    behind = None
    for part in outs:
        grads = part[2]
        if behind is not None:
            grads, _ = lax.optimization_barrier((grads, behind))
        behind = lax.psum_scatter(grads, "fsdp", scatter_dimension=2, tiled=True)
        grad_sums.append(behind)
    y_part = functools.reduce(lambda one, two: one + two, [part[0] for part in outs])
    dx_part = functools.reduce(lambda one, two: one + two, [part[1] for part in outs])
    dx_sum = line_scatter(dx_part, tp_count, 4)
    rows_grad_sum = dx_sum[:, : emb.shape[1]]
    gates_grad = dx_sum[:, emb.shape[1] : emb.shape[1] + expert_count]
    gates_inner = jnp.sum(gates * gates_grad, axis=-1, keepdims=True)
    logits_grad = (gates * (gates_grad - gates_inner)).astype(jnp.bfloat16)
    router_grad_part = contract_first(normed_low, logits_grad)
    normed_two_grad = rows_grad_sum + contract_last(logits_grad, router_w[:, :expert_count])
    mid_from_norm, gain_two_grad = rms_backward(normed_two_grad, mid_x, inverse_two, gain_two)
    mid_grad = out_grad + mid_from_norm
    branch_grad = (resid_scale * mid_grad).astype(jnp.bfloat16)
    branch_grad_rows = line_gather(branch_grad, tp_count, 5)
    moe_sum = line_scatter(y_part, tp_count, 6)
    out = (mid_x + resid_scale * moe_sum).astype(jnp.bfloat16)
    out_w_grad = contract_first(branch_grad_rows, mixed_rows)
    mixed_grad = jnp.dot(branch_grad_rows, out_w, preferred_element_type=jnp.float32).astype(
        jnp.bfloat16
    )
    query_grad, key_grad, value_grad = lax.map(
        attend_backward,
        (
            seq_queries,
            seq_keys,
            seq_values,
            segment_ids,
            logsum,
            mixed_grad.reshape(seq_count, SEQ, -1),
        ),
    )
    query_proj_grad = (
        rotate(query_grad.reshape(group_size, heads_here, HEAD_DIM), cosine_table, -sine_table)
        .astype(jnp.bfloat16)
        .reshape(group_size, -1)
    )
    key_proj_grad = (
        rotate(key_grad.reshape(group_size, kv_here, HEAD_DIM), cosine_table, -sine_table)
        .astype(jnp.bfloat16)
        .reshape(group_size, -1)
    )
    value_proj_grad = value_grad.reshape(group_size, -1).astype(jnp.bfloat16)
    qkv_grad = jnp.concatenate([query_proj_grad, key_proj_grad, value_proj_grad], axis=1)
    qkv_w_grad = contract_first(group_rows, qkv_grad)
    qkv_w = attn_w[:, : q_width + 2 * kv_width]
    normed_one_grad = line_scatter(contract_last(qkv_grad, qkv_w), tp_count, 7)
    start_from_norm, gain_one_grad = rms_backward(normed_one_grad, start_x, inverse_one, gain_one)
    grad_emb = emb_scale * (mid_grad + start_from_norm)
    attn_grads = jnp.concatenate([qkv_w_grad, out_w_grad], axis=1).astype(jnp.bfloat16)
    attn_grads, grad_sums[-1] = lax.optimization_barrier((attn_grads, grad_sums[-1]))
    attn_sum = lax.psum_scatter(attn_grads, "fsdp", scatter_dimension=0, tiled=True).astype(jnp.float32)
    gain_one_sum, gain_two_sum, router_sum = lax.psum(
        (gain_one_grad, gain_two_grad, router_grad_part), ("fsdp", "tp")
    )
    router_rows = w_router.shape[0]
    router_own = lax.dynamic_slice_in_dim(
        router_sum, lax.axis_index("fsdp") * router_rows, router_rows, 0
    )
    expert_sum = jnp.concatenate(grad_sums, axis=0).astype(jnp.float32)
    return (
        out,
        grad_emb,
        gain_one_sum,
        attn_sum[:, :q_width],
        attn_sum[:, q_width : q_width + kv_width],
        attn_sum[:, q_width + kv_width : q_width + 2 * kv_width],
        attn_sum[:, q_width + 2 * kv_width :],
        gain_two_sum,
        router_own,
        expert_sum[:, 0],
        expert_sum[:, 1],
        expert_sum[:, 2],
    )


def solution(mesh):
    return jax.shard_map(
        local,
        mesh=mesh,
        in_specs=(
            P(("fsdp", "tp"), None),
            P("fsdp", None),
            P("fsdp", None),
            P(),
            P("fsdp", "tp"),
            P("fsdp", "tp"),
            P("fsdp", "tp"),
            P("fsdp", "tp"),
            P(),
            P("fsdp", None),
            P("tp", "fsdp", None),
            P("tp", "fsdp", None),
            P("tp", "fsdp", None),
            P(("fsdp", "tp"), None),
        ),
        out_specs=(
            P(("fsdp", "tp"), None),
            P(("fsdp", "tp"), None),
            P(),
            P("fsdp", "tp"),
            P("fsdp", "tp"),
            P("fsdp", "tp"),
            P("fsdp", "tp"),
            P(),
            P("fsdp", None),
            P("tp", "fsdp", None),
            P("tp", "fsdp", None),
            P("tp", "fsdp", None),
        ),
        check_vma=False,
    )
```

```python
import functools

import jax
import jax.numpy as jnp
from jax import lax
from jax.experimental import pallas as pl
from jax.experimental.pallas import tpu as pltpu
from jax.sharding import PartitionSpec as P

HEAD_DIM = 64
SEQ = 512


emb_scale = 12.0
resid_scale = 0.22
attn_scale = 0.015625
norm_eps = 1e-06
rope_base = 10000.0
masked_value = -1e30


def contract_last(left_op, right_op):
    return lax.dot_general(
        left_op, right_op, (((1,), (1,)), ((), ())), preferred_element_type=jnp.float32
    )


def contract_first(left_op, right_op):
    return lax.dot_general(
        left_op, right_op, (((0,), (0,)), ((), ())), preferred_element_type=jnp.float32
    )


def rms_forward(values, gain_vec):
    inverse = lax.rsqrt(jnp.mean(values * values, axis=-1, keepdims=True) + norm_eps)
    return (values * inverse * gain_vec, inverse)


def rms_backward(incoming, values, inverse, gain_vec):
    scaled = values * inverse
    gain_grad = jnp.sum(incoming * scaled, axis=0)
    weighted = incoming * gain_vec
    row_inner = jnp.mean(weighted * scaled, axis=-1, keepdims=True)
    return (inverse * (weighted - scaled * row_inner), gain_grad)


def line_barrier(me, count):
    barrier = pltpu.get_barrier_semaphore()

    @pl.when(me > 0)
    def _():
        pl.semaphore_signal(barrier, inc=1, device_id={"tp": me - 1})

    @pl.when(me < count - 1)
    def _():
        pl.semaphore_signal(barrier, inc=1, device_id={"tp": me + 1})

    pl.semaphore_wait(barrier, jnp.where((me > 0) & (me < count - 1), 2, 1))


def line_gather_kernel(count, x_ref, o_ref, send_sem, recv_sem, own_sem):
    rows = x_ref.shape[0]
    me = lax.axis_index("tp")
    line_barrier(me, count)

    def part(chunk):
        return o_ref.at[pl.ds(pl.multiple_of(chunk * rows, rows), rows)]

    def hop(way, step, chunk):
        return pltpu.make_async_remote_copy(
            src_ref=x_ref if step == 0 else part(chunk),
            dst_ref=part(chunk),
            send_sem=send_sem.at[way, step],
            recv_sem=recv_sem.at[way, step],
            device_id={"tp": me + 1 if way == 0 else me - 1},
        )

    own = pltpu.make_async_copy(x_ref, part(me), own_sem)
    sends = [[(me >= step) & (me < count - 1) for step in range(count - 1)],
             [(me + step < count) & (me > 0) for step in range(count - 1)]]
    gets = [[me - 1 - step >= 0 for step in range(count - 1)],
            [me + 1 + step < count for step in range(count - 1)]]
    for step in range(count - 1):

        @pl.when(sends[0][step])
        def _():
            hop(0, step, me - step).start()

        @pl.when(sends[1][step])
        def _():
            hop(1, step, me + step).start()

        if step == 0:
            own.start()

        @pl.when(gets[0][step])
        def _():
            hop(0, step, me - 1 - step).wait_recv()

        @pl.when(gets[1][step])
        def _():
            hop(1, step, me + 1 + step).wait_recv()

    own.wait()
    for step in range(count - 1):

        @pl.when(sends[0][step])
        def _():
            hop(0, step, me - step).wait_send()

        @pl.when(sends[1][step])
        def _():
            hop(1, step, me + step).wait_send()


def line_gather(rows_in, count, ident):
    rows, width = rows_in.shape
    return pl.pallas_call(
        functools.partial(line_gather_kernel, count),
        out_shape=jax.ShapeDtypeStruct((rows * count, width), rows_in.dtype),
        in_specs=[pl.BlockSpec(memory_space=pltpu.VMEM)],
        out_specs=pl.BlockSpec(memory_space=pl.ANY),
        scratch_shapes=[
            pltpu.SemaphoreType.DMA((2, count - 1)),
            pltpu.SemaphoreType.DMA((2, count - 1)),
            pltpu.SemaphoreType.DMA,
        ],
        compiler_params=pltpu.CompilerParams(collective_id=ident, has_side_effects=True),
        cost_estimate=pl.CostEstimate(flops=0, transcendentals=0, bytes_accessed=150_000_000),
    )(rows_in)


def line_scatter_kernel(count, x_ref, o_ref, recv, send, send_sem, recv_sem):
    rows = o_ref.shape[0]
    me = lax.axis_index("tp")
    line_barrier(me, count)

    def block(dest):
        return x_ref[pl.ds(pl.multiple_of(dest * rows, rows), rows), :].astype(jnp.float32)

    def hop(way, step):
        return pltpu.make_async_remote_copy(
            src_ref=send.at[way, step],
            dst_ref=recv.at[way, step],
            send_sem=send_sem.at[way, step],
            recv_sem=recv_sem.at[way, step],
            device_id={"tp": me + 1 if way == 0 else me - 1},
        )

    behind = (me, count - 1 - me)
    has_next = (me < count - 1, me > 0)
    has_prev = (me > 0, me < count - 1)
    for step in range(count - 1):
        for way in range(2):
            dest = count - 1 - step + me if way == 0 else step - (count - 1 - me)

            @pl.when(has_next[way] & (step >= behind[way]) & (behind[way] == 0))
            def _():
                send[way, step] = block(dest).astype(send.dtype)
                hop(way, step).start()

            if step > 0:

                @pl.when(has_next[way] & (step >= behind[way]) & (behind[way] > 0))
                def _():
                    total = block(dest) + recv[way, step - 1].astype(jnp.float32)
                    send[way, step] = total.astype(send.dtype)
                    hop(way, step).start()

        for way in range(2):

            @pl.when(has_prev[way] & (step >= behind[way] - 1))
            def _():
                hop(way, step).wait_recv()

    o_ref[...] = block(me)
    for way in range(2):

        @pl.when(has_prev[way])
        def _():
            o_ref[...] += recv[way, count - 2].astype(jnp.float32)

    for step in range(count - 1):
        for way in range(2):

            @pl.when(has_next[way] & (step >= behind[way]))
            def _():
                hop(way, step).wait_send()


def line_scatter(partial_rows, count, ident):
    rows, width = partial_rows.shape[0] // count, partial_rows.shape[1]
    return pl.pallas_call(
        functools.partial(line_scatter_kernel, count),
        out_shape=jax.ShapeDtypeStruct((rows, width), jnp.float32),
        in_specs=[pl.BlockSpec(memory_space=pltpu.VMEM)],
        out_specs=pl.BlockSpec(memory_space=pltpu.VMEM),
        scratch_shapes=[
            pltpu.VMEM((2, count - 1, rows, width), jnp.bfloat16),
            pltpu.VMEM((2, count - 1, rows, width), jnp.bfloat16),
            pltpu.SemaphoreType.DMA((2, count - 1)),
            pltpu.SemaphoreType.DMA((2, count - 1)),
        ],
        compiler_params=pltpu.CompilerParams(
            collective_id=ident, has_side_effects=True, vmem_limit_bytes=56 << 20
        ),
        cost_estimate=pl.CostEstimate(flops=0, transcendentals=0, bytes_accessed=150_000_000),
    )(partial_rows)


SLOTS = 256


def experts_kernel(
    first_expert,
    capacity,
    meta,
    place_row,
    place_cols,
    gate_row,
    x_ref,
    g_ref,
    weights,
    y_ref,
    dx_ref,
    grads,
):
    step = pl.program_id(0)
    expert = step + first_expert
    group, width = x_ref.shape
    tail = dx_ref.shape[1] - width

    @pl.when(step == 0)
    def _():
        y_ref[...] = jnp.zeros_like(y_ref)
        dx_ref[...] = jnp.zeros_like(dx_ref)

    lanes = lax.broadcasted_iota(jnp.int32, place_cols.shape, 1)
    place_col = jnp.sum(jnp.where(lanes == expert, place_cols[...], 0), axis=1, keepdims=True)
    column = expert + meta[meta.shape[0] - 1]
    mark = jnp.where(lax.broadcasted_iota(jnp.int32, (1, tail), 1) == column, 1.0, 0.0)

    def run(base, span):
        slots = lax.broadcasted_iota(jnp.int32, (span, group), 0) + base
        hit = slots == place_row[0]
        pick = jnp.where(hit, 1.0, 0.0).astype(jnp.bfloat16)
        scale = jnp.sum(jnp.where(hit, gate_row[0], 0.0), axis=1, keepdims=True)
        x_taken = jnp.dot(pick, x_ref[...], preferred_element_type=jnp.float32).astype(jnp.bfloat16)
        g_taken = jnp.dot(pick, g_ref[...], preferred_element_type=jnp.float32).astype(jnp.bfloat16)
        gate_pre = jnp.dot(x_taken, weights[0, 0], preferred_element_type=jnp.float32)
        up_pre = jnp.dot(x_taken, weights[0, 1], preferred_element_type=jnp.float32)
        raw = jnp.dot(g_taken, weights[0, 2], preferred_element_type=jnp.float32)
        sig = jax.nn.sigmoid(gate_pre)
        silu = gate_pre * sig
        act = (silu * up_pre).astype(jnp.bfloat16).astype(jnp.float32)
        slot_grad = jnp.sum(act * raw, axis=1, keepdims=True)
        act_grad = raw * scale
        act_scaled = (act * scale).astype(jnp.bfloat16)
        gate_grad = (act_grad * up_pre * sig * (1.0 + gate_pre * (1.0 - sig))).astype(jnp.bfloat16)
        up_grad = (act_grad * silu).astype(jnp.bfloat16)
        extra = (slot_grad * mark).astype(jnp.bfloat16)
        rows_out = contract_last(act_scaled, weights[0, 2]).astype(jnp.bfloat16)
        rows_in = (
            contract_last(gate_grad, weights[0, 0]) + contract_last(up_grad, weights[0, 1])
        ).astype(jnp.bfloat16)
        for slot, left_op, right_op in (
            (0, x_taken, gate_grad),
            (1, x_taken, up_grad),
            (2, g_taken, act_scaled),
        ):
            grad = contract_first(left_op, right_op)
            if base > 0:
                grad = grad + grads[0, slot].astype(jnp.float32)
            grads[0, slot] = grad.astype(jnp.bfloat16)
        block = min(256, group)
        for start in range(0, group, block):
            back = jnp.where(
                lax.broadcasted_iota(jnp.int32, (block, span), 1) + base
                == place_col[start : start + block],
                1.0,
                0.0,
            ).astype(jnp.bfloat16)
            for target, low_col, addend in (
                (y_ref, 0, rows_out),
                (dx_ref, 0, rows_in),
                (dx_ref, width, extra),
            ):
                area = (slice(start, start + block), slice(low_col, low_col + addend.shape[1]))
                target[area] = (
                    target[area].astype(jnp.float32)
                    + jnp.dot(back, addend, preferred_element_type=jnp.float32)
                ).astype(target.dtype)

    run(0, min(SLOTS, capacity))
    for base in range(SLOTS, capacity, SLOTS):
        span = min(SLOTS, -(-(capacity - base) // 16) * 16)

        @pl.when(meta[expert] > base)
        def _():
            run(base, span)


def experts_step(meta, place_rows, place_cols, gate_rows, x_rows, g_rows, weights, first, capacity):
    group, width = x_rows.shape
    count, _, _, hidden = weights.shape
    keep = jnp.float32 if group <= 1024 else jnp.bfloat16
    tail = 128

    def whole(shape):
        return pl.BlockSpec(
            shape, lambda step, meta: (0,) * len(shape), pipeline_mode=pl.Buffered(1)
        )

    def row(shape):
        return pl.BlockSpec(shape, lambda step, meta: (step + first, 0, 0))

    def big():
        return pl.BlockSpec((1, 3, width, hidden), lambda step, meta: (step, 0, 0, 0))

    return pl.pallas_call(
        functools.partial(experts_kernel, first, capacity),
        grid_spec=pltpu.PrefetchScalarGridSpec(
            num_scalar_prefetch=1,
            grid=(count,),
            in_specs=[
                row((1, 1, group)),
                whole(place_cols.shape),
                row((1, 1, group)),
                whole(x_rows.shape),
                whole(g_rows.shape),
                big(),
            ],
            out_specs=[
                whole((group, width)),
                whole((group, width + tail)),
                big(),
            ],
        ),
        out_shape=[
            jax.ShapeDtypeStruct((group, width), keep),
            jax.ShapeDtypeStruct((group, width + tail), keep),
            jax.ShapeDtypeStruct(weights.shape, jnp.bfloat16),
        ],
        compiler_params=pltpu.CompilerParams(
            dimension_semantics=("arbitrary",), vmem_limit_bytes=63 << 20
        ),
        cost_estimate=pl.CostEstimate(
            flops=count * 17 * 2 * 408 * width * hidden,
            transcendentals=count * 408 * hidden,
            bytes_accessed=count * 12 * width * hidden,
        ),
    )(meta, place_rows, place_cols, gate_rows, x_rows, g_rows, weights)


def rotate_head(values, cosine, sine, sign):
    half = values.shape[-1] // 2
    other = jnp.concatenate([values[:, half:], values[:, :half]], axis=1)
    return values * cosine + other * (sine * sign)


def segment_bias(seg_row, seg_col):
    shape = (seg_col.shape[0], seg_row.shape[1])
    keys = lax.broadcasted_iota(jnp.int32, shape, 0)
    queries = lax.broadcasted_iota(jnp.int32, shape, 1)
    return jnp.where((keys <= queries) & (seg_col == seg_row), 0.0, masked_value)


def attend_kernel(
    x_ref,
    w_ref,
    seg_row,
    seg_col,
    cos_ref,
    sin_ref,
    q_ref,
    k_ref,
    v_ref,
    mixed_ref,
    logsum_ref,
    branch_ref,
    bias,
    v_turned,
    mixed_heads,
):
    heads, kv_heads = q_ref.shape[0], k_ref.shape[0]
    per_kv = heads // kv_heads
    block = SEQ // 2
    edge = (heads + 2 * kv_heads) * HEAD_DIM
    proj = jnp.dot(x_ref[...], w_ref[:, :edge], preferred_element_type=jnp.float32)
    cosine, sine = cos_ref[...], sin_ref[...]
    for head in range(heads + 2 * kv_heads):
        part = proj[:, head * HEAD_DIM : (head + 1) * HEAD_DIM]
        if head < heads:
            q_ref[head] = rotate_head(part, cosine, sine, 1.0).astype(jnp.bfloat16)
        elif head < heads + kv_heads:
            k_ref[head - heads] = rotate_head(part, cosine, sine, 1.0).astype(jnp.bfloat16)
        else:
            v_ref[head - heads - kv_heads] = part.astype(jnp.bfloat16)
            v_turned[head - heads - kv_heads] = part.T.astype(jnp.bfloat16)
    bias[...] = segment_bias(seg_row[0], seg_col[0])

    def one_head(head, carry):
        kv = head // per_kv
        for part in range(2):
            span, low = block * (part + 1), block * part
            scores = contract_last(k_ref[kv, :span], q_ref[head, low : low + block]) * attn_scale
            scores = scores + bias[:span, low : low + block]
            top = jnp.max(scores, axis=0, keepdims=True)
            raised = jnp.exp(scores - top)
            total = jnp.sum(raised, axis=0, keepdims=True)
            probs = (raised * (1.0 / total)).astype(jnp.bfloat16)
            turned = jnp.dot(v_turned[kv, :, :span], probs, preferred_element_type=jnp.float32)
            mixed_heads[head, low : low + block, :] = turned.T.astype(jnp.bfloat16)
            logsum_ref[0, pl.ds(head, 1), low : low + block] = top + jnp.log(total)
        return carry

    lax.fori_loop(0, heads, one_head, 0)
    for head in range(heads):
        mixed_ref[:, head * HEAD_DIM : (head + 1) * HEAD_DIM] = mixed_heads[head]
    branch_ref[...] = contract_last(
        mixed_ref[...], w_ref[:, edge : edge + heads * HEAD_DIM]
    ).astype(jnp.bfloat16)


def attend_back_kernel(
    x_ref,
    w_ref,
    seg_row,
    seg_col,
    cos_ref,
    sin_ref,
    q_ref,
    k_ref,
    v_ref,
    mixed_ref,
    logsum_ref,
    branch_grad,
    dx_ref,
    dw_ref,
    bias,
    k_turned,
    mixed_grads,
    q_grads,
    kv_grads,
    qkv_grad,
    dw_acc,
):
    heads, kv_heads = q_ref.shape[0], k_ref.shape[0]
    per_kv = heads // kv_heads
    block = SEQ // 2
    edge = (heads + 2 * kv_heads) * HEAD_DIM
    step = pl.program_id(0)
    out_edge = edge + heads * HEAD_DIM
    grad = jnp.dot(
        branch_grad[...], w_ref[:, edge:out_edge], preferred_element_type=jnp.float32
    ).astype(jnp.bfloat16)
    for head in range(heads):
        mixed_grads[head] = grad[:, head * HEAD_DIM : (head + 1) * HEAD_DIM]
    for kv in range(kv_heads):
        k_turned[kv] = k_ref[kv].astype(jnp.float32).T.astype(jnp.bfloat16)
    bias[...] = segment_bias(seg_row[0], seg_col[0])
    kv_grads[...] = jnp.zeros_like(kv_grads)

    def one_head(head, carry):
        kv = head // per_kv
        for part in range(2):
            span, low = block * (part + 1), block * part
            high = low + block
            scores = contract_last(k_ref[kv, :span], q_ref[head, low:high]) * attn_scale
            scores = scores + bias[:span, low:high]
            probs = jnp.exp(scores - logsum_ref[0, pl.ds(head, 1), low:high])
            probs_grad = contract_last(v_ref[kv, :span], mixed_grads[head, low:high])
            inner = jnp.sum(probs * probs_grad, axis=0, keepdims=True)
            score_grad = (probs * (probs_grad - inner)).astype(jnp.bfloat16)
            turned = jnp.dot(k_turned[kv, :, :span], score_grad, preferred_element_type=jnp.float32)
            q_grads[head, low:high, :] = turned.T * attn_scale
            kv_grads[0, kv, :span, :] += jnp.dot(
                score_grad, q_ref[head, low:high], preferred_element_type=jnp.float32
            )
            kv_grads[1, kv, :span, :] += jnp.dot(
                probs.astype(jnp.bfloat16), mixed_grads[head, low:high],
                preferred_element_type=jnp.float32,
            )
        return carry

    lax.fori_loop(0, heads, one_head, 0)
    cosine, sine = cos_ref[...], sin_ref[...]
    for head in range(heads + 2 * kv_heads):
        if head < heads:
            part = rotate_head(q_grads[head], cosine, sine, -1.0)
        elif head < heads + kv_heads:
            part = rotate_head(kv_grads[0, head - heads] * attn_scale, cosine, sine, -1.0)
        else:
            part = kv_grads[1, head - heads - kv_heads]
        qkv_grad[:, head * HEAD_DIM : (head + 1) * HEAD_DIM] = part.astype(jnp.bfloat16)
    dx_ref[...] = contract_last(qkv_grad[...], w_ref[:, :edge]).astype(jnp.bfloat16)
    qkv_part = contract_first(x_ref[...], qkv_grad[...])
    out_part = contract_first(branch_grad[...], mixed_ref[...])

    @pl.when(step == 0)
    def _():
        dw_acc[:, :edge] = qkv_part
        dw_acc[:, edge:out_edge] = out_part

    @pl.when(step > 0)
    def _():
        dw_acc[:, :edge] += qkv_part
        dw_acc[:, edge:out_edge] += out_part

    @pl.when(step == pl.num_programs(0) - 1)
    def _():
        dw_ref[...] = dw_acc[...].astype(jnp.bfloat16)


def fixed(shape):
    return pl.BlockSpec(shape, lambda seq: (0,) * len(shape), pipeline_mode=pl.Buffered(1))


def by_row(width):
    return pl.BlockSpec((SEQ, width), lambda seq: (seq, 0))


def by_head(heads):
    return pl.BlockSpec((heads, SEQ, HEAD_DIM), lambda seq: (0, seq, 0))


def attend_tables():
    half = HEAD_DIM // 2
    positions = jnp.arange(SEQ).astype(jnp.float32)
    frequency = rope_base ** (-jnp.arange(half).astype(jnp.float32) * 2.0 / HEAD_DIM)
    angles = positions[:, None] * frequency[None, :]
    cosine, sine = jnp.cos(angles), jnp.sin(angles)
    return (
        jnp.concatenate([cosine, cosine], axis=1),
        jnp.concatenate([-sine, sine], axis=1),
    )


def attend(rows, weights, segments, tables, heads, kv_heads):
    group, width = rows.shape
    seqs = group // SEQ
    return pl.pallas_call(
        attend_kernel,
        grid=(seqs,),
        in_specs=[
            by_row(width),
            fixed(weights.shape),
            pl.BlockSpec((1, 1, SEQ), lambda seq: (seq, 0, 0)),
            pl.BlockSpec((1, SEQ, 1), lambda seq: (seq, 0, 0)),
            fixed(tables[0].shape),
            fixed(tables[1].shape),
        ],
        out_specs=[
            by_head(heads),
            by_head(kv_heads),
            by_head(kv_heads),
            by_row(heads * HEAD_DIM),
            pl.BlockSpec((1, heads, SEQ), lambda seq: (seq, 0, 0)),
            by_row(width),
        ],
        out_shape=[
            jax.ShapeDtypeStruct((heads, group, HEAD_DIM), jnp.bfloat16),
            jax.ShapeDtypeStruct((kv_heads, group, HEAD_DIM), jnp.bfloat16),
            jax.ShapeDtypeStruct((kv_heads, group, HEAD_DIM), jnp.bfloat16),
            jax.ShapeDtypeStruct((group, heads * HEAD_DIM), jnp.bfloat16),
            jax.ShapeDtypeStruct((seqs, heads, SEQ), jnp.float32),
            jax.ShapeDtypeStruct((group, width), jnp.bfloat16),
        ],
        scratch_shapes=[
            pltpu.VMEM((SEQ, SEQ), jnp.float32),
            pltpu.VMEM((kv_heads, HEAD_DIM, SEQ), jnp.bfloat16),
            pltpu.VMEM((heads, SEQ, HEAD_DIM), jnp.bfloat16),
        ],
        compiler_params=pltpu.CompilerParams(
            dimension_semantics=("arbitrary",), vmem_limit_bytes=56 << 20
        ),
        cost_estimate=pl.CostEstimate(
            flops=10_000_000_000, transcendentals=3_000_000, bytes_accessed=60_000_000
        ),
    )(rows, weights, segments[:, None, :], segments[:, :, None], *tables)


def attend_back(rows, weights, segments, tables, kept, branch_grad):
    queries, keys, values, mixed, logsum = kept
    group, width = rows.shape
    heads, kv_heads = queries.shape[0], keys.shape[0]
    used = 2 * (heads + kv_heads) * HEAD_DIM
    return pl.pallas_call(
        attend_back_kernel,
        grid=(group // SEQ,),
        in_specs=[
            by_row(width),
            fixed(weights.shape),
            pl.BlockSpec((1, 1, SEQ), lambda seq: (seq, 0, 0)),
            pl.BlockSpec((1, SEQ, 1), lambda seq: (seq, 0, 0)),
            fixed(tables[0].shape),
            fixed(tables[1].shape),
            by_head(heads),
            by_head(kv_heads),
            by_head(kv_heads),
            by_row(heads * HEAD_DIM),
            pl.BlockSpec((1, heads, SEQ), lambda seq: (seq, 0, 0)),
            by_row(width),
        ],
        out_specs=[by_row(width), fixed((width, used))],
        out_shape=[
            jax.ShapeDtypeStruct((group, width), jnp.bfloat16),
            jax.ShapeDtypeStruct((width, used), jnp.bfloat16),
        ],
        scratch_shapes=[
            pltpu.VMEM((SEQ, SEQ), jnp.float32),
            pltpu.VMEM((kv_heads, HEAD_DIM, SEQ), jnp.bfloat16),
            pltpu.VMEM((heads, SEQ, HEAD_DIM), jnp.bfloat16),
            pltpu.VMEM((heads, SEQ, HEAD_DIM), jnp.float32),
            pltpu.VMEM((2, kv_heads, SEQ, HEAD_DIM), jnp.float32),
            pltpu.VMEM((SEQ, used - heads * HEAD_DIM), jnp.bfloat16),
            pltpu.VMEM((width, used), jnp.float32),
        ],
        compiler_params=pltpu.CompilerParams(
            dimension_semantics=("arbitrary",), vmem_limit_bytes=60 << 20
        ),
        cost_estimate=pl.CostEstimate(
            flops=20_000_000_000, transcendentals=3_000_000, bytes_accessed=100_000_000
        ),
    )(rows, weights, segments[:, None, :], segments[:, :, None], *tables,
      queries, keys, values, mixed, logsum, branch_grad)


def total_kernel(tp_count, fsdp_count, x_ref, o_ref, tp_got, fsdp_got, send_sem, recv_sem):
    tp_me, fsdp_me = lax.axis_index("tp"), lax.axis_index("fsdp")
    barrier = pltpu.get_barrier_semaphore()
    for shift in range(1, tp_count):
        pl.semaphore_signal(barrier, inc=1, device_id={"tp": lax.rem(tp_me + shift, tp_count)})
    for shift in range(1, fsdp_count):
        pl.semaphore_signal(
            barrier, inc=1, device_id={"fsdp": lax.rem(fsdp_me + shift, fsdp_count)}
        )
    pl.semaphore_wait(barrier, tp_count + fsdp_count - 2)

    def exchange(axis, me, count, source, got, base):
        copies = []
        for shift in range(1, count):
            copies.append(
                pltpu.make_async_remote_copy(
                    src_ref=source,
                    dst_ref=got.at[me],
                    send_sem=send_sem.at[base + shift],
                    recv_sem=recv_sem.at[base + shift],
                    device_id={axis: lax.rem(me + shift, count)},
                )
            )
            copies[-1].start()
        got[me] = source[...]
        for copy in copies:
            copy.wait()
        total = got[0]
        for index in range(1, count):
            total = total + got[index]
        return total

    o_ref[...] = exchange("tp", tp_me, tp_count, x_ref, tp_got, 0)
    o_ref[...] = exchange("fsdp", fsdp_me, fsdp_count, o_ref, fsdp_got, tp_count)


def total_everywhere(values, ident):
    tp_count, fsdp_count = lax.axis_size("tp"), lax.axis_size("fsdp")
    return pl.pallas_call(
        functools.partial(total_kernel, tp_count, fsdp_count),
        out_shape=jax.ShapeDtypeStruct(values.shape, values.dtype),
        in_specs=[pl.BlockSpec(memory_space=pltpu.VMEM)],
        out_specs=pl.BlockSpec(memory_space=pltpu.VMEM),
        scratch_shapes=[
            pltpu.VMEM((tp_count,) + values.shape, values.dtype),
            pltpu.VMEM((fsdp_count,) + values.shape, values.dtype),
            pltpu.SemaphoreType.DMA((tp_count + fsdp_count,)),
            pltpu.SemaphoreType.DMA((tp_count + fsdp_count,)),
        ],
        compiler_params=pltpu.CompilerParams(collective_id=ident, has_side_effects=True),
    )(values)


def widen_kernel(packed, *refs):
    for slot, target in enumerate(refs[-3:]):
        target[0] = packed[0, slot].astype(jnp.float32)


def widen(packed, count, first, held):
    span, _, rows, width = packed.shape
    shape = jax.ShapeDtypeStruct((count, rows, width), jnp.float32)
    return pl.pallas_call(
        widen_kernel,
        grid=(span,),
        in_specs=[pl.BlockSpec((1, 3, rows, width), lambda step: (step, 0, 0, 0))]
        + [pl.BlockSpec(memory_space=pl.ANY)] * len(held),
        out_specs=[pl.BlockSpec((1, rows, width), lambda step: (step + first, 0, 0))] * 3,
        out_shape=[shape] * 3,
        input_output_aliases={1 + index: index for index in range(len(held))},
    )(packed, *held)


def shifted_gather(block, count, me):
    rows = block.shape[0]
    whole = jnp.zeros((rows * count, block.shape[1]), block.dtype)
    whole = lax.dynamic_update_slice_in_dim(whole, block, me * rows, 0)
    for shift in range(1, count):
        got = lax.ppermute(block, "tp", [(i, (i + shift) % count) for i in range(count)])
        whole = lax.dynamic_update_slice_in_dim(
            whole, got, lax.rem(me + count - shift, count) * rows, 0
        )
    return whole


def shifted_scatter(partial_rows, count, me):
    rows = partial_rows.shape[0] // count
    total = lax.dynamic_slice_in_dim(partial_rows, me * rows, rows, 0).astype(jnp.float32)
    for shift in range(1, count):
        block = lax.dynamic_slice_in_dim(
            partial_rows, lax.rem(me + shift, count) * rows, rows, 0
        ).astype(jnp.bfloat16)
        got = lax.ppermute(block, "tp", [(i, (i + shift) % count) for i in range(count)])
        total = total + got.astype(jnp.float32)
    return total


CHUNKS = 2


def local(
    emb,
    segment_ids,
    routes,
    norm1_gain,
    w_query,
    w_key,
    w_value,
    w_out,
    norm2_gain,
    w_router,
    w_gate,
    w_up,
    w_down,
    cotangent,
):
    local_rows, width = emb.shape
    tp_count = lax.axis_size("tp")
    tp_index = lax.axis_index("tp")
    experts_here = w_gate.shape[0]
    expert_count = w_router.shape[1]
    q_width, kv_width = w_query.shape[1], w_key.shape[1]
    used = 2 * (q_width + kv_width)
    lane_pad = 128 - expert_count
    attn_w = lax.all_gather(
        jnp.concatenate(
            [w_query, w_key, w_value, w_out, jnp.pad(w_router, ((0, 0), (0, lane_pad)))], axis=1
        ),
        "fsdp",
        axis=0,
        tiled=True,
    )
    router_w = attn_w[:, used : used + expert_count]
    stacked = jnp.stack([w_gate, w_up, w_down], axis=1)
    edges = [experts_here * part // CHUNKS for part in range(CHUNKS + 1)]
    pieces = [
        lax.all_gather(stacked[low:high], "fsdp", axis=2, tiled=True)
        for low, high in zip(edges[:-1], edges[1:])
    ]

    gain_one = norm1_gain.astype(jnp.float32)
    gain_two = norm2_gain.astype(jnp.float32)
    start_x = emb.astype(jnp.float32) * emb_scale
    normed_one, inverse_one = rms_forward(start_x, gain_one)
    group_rows = line_gather(normed_one.astype(jnp.bfloat16), tp_count, 0)
    out_grad = cotangent.astype(jnp.float32)
    moe_grad_rows = shifted_gather((resid_scale * out_grad).astype(jnp.bfloat16), tp_count, tp_index)
    group_size = group_rows.shape[0]

    capacity = group_size * routes.shape[1] // expert_count * 2
    all_experts = jnp.arange(expert_count, dtype=jnp.int32)
    member_all = jnp.any(routes[:, :, None] == all_experts[None, None, :], axis=1)
    own_member = lax.dynamic_slice_in_dim(member_all, tp_index * local_rows, local_rows, 0)
    member = lax.dynamic_slice_in_dim(member_all, tp_index * experts_here, experts_here, 1)
    ids = jnp.arange(group_size)
    earlier = (ids[:, None] > ids[None, :]).astype(jnp.bfloat16)
    ranks = jnp.dot(earlier, member.astype(jnp.bfloat16), preferred_element_type=jnp.float32)
    places = jnp.where(member, ranks.astype(jnp.int32), -1)
    meta = jnp.concatenate(
        [jnp.sum(member.astype(jnp.int32), axis=0), (tp_index * experts_here)[None]]
    )

    tables = attend_tables()
    heads_here, kv_here = q_width // HEAD_DIM, kv_width // HEAD_DIM
    *kept, branch_part = attend(group_rows, attn_w, segment_ids, tables, heads_here, kv_here)
    attn_branch = line_scatter(branch_part, tp_count, 2)
    mid_x = start_x + resid_scale * attn_branch
    normed_two, inverse_two = rms_forward(mid_x, gain_two)
    normed_low = normed_two.astype(jnp.bfloat16)
    moe_rows = line_gather(normed_low, tp_count, 3)

    def gates_of(rows, inside):
        logits = jnp.dot(rows, router_w, preferred_element_type=jnp.float32)
        top = jnp.max(jnp.where(inside, logits, masked_value), axis=-1, keepdims=True)
        raised = jnp.where(inside, jnp.exp(jnp.where(inside, logits - top, 0.0)), 0.0)
        return raised / jnp.sum(raised, axis=-1, keepdims=True)

    gates = gates_of(normed_low, own_member)
    gates_here = lax.dynamic_slice_in_dim(
        gates_of(moe_rows, member_all).astype(jnp.bfloat16).astype(jnp.float32),
        tp_index * experts_here,
        experts_here,
        1,
    )
    place_rows = places.T[:, None, :]
    gate_rows = gates_here.T[:, None, :]

    outs = []
    for first, piece in zip(edges[:-1], pieces):
        outs.append(
            experts_step(
                meta,
                place_rows,
                places,
                gate_rows,
                moe_rows,
                moe_grad_rows,
                piece,
                first,
                capacity,
            )
        )
    grad_sums = [
        lax.psum_scatter(part[2], "fsdp", scatter_dimension=2, tiled=True) for part in outs
    ]
    y_part = functools.reduce(lambda one, two: one + two, [part[0] for part in outs])
    dx_part = functools.reduce(lambda one, two: one + two, [part[1] for part in outs])
    dx_sum = line_scatter(dx_part, tp_count, 4)
    moe_sum = shifted_scatter(y_part, tp_count, tp_index)
    out = (mid_x + resid_scale * moe_sum).astype(jnp.bfloat16)
    gates_grad = dx_sum[:, width : width + expert_count]
    gates_inner = jnp.sum(gates * gates_grad, axis=-1, keepdims=True)
    logits_grad = (gates * (gates_grad - gates_inner)).astype(jnp.bfloat16)
    normed_two_grad = dx_sum[:, :width] + contract_last(logits_grad, router_w)
    mid_from_norm, gain_two_grad = rms_backward(normed_two_grad, mid_x, inverse_two, gain_two)
    mid_grad = out_grad + mid_from_norm
    branch_grad = (resid_scale * mid_grad).astype(jnp.bfloat16)
    sent = line_gather(
        jnp.concatenate([branch_grad, jnp.pad(logits_grad, ((0, 0), (0, lane_pad)))], axis=1),
        tp_count,
        5,
    )
    router_grad = contract_first(moe_rows, sent[:, width:])
    dx_one, attn_dw = attend_back(
        group_rows, attn_w, segment_ids, tables, kept, sent
    )
    attn_grads = jnp.concatenate([attn_dw, router_grad.astype(jnp.bfloat16)], axis=1)
    normed_one_grad = line_scatter(dx_one, tp_count, 7)
    start_from_norm, gain_one_grad = rms_backward(normed_one_grad, start_x, inverse_one, gain_one)
    grad_emb = emb_scale * (mid_grad + start_from_norm)
    gain_sums = total_everywhere(
        jnp.concatenate([gain_one_grad, gain_two_grad]).reshape(8, -1), 8
    ).reshape(2, width)
    attn_sum = lax.psum_scatter(attn_grads, "fsdp", scatter_dimension=0, tiled=True).astype(
        jnp.float32
    )
    expert_sums = ()
    for first, part in zip(edges[:-1], grad_sums):
        expert_sums = widen(part, experts_here, first, expert_sums)
    return (
        out,
        grad_emb,
        gain_sums[0],
        attn_sum[:, :q_width],
        attn_sum[:, q_width : q_width + kv_width],
        attn_sum[:, q_width + kv_width : q_width + 2 * kv_width],
        attn_sum[:, q_width + 2 * kv_width : used],
        gain_sums[1],
        attn_sum[:, used : used + expert_count],
        *expert_sums,
    )


def solution(mesh):
    return jax.shard_map(
        local,
        mesh=mesh,
        in_specs=(
            P(("fsdp", "tp"), None),
            P("fsdp", None),
            P("fsdp", None),
            P(),
            P("fsdp", "tp"),
            P("fsdp", "tp"),
            P("fsdp", "tp"),
            P("fsdp", "tp"),
            P(),
            P("fsdp", None),
            P("tp", "fsdp", None),
            P("tp", "fsdp", None),
            P("tp", "fsdp", None),
            P(("fsdp", "tp"), None),
        ),
        out_specs=(
            P(("fsdp", "tp"), None),
            P(("fsdp", "tp"), None),
            P(),
            P("fsdp", "tp"),
            P("fsdp", "tp"),
            P("fsdp", "tp"),
            P("fsdp", "tp"),
            P(),
            P("fsdp", None),
            P("tp", "fsdp", None),
            P("tp", "fsdp", None),
            P("tp", "fsdp", None),
        ),
        check_vma=False,
    )
```

```python
import functools

import jax
import jax.numpy as jnp
from jax import lax
from jax.experimental import pallas as pl
from jax.experimental.pallas import tpu as pltpu
from jax.sharding import PartitionSpec as P

HEAD_DIM = 64
SEQ = 512


emb_scale = 12.0
resid_scale = 0.22
attn_scale = 0.015625
norm_eps = 1e-06
rope_base = 10000.0
masked_value = -1e30


def contract_last(left_op, right_op):
    return lax.dot_general(
        left_op, right_op, (((1,), (1,)), ((), ())), preferred_element_type=jnp.float32
    )


def contract_first(left_op, right_op):
    return lax.dot_general(
        left_op, right_op, (((0,), (0,)), ((), ())), preferred_element_type=jnp.float32
    )


def rms_forward(values, gain_vec):
    inverse = lax.rsqrt(jnp.mean(values * values, axis=-1, keepdims=True) + norm_eps)
    return (values * inverse * gain_vec, inverse)


def rms_backward(incoming, values, inverse, gain_vec):
    scaled = values * inverse
    gain_grad = jnp.sum(incoming * scaled, axis=0)
    weighted = incoming * gain_vec
    row_inner = jnp.mean(weighted * scaled, axis=-1, keepdims=True)
    return (inverse * (weighted - scaled * row_inner), gain_grad)


def line_signal(barrier, me, count):
    @pl.when(me > 0)
    def _():
        pl.semaphore_signal(barrier, inc=1, device_id={"tp": me - 1})

    @pl.when(me < count - 1)
    def _():
        pl.semaphore_signal(barrier, inc=1, device_id={"tp": me + 1})

    return jnp.where((me > 0) & (me < count - 1), 2, 1)


class Plane:
    def __init__(self, count):
        self.me = lax.axis_index("fsdp")
        self.core = lax.rem(self.me, 2)
        self.chip = lax.div(self.me, 2)
        self.chips = count // 2
        self.partner = self.me + 1 - 2 * self.core

    def chip_at(self, shift):
        return lax.rem(self.chip + shift + self.chips, self.chips)

    def peer(self, shift):
        return self.chip_at(shift) * 2 + self.core

    def signal(self, barrier):
        for shift in range(1, self.chips):
            pl.semaphore_signal(barrier, inc=1, device_id={"fsdp": self.peer(shift)})
        pl.semaphore_signal(barrier, inc=1, device_id={"fsdp": self.partner})
        return self.chips


def rows_of(ref, index, rows):
    return ref.at[pl.ds(pl.multiple_of(index * rows, rows), rows)]


class LineGather:
    def __init__(self, count, x_ref, o_ref, send_sem, recv_sem, own_sem):
        self.count, self.x_ref, self.o_ref = count, x_ref, o_ref
        self.send_sem, self.recv_sem = send_sem, recv_sem
        self.rows = x_ref.shape[0]
        me = self.me = lax.axis_index("tp")
        self.own = pltpu.make_async_copy(x_ref, rows_of(o_ref, me, self.rows), own_sem)
        steps = range(count - 1)
        self.sends = [
            [(me >= step) & (me < count - 1) for step in steps],
            [(me + step < count) & (me > 0) for step in steps],
        ]
        self.gets = [
            [me - 1 - step >= 0 for step in steps],
            [me + 1 + step < count for step in steps],
        ]

    def hop(self, way, step, chunk):
        part = rows_of(self.o_ref, chunk, self.rows)
        return pltpu.make_async_remote_copy(
            src_ref=self.x_ref if step == 0 else part,
            dst_ref=part,
            send_sem=self.send_sem.at[way, step],
            recv_sem=self.recv_sem.at[way, step],
            device_id={"tp": self.me + 1 if way == 0 else self.me - 1},
        )

    def start(self, step):
        @pl.when(self.sends[0][step])
        def _():
            self.hop(0, step, self.me - step).start()

        @pl.when(self.sends[1][step])
        def _():
            self.hop(1, step, self.me + step).start()

        if step == 0:
            self.own.start()

    def arrive(self, step):
        @pl.when(self.gets[0][step])
        def _():
            self.hop(0, step, self.me - 1 - step).wait_recv()

        @pl.when(self.gets[1][step])
        def _():
            self.hop(1, step, self.me + 1 + step).wait_recv()

    def finish(self):
        self.own.wait()
        for step in range(self.count - 1):

            @pl.when(self.sends[0][step])
            def _():
                self.hop(0, step, self.me - step).wait_send()

            @pl.when(self.sends[1][step])
            def _():
                self.hop(1, step, self.me + step).wait_send()


def line_gather_kernel(count, x_ref, o_ref, *sems):
    barrier = pltpu.get_barrier_semaphore()
    pl.semaphore_wait(barrier, line_signal(barrier, lax.axis_index("tp"), count))
    line = LineGather(count, x_ref, o_ref, *sems)
    for step in range(count - 1):
        line.start(step)
        line.arrive(step)
    line.finish()


def line_sems(count):
    return [
        pltpu.SemaphoreType.DMA((2, count - 1)),
        pltpu.SemaphoreType.DMA((2, count - 1)),
    ]


def line_gather(rows_in, count, ident):
    rows, width = rows_in.shape
    return pl.pallas_call(
        functools.partial(line_gather_kernel, count),
        out_shape=jax.ShapeDtypeStruct((rows * count, width), rows_in.dtype),
        in_specs=[pl.BlockSpec(memory_space=pltpu.VMEM)],
        out_specs=pl.BlockSpec(memory_space=pl.ANY),
        scratch_shapes=line_sems(count) + [pltpu.SemaphoreType.DMA],
        compiler_params=pltpu.CompilerParams(collective_id=ident, has_side_effects=True),
        cost_estimate=pl.CostEstimate(flops=0, transcendentals=0, bytes_accessed=150_000_000),
    )(rows_in)


def gather_both_kernel(
    tp_count, fsdp_count, x_ref, w_ref, o_ref, wo_ref,
    line_send, line_recv, own_sem, out_send, out_recv, on_send, on_recv, kept_sem,
):
    plane = Plane(fsdp_count)
    barrier = pltpu.get_barrier_semaphore()
    waits = line_signal(barrier, lax.axis_index("tp"), tp_count) + plane.signal(barrier)
    pl.semaphore_wait(barrier, waits)
    line = LineGather(tp_count, x_ref, o_ref, line_send, line_recv, own_sem)
    rows = w_ref.shape[0]

    def outward(shift, target, source_device):
        return pltpu.make_async_remote_copy(
            src_ref=w_ref,
            dst_ref=rows_of(wo_ref, source_device, rows),
            send_sem=out_send.at[shift],
            recv_sem=out_recv.at[shift],
            device_id={"fsdp": target},
        )

    def onward(shift, source_device):
        part = rows_of(wo_ref, source_device, rows)
        return pltpu.make_async_remote_copy(
            src_ref=part,
            dst_ref=part,
            send_sem=on_send.at[shift - 1],
            recv_sem=on_recv.at[shift - 1],
            device_id={"fsdp": plane.partner},
        )

    kept = pltpu.make_async_copy(w_ref, rows_of(wo_ref, plane.me, rows), kept_sem)
    line.start(0)
    for shift in range(1, plane.chips):
        outward(shift, plane.peer(shift), plane.me).start()
    outward(0, plane.partner, plane.me).start()
    kept.start()
    for shift in range(1, plane.chips):
        outward(shift, plane.peer(shift), plane.peer(-shift)).wait_recv()
        onward(shift, plane.peer(-shift)).start()
    line.arrive(0)
    for step in range(1, tp_count - 1):
        line.start(step)
        line.arrive(step)
    outward(0, plane.partner, plane.partner).wait_recv()
    for shift in range(1, plane.chips):
        onward(shift, plane.chip_at(-shift) * 2 + 1 - plane.core).wait_recv()
    for shift in range(1, plane.chips):
        outward(shift, plane.peer(shift), plane.me).wait_send()
        onward(shift, plane.peer(-shift)).wait_send()
    outward(0, plane.partner, plane.me).wait_send()
    kept.wait()
    line.finish()


def gather_both(rows_in, weights, tp_count, fsdp_count, ident):
    chips = fsdp_count // 2
    return pl.pallas_call(
        functools.partial(gather_both_kernel, tp_count, fsdp_count),
        out_shape=[
            jax.ShapeDtypeStruct((rows_in.shape[0] * tp_count, rows_in.shape[1]), rows_in.dtype),
            jax.ShapeDtypeStruct((weights.shape[0] * fsdp_count, weights.shape[1]), weights.dtype),
        ],
        in_specs=[pl.BlockSpec(memory_space=pltpu.VMEM)] * 2,
        out_specs=[pl.BlockSpec(memory_space=pl.ANY)] * 2,
        scratch_shapes=line_sems(tp_count)
        + [
            pltpu.SemaphoreType.DMA,
            pltpu.SemaphoreType.DMA((chips,)),
            pltpu.SemaphoreType.DMA((chips,)),
            pltpu.SemaphoreType.DMA((chips - 1,)),
            pltpu.SemaphoreType.DMA((chips - 1,)),
            pltpu.SemaphoreType.DMA,
        ],
        compiler_params=pltpu.CompilerParams(collective_id=ident, has_side_effects=True),
        cost_estimate=pl.CostEstimate(flops=0, transcendentals=0, bytes_accessed=150_000_000),
    )(rows_in, weights)


class LineScatter:
    def __init__(self, count, x_refs, o_ref, recv, send, send_sem, recv_sem):
        self.count, self.x_refs, self.o_ref = count, x_refs, o_ref
        self.recv, self.send = recv, send
        self.send_sem, self.recv_sem = send_sem, recv_sem
        self.rows = o_ref.shape[0]
        me = self.me = lax.axis_index("tp")
        self.behind = (me, count - 1 - me)
        self.has_next = (me < count - 1, me > 0)
        self.has_prev = (me > 0, me < count - 1)

    def block(self, dest):
        area = pl.ds(pl.multiple_of(dest * self.rows, self.rows), self.rows)
        total = self.x_refs[0][area, :].astype(jnp.float32)
        for x_ref in self.x_refs[1:]:
            total = total + x_ref[area, :].astype(jnp.float32)
        return total

    def hop(self, way, step):
        return pltpu.make_async_remote_copy(
            src_ref=self.send.at[way, step],
            dst_ref=self.recv.at[way, step],
            send_sem=self.send_sem.at[way, step],
            recv_sem=self.recv_sem.at[way, step],
            device_id={"tp": self.me + 1 if way == 0 else self.me - 1},
        )

    def start(self, step):
        count, me, send = self.count, self.me, self.send
        for way in range(2):
            dest = count - 1 - step + me if way == 0 else step - (count - 1 - me)
            active = self.has_next[way] & (step >= self.behind[way])

            @pl.when(active & (self.behind[way] == 0))
            def _():
                send[way, step] = self.block(dest).astype(send.dtype)
                self.hop(way, step).start()

            if step > 0:

                @pl.when(active & (self.behind[way] > 0))
                def _():
                    total = self.block(dest) + self.recv[way, step - 1].astype(jnp.float32)
                    send[way, step] = total.astype(send.dtype)
                    self.hop(way, step).start()

    def arrive(self, step):
        for way in range(2):

            @pl.when(self.has_prev[way] & (step >= self.behind[way] - 1))
            def _():
                self.hop(way, step).wait_recv()

    def finish(self):
        self.o_ref[...] = self.block(self.me)
        for way in range(2):

            @pl.when(self.has_prev[way])
            def _():
                self.o_ref[...] += self.recv[way, self.count - 2].astype(jnp.float32)

        for step in range(self.count - 1):
            for way in range(2):

                @pl.when(self.has_next[way] & (step >= self.behind[way]))
                def _():
                    self.hop(way, step).wait_send()


def line_scatter_kernel(count, parts, *refs):
    barrier = pltpu.get_barrier_semaphore()
    pl.semaphore_wait(barrier, line_signal(barrier, lax.axis_index("tp"), count))
    line = LineScatter(count, refs[:parts], *refs[parts:])
    for step in range(count - 1):
        line.start(step)
        line.arrive(step)
    line.finish()


def line_buffers(count, rows, width):
    return [
        pltpu.VMEM((2, count - 1, rows, width), jnp.bfloat16),
        pltpu.VMEM((2, count - 1, rows, width), jnp.bfloat16),
    ] + line_sems(count)


def line_scatter(parts, count, ident):
    rows, width = parts[0].shape[0] // count, parts[0].shape[1]
    return pl.pallas_call(
        functools.partial(line_scatter_kernel, count, len(parts)),
        out_shape=jax.ShapeDtypeStruct((rows, width), jnp.float32),
        in_specs=[pl.BlockSpec(memory_space=pltpu.VMEM)] * len(parts),
        out_specs=pl.BlockSpec(memory_space=pltpu.VMEM),
        scratch_shapes=line_buffers(count, rows, width),
        compiler_params=pltpu.CompilerParams(
            collective_id=ident, has_side_effects=True, vmem_limit_bytes=60 << 20
        ),
        cost_estimate=pl.CostEstimate(flops=0, transcendentals=0, bytes_accessed=150_000_000),
    )(*parts)


def scatter_both_kernel(
    tp_count, fsdp_count, x_ref, w_ref, o_ref, wo_ref,
    line_recv, line_send, line_send_sem, line_recv_sem,
    pair_got, chip_sums, chip_got, pair_send, pair_recv, chip_send, chip_recv,
):
    plane = Plane(fsdp_count)
    barrier = pltpu.get_barrier_semaphore()
    waits = line_signal(barrier, lax.axis_index("tp"), tp_count) + plane.signal(barrier)
    pl.semaphore_wait(barrier, waits)
    line = LineScatter(
        tp_count, [x_ref], o_ref, line_recv, line_send, line_send_sem, line_recv_sem
    )
    rows = wo_ref.shape[0]

    def to_pair(shift):
        return pltpu.make_async_remote_copy(
            src_ref=rows_of(w_ref, plane.chip_at(shift) * 2 + 1 - plane.core, rows),
            dst_ref=pair_got.at[shift],
            send_sem=pair_send.at[shift],
            recv_sem=pair_recv.at[shift],
            device_id={"fsdp": plane.partner},
        )

    def to_chip(shift):
        return pltpu.make_async_remote_copy(
            src_ref=chip_sums.at[shift - 1],
            dst_ref=chip_got.at[shift - 1],
            send_sem=chip_send.at[shift - 1],
            recv_sem=chip_recv.at[shift - 1],
            device_id={"fsdp": plane.peer(shift)},
        )

    def both_cores(shift):
        own = pl.ds(pl.multiple_of(plane.peer(shift) * rows, rows), rows)
        return w_ref[own, :].astype(jnp.float32) + pair_got[shift].astype(jnp.float32)

    line.start(0)
    order = list(range(1, plane.chips)) + [0]
    for shift in order:
        to_pair(shift).start()
    for shift in order:
        to_pair(shift).wait_recv()
        if shift > 0:
            chip_sums[shift - 1] = both_cores(shift).astype(chip_sums.dtype)
            to_chip(shift).start()
    line.arrive(0)
    for step in range(1, tp_count - 1):
        line.start(step)
        line.arrive(step)
    total = both_cores(0)
    for shift in range(1, plane.chips):
        to_chip(shift).wait_recv()
        total = total + chip_got[shift - 1].astype(jnp.float32)
    wo_ref[...] = total
    line.finish()
    for shift in order:
        to_pair(shift).wait_send()
        if shift > 0:
            to_chip(shift).wait_send()


def scatter_both(partial_rows, weight_grads, tp_count, fsdp_count, ident):
    rows, width = partial_rows.shape[0] // tp_count, partial_rows.shape[1]
    w_rows, w_width = weight_grads.shape[0] // fsdp_count, weight_grads.shape[1]
    chips = fsdp_count // 2
    return pl.pallas_call(
        functools.partial(scatter_both_kernel, tp_count, fsdp_count),
        out_shape=[
            jax.ShapeDtypeStruct((rows, width), jnp.float32),
            jax.ShapeDtypeStruct((w_rows, w_width), jnp.float32),
        ],
        in_specs=[pl.BlockSpec(memory_space=pltpu.VMEM)] * 2,
        out_specs=[pl.BlockSpec(memory_space=pltpu.VMEM)] * 2,
        scratch_shapes=line_buffers(tp_count, rows, width)
        + [
            pltpu.VMEM((chips, w_rows, w_width), jnp.bfloat16),
            pltpu.VMEM((chips - 1, w_rows, w_width), jnp.bfloat16),
            pltpu.VMEM((chips - 1, w_rows, w_width), jnp.bfloat16),
            pltpu.SemaphoreType.DMA((chips,)),
            pltpu.SemaphoreType.DMA((chips,)),
            pltpu.SemaphoreType.DMA((chips - 1,)),
            pltpu.SemaphoreType.DMA((chips - 1,)),
        ],
        compiler_params=pltpu.CompilerParams(
            collective_id=ident, has_side_effects=True, vmem_limit_bytes=60 << 20
        ),
        cost_estimate=pl.CostEstimate(flops=0, transcendentals=0, bytes_accessed=150_000_000),
    )(partial_rows, weight_grads)


def pack_kernel(*refs):
    for slot, source in enumerate(refs[:-1]):
        refs[-1][0, slot] = source[0]


def pack(stacks, low, high):
    _, rows, width = stacks[0].shape
    return pl.pallas_call(
        pack_kernel,
        grid=(high - low,),
        in_specs=[pl.BlockSpec((1, rows, width), lambda step: (step + low, 0, 0))] * len(stacks),
        out_specs=pl.BlockSpec((1, len(stacks), rows, width), lambda step: (step, 0, 0, 0)),
        out_shape=jax.ShapeDtypeStruct((high - low, len(stacks), rows, width), jnp.bfloat16),
    )(*stacks)


SLOTS = 256


def experts_kernel(
    first_expert,
    capacity,
    meta,
    place_row,
    place_cols,
    gate_row,
    x_ref,
    g_ref,
    weights,
    y_out,
    dx_out,
    grads,
    *totals,
):
    y_ref, dx_ref = totals or (y_out, dx_out)
    step = pl.program_id(0)
    expert = step + first_expert
    group, width = x_ref.shape
    tail = dx_ref.shape[1] - width

    @pl.when(step == 0)
    def _():
        y_ref[...] = jnp.zeros_like(y_ref)
        dx_ref[...] = jnp.zeros_like(dx_ref)

    lanes = lax.broadcasted_iota(jnp.int32, place_cols.shape, 1)
    place_col = jnp.sum(jnp.where(lanes == expert, place_cols[...], 0), axis=1, keepdims=True)
    column = expert + meta[meta.shape[0] - 1]
    mark = jnp.where(lax.broadcasted_iota(jnp.int32, (1, tail), 1) == column, 1.0, 0.0)

    def run(base, span):
        slots = lax.broadcasted_iota(jnp.int32, (span, group), 0) + base
        hit = slots == place_row[0]
        pick = jnp.where(hit, 1.0, 0.0).astype(jnp.bfloat16)
        scale = jnp.sum(jnp.where(hit, gate_row[0], 0.0), axis=1, keepdims=True)
        x_taken = jnp.dot(pick, x_ref[...], preferred_element_type=jnp.float32).astype(jnp.bfloat16)
        g_taken = jnp.dot(pick, g_ref[...], preferred_element_type=jnp.float32).astype(jnp.bfloat16)
        gate_pre = jnp.dot(x_taken, weights[0, 0], preferred_element_type=jnp.float32)
        up_pre = jnp.dot(x_taken, weights[0, 1], preferred_element_type=jnp.float32)
        raw = jnp.dot(g_taken, weights[0, 2], preferred_element_type=jnp.float32)
        sig = jax.nn.sigmoid(gate_pre)
        silu = gate_pre * sig
        act = (silu * up_pre).astype(jnp.bfloat16).astype(jnp.float32)
        slot_grad = jnp.sum(act * raw, axis=1, keepdims=True)
        act_grad = raw * scale
        act_scaled = (act * scale).astype(jnp.bfloat16)
        gate_grad = (act_grad * up_pre * sig * (1.0 + gate_pre * (1.0 - sig))).astype(jnp.bfloat16)
        up_grad = (act_grad * silu).astype(jnp.bfloat16)
        extra = (slot_grad * mark).astype(jnp.bfloat16)
        rows_out = contract_last(act_scaled, weights[0, 2]).astype(jnp.bfloat16)
        rows_in = (
            contract_last(gate_grad, weights[0, 0]) + contract_last(up_grad, weights[0, 1])
        ).astype(jnp.bfloat16)
        for slot, left_op, right_op in (
            (0, x_taken, gate_grad),
            (1, x_taken, up_grad),
            (2, g_taken, act_scaled),
        ):
            grad = contract_first(left_op, right_op)
            if base > 0:
                grad = grad + grads[0, slot].astype(jnp.float32)
            grads[0, slot] = grad.astype(jnp.bfloat16)
        block = min(256, group)
        for start in range(0, group, block):
            back = jnp.where(
                lax.broadcasted_iota(jnp.int32, (block, span), 1) + base
                == place_col[start : start + block],
                1.0,
                0.0,
            ).astype(jnp.bfloat16)
            for target, low_col, addend in (
                (y_ref, 0, rows_out),
                (dx_ref, 0, rows_in),
                (dx_ref, width, extra),
            ):
                area = (slice(start, start + block), slice(low_col, low_col + addend.shape[1]))
                target[area] = (
                    target[area].astype(jnp.float32)
                    + jnp.dot(back, addend, preferred_element_type=jnp.float32)
                ).astype(target.dtype)

    run(0, min(SLOTS, capacity))
    for base in range(SLOTS, capacity, SLOTS):
        span = min(SLOTS, -(-(capacity - base) // 16) * 16)

        @pl.when(meta[expert] > base)
        def _():
            run(base, span)

    @pl.when((step == pl.num_programs(0) - 1) & (len(totals) > 0))
    def _():
        y_out[...] = y_ref[...].astype(y_out.dtype)
        dx_out[...] = dx_ref[...].astype(dx_out.dtype)


def experts_step(meta, place_rows, place_cols, gate_rows, x_rows, g_rows, weights, first, count, skip, capacity):
    group, width = x_rows.shape
    hidden = weights.shape[-1]
    totals = [pltpu.VMEM((group, width), jnp.float32), pltpu.VMEM((group, width + 128), jnp.float32)]
    tail = 128

    def whole(shape):
        return pl.BlockSpec(
            shape, lambda step, meta: (0,) * len(shape), pipeline_mode=pl.Buffered(1)
        )

    def row(shape):
        return pl.BlockSpec(shape, lambda step, meta: (step + first, 0, 0))

    def big(offset):
        return pl.BlockSpec((1, 3, width, hidden), lambda step, meta: (step + offset, 0, 0, 0))

    return pl.pallas_call(
        functools.partial(experts_kernel, first, capacity),
        grid_spec=pltpu.PrefetchScalarGridSpec(
            num_scalar_prefetch=1,
            grid=(count,),
            in_specs=[
                row((1, 1, group)),
                whole(place_cols.shape),
                row((1, 1, group)),
                whole(x_rows.shape),
                whole(g_rows.shape),
                big(skip),
            ],
            out_specs=[
                whole((group, width)),
                whole((group, width + tail)),
                big(0),
            ],
            scratch_shapes=totals if group <= 1024 else [],
        ),
        out_shape=[
            jax.ShapeDtypeStruct((group, width), jnp.bfloat16),
            jax.ShapeDtypeStruct((group, width + tail), jnp.bfloat16),
            jax.ShapeDtypeStruct((count, 3, width, hidden), jnp.bfloat16),
        ],
        compiler_params=pltpu.CompilerParams(
            dimension_semantics=("arbitrary",), vmem_limit_bytes=63 << 20
        ),
        cost_estimate=pl.CostEstimate(
            flops=count * 17 * 2 * 408 * width * hidden,
            transcendentals=count * 408 * hidden,
            bytes_accessed=count * 12 * width * hidden,
        ),
    )(meta, place_rows, place_cols, gate_rows, x_rows, g_rows, weights)


def rotate_head(values, cosine, sine, sign):
    half = values.shape[-1] // 2
    other = jnp.concatenate([values[:, half:], values[:, :half]], axis=1)
    return values * cosine + other * (sine * sign)


def segment_bias(seg_row, seg_col):
    shape = (seg_col.shape[0], seg_row.shape[1])
    keys = lax.broadcasted_iota(jnp.int32, shape, 0)
    queries = lax.broadcasted_iota(jnp.int32, shape, 1)
    return jnp.where((keys <= queries) & (seg_col == seg_row), 0.0, masked_value)


def attend_kernel(
    x_ref,
    w_ref,
    seg_row,
    seg_col,
    cos_ref,
    sin_ref,
    q_ref,
    k_ref,
    v_ref,
    mixed_ref,
    logsum_ref,
    branch_ref,
    bias,
    v_turned,
    mixed_heads,
):
    heads, kv_heads = q_ref.shape[0], k_ref.shape[0]
    per_kv = heads // kv_heads
    block = SEQ // 2
    edge = (heads + 2 * kv_heads) * HEAD_DIM
    proj = jnp.dot(x_ref[...], w_ref[:, :edge], preferred_element_type=jnp.float32)
    cosine, sine = cos_ref[...], sin_ref[...]
    for head in range(heads + 2 * kv_heads):
        part = proj[:, head * HEAD_DIM : (head + 1) * HEAD_DIM]
        if head < heads:
            q_ref[head] = rotate_head(part, cosine, sine, 1.0).astype(jnp.bfloat16)
        elif head < heads + kv_heads:
            k_ref[head - heads] = rotate_head(part, cosine, sine, 1.0).astype(jnp.bfloat16)
        else:
            v_ref[head - heads - kv_heads] = part.astype(jnp.bfloat16)
            v_turned[head - heads - kv_heads] = part.T.astype(jnp.bfloat16)
    bias[...] = segment_bias(seg_row[0], seg_col[0])

    def one_head(head, carry):
        kv = head // per_kv
        for part in range(2):
            span, low = block * (part + 1), block * part
            scores = contract_last(k_ref[kv, :span], q_ref[head, low : low + block]) * attn_scale
            scores = scores + bias[:span, low : low + block]
            top = jnp.max(scores, axis=0, keepdims=True)
            raised = jnp.exp(scores - top)
            total = jnp.sum(raised, axis=0, keepdims=True)
            probs = (raised * (1.0 / total)).astype(jnp.bfloat16)
            turned = jnp.dot(v_turned[kv, :, :span], probs, preferred_element_type=jnp.float32)
            mixed_heads[head, low : low + block, :] = turned.T.astype(jnp.bfloat16)
            logsum_ref[0, pl.ds(head, 1), low : low + block] = top + jnp.log(total)
        return carry

    lax.fori_loop(0, heads, one_head, 0)
    for head in range(heads):
        mixed_ref[:, head * HEAD_DIM : (head + 1) * HEAD_DIM] = mixed_heads[head]
    branch_ref[...] = contract_last(
        mixed_ref[...], w_ref[:, edge : edge + heads * HEAD_DIM]
    ).astype(jnp.bfloat16)


def attend_back_kernel(
    x_ref,
    w_ref,
    seg_row,
    seg_col,
    cos_ref,
    sin_ref,
    q_ref,
    k_ref,
    v_ref,
    mixed_ref,
    logsum_ref,
    moe_rows,
    branch_grad,
    dx_ref,
    dw_ref,
    bias,
    k_turned,
    mixed_grads,
    q_grads,
    kv_grads,
    qkv_grad,
    dw_acc,
):
    heads, kv_heads = q_ref.shape[0], k_ref.shape[0]
    per_kv = heads // kv_heads
    block = SEQ // 2
    edge = (heads + 2 * kv_heads) * HEAD_DIM
    step = pl.program_id(0)
    out_edge = edge + heads * HEAD_DIM
    width = x_ref.shape[1]
    grad = jnp.dot(
        branch_grad[:, :width], w_ref[:, edge:out_edge], preferred_element_type=jnp.float32
    ).astype(jnp.bfloat16)
    for head in range(heads):
        mixed_grads[head] = grad[:, head * HEAD_DIM : (head + 1) * HEAD_DIM]
    for kv in range(kv_heads):
        k_turned[kv] = k_ref[kv].astype(jnp.float32).T.astype(jnp.bfloat16)
    bias[...] = segment_bias(seg_row[0], seg_col[0])
    kv_grads[...] = jnp.zeros_like(kv_grads)

    def one_head(head, carry):
        kv = head // per_kv
        for part in range(2):
            span, low = block * (part + 1), block * part
            high = low + block
            scores = contract_last(k_ref[kv, :span], q_ref[head, low:high]) * attn_scale
            scores = scores + bias[:span, low:high]
            probs = jnp.exp(scores - logsum_ref[0, pl.ds(head, 1), low:high])
            probs_grad = contract_last(v_ref[kv, :span], mixed_grads[head, low:high])
            inner = jnp.sum(probs * probs_grad, axis=0, keepdims=True)
            score_grad = (probs * (probs_grad - inner)).astype(jnp.bfloat16)
            turned = jnp.dot(k_turned[kv, :, :span], score_grad, preferred_element_type=jnp.float32)
            q_grads[head, low:high, :] = turned.T * attn_scale
            kv_grads[0, kv, :span, :] += jnp.dot(
                score_grad, q_ref[head, low:high], preferred_element_type=jnp.float32
            )
            kv_grads[1, kv, :span, :] += jnp.dot(
                probs.astype(jnp.bfloat16), mixed_grads[head, low:high],
                preferred_element_type=jnp.float32,
            )
        return carry

    lax.fori_loop(0, heads, one_head, 0)
    cosine, sine = cos_ref[...], sin_ref[...]
    for head in range(heads + 2 * kv_heads):
        if head < heads:
            part = rotate_head(q_grads[head], cosine, sine, -1.0)
        elif head < heads + kv_heads:
            part = rotate_head(kv_grads[0, head - heads] * attn_scale, cosine, sine, -1.0)
        else:
            part = kv_grads[1, head - heads - kv_heads]
        qkv_grad[:, head * HEAD_DIM : (head + 1) * HEAD_DIM] = part.astype(jnp.bfloat16)
    dx_ref[...] = contract_last(qkv_grad[...], w_ref[:, :edge]).astype(jnp.bfloat16)
    for low, high, left_op, right_op in (
        (0, edge, x_ref[...], qkv_grad[...]),
        (edge, out_edge, branch_grad[:, :width], mixed_ref[...]),
        (out_edge, dw_acc.shape[1], moe_rows[...], branch_grad[:, width:]),
    ):
        part = contract_first(left_op, right_op)

        @pl.when(step == 0)
        def _():
            dw_acc[:, low:high] = part

        @pl.when(step > 0)
        def _():
            dw_acc[:, low:high] += part

    @pl.when(step == pl.num_programs(0) - 1)
    def _():
        dw_ref[...] = dw_acc[...].astype(jnp.bfloat16)


def fixed(shape):
    return pl.BlockSpec(shape, lambda seq: (0,) * len(shape), pipeline_mode=pl.Buffered(1))


def by_row(width):
    return pl.BlockSpec((SEQ, width), lambda seq: (seq, 0))


def by_head(heads):
    return pl.BlockSpec((heads, SEQ, HEAD_DIM), lambda seq: (0, seq, 0))


def attend_tables():
    half = HEAD_DIM // 2
    positions = jnp.arange(SEQ).astype(jnp.float32)
    frequency = rope_base ** (-jnp.arange(half).astype(jnp.float32) * 2.0 / HEAD_DIM)
    angles = positions[:, None] * frequency[None, :]
    cosine, sine = jnp.cos(angles), jnp.sin(angles)
    return (
        jnp.concatenate([cosine, cosine], axis=1),
        jnp.concatenate([-sine, sine], axis=1),
    )


def attend(rows, weights, segments, tables, heads, kv_heads):
    group, width = rows.shape
    seqs = group // SEQ
    return pl.pallas_call(
        attend_kernel,
        grid=(seqs,),
        in_specs=[
            by_row(width),
            fixed(weights.shape),
            pl.BlockSpec((1, 1, SEQ), lambda seq: (seq, 0, 0)),
            pl.BlockSpec((1, SEQ, 1), lambda seq: (seq, 0, 0)),
            fixed(tables[0].shape),
            fixed(tables[1].shape),
        ],
        out_specs=[
            by_head(heads),
            by_head(kv_heads),
            by_head(kv_heads),
            by_row(heads * HEAD_DIM),
            pl.BlockSpec((1, heads, SEQ), lambda seq: (seq, 0, 0)),
            by_row(width),
        ],
        out_shape=[
            jax.ShapeDtypeStruct((heads, group, HEAD_DIM), jnp.bfloat16),
            jax.ShapeDtypeStruct((kv_heads, group, HEAD_DIM), jnp.bfloat16),
            jax.ShapeDtypeStruct((kv_heads, group, HEAD_DIM), jnp.bfloat16),
            jax.ShapeDtypeStruct((group, heads * HEAD_DIM), jnp.bfloat16),
            jax.ShapeDtypeStruct((seqs, heads, SEQ), jnp.float32),
            jax.ShapeDtypeStruct((group, width), jnp.bfloat16),
        ],
        scratch_shapes=[
            pltpu.VMEM((SEQ, SEQ), jnp.float32),
            pltpu.VMEM((kv_heads, HEAD_DIM, SEQ), jnp.bfloat16),
            pltpu.VMEM((heads, SEQ, HEAD_DIM), jnp.bfloat16),
        ],
        compiler_params=pltpu.CompilerParams(
            dimension_semantics=("arbitrary",), vmem_limit_bytes=56 << 20
        ),
        cost_estimate=pl.CostEstimate(
            flops=10_000_000_000, transcendentals=3_000_000, bytes_accessed=60_000_000
        ),
    )(rows, weights, segments[:, None, :], segments[:, :, None], *tables)


def attend_back(rows, weights, segments, tables, kept, moe_rows, branch_grad):
    queries, keys, values, mixed, logsum = kept
    group, width = rows.shape
    heads, kv_heads = queries.shape[0], keys.shape[0]
    used = weights.shape[1]
    edge = (heads + 2 * kv_heads) * HEAD_DIM
    return pl.pallas_call(
        attend_back_kernel,
        grid=(group // SEQ,),
        in_specs=[
            by_row(width),
            fixed(weights.shape),
            pl.BlockSpec((1, 1, SEQ), lambda seq: (seq, 0, 0)),
            pl.BlockSpec((1, SEQ, 1), lambda seq: (seq, 0, 0)),
            fixed(tables[0].shape),
            fixed(tables[1].shape),
            by_head(heads),
            by_head(kv_heads),
            by_head(kv_heads),
            by_row(heads * HEAD_DIM),
            pl.BlockSpec((1, heads, SEQ), lambda seq: (seq, 0, 0)),
            by_row(width),
            by_row(branch_grad.shape[1]),
        ],
        out_specs=[by_row(width), fixed((width, used))],
        out_shape=[
            jax.ShapeDtypeStruct((group, width), jnp.bfloat16),
            jax.ShapeDtypeStruct((width, used), jnp.bfloat16),
        ],
        scratch_shapes=[
            pltpu.VMEM((SEQ, SEQ), jnp.float32),
            pltpu.VMEM((kv_heads, HEAD_DIM, SEQ), jnp.bfloat16),
            pltpu.VMEM((heads, SEQ, HEAD_DIM), jnp.bfloat16),
            pltpu.VMEM((heads, SEQ, HEAD_DIM), jnp.float32),
            pltpu.VMEM((2, kv_heads, SEQ, HEAD_DIM), jnp.float32),
            pltpu.VMEM((SEQ, edge), jnp.bfloat16),
            pltpu.VMEM((width, used), jnp.float32),
        ],
        compiler_params=pltpu.CompilerParams(
            dimension_semantics=("arbitrary",), vmem_limit_bytes=60 << 20
        ),
        cost_estimate=pl.CostEstimate(
            flops=20_000_000_000, transcendentals=3_000_000, bytes_accessed=100_000_000
        ),
    )(rows, weights, segments[:, None, :], segments[:, :, None], *tables,
      queries, keys, values, mixed, logsum, moe_rows, branch_grad)


def total_kernel(tp_count, fsdp_count, x_ref, o_ref, tp_got, fsdp_got, send_sem, recv_sem):
    tp_me, fsdp_me = lax.axis_index("tp"), lax.axis_index("fsdp")
    barrier = pltpu.get_barrier_semaphore()
    for shift in range(1, tp_count):
        pl.semaphore_signal(barrier, inc=1, device_id={"tp": lax.rem(tp_me + shift, tp_count)})
    for shift in range(1, fsdp_count):
        pl.semaphore_signal(
            barrier, inc=1, device_id={"fsdp": lax.rem(fsdp_me + shift, fsdp_count)}
        )
    pl.semaphore_wait(barrier, tp_count + fsdp_count - 2)

    def exchange(axis, me, count, source, got, base):
        copies = []
        for shift in range(1, count):
            copies.append(
                pltpu.make_async_remote_copy(
                    src_ref=source,
                    dst_ref=got.at[me],
                    send_sem=send_sem.at[base + shift],
                    recv_sem=recv_sem.at[base + shift],
                    device_id={axis: lax.rem(me + shift, count)},
                )
            )
            copies[-1].start()
        got[me] = source[...]
        for copy in copies:
            copy.wait()
        total = got[0]
        for index in range(1, count):
            total = total + got[index]
        return total

    o_ref[...] = exchange("tp", tp_me, tp_count, x_ref, tp_got, 0)
    o_ref[...] = exchange("fsdp", fsdp_me, fsdp_count, o_ref, fsdp_got, tp_count)


def total_everywhere(values, ident):
    tp_count, fsdp_count = lax.axis_size("tp"), lax.axis_size("fsdp")
    return pl.pallas_call(
        functools.partial(total_kernel, tp_count, fsdp_count),
        out_shape=jax.ShapeDtypeStruct(values.shape, values.dtype),
        in_specs=[pl.BlockSpec(memory_space=pltpu.VMEM)],
        out_specs=pl.BlockSpec(memory_space=pltpu.VMEM),
        scratch_shapes=[
            pltpu.VMEM((tp_count,) + values.shape, values.dtype),
            pltpu.VMEM((fsdp_count,) + values.shape, values.dtype),
            pltpu.SemaphoreType.DMA((tp_count + fsdp_count,)),
            pltpu.SemaphoreType.DMA((tp_count + fsdp_count,)),
        ],
        compiler_params=pltpu.CompilerParams(collective_id=ident, has_side_effects=True),
    )(values)


def widen_kernel(packed, *refs):
    for slot, target in enumerate(refs[-3:]):
        target[0] = packed[0, slot].astype(jnp.float32)


def widen(packed, count, first, held):
    span, _, rows, width = packed.shape
    shape = jax.ShapeDtypeStruct((count, rows, width), jnp.float32)
    return pl.pallas_call(
        widen_kernel,
        grid=(span,),
        in_specs=[pl.BlockSpec((1, 3, rows, width), lambda step: (step, 0, 0, 0))]
        + [pl.BlockSpec(memory_space=pl.ANY)] * len(held),
        out_specs=[pl.BlockSpec((1, rows, width), lambda step: (step + first, 0, 0))] * 3,
        out_shape=[shape] * 3,
        input_output_aliases={1 + index: index for index in range(len(held))},
    )(packed, *held)


def shifted_gather(block, count, me):
    rows = block.shape[0]
    whole = jnp.zeros((rows * count, block.shape[1]), block.dtype)
    whole = lax.dynamic_update_slice_in_dim(whole, block, me * rows, 0)
    for shift in range(1, count):
        got = lax.ppermute(block, "tp", [(i, (i + shift) % count) for i in range(count)])
        whole = lax.dynamic_update_slice_in_dim(
            whole, got, lax.rem(me + count - shift, count) * rows, 0
        )
    return whole


def shifted_scatter(partial_rows, count, me):
    rows = partial_rows.shape[0] // count
    total = lax.dynamic_slice_in_dim(partial_rows, me * rows, rows, 0).astype(jnp.float32)
    for shift in range(1, count):
        block = lax.dynamic_slice_in_dim(
            partial_rows, lax.rem(me + shift, count) * rows, rows, 0
        ).astype(jnp.bfloat16)
        got = lax.ppermute(block, "tp", [(i, (i + shift) % count) for i in range(count)])
        total = total + got.astype(jnp.float32)
    return total


GATHERS = 2
RUNS = (0, 2, 5, 10)


def local(
    emb,
    segment_ids,
    routes,
    norm1_gain,
    w_query,
    w_key,
    w_value,
    w_out,
    norm2_gain,
    w_router,
    w_gate,
    w_up,
    w_down,
    cotangent,
):
    local_rows, width = emb.shape
    tp_count = lax.axis_size("tp")
    tp_index = lax.axis_index("tp")
    experts_here = w_gate.shape[0]
    expert_count = w_router.shape[1]
    q_width, kv_width = w_query.shape[1], w_key.shape[1]
    used = 2 * (q_width + kv_width)
    lane_pad = 128 - expert_count
    edges = [experts_here * part // GATHERS for part in range(GATHERS + 1)]
    pieces = [
        lax.all_gather(pack([w_gate, w_up, w_down], low, high), "fsdp", axis=2, tiled=True)
        for low, high in zip(edges[:-1], edges[1:])
    ]
    gain_one = norm1_gain.astype(jnp.float32)
    gain_two = norm2_gain.astype(jnp.float32)
    start_x = emb.astype(jnp.float32) * emb_scale
    normed_one, inverse_one = rms_forward(start_x, gain_one)
    fsdp_count = lax.axis_size("fsdp")
    group_rows, attn_w = gather_both(
        normed_one.astype(jnp.bfloat16),
        jnp.concatenate(
            [w_query, w_key, w_value, w_out, jnp.pad(w_router, ((0, 0), (0, lane_pad)))], axis=1
        ),
        tp_count,
        fsdp_count,
        0,
    )
    router_w = attn_w[:, used : used + expert_count]
    out_grad = cotangent.astype(jnp.float32)
    moe_grad = (resid_scale * out_grad).astype(jnp.bfloat16)
    moe_grad, group_rows = lax.optimization_barrier((moe_grad, group_rows))
    moe_grad_rows = shifted_gather(moe_grad, tp_count, tp_index)
    group_size = group_rows.shape[0]

    capacity = group_size * routes.shape[1] // expert_count * 2
    all_experts = jnp.arange(expert_count, dtype=jnp.int32)
    member_all = jnp.any(routes[:, :, None] == all_experts[None, None, :], axis=1)
    own_member = lax.dynamic_slice_in_dim(member_all, tp_index * local_rows, local_rows, 0)
    member = lax.dynamic_slice_in_dim(member_all, tp_index * experts_here, experts_here, 1)
    ids = jnp.arange(group_size)
    earlier = (ids[:, None] > ids[None, :]).astype(jnp.bfloat16)
    ranks = jnp.dot(earlier, member.astype(jnp.bfloat16), preferred_element_type=jnp.float32)
    places = jnp.where(member, ranks.astype(jnp.int32), -1)
    meta = jnp.concatenate(
        [jnp.sum(member.astype(jnp.int32), axis=0), (tp_index * experts_here)[None]]
    )

    tables = attend_tables()
    heads_here, kv_here = q_width // HEAD_DIM, kv_width // HEAD_DIM
    *kept, branch_part = attend(group_rows, attn_w, segment_ids, tables, heads_here, kv_here)
    attn_branch = line_scatter([branch_part], tp_count, 2)
    mid_x = start_x + resid_scale * attn_branch
    normed_two, inverse_two = rms_forward(mid_x, gain_two)
    normed_low = normed_two.astype(jnp.bfloat16)
    moe_rows = line_gather(normed_low, tp_count, 3)

    def gates_of(rows, inside):
        logits = jnp.dot(rows, router_w, preferred_element_type=jnp.float32)
        top = jnp.max(jnp.where(inside, logits, masked_value), axis=-1, keepdims=True)
        raised = jnp.where(inside, jnp.exp(jnp.where(inside, logits - top, 0.0)), 0.0)
        return raised / jnp.sum(raised, axis=-1, keepdims=True)

    gates = gates_of(normed_low, own_member)
    gates_here = lax.dynamic_slice_in_dim(
        gates_of(moe_rows, member_all).astype(jnp.bfloat16).astype(jnp.float32),
        tp_index * experts_here,
        experts_here,
        1,
    )
    place_rows = places.T[:, None, :]
    gate_rows = gates_here.T[:, None, :]

    outs = []
    runs = sorted({edge * experts_here // RUNS[-1] for edge in RUNS} | set(edges))
    for first, last in zip(runs[:-1], runs[1:]):
        home = max(index for index in range(GATHERS) if edges[index] <= first)
        outs.append(
            experts_step(
                meta,
                place_rows,
                places,
                gate_rows,
                moe_rows,
                moe_grad_rows,
                pieces[home],
                first,
                last - first,
                first - edges[home],
                capacity,
            )
        )
    grad_sums = [
        lax.psum_scatter(part[2], "fsdp", scatter_dimension=2, tiled=True) for part in outs
    ]
    dx_sum = line_scatter([part[1] for part in outs], tp_count, 4)
    gates_grad = dx_sum[:, width : width + expert_count]
    gates_inner = jnp.sum(gates * gates_grad, axis=-1, keepdims=True)
    logits_grad = (gates * (gates_grad - gates_inner)).astype(jnp.bfloat16)
    normed_two_grad = dx_sum[:, :width] + contract_last(logits_grad, router_w)
    mid_from_norm, gain_two_grad = rms_backward(normed_two_grad, mid_x, inverse_two, gain_two)
    mid_grad = out_grad + mid_from_norm
    branch_grad = (resid_scale * mid_grad).astype(jnp.bfloat16)
    sent = line_gather(
        jnp.concatenate([branch_grad, jnp.pad(logits_grad, ((0, 0), (0, lane_pad)))], axis=1),
        tp_count,
        5,
    )
    y_parts, sent = lax.optimization_barrier(([part[0] for part in outs], sent))
    y_part = functools.reduce(
        lambda one, two: one + two, [part.astype(jnp.float32) for part in y_parts]
    )
    moe_sum = shifted_scatter(y_part, tp_count, tp_index)
    out = (mid_x + resid_scale * moe_sum).astype(jnp.bfloat16)
    dx_one, attn_grads = attend_back(group_rows, attn_w, segment_ids, tables, kept, moe_rows, sent)
    normed_one_grad, attn_sum = scatter_both(dx_one, attn_grads, tp_count, fsdp_count, 7)
    start_from_norm, gain_one_grad = rms_backward(normed_one_grad, start_x, inverse_one, gain_one)
    grad_emb = emb_scale * (mid_grad + start_from_norm)
    gain_sums = total_everywhere(
        jnp.concatenate([gain_one_grad, gain_two_grad]).reshape(8, -1), 8
    ).reshape(2, width)
    expert_sums = ()
    for first, part in zip(runs[:-1], grad_sums):
        expert_sums = widen(part, experts_here, first, expert_sums)
    return (
        out,
        grad_emb,
        gain_sums[0],
        attn_sum[:, :q_width],
        attn_sum[:, q_width : q_width + kv_width],
        attn_sum[:, q_width + kv_width : q_width + 2 * kv_width],
        attn_sum[:, q_width + 2 * kv_width : used],
        gain_sums[1],
        attn_sum[:, used : used + expert_count],
        *expert_sums,
    )


def solution(mesh):
    return jax.shard_map(
        local,
        mesh=mesh,
        in_specs=(
            P(("fsdp", "tp"), None),
            P("fsdp", None),
            P("fsdp", None),
            P(),
            P("fsdp", "tp"),
            P("fsdp", "tp"),
            P("fsdp", "tp"),
            P("fsdp", "tp"),
            P(),
            P("fsdp", None),
            P("tp", "fsdp", None),
            P("tp", "fsdp", None),
            P("tp", "fsdp", None),
            P(("fsdp", "tp"), None),
        ),
        out_specs=(
            P(("fsdp", "tp"), None),
            P(("fsdp", "tp"), None),
            P(),
            P("fsdp", "tp"),
            P("fsdp", "tp"),
            P("fsdp", "tp"),
            P("fsdp", "tp"),
            P(),
            P("fsdp", None),
            P("tp", "fsdp", None),
            P("tp", "fsdp", None),
            P("tp", "fsdp", None),
        ),
        check_vma=False,
    )
```

```python
import functools

import jax
import jax.numpy as jnp
from jax import lax
from jax.experimental import pallas as pl
from jax.experimental.pallas import tpu as pltpu
from jax.sharding import PartitionSpec as P

HEAD_DIM = 64
SEQ = 512


emb_scale = 12.0
resid_scale = 0.22
attn_scale = 0.015625
norm_eps = 1e-06
rope_base = 10000.0
masked_value = -1e30


def contract_last(left_op, right_op):
    return lax.dot_general(
        left_op, right_op, (((1,), (1,)), ((), ())), preferred_element_type=jnp.float32
    )


def contract_first(left_op, right_op):
    return lax.dot_general(
        left_op, right_op, (((0,), (0,)), ((), ())), preferred_element_type=jnp.float32
    )


def line_signal(barrier, me, count):
    @pl.when(me > 0)
    def _():
        pl.semaphore_signal(barrier, inc=1, device_id={"tp": me - 1})

    @pl.when(me < count - 1)
    def _():
        pl.semaphore_signal(barrier, inc=1, device_id={"tp": me + 1})

    return jnp.where((me > 0) & (me < count - 1), 2, 1)


class Plane:
    def __init__(self, count):
        self.me = lax.axis_index("fsdp")
        self.core = lax.rem(self.me, 2)
        self.chip = lax.div(self.me, 2)
        self.chips = count // 2
        self.partner = self.me + 1 - 2 * self.core

    def chip_at(self, shift):
        return lax.rem(self.chip + shift + self.chips, self.chips)

    def peer(self, shift):
        return self.chip_at(shift) * 2 + self.core

    def signal(self, barrier):
        for shift in range(1, self.chips):
            pl.semaphore_signal(barrier, inc=1, device_id={"fsdp": self.peer(shift)})
        pl.semaphore_signal(barrier, inc=1, device_id={"fsdp": self.partner})
        return self.chips


def rows_of(ref, index, rows):
    return ref.at[pl.ds(pl.multiple_of(index * rows, rows), rows)]


class LineGather:
    def __init__(self, count, o_ref, send_sem, recv_sem):
        self.count, self.o_ref = count, o_ref
        self.send_sem, self.recv_sem = send_sem, recv_sem
        self.rows = o_ref.shape[0] // count
        me = self.me = lax.axis_index("tp")
        steps = range(count - 1)
        self.sends = [
            [(me >= step) & (me < count - 1) for step in steps],
            [(me + step < count) & (me > 0) for step in steps],
        ]
        self.gets = [
            [me - 1 - step >= 0 for step in steps],
            [me + 1 + step < count for step in steps],
        ]

    def hop(self, way, step, chunk):
        part = rows_of(self.o_ref, chunk, self.rows)
        return pltpu.make_async_remote_copy(
            src_ref=part,
            dst_ref=part,
            send_sem=self.send_sem.at[way, step],
            recv_sem=self.recv_sem.at[way, step],
            device_id={"tp": self.me + 1 if way == 0 else self.me - 1},
        )

    def start(self, step):
        @pl.when(self.sends[0][step])
        def _():
            self.hop(0, step, self.me - step).start()

        @pl.when(self.sends[1][step])
        def _():
            self.hop(1, step, self.me + step).start()

    def arrive(self, step):
        @pl.when(self.gets[0][step])
        def _():
            self.hop(0, step, self.me - 1 - step).wait_recv()

        @pl.when(self.gets[1][step])
        def _():
            self.hop(1, step, self.me + 1 + step).wait_recv()

    def finish(self):
        for step in range(self.count - 1):

            @pl.when(self.sends[0][step])
            def _():
                self.hop(0, step, self.me - step).wait_send()

            @pl.when(self.sends[1][step])
            def _():
                self.hop(1, step, self.me + step).wait_send()


def line_sems(count):
    return [
        pltpu.SemaphoreType.DMA((2, count - 1)),
        pltpu.SemaphoreType.DMA((2, count - 1)),
    ]


class LineScatter:
    def __init__(self, count, x_refs, o_ref, recv, send, send_sem, recv_sem):
        self.count, self.x_refs, self.o_ref = count, x_refs, o_ref
        self.recv, self.send = recv, send
        self.send_sem, self.recv_sem = send_sem, recv_sem
        self.rows = o_ref.shape[0]
        me = self.me = lax.axis_index("tp")
        self.behind = (me, count - 1 - me)
        self.has_next = (me < count - 1, me > 0)
        self.has_prev = (me > 0, me < count - 1)

    def block(self, dest):
        area = pl.ds(pl.multiple_of(dest * self.rows, self.rows), self.rows)
        total = self.x_refs[0][area, :].astype(jnp.float32)
        for x_ref in self.x_refs[1:]:
            total = total + x_ref[area, :].astype(jnp.float32)
        return total

    def hop(self, way, step):
        return pltpu.make_async_remote_copy(
            src_ref=self.send.at[way, step],
            dst_ref=self.recv.at[way, step],
            send_sem=self.send_sem.at[way, step],
            recv_sem=self.recv_sem.at[way, step],
            device_id={"tp": self.me + 1 if way == 0 else self.me - 1},
        )

    def start(self, step):
        count, me, send = self.count, self.me, self.send
        for way in range(2):
            dest = count - 1 - step + me if way == 0 else step - (count - 1 - me)
            active = self.has_next[way] & (step >= self.behind[way])

            @pl.when(active & (self.behind[way] == 0))
            def _():
                send[way, step] = self.block(dest).astype(send.dtype)
                self.hop(way, step).start()

            if step > 0:

                @pl.when(active & (self.behind[way] > 0))
                def _():
                    total = self.block(dest) + self.recv[way, step - 1].astype(jnp.float32)
                    send[way, step] = total.astype(send.dtype)
                    self.hop(way, step).start()

    def arrive(self, step):
        for way in range(2):

            @pl.when(self.has_prev[way] & (step >= self.behind[way] - 1))
            def _():
                self.hop(way, step).wait_recv()

    def collect(self):
        self.o_ref[...] = self.block(self.me)
        for way in range(2):

            @pl.when(self.has_prev[way])
            def _():
                self.o_ref[...] += self.recv[way, self.count - 2].astype(jnp.float32)

    def finish(self):
        for step in range(self.count - 1):
            for way in range(2):

                @pl.when(self.has_next[way] & (step >= self.behind[way]))
                def _():
                    self.hop(way, step).wait_send()


def line_buffers(count, rows, width):
    return [
        pltpu.VMEM((2, count - 1, rows, width), jnp.bfloat16),
        pltpu.VMEM((2, count - 1, rows, width), jnp.bfloat16),
    ] + line_sems(count)


def own_rows(rows):
    return pl.ds(pl.multiple_of(lax.axis_index("tp") * rows, rows), rows)


def inverse_norm(values):
    return lax.rsqrt(jnp.mean(values * values, axis=-1, keepdims=True) + norm_eps)


def rms_back(incoming, values, gain_row):
    inverse = inverse_norm(values)
    scaled = values * inverse
    gain_grad = jnp.sum(incoming * scaled, axis=0, keepdims=True)
    weighted = incoming * gain_row
    row_inner = jnp.mean(weighted * scaled, axis=-1, keepdims=True)
    return inverse * (weighted - scaled * row_inner), gain_grad


def enter_kernel(count):
    barrier = pltpu.get_barrier_semaphore()
    pl.semaphore_wait(barrier, line_signal(barrier, lax.axis_index("tp"), count))


def remote_params(ident, limit=60):
    return pltpu.CompilerParams(
        collective_id=ident, has_side_effects=True, vmem_limit_bytes=limit << 20
    )


IN_VMEM = pl.BlockSpec(memory_space=pltpu.VMEM)
IN_PLACE = pl.BlockSpec(memory_space=pl.ANY)
TRANSFER = pl.CostEstimate(flops=0, transcendentals=0, bytes_accessed=150_000_000)


def norm_gather_kernel(count, emb_ref, gain_ref, rows_ref, *sems):
    enter_kernel(count)
    line = LineGather(count, rows_ref, *sems)
    start_x = emb_ref[...].astype(jnp.float32) * emb_scale
    normed = start_x * inverse_norm(start_x) * gain_ref[...]
    rows_ref[own_rows(line.rows), :] = normed.astype(jnp.bfloat16)
    for step in range(count - 1):
        line.start(step)
        line.arrive(step)
    line.finish()


def norm_gather(emb, gain_row, count, ident):
    rows, width = emb.shape
    return pl.pallas_call(
        functools.partial(norm_gather_kernel, count),
        out_shape=jax.ShapeDtypeStruct((rows * count, width), jnp.bfloat16),
        in_specs=[IN_VMEM] * 2,
        out_specs=IN_VMEM,
        scratch_shapes=line_sems(count),
        compiler_params=remote_params(ident, 32),
        cost_estimate=TRANSFER,
    )(emb, gain_row)


def mid_kernel(
    count, part_ref, emb_ref, gain_ref, router_ref, mask_ref,
    mid_ref, rows_ref, gates_ref, own_gates,
    recv, send, sum_send, sum_recv, row_send, row_recv,
):
    enter_kernel(count)
    total = LineScatter(count, [part_ref], mid_ref, recv, send, sum_send, sum_recv)
    line = LineGather(count, rows_ref, row_send, row_recv)
    rows = line.rows
    for step in range(count - 1):
        total.start(step)
        total.arrive(step)
    total.collect()
    mid = emb_ref[...].astype(jnp.float32) * emb_scale + resid_scale * mid_ref[...]
    mid_ref[...] = mid
    own = own_rows(rows)
    rows_ref[own, :] = (mid * inverse_norm(mid) * gain_ref[...]).astype(jnp.bfloat16)

    def find_gates(chunk):
        area = pl.ds(pl.multiple_of(chunk * rows, rows), rows)
        logits = jnp.dot(rows_ref[area, :], router_ref[...], preferred_element_type=jnp.float32)
        inside = mask_ref[area, :] > 0.0
        top = jnp.max(jnp.where(inside, logits, masked_value), axis=-1, keepdims=True)
        raised = jnp.where(inside, jnp.exp(jnp.where(inside, logits - top, 0.0)), 0.0)
        gates = raised / jnp.sum(raised, axis=-1, keepdims=True)
        gates_ref[:, area] = gates.T
        return gates

    for step in range(count - 1):
        line.start(step)
        if step == 0:
            own_gates[...] = find_gates(line.me)
        line.arrive(step)

        @pl.when(line.gets[0][step])
        def _():
            find_gates(line.me - 1 - step)

        @pl.when(line.gets[1][step])
        def _():
            find_gates(line.me + 1 + step)

    line.finish()
    total.finish()


def find_mid(part, emb, gain_row, weights, used, mask, count, ident):
    rows, width = emb.shape
    group = rows * count
    return pl.pallas_call(
        functools.partial(mid_kernel, count),
        grid=(1,),
        out_shape=[
            jax.ShapeDtypeStruct((rows, width), jnp.float32),
            jax.ShapeDtypeStruct((group, width), jnp.bfloat16),
            jax.ShapeDtypeStruct((128, group), jnp.float32),
            jax.ShapeDtypeStruct((rows, 128), jnp.float32),
        ],
        in_specs=[
            IN_VMEM,
            IN_VMEM,
            IN_VMEM,
            pl.BlockSpec((width, 128), lambda step: (0, used // 128)),
            IN_VMEM,
        ],
        out_specs=[IN_VMEM] * 4,
        scratch_shapes=line_buffers(count, rows, width) + line_sems(count),
        compiler_params=remote_params(ident),
        cost_estimate=TRANSFER,
    )(part, emb, gain_row, weights, mask)


def moe_back_kernel(count, runs, *refs):
    dx_parts, y_parts, refs = refs[:runs], refs[runs : 2 * runs], refs[2 * runs :]
    (
        mid_ref, cotangent_ref, own_gates, gain_ref, router_ref,
        y_ref, mid_grad, gain_grad, sent_ref,
        sum_ref, recv, send, sum_send, sum_recv, row_send, row_recv,
    ) = refs
    enter_kernel(count)
    total = LineScatter(count, dx_parts, sum_ref, recv, send, sum_send, sum_recv)
    line = LineGather(count, sent_ref, row_send, row_recv)
    rows, width = mid_ref.shape
    for step in range(count - 1):
        total.start(step)
        if step == 0:
            for chunk in range(count):
                area = slice(chunk * rows, (chunk + 1) * rows)
                whole = y_parts[0][area, :].astype(jnp.float32)
                for y_part in y_parts[1:]:
                    whole = whole + y_part[area, :].astype(jnp.float32)
                y_ref[area, :] = whole.astype(y_ref.dtype)
        total.arrive(step)
    total.collect()
    gates = own_gates[...]
    gates_grad = sum_ref[:, width:]
    gates_inner = jnp.sum(gates * gates_grad, axis=-1, keepdims=True)
    logits_grad = (gates * (gates_grad - gates_inner)).astype(jnp.bfloat16)
    incoming = sum_ref[:, :width] + contract_last(logits_grad, router_ref[...])
    from_norm, gain_part = rms_back(incoming, mid_ref[...], gain_ref[...])
    grad = cotangent_ref[...].astype(jnp.float32) + from_norm
    mid_grad[...] = grad
    gain_grad[...] = gain_part
    own = own_rows(rows)
    sent_ref[own, :width] = (resid_scale * grad).astype(jnp.bfloat16)
    sent_ref[own, width:] = logits_grad
    for step in range(count - 1):
        line.start(step)
        line.arrive(step)
    line.finish()
    total.finish()


def find_mid_grad(dx_parts, y_parts, mid, cotangent, own_gates, gain_row, weights, used, count, ident):
    rows, width = mid.shape
    runs, group = len(dx_parts), rows * count
    wide = dx_parts[0].shape[1]
    return pl.pallas_call(
        functools.partial(moe_back_kernel, count, runs),
        grid=(1,),
        out_shape=[
            jax.ShapeDtypeStruct((group, width), jnp.bfloat16),
            jax.ShapeDtypeStruct((rows, width), jnp.float32),
            jax.ShapeDtypeStruct((1, width), jnp.float32),
            jax.ShapeDtypeStruct((group, wide), jnp.bfloat16),
        ],
        in_specs=[IN_VMEM] * (2 * runs + 4)
        + [pl.BlockSpec((width, 128), lambda step: (0, used // 128))],
        out_specs=[IN_VMEM] * 4,
        scratch_shapes=[pltpu.VMEM((rows, wide), jnp.float32)]
        + line_buffers(count, rows, wide)
        + line_sems(count),
        compiler_params=remote_params(ident, 62),
        cost_estimate=TRANSFER,
    )(*dx_parts, *y_parts, mid, cotangent, own_gates, gain_row, weights)


def finish_kernel(tp_count, fsdp_count, runs, *refs):
    x_ref, w_ref, emb_ref, gain_ref, mid_grad, gain_two = refs[:6]
    packed, refs = refs[6 : 6 + runs], refs[6 + runs :]
    (
        grad_ref, w_sum, gains_ref, *wide,
        line_recv, line_send, line_send_sem, line_recv_sem,
        pair_got, chip_sums, chip_got, pair_send, pair_recv, chip_send, chip_recv,
        tp_got, fsdp_got, small_send, small_recv, narrow, broad, in_sem, out_sem,
    ) = refs
    plane = Plane(fsdp_count)
    tp_me, fsdp_me = lax.axis_index("tp"), plane.me
    barrier = pltpu.get_barrier_semaphore()
    for shift in range(1, tp_count):
        pl.semaphore_signal(barrier, inc=1, device_id={"tp": lax.rem(tp_me + shift, tp_count)})
    for shift in range(1, fsdp_count):
        pl.semaphore_signal(
            barrier, inc=1, device_id={"fsdp": lax.rem(fsdp_me + shift, fsdp_count)}
        )
    pl.semaphore_wait(barrier, tp_count + fsdp_count - 2)
    line = LineScatter(
        tp_count, [x_ref], grad_ref, line_recv, line_send, line_send_sem, line_recv_sem
    )
    rows = w_sum.shape[0]

    def to_pair(shift):
        return pltpu.make_async_remote_copy(
            src_ref=rows_of(w_ref, plane.chip_at(shift) * 2 + 1 - plane.core, rows),
            dst_ref=pair_got.at[shift],
            send_sem=pair_send.at[shift],
            recv_sem=pair_recv.at[shift],
            device_id={"fsdp": plane.partner},
        )

    def to_chip(shift):
        return pltpu.make_async_remote_copy(
            src_ref=chip_sums.at[shift - 1],
            dst_ref=chip_got.at[shift - 1],
            send_sem=chip_send.at[shift - 1],
            recv_sem=chip_recv.at[shift - 1],
            device_id={"fsdp": plane.peer(shift)},
        )

    def both_cores(shift):
        own = pl.ds(pl.multiple_of(plane.peer(shift) * rows, rows), rows)
        return w_ref[own, :].astype(jnp.float32) + pair_got[shift].astype(jnp.float32)

    def exchange(axis, me, count, got, base):
        copies = []
        for shift in range(1, count):
            copies.append(
                pltpu.make_async_remote_copy(
                    src_ref=gains_ref,
                    dst_ref=got.at[me],
                    send_sem=small_send.at[base + shift],
                    recv_sem=small_recv.at[base + shift],
                    device_id={axis: lax.rem(me + shift, count)},
                )
            )
            copies[-1].start()
        got[me] = gains_ref[...]
        for copy in copies:
            copy.wait()
        total = got[0]
        for index in range(1, count):
            total = total + got[index]
        return total

    def widen_run(run):
        base = sum(packed[index].shape[0] for index in range(run))

        def one(index, carry):
            fetch = pltpu.make_async_copy(packed[run].at[index], narrow, in_sem)
            fetch.start()
            fetch.wait()
            puts = []
            for slot in range(3):
                broad[slot] = narrow[slot].astype(jnp.float32)
                puts.append(
                    pltpu.make_async_copy(
                        broad.at[slot], wide[slot].at[base + index], out_sem.at[slot]
                    )
                )
                puts[-1].start()
            for put in puts:
                put.wait()
            return carry

        lax.fori_loop(0, packed[run].shape[0], one, 0)

    line.start(0)
    order = list(range(1, plane.chips)) + [0]
    for shift in order:
        to_pair(shift).start()
    for shift in order:
        to_pair(shift).wait_recv()
        if shift > 0:
            chip_sums[shift - 1] = both_cores(shift).astype(chip_sums.dtype)
            to_chip(shift).start()
    if runs > 0:
        widen_run(0)
    line.arrive(0)
    for step in range(1, tp_count - 1):
        line.start(step)
        if step < runs:
            widen_run(step)
        line.arrive(step)
    line.collect()
    from_norm, gain_one = rms_back(
        grad_ref[...], emb_ref[...].astype(jnp.float32) * emb_scale, gain_ref[...]
    )
    gains_ref[...] = jnp.zeros_like(gains_ref)
    gains_ref[0:1, :] = gain_one
    gains_ref[1:2, :] = gain_two[...]
    grad_ref[...] = emb_scale * (mid_grad[...] + from_norm)
    total = both_cores(0)
    for shift in range(1, plane.chips):
        to_chip(shift).wait_recv()
        total = total + chip_got[shift - 1].astype(jnp.float32)
    w_sum[...] = total
    gains_ref[...] = exchange("tp", tp_me, tp_count, tp_got, 0)
    gains_ref[...] = exchange("fsdp", fsdp_me, fsdp_count, fsdp_got, tp_count)
    line.finish()
    for shift in order:
        to_pair(shift).wait_send()
        if shift > 0:
            to_chip(shift).wait_send()


def finish(dx_rows, weight_grads, emb, gain_row, mid_grad, gain_two, packed, experts, ident):
    tp_count, fsdp_count = lax.axis_size("tp"), lax.axis_size("fsdp")
    rows, width = emb.shape
    w_rows, w_width = weight_grads.shape[0] // fsdp_count, weight_grads.shape[1]
    chips, runs = fsdp_count // 2, len(packed)
    shares, hidden = packed[0].shape[2:] if runs else (8, 128)
    wide = [jax.ShapeDtypeStruct((experts, shares, hidden), jnp.float32)] * (3 if runs else 0)
    return pl.pallas_call(
        functools.partial(finish_kernel, tp_count, fsdp_count, runs),
        out_shape=[
            jax.ShapeDtypeStruct((rows, width), jnp.float32),
            jax.ShapeDtypeStruct((w_rows, w_width), jnp.float32),
            jax.ShapeDtypeStruct((8, width), jnp.float32),
            *wide,
        ],
        in_specs=[IN_VMEM] * 6 + [IN_PLACE] * runs,
        out_specs=[IN_VMEM] * 3 + [IN_PLACE] * len(wide),
        scratch_shapes=line_buffers(tp_count, rows, width)
        + [
            pltpu.VMEM((chips, w_rows, w_width), jnp.bfloat16),
            pltpu.VMEM((chips - 1, w_rows, w_width), jnp.bfloat16),
            pltpu.VMEM((chips - 1, w_rows, w_width), jnp.bfloat16),
            pltpu.SemaphoreType.DMA((chips,)),
            pltpu.SemaphoreType.DMA((chips,)),
            pltpu.SemaphoreType.DMA((chips - 1,)),
            pltpu.SemaphoreType.DMA((chips - 1,)),
            pltpu.VMEM((tp_count, 8, width), jnp.float32),
            pltpu.VMEM((fsdp_count, 8, width), jnp.float32),
            pltpu.SemaphoreType.DMA((tp_count + fsdp_count,)),
            pltpu.SemaphoreType.DMA((tp_count + fsdp_count,)),
            pltpu.VMEM((3, shares, hidden), jnp.bfloat16),
            pltpu.VMEM((3, shares, hidden), jnp.float32),
            pltpu.SemaphoreType.DMA,
            pltpu.SemaphoreType.DMA((3,)),
        ],
        compiler_params=remote_params(ident),
        cost_estimate=TRANSFER,
    )(dx_rows, weight_grads, emb, gain_row, mid_grad, gain_two, *packed)


def pack_kernel(low, *refs):
    sources, target, held, in_sem, out_sem = refs[:-4], *refs[-4:]
    span = target.shape[0]
    gets = [
        pltpu.make_async_copy(source.at[pl.ds(low, span)], held.at[slot], in_sem.at[slot])
        for slot, source in enumerate(sources)
    ]
    puts = [
        pltpu.make_async_copy(held.at[slot], target.at[:, slot], out_sem.at[slot])
        for slot in range(len(sources))
    ]
    for get in gets:
        get.start()
    for get, put in zip(gets, puts):
        get.wait()
        put.start()
    for put in puts:
        put.wait()


def pack(stacks, low, high):
    _, rows, width = stacks[0].shape
    count, span = len(stacks), high - low
    return pl.pallas_call(
        functools.partial(pack_kernel, low),
        in_specs=[IN_PLACE] * count,
        out_specs=IN_PLACE,
        out_shape=jax.ShapeDtypeStruct((span, count, rows, width), jnp.bfloat16),
        scratch_shapes=[
            pltpu.VMEM((count, span, rows, width), jnp.bfloat16),
            pltpu.SemaphoreType.DMA((count,)),
            pltpu.SemaphoreType.DMA((count,)),
        ],
    )(*stacks)


def join_kernel(*refs):
    low = 0
    for source in refs[:-1]:
        refs[-1][:, low : low + source.shape[1]] = source[...]
        low += source.shape[1]
    if low < refs[-1].shape[1]:
        refs[-1][:, low:] = jnp.zeros((refs[-1].shape[0], refs[-1].shape[1] - low), jnp.bfloat16)


def join(parts, width):
    return pl.pallas_call(
        join_kernel,
        in_specs=[IN_VMEM] * len(parts),
        out_specs=IN_VMEM,
        out_shape=jax.ShapeDtypeStruct((parts[0].shape[0], width), jnp.bfloat16),
    )(*parts)


SLOTS = 256


def experts_kernel(
    first_expert,
    capacity,
    meta,
    place_row,
    place_cols,
    gate_rows,
    x_ref,
    weights,
    *refs,
):
    g_blocks, (y_ref, dx_ref, grads, g_ref, g_sem) = refs[:-5], refs[-5:]
    step = pl.program_id(0)
    expert = step + first_expert
    group, width = x_ref.shape
    tail = dx_ref.shape[1] - width

    @pl.when(step == 0)
    def _():
        count, rows = len(g_blocks), g_blocks[0].shape[0]
        copies = []
        for shift, block in enumerate(g_blocks):
            home = lax.rem(meta[meta.shape[0] - 1] + count - shift, count)
            copies.append(pltpu.make_async_copy(block, rows_of(g_ref, home, rows), g_sem.at[shift]))
            copies[-1].start()
        y_ref[...] = jnp.zeros_like(y_ref)
        dx_ref[...] = jnp.zeros_like(dx_ref)
        for copy in copies:
            copy.wait()

    lanes = lax.broadcasted_iota(jnp.int32, place_cols.shape, 1)
    place_col = jnp.sum(jnp.where(lanes == expert, place_cols[...], 0), axis=1, keepdims=True)
    column = expert + meta[meta.shape[0] - 2]
    gate_row = gate_rows[pl.ds(column, 1), :].astype(jnp.bfloat16).astype(jnp.float32)
    mark = jnp.where(lax.broadcasted_iota(jnp.int32, (1, tail), 1) == column, 1.0, 0.0)

    def run(base, span):
        slots = lax.broadcasted_iota(jnp.int32, (span, group), 0) + base
        hit = slots == place_row[0]
        pick = jnp.where(hit, 1.0, 0.0).astype(jnp.bfloat16)
        scale = jnp.sum(jnp.where(hit, gate_row, 0.0), axis=1, keepdims=True)
        x_taken = jnp.dot(pick, x_ref[...], preferred_element_type=jnp.float32).astype(jnp.bfloat16)
        g_taken = jnp.dot(pick, g_ref[...], preferred_element_type=jnp.float32).astype(jnp.bfloat16)
        gate_pre = jnp.dot(x_taken, weights[0, 0], preferred_element_type=jnp.float32)
        up_pre = jnp.dot(x_taken, weights[0, 1], preferred_element_type=jnp.float32)
        raw = jnp.dot(g_taken, weights[0, 2], preferred_element_type=jnp.float32)
        sig = jax.nn.sigmoid(gate_pre)
        silu = gate_pre * sig
        act = (silu * up_pre).astype(jnp.bfloat16).astype(jnp.float32)
        slot_grad = jnp.sum(act * raw, axis=1, keepdims=True)
        act_grad = raw * scale
        act_scaled = (act * scale).astype(jnp.bfloat16)
        gate_grad = (act_grad * up_pre * sig * (1.0 + gate_pre * (1.0 - sig))).astype(jnp.bfloat16)
        up_grad = (act_grad * silu).astype(jnp.bfloat16)
        extra = (slot_grad * mark).astype(jnp.bfloat16)
        rows_out = contract_last(act_scaled, weights[0, 2]).astype(jnp.bfloat16)
        rows_in = (
            contract_last(gate_grad, weights[0, 0]) + contract_last(up_grad, weights[0, 1])
        ).astype(jnp.bfloat16)
        for slot, left_op, right_op in (
            (0, x_taken, gate_grad),
            (1, x_taken, up_grad),
            (2, g_taken, act_scaled),
        ):
            grad = contract_first(left_op, right_op)
            if base > 0:
                grad = grad + grads[0, slot].astype(jnp.float32)
            grads[0, slot] = grad.astype(jnp.bfloat16)
        block = min(256, group)
        for start in range(0, group, block):
            back = jnp.where(
                lax.broadcasted_iota(jnp.int32, (block, span), 1) + base
                == place_col[start : start + block],
                1.0,
                0.0,
            ).astype(jnp.bfloat16)
            for target, low_col, addend in (
                (y_ref, 0, rows_out),
                (dx_ref, 0, rows_in),
                (dx_ref, width, extra),
            ):
                area = (slice(start, start + block), slice(low_col, low_col + addend.shape[1]))
                target[area] = (
                    target[area].astype(jnp.float32)
                    + jnp.dot(back, addend, preferred_element_type=jnp.float32)
                ).astype(target.dtype)

    run(0, min(SLOTS, capacity))
    for base in range(SLOTS, capacity, SLOTS):
        span = min(SLOTS, -(-(capacity - base) // 16) * 16)

        @pl.when(meta[expert] > base)
        def _():
            run(base, span)


def experts_step(meta, place_rows, place_cols, gate_rows, x_rows, g_blocks, weights, first, count, skip, capacity):
    group, width = x_rows.shape
    hidden = weights.shape[-1]
    tail = 128

    def whole(shape):
        return pl.BlockSpec(
            shape, lambda step, meta: (0,) * len(shape), pipeline_mode=pl.Buffered(1)
        )

    def row(shape):
        return pl.BlockSpec(shape, lambda step, meta: (step + first, 0, 0))

    def big(offset):
        return pl.BlockSpec((1, 3, width, hidden), lambda step, meta: (step + offset, 0, 0, 0))

    return pl.pallas_call(
        functools.partial(experts_kernel, first, capacity),
        grid_spec=pltpu.PrefetchScalarGridSpec(
            num_scalar_prefetch=1,
            grid=(count,),
            in_specs=[
                row((1, 1, group)),
                whole(place_cols.shape),
                whole(gate_rows.shape),
                whole(x_rows.shape),
                big(skip),
            ]
            + [IN_PLACE] * len(g_blocks),
            out_specs=[
                whole((group, width)),
                whole((group, width + tail)),
                big(0),
            ],
            scratch_shapes=[
                pltpu.VMEM((group, width), jnp.bfloat16),
                pltpu.SemaphoreType.DMA((len(g_blocks),)),
            ],
        ),
        out_shape=[
            jax.ShapeDtypeStruct((group, width), jnp.bfloat16),
            jax.ShapeDtypeStruct((group, width + tail), jnp.bfloat16),
            jax.ShapeDtypeStruct((count, 3, width, hidden), jnp.bfloat16),
        ],
        compiler_params=pltpu.CompilerParams(
            dimension_semantics=("arbitrary",), vmem_limit_bytes=63 << 20
        ),
        cost_estimate=pl.CostEstimate(
            flops=count * 17 * 2 * 408 * width * hidden,
            transcendentals=count * 408 * hidden,
            bytes_accessed=count * 12 * width * hidden,
        ),
    )(meta, place_rows, place_cols, gate_rows, x_rows, weights, *g_blocks)


def rotate_head(values, cosine, sine, sign):
    half = values.shape[-1] // 2
    other = jnp.concatenate([values[:, half:], values[:, :half]], axis=1)
    return values * cosine + other * (sine * sign)


def segment_bias(seg_row, seg_col):
    shape = (seg_col.shape[0], seg_row.shape[1])
    keys = lax.broadcasted_iota(jnp.int32, shape, 0)
    queries = lax.broadcasted_iota(jnp.int32, shape, 1)
    return jnp.where((keys <= queries) & (seg_col == seg_row), 0.0, masked_value)


def attend_kernel(
    x_ref,
    w_ref,
    seg_row,
    seg_col,
    cos_ref,
    sin_ref,
    q_ref,
    k_ref,
    v_ref,
    mixed_ref,
    logsum_ref,
    branch_ref,
    bias,
    v_turned,
    mixed_heads,
):
    heads, kv_heads = q_ref.shape[0], k_ref.shape[0]
    per_kv = heads // kv_heads
    block = SEQ // 2
    edge = (heads + 2 * kv_heads) * HEAD_DIM
    proj = jnp.dot(x_ref[...], w_ref[:, :edge], preferred_element_type=jnp.float32)
    cosine, sine = cos_ref[...], sin_ref[...]
    for head in range(heads + 2 * kv_heads):
        part = proj[:, head * HEAD_DIM : (head + 1) * HEAD_DIM]
        if head < heads:
            q_ref[head] = rotate_head(part, cosine, sine, 1.0).astype(jnp.bfloat16)
        elif head < heads + kv_heads:
            k_ref[head - heads] = rotate_head(part, cosine, sine, 1.0).astype(jnp.bfloat16)
        else:
            v_ref[head - heads - kv_heads] = part.astype(jnp.bfloat16)
            v_turned[head - heads - kv_heads] = part.T.astype(jnp.bfloat16)
    bias[...] = segment_bias(seg_row[0], seg_col[0])

    def one_head(head, carry):
        kv = head // per_kv
        for part in range(2):
            span, low = block * (part + 1), block * part
            scores = contract_last(k_ref[kv, :span], q_ref[head, low : low + block]) * attn_scale
            scores = scores + bias[:span, low : low + block]
            top = jnp.max(scores, axis=0, keepdims=True)
            raised = jnp.exp(scores - top)
            total = jnp.sum(raised, axis=0, keepdims=True)
            probs = (raised * (1.0 / total)).astype(jnp.bfloat16)
            turned = jnp.dot(v_turned[kv, :, :span], probs, preferred_element_type=jnp.float32)
            mixed_heads[head, low : low + block, :] = turned.T.astype(jnp.bfloat16)
            logsum_ref[0, pl.ds(head, 1), low : low + block] = top + jnp.log(total)
        return carry

    lax.fori_loop(0, heads, one_head, 0)
    for head in range(heads):
        mixed_ref[:, head * HEAD_DIM : (head + 1) * HEAD_DIM] = mixed_heads[head]
    branch_ref[...] = contract_last(
        mixed_ref[...], w_ref[:, edge : edge + heads * HEAD_DIM]
    ).astype(jnp.bfloat16)


def attend_back_kernel(
    x_ref,
    w_ref,
    seg_row,
    seg_col,
    cos_ref,
    sin_ref,
    q_ref,
    k_ref,
    v_ref,
    mixed_ref,
    logsum_ref,
    moe_rows,
    branch_grad,
    dx_ref,
    dw_ref,
    bias,
    k_turned,
    mixed_grads,
    q_grads,
    kv_grads,
    qkv_grad,
    dw_acc,
):
    heads, kv_heads = q_ref.shape[0], k_ref.shape[0]
    per_kv = heads // kv_heads
    block = SEQ // 2
    edge = (heads + 2 * kv_heads) * HEAD_DIM
    step = pl.program_id(0)
    out_edge = edge + heads * HEAD_DIM
    width = x_ref.shape[1]
    grad = jnp.dot(
        branch_grad[:, :width], w_ref[:, edge:out_edge], preferred_element_type=jnp.float32
    ).astype(jnp.bfloat16)
    for head in range(heads):
        mixed_grads[head] = grad[:, head * HEAD_DIM : (head + 1) * HEAD_DIM]
    for kv in range(kv_heads):
        k_turned[kv] = k_ref[kv].astype(jnp.float32).T.astype(jnp.bfloat16)
    bias[...] = segment_bias(seg_row[0], seg_col[0])
    kv_grads[...] = jnp.zeros_like(kv_grads)

    def one_head(head, carry):
        kv = head // per_kv
        for part in range(2):
            span, low = block * (part + 1), block * part
            high = low + block
            scores = contract_last(k_ref[kv, :span], q_ref[head, low:high]) * attn_scale
            scores = scores + bias[:span, low:high]
            probs = jnp.exp(scores - logsum_ref[0, pl.ds(head, 1), low:high])
            probs_grad = contract_last(v_ref[kv, :span], mixed_grads[head, low:high])
            inner = jnp.sum(probs * probs_grad, axis=0, keepdims=True)
            score_grad = (probs * (probs_grad - inner)).astype(jnp.bfloat16)
            turned = jnp.dot(k_turned[kv, :, :span], score_grad, preferred_element_type=jnp.float32)
            q_grads[head, low:high, :] = turned.T * attn_scale
            kv_grads[0, kv, :span, :] += jnp.dot(
                score_grad, q_ref[head, low:high], preferred_element_type=jnp.float32
            )
            kv_grads[1, kv, :span, :] += jnp.dot(
                probs.astype(jnp.bfloat16), mixed_grads[head, low:high],
                preferred_element_type=jnp.float32,
            )
        return carry

    lax.fori_loop(0, heads, one_head, 0)
    cosine, sine = cos_ref[...], sin_ref[...]
    for head in range(heads + 2 * kv_heads):
        if head < heads:
            part = rotate_head(q_grads[head], cosine, sine, -1.0)
        elif head < heads + kv_heads:
            part = rotate_head(kv_grads[0, head - heads] * attn_scale, cosine, sine, -1.0)
        else:
            part = kv_grads[1, head - heads - kv_heads]
        qkv_grad[:, head * HEAD_DIM : (head + 1) * HEAD_DIM] = part.astype(jnp.bfloat16)
    dx_ref[...] = contract_last(qkv_grad[...], w_ref[:, :edge]).astype(jnp.bfloat16)
    for low, high, left_op, right_op in (
        (0, edge, x_ref[...], qkv_grad[...]),
        (edge, out_edge, branch_grad[:, :width], mixed_ref[...]),
        (out_edge, dw_acc.shape[1], moe_rows[...], branch_grad[:, width:]),
    ):
        part = contract_first(left_op, right_op)

        @pl.when(step == 0)
        def _():
            dw_acc[:, low:high] = part

        @pl.when(step > 0)
        def _():
            dw_acc[:, low:high] += part

    @pl.when(step == pl.num_programs(0) - 1)
    def _():
        dw_ref[...] = dw_acc[...].astype(jnp.bfloat16)


def fixed(shape):
    return pl.BlockSpec(shape, lambda seq: (0,) * len(shape), pipeline_mode=pl.Buffered(1))


def by_row(width):
    return pl.BlockSpec((SEQ, width), lambda seq: (seq, 0))


def by_head(heads):
    return pl.BlockSpec((heads, SEQ, HEAD_DIM), lambda seq: (0, seq, 0))


def attend_tables():
    half = HEAD_DIM // 2
    positions = jnp.arange(SEQ).astype(jnp.float32)
    frequency = rope_base ** (-jnp.arange(half).astype(jnp.float32) * 2.0 / HEAD_DIM)
    angles = positions[:, None] * frequency[None, :]
    cosine, sine = jnp.cos(angles), jnp.sin(angles)
    return (
        jnp.concatenate([cosine, cosine], axis=1),
        jnp.concatenate([-sine, sine], axis=1),
    )


def attend(rows, weights, segments, tables, heads, kv_heads):
    group, width = rows.shape
    seqs = group // SEQ
    return pl.pallas_call(
        attend_kernel,
        grid=(seqs,),
        in_specs=[
            by_row(width),
            fixed(weights.shape),
            pl.BlockSpec((1, 1, SEQ), lambda seq: (seq, 0, 0)),
            pl.BlockSpec((1, SEQ, 1), lambda seq: (seq, 0, 0)),
            fixed(tables[0].shape),
            fixed(tables[1].shape),
        ],
        out_specs=[
            by_head(heads),
            by_head(kv_heads),
            by_head(kv_heads),
            by_row(heads * HEAD_DIM),
            pl.BlockSpec((1, heads, SEQ), lambda seq: (seq, 0, 0)),
            by_row(width),
        ],
        out_shape=[
            jax.ShapeDtypeStruct((heads, group, HEAD_DIM), jnp.bfloat16),
            jax.ShapeDtypeStruct((kv_heads, group, HEAD_DIM), jnp.bfloat16),
            jax.ShapeDtypeStruct((kv_heads, group, HEAD_DIM), jnp.bfloat16),
            jax.ShapeDtypeStruct((group, heads * HEAD_DIM), jnp.bfloat16),
            jax.ShapeDtypeStruct((seqs, heads, SEQ), jnp.float32),
            jax.ShapeDtypeStruct((group, width), jnp.bfloat16),
        ],
        scratch_shapes=[
            pltpu.VMEM((SEQ, SEQ), jnp.float32),
            pltpu.VMEM((kv_heads, HEAD_DIM, SEQ), jnp.bfloat16),
            pltpu.VMEM((heads, SEQ, HEAD_DIM), jnp.bfloat16),
        ],
        compiler_params=pltpu.CompilerParams(
            dimension_semantics=("arbitrary",), vmem_limit_bytes=56 << 20
        ),
        cost_estimate=pl.CostEstimate(
            flops=10_000_000_000, transcendentals=3_000_000, bytes_accessed=60_000_000
        ),
    )(rows, weights, segments[:, None, :], segments[:, :, None], *tables)


def attend_back(rows, weights, segments, tables, kept, moe_rows, branch_grad):
    queries, keys, values, mixed, logsum = kept
    group, width = rows.shape
    heads, kv_heads = queries.shape[0], keys.shape[0]
    used = weights.shape[1]
    edge = (heads + 2 * kv_heads) * HEAD_DIM
    return pl.pallas_call(
        attend_back_kernel,
        grid=(group // SEQ,),
        in_specs=[
            by_row(width),
            fixed(weights.shape),
            pl.BlockSpec((1, 1, SEQ), lambda seq: (seq, 0, 0)),
            pl.BlockSpec((1, SEQ, 1), lambda seq: (seq, 0, 0)),
            fixed(tables[0].shape),
            fixed(tables[1].shape),
            by_head(heads),
            by_head(kv_heads),
            by_head(kv_heads),
            by_row(heads * HEAD_DIM),
            pl.BlockSpec((1, heads, SEQ), lambda seq: (seq, 0, 0)),
            by_row(width),
            by_row(branch_grad.shape[1]),
        ],
        out_specs=[by_row(width), fixed((width, used))],
        out_shape=[
            jax.ShapeDtypeStruct((group, width), jnp.bfloat16),
            jax.ShapeDtypeStruct((width, used), jnp.bfloat16),
        ],
        scratch_shapes=[
            pltpu.VMEM((SEQ, SEQ), jnp.float32),
            pltpu.VMEM((kv_heads, HEAD_DIM, SEQ), jnp.bfloat16),
            pltpu.VMEM((heads, SEQ, HEAD_DIM), jnp.bfloat16),
            pltpu.VMEM((heads, SEQ, HEAD_DIM), jnp.float32),
            pltpu.VMEM((2, kv_heads, SEQ, HEAD_DIM), jnp.float32),
            pltpu.VMEM((SEQ, edge), jnp.bfloat16),
            pltpu.VMEM((width, used), jnp.float32),
        ],
        compiler_params=pltpu.CompilerParams(
            dimension_semantics=("arbitrary",), vmem_limit_bytes=60 << 20
        ),
        cost_estimate=pl.CostEstimate(
            flops=20_000_000_000, transcendentals=3_000_000, bytes_accessed=100_000_000
        ),
    )(rows, weights, segments[:, None, :], segments[:, :, None], *tables,
      queries, keys, values, mixed, logsum, moe_rows, branch_grad)


def widen_kernel(packed, *refs):
    for slot, target in enumerate(refs[-3:]):
        target[0] = packed[0, slot].astype(jnp.float32)


def widen(packed, count, first, held):
    span, _, rows, width = packed.shape
    shape = jax.ShapeDtypeStruct((count, rows, width), jnp.float32)
    return pl.pallas_call(
        widen_kernel,
        grid=(span,),
        in_specs=[pl.BlockSpec((1, 3, rows, width), lambda step: (step, 0, 0, 0))]
        + [pl.BlockSpec(memory_space=pl.ANY)] * len(held),
        out_specs=[pl.BlockSpec((1, rows, width), lambda step: (step + first, 0, 0))] * 3,
        out_shape=[shape] * 3,
        input_output_aliases={1 + index: index for index in range(len(held))},
    )(packed, *held)


def shifted_blocks(block, count):
    return [block] + [
        lax.ppermute(block, "tp", [(i, (i + shift) % count) for i in range(count)])
        for shift in range(1, count)
    ]


def shifted_scatter(partial_rows, count, me):
    rows = partial_rows.shape[0] // count
    total = lax.dynamic_slice_in_dim(partial_rows, me * rows, rows, 0).astype(jnp.float32)
    for shift in range(1, count):
        block = lax.dynamic_slice_in_dim(
            partial_rows, lax.rem(me + shift, count) * rows, rows, 0
        ).astype(jnp.bfloat16)
        got = lax.ppermute(block, "tp", [(i, (i + shift) % count) for i in range(count)])
        total = total + got.astype(jnp.float32)
    return total


RUNS = (0, 2, 5, 10)


def local(
    emb,
    segment_ids,
    routes,
    norm1_gain,
    w_query,
    w_key,
    w_value,
    w_out,
    norm2_gain,
    w_router,
    w_gate,
    w_up,
    w_down,
    cotangent,
):
    local_rows, _ = emb.shape
    tp_count, tp_index = lax.axis_size("tp"), lax.axis_index("tp")
    experts_here = w_gate.shape[0]
    expert_count = w_router.shape[1]
    q_width, kv_width = w_query.shape[1], w_key.shape[1]
    used = 2 * (q_width + kv_width)
    group_size = local_rows * tp_count
    gathers = 2 if group_size <= 1024 else 1

    moe_grad = (resid_scale * cotangent.astype(jnp.float32)).astype(jnp.bfloat16)
    moe_grad_blocks = shifted_blocks(moe_grad, tp_count)
    attn_w = lax.all_gather(
        join([w_query, w_key, w_value, w_out, w_router], used + 128), "fsdp", axis=0, tiled=True
    )
    edges = [experts_here * part // gathers for part in range(gathers + 1)]
    pieces = [
        lax.all_gather(pack([w_gate, w_up, w_down], low, high), "fsdp", axis=2, tiled=True)
        for low, high in zip(edges[:-1], edges[1:])
    ]
    gain_one = norm1_gain.astype(jnp.float32)[None, :]
    gain_two = norm2_gain.astype(jnp.float32)[None, :]
    group_rows = norm_gather(emb, gain_one, tp_count, 0)

    capacity = group_size * routes.shape[1] // expert_count * 2
    lanes = jnp.arange(128, dtype=jnp.int32)
    member_all = jnp.any(routes[:, :, None] == lanes[None, None, :], axis=1)
    member = lax.dynamic_slice_in_dim(member_all, tp_index * experts_here, experts_here, 1)
    ids = jnp.arange(group_size)
    earlier = (ids[:, None] > ids[None, :]).astype(jnp.bfloat16)
    ranks = jnp.dot(earlier, member.astype(jnp.bfloat16), preferred_element_type=jnp.float32)
    places = jnp.where(member, ranks.astype(jnp.int32), -1)
    meta = jnp.concatenate(
        [jnp.sum(member.astype(jnp.int32), axis=0), jnp.stack([tp_index * experts_here, tp_index])]
    )
    place_rows = places.T[:, None, :]

    tables = attend_tables()
    heads_here, kv_here = q_width // HEAD_DIM, kv_width // HEAD_DIM
    *kept, branch_part = attend(group_rows, attn_w, segment_ids, tables, heads_here, kv_here)
    mid_x, moe_rows, gate_rows, own_gates = find_mid(
        branch_part, emb, gain_two, attn_w, used, member_all.astype(jnp.float32), tp_count, 1
    )

    outs = []
    runs = edges
    if gathers > 1:
        runs = sorted({edge * experts_here // RUNS[-1] for edge in RUNS} | set(edges))
    for first, last in zip(runs[:-1], runs[1:]):
        home = max(index for index in range(gathers) if edges[index] <= first)
        outs.append(
            experts_step(
                meta,
                place_rows,
                places,
                gate_rows,
                moe_rows,
                moe_grad_blocks,
                pieces[home],
                first,
                last - first,
                first - edges[home],
                capacity,
            )
        )
    grad_sums = [
        lax.psum_scatter(part[2], "fsdp", scatter_dimension=2, tiled=True) for part in outs
    ]
    y_part, mid_grad, gain_two_grad, sent = find_mid_grad(
        [part[1] for part in outs],
        [part[0] for part in outs],
        mid_x,
        cotangent,
        own_gates,
        gain_two,
        attn_w,
        used,
        tp_count,
        2,
    )
    moe_sum = shifted_scatter(y_part, tp_count, tp_index)
    out = (mid_x + resid_scale * moe_sum).astype(jnp.bfloat16)
    dx_one, attn_grads = attend_back(group_rows, attn_w, segment_ids, tables, kept, moe_rows, sent)
    grad_emb, attn_sum, gain_sums, *expert_sums = finish(
        dx_one,
        attn_grads,
        emb,
        gain_one,
        mid_grad,
        gain_two_grad,
        grad_sums[:-1],
        experts_here,
        3,
    )
    expert_sums = widen(grad_sums[-1], experts_here, runs[-2], expert_sums)
    return (
        out,
        grad_emb,
        gain_sums[0],
        attn_sum[:, :q_width],
        attn_sum[:, q_width : q_width + kv_width],
        attn_sum[:, q_width + kv_width : q_width + 2 * kv_width],
        attn_sum[:, q_width + 2 * kv_width : used],
        gain_sums[1],
        attn_sum[:, used : used + expert_count],
        *expert_sums,
    )


def solution(mesh):
    return jax.shard_map(
        local,
        mesh=mesh,
        in_specs=(
            P(("fsdp", "tp"), None),
            P("fsdp", None),
            P("fsdp", None),
            P(),
            P("fsdp", "tp"),
            P("fsdp", "tp"),
            P("fsdp", "tp"),
            P("fsdp", "tp"),
            P(),
            P("fsdp", None),
            P("tp", "fsdp", None),
            P("tp", "fsdp", None),
            P("tp", "fsdp", None),
            P(("fsdp", "tp"), None),
        ),
        out_specs=(
            P(("fsdp", "tp"), None),
            P(("fsdp", "tp"), None),
            P(),
            P("fsdp", "tp"),
            P("fsdp", "tp"),
            P("fsdp", "tp"),
            P("fsdp", "tp"),
            P(),
            P("fsdp", None),
            P("tp", "fsdp", None),
            P("tp", "fsdp", None),
            P("tp", "fsdp", None),
        ),
        check_vma=False,
    )
```

```python
import functools

import jax
import jax.numpy as jnp
from jax import lax
from jax.experimental import pallas as pl
from jax.experimental.pallas import tpu as pltpu
from jax.sharding import PartitionSpec as P

HEAD_DIM = 64
SEQ = 512


emb_scale = 12.0
resid_scale = 0.22
attn_scale = 0.015625
norm_eps = 1e-06
rope_base = 10000.0
masked_value = -1e30


def contract_last(left_op, right_op):
    return lax.dot_general(
        left_op, right_op, (((1,), (1,)), ((), ())), preferred_element_type=jnp.float32
    )


def contract_first(left_op, right_op):
    return lax.dot_general(
        left_op, right_op, (((0,), (0,)), ((), ())), preferred_element_type=jnp.float32
    )


def line_signal(barrier, me, count):
    @pl.when(me > 0)
    def _():
        pl.semaphore_signal(barrier, inc=1, device_id={"tp": me - 1})

    @pl.when(me < count - 1)
    def _():
        pl.semaphore_signal(barrier, inc=1, device_id={"tp": me + 1})

    return jnp.where((me > 0) & (me < count - 1), 2, 1)


class Plane:
    def __init__(self, count):
        self.me = lax.axis_index("fsdp")
        self.core = lax.rem(self.me, 2)
        self.chip = lax.div(self.me, 2)
        self.chips = count // 2
        self.partner = self.me + 1 - 2 * self.core

    def chip_at(self, shift):
        return lax.rem(self.chip + shift + self.chips, self.chips)

    def peer(self, shift):
        return self.chip_at(shift) * 2 + self.core

    def signal(self, barrier):
        for shift in range(1, self.chips):
            pl.semaphore_signal(barrier, inc=1, device_id={"fsdp": self.peer(shift)})
        pl.semaphore_signal(barrier, inc=1, device_id={"fsdp": self.partner})
        return self.chips


def rows_of(ref, index, rows):
    return ref.at[pl.ds(pl.multiple_of(index * rows, rows), rows)]


class LineGather:
    def __init__(self, count, o_ref, send_sem, recv_sem):
        self.count, self.o_ref = count, o_ref
        self.send_sem, self.recv_sem = send_sem, recv_sem
        self.rows = o_ref.shape[0] // count
        me = self.me = lax.axis_index("tp")
        steps = range(count - 1)
        self.sends = [
            [(me >= step) & (me < count - 1) for step in steps],
            [(me + step < count) & (me > 0) for step in steps],
        ]
        self.gets = [
            [me - 1 - step >= 0 for step in steps],
            [me + 1 + step < count for step in steps],
        ]

    def hop(self, way, step, chunk):
        part = rows_of(self.o_ref, chunk, self.rows)
        return pltpu.make_async_remote_copy(
            src_ref=part,
            dst_ref=part,
            send_sem=self.send_sem.at[way, step],
            recv_sem=self.recv_sem.at[way, step],
            device_id={"tp": self.me + 1 if way == 0 else self.me - 1},
        )

    def start(self, step):
        @pl.when(self.sends[0][step])
        def _():
            self.hop(0, step, self.me - step).start()

        @pl.when(self.sends[1][step])
        def _():
            self.hop(1, step, self.me + step).start()

    def arrive(self, step):
        @pl.when(self.gets[0][step])
        def _():
            self.hop(0, step, self.me - 1 - step).wait_recv()

        @pl.when(self.gets[1][step])
        def _():
            self.hop(1, step, self.me + 1 + step).wait_recv()

    def finish(self):
        for step in range(self.count - 1):

            @pl.when(self.sends[0][step])
            def _():
                self.hop(0, step, self.me - step).wait_send()

            @pl.when(self.sends[1][step])
            def _():
                self.hop(1, step, self.me + step).wait_send()


def line_sems(count):
    return [
        pltpu.SemaphoreType.DMA((2, count - 1)),
        pltpu.SemaphoreType.DMA((2, count - 1)),
    ]


class LineScatter:
    def __init__(self, count, x_refs, o_ref, recv, send, send_sem, recv_sem):
        self.count, self.x_refs, self.o_ref = count, x_refs, o_ref
        self.recv, self.send = recv, send
        self.send_sem, self.recv_sem = send_sem, recv_sem
        self.rows = o_ref.shape[0]
        me = self.me = lax.axis_index("tp")
        self.behind = (me, count - 1 - me)
        self.has_next = (me < count - 1, me > 0)
        self.has_prev = (me > 0, me < count - 1)

    def block(self, dest):
        area = pl.ds(pl.multiple_of(dest * self.rows, self.rows), self.rows)
        total = self.x_refs[0][area, :].astype(jnp.float32)
        for x_ref in self.x_refs[1:]:
            total = total + x_ref[area, :].astype(jnp.float32)
        return total

    def hop(self, way, step):
        return pltpu.make_async_remote_copy(
            src_ref=self.send.at[way, step],
            dst_ref=self.recv.at[way, step],
            send_sem=self.send_sem.at[way, step],
            recv_sem=self.recv_sem.at[way, step],
            device_id={"tp": self.me + 1 if way == 0 else self.me - 1},
        )

    def start(self, step):
        count, me, send = self.count, self.me, self.send
        for way in range(2):
            dest = count - 1 - step + me if way == 0 else step - (count - 1 - me)
            active = self.has_next[way] & (step >= self.behind[way])

            @pl.when(active & (self.behind[way] == 0))
            def _():
                send[way, step] = self.block(dest).astype(send.dtype)
                self.hop(way, step).start()

            if step > 0:

                @pl.when(active & (self.behind[way] > 0))
                def _():
                    total = self.block(dest) + self.recv[way, step - 1].astype(jnp.float32)
                    send[way, step] = total.astype(send.dtype)
                    self.hop(way, step).start()

    def arrive(self, step):
        for way in range(2):

            @pl.when(self.has_prev[way] & (step >= self.behind[way] - 1))
            def _():
                self.hop(way, step).wait_recv()

    def collect(self):
        self.o_ref[...] = self.block(self.me)
        for way in range(2):

            @pl.when(self.has_prev[way])
            def _():
                self.o_ref[...] += self.recv[way, self.count - 2].astype(jnp.float32)

    def finish(self):
        for step in range(self.count - 1):
            for way in range(2):

                @pl.when(self.has_next[way] & (step >= self.behind[way]))
                def _():
                    self.hop(way, step).wait_send()


def line_buffers(count, rows, width):
    return [
        pltpu.VMEM((2, count - 1, rows, width), jnp.bfloat16),
        pltpu.VMEM((2, count - 1, rows, width), jnp.bfloat16),
    ] + line_sems(count)


def own_rows(rows):
    return pl.ds(pl.multiple_of(lax.axis_index("tp") * rows, rows), rows)


def inverse_norm(values):
    return lax.rsqrt(jnp.mean(values * values, axis=-1, keepdims=True) + norm_eps)


def rms_back(incoming, values, gain_row):
    inverse = inverse_norm(values)
    scaled = values * inverse
    gain_grad = jnp.sum(incoming * scaled, axis=0, keepdims=True)
    weighted = incoming * gain_row
    row_inner = jnp.mean(weighted * scaled, axis=-1, keepdims=True)
    return inverse * (weighted - scaled * row_inner), gain_grad


def enter_kernel(count):
    barrier = pltpu.get_barrier_semaphore()
    pl.semaphore_wait(barrier, line_signal(barrier, lax.axis_index("tp"), count))


def remote_params(ident, limit=60):
    return pltpu.CompilerParams(
        collective_id=ident, has_side_effects=True, vmem_limit_bytes=limit << 20
    )


IN_VMEM = pl.BlockSpec(memory_space=pltpu.VMEM)
IN_PLACE = pl.BlockSpec(memory_space=pl.ANY)
TRANSFER = pl.CostEstimate(flops=0, transcendentals=0, bytes_accessed=150_000_000)


def norm_gather_kernel(
    count, emb_ref, gain_ref, routes_ref, rows_ref, mask_ref, cols_ref, turned_ref, counts_ref, *sems
):
    enter_kernel(count)
    line = LineGather(count, rows_ref, *sems)
    start_x = emb_ref[...].astype(jnp.float32) * emb_scale
    normed = start_x * inverse_norm(start_x) * gain_ref[...]
    rows_ref[own_rows(line.rows), :] = normed.astype(jnp.bfloat16)
    for step in range(count - 1):
        line.start(step)
        if step == 0:
            place_routes(line.rows, routes_ref, mask_ref, cols_ref, turned_ref, counts_ref)
        line.arrive(step)
    line.finish()


def place_routes(rows, routes_ref, mask_ref, cols_ref, turned_ref, counts_ref):
    group, lanes = mask_ref.shape
    columns = lax.broadcasted_iota(jnp.int32, (rows, lanes), 1)
    for low in range(0, group, rows):
        area = slice(low, low + rows)
        mask = jnp.zeros((rows, lanes), jnp.float32)
        for choice in range(routes_ref.shape[1]):
            mask = jnp.where(routes_ref[area, choice : choice + 1] == columns, 1.0, mask)
        mask_ref[area, :] = mask
    counts_ref[...] = jnp.sum(mask_ref[...], axis=0, keepdims=True).astype(jnp.int32)
    member = mask_ref[...].astype(jnp.bfloat16)
    for low in range(0, group, rows):
        area = slice(low, low + rows)
        here = lax.broadcasted_iota(jnp.int32, (rows, group), 0) + low
        earlier = here > lax.broadcasted_iota(jnp.int32, (rows, group), 1)
        ranks = jnp.dot(
            jnp.where(earlier, 1.0, 0.0).astype(jnp.bfloat16),
            member,
            preferred_element_type=jnp.float32,
        )
        places = jnp.where(mask_ref[area, :] > 0.0, ranks, -1.0)
        cols_ref[area, :] = places.astype(jnp.int32)
        turned_ref[:, area] = places.T.astype(jnp.int32)


def norm_gather(emb, gain_row, routes, count, ident):
    rows, width = emb.shape
    group = rows * count
    return pl.pallas_call(
        functools.partial(norm_gather_kernel, count),
        out_shape=[
            jax.ShapeDtypeStruct((group, width), jnp.bfloat16),
            jax.ShapeDtypeStruct((group, 128), jnp.float32),
            jax.ShapeDtypeStruct((group, 128), jnp.int32),
            jax.ShapeDtypeStruct((128, group), jnp.int32),
            jax.ShapeDtypeStruct((1, 128), jnp.int32),
        ],
        in_specs=[IN_VMEM] * 3,
        out_specs=[IN_VMEM] * 5,
        scratch_shapes=line_sems(count),
        compiler_params=remote_params(ident, 48),
        cost_estimate=TRANSFER,
    )(emb, gain_row, routes)


def mid_kernel(
    count, part_ref, emb_ref, gain_ref, router_ref, mask_ref,
    mid_ref, rows_ref, gates_ref, own_gates,
    recv, send, sum_send, sum_recv, row_send, row_recv,
):
    enter_kernel(count)
    total = LineScatter(count, [part_ref], mid_ref, recv, send, sum_send, sum_recv)
    line = LineGather(count, rows_ref, row_send, row_recv)
    rows = line.rows
    for step in range(count - 1):
        total.start(step)
        total.arrive(step)
    total.collect()
    mid = emb_ref[...].astype(jnp.float32) * emb_scale + resid_scale * mid_ref[...]
    mid_ref[...] = mid
    own = own_rows(rows)
    rows_ref[own, :] = (mid * inverse_norm(mid) * gain_ref[...]).astype(jnp.bfloat16)

    def find_gates(chunk):
        area = pl.ds(pl.multiple_of(chunk * rows, rows), rows)
        logits = jnp.dot(rows_ref[area, :], router_ref[...], preferred_element_type=jnp.float32)
        inside = mask_ref[area, :] > 0.0
        top = jnp.max(jnp.where(inside, logits, masked_value), axis=-1, keepdims=True)
        raised = jnp.where(inside, jnp.exp(jnp.where(inside, logits - top, 0.0)), 0.0)
        gates = raised / jnp.sum(raised, axis=-1, keepdims=True)
        gates_ref[:, area] = gates.T
        return gates

    for step in range(count - 1):
        line.start(step)
        if step == 0:
            own_gates[...] = find_gates(line.me)
        line.arrive(step)

        @pl.when(line.gets[0][step])
        def _():
            find_gates(line.me - 1 - step)

        @pl.when(line.gets[1][step])
        def _():
            find_gates(line.me + 1 + step)

    line.finish()
    total.finish()


def find_mid(part, emb, gain_row, weights, used, mask, count, ident):
    rows, width = emb.shape
    group = rows * count
    return pl.pallas_call(
        functools.partial(mid_kernel, count),
        grid=(1,),
        out_shape=[
            jax.ShapeDtypeStruct((rows, width), jnp.float32),
            jax.ShapeDtypeStruct((group, width), jnp.bfloat16),
            jax.ShapeDtypeStruct((128, group), jnp.float32),
            jax.ShapeDtypeStruct((rows, 128), jnp.float32),
        ],
        in_specs=[
            IN_VMEM,
            IN_VMEM,
            IN_VMEM,
            pl.BlockSpec((width, 128), lambda step: (0, used // 128)),
            IN_VMEM,
        ],
        out_specs=[IN_VMEM] * 4,
        scratch_shapes=line_buffers(count, rows, width) + line_sems(count),
        compiler_params=remote_params(ident),
        cost_estimate=TRANSFER,
    )(part, emb, gain_row, weights, mask)


def moe_back_kernel(count, runs, *refs):
    dx_parts, y_parts, refs = refs[:runs], refs[runs : 2 * runs], refs[2 * runs :]
    (
        mid_ref, cotangent_ref, own_gates, gain_ref, router_ref,
        y_ref, mid_grad, gain_grad, sent_ref,
        sum_ref, recv, send, sum_send, sum_recv, row_send, row_recv,
    ) = refs
    enter_kernel(count)
    total = LineScatter(count, dx_parts, sum_ref, recv, send, sum_send, sum_recv)
    line = LineGather(count, sent_ref, row_send, row_recv)
    rows, width = mid_ref.shape
    for step in range(count - 1):
        total.start(step)
        if step == 0:
            for chunk in range(count):
                area = slice(chunk * rows, (chunk + 1) * rows)
                whole = y_parts[0][area, :].astype(jnp.float32)
                for y_part in y_parts[1:]:
                    whole = whole + y_part[area, :].astype(jnp.float32)
                y_ref[area, :] = whole.astype(y_ref.dtype)
        total.arrive(step)
    total.collect()
    gates = own_gates[...]
    gates_grad = sum_ref[:, width:]
    gates_inner = jnp.sum(gates * gates_grad, axis=-1, keepdims=True)
    logits_grad = (gates * (gates_grad - gates_inner)).astype(jnp.bfloat16)
    incoming = sum_ref[:, :width] + contract_last(logits_grad, router_ref[...])
    from_norm, gain_part = rms_back(incoming, mid_ref[...], gain_ref[...])
    grad = cotangent_ref[...].astype(jnp.float32) + from_norm
    mid_grad[...] = grad
    gain_grad[...] = gain_part
    own = own_rows(rows)
    sent_ref[own, :width] = (resid_scale * grad).astype(jnp.bfloat16)
    sent_ref[own, width:] = logits_grad
    for step in range(count - 1):
        line.start(step)
        line.arrive(step)
    line.finish()
    total.finish()


def find_mid_grad(dx_parts, y_parts, mid, cotangent, own_gates, gain_row, weights, used, count, ident):
    rows, width = mid.shape
    runs, group = len(dx_parts), rows * count
    wide = dx_parts[0].shape[1]
    return pl.pallas_call(
        functools.partial(moe_back_kernel, count, runs),
        grid=(1,),
        out_shape=[
            jax.ShapeDtypeStruct((group, width), jnp.bfloat16),
            jax.ShapeDtypeStruct((rows, width), jnp.float32),
            jax.ShapeDtypeStruct((1, width), jnp.float32),
            jax.ShapeDtypeStruct((group, wide), jnp.bfloat16),
        ],
        in_specs=[IN_VMEM] * (2 * runs + 4)
        + [pl.BlockSpec((width, 128), lambda step: (0, used // 128))],
        out_specs=[IN_VMEM] * 4,
        scratch_shapes=[pltpu.VMEM((rows, wide), jnp.float32)]
        + line_buffers(count, rows, wide)
        + line_sems(count),
        compiler_params=remote_params(ident, 62),
        cost_estimate=TRANSFER,
    )(*dx_parts, *y_parts, mid, cotangent, own_gates, gain_row, weights)


def finish_kernel(tp_count, fsdp_count, *refs):
    x_ref, w_ref, emb_ref, gain_ref, mid_grad, gain_two, *refs = refs
    (
        grad_ref, w_sum, gains_ref,
        line_recv, line_send, line_send_sem, line_recv_sem,
        pair_got, chip_sums, chip_got, pair_send, pair_recv, chip_send, chip_recv,
        tp_got, fsdp_got, small_send, small_recv,
    ) = refs
    plane = Plane(fsdp_count)
    tp_me, fsdp_me = lax.axis_index("tp"), plane.me
    barrier = pltpu.get_barrier_semaphore()
    for shift in range(1, tp_count):
        pl.semaphore_signal(barrier, inc=1, device_id={"tp": lax.rem(tp_me + shift, tp_count)})
    for shift in range(1, fsdp_count):
        pl.semaphore_signal(
            barrier, inc=1, device_id={"fsdp": lax.rem(fsdp_me + shift, fsdp_count)}
        )
    pl.semaphore_wait(barrier, tp_count + fsdp_count - 2)
    line = LineScatter(
        tp_count, [x_ref], grad_ref, line_recv, line_send, line_send_sem, line_recv_sem
    )
    rows = w_sum.shape[0]

    def to_pair(shift):
        return pltpu.make_async_remote_copy(
            src_ref=rows_of(w_ref, plane.chip_at(shift) * 2 + 1 - plane.core, rows),
            dst_ref=pair_got.at[shift],
            send_sem=pair_send.at[shift],
            recv_sem=pair_recv.at[shift],
            device_id={"fsdp": plane.partner},
        )

    def to_chip(shift):
        return pltpu.make_async_remote_copy(
            src_ref=chip_sums.at[shift - 1],
            dst_ref=chip_got.at[shift - 1],
            send_sem=chip_send.at[shift - 1],
            recv_sem=chip_recv.at[shift - 1],
            device_id={"fsdp": plane.peer(shift)},
        )

    def both_cores(shift):
        own = pl.ds(pl.multiple_of(plane.peer(shift) * rows, rows), rows)
        return w_ref[own, :].astype(jnp.float32) + pair_got[shift].astype(jnp.float32)

    def exchange(axis, me, count, got, base):
        copies = []
        for shift in range(1, count):
            copies.append(
                pltpu.make_async_remote_copy(
                    src_ref=gains_ref,
                    dst_ref=got.at[me],
                    send_sem=small_send.at[base + shift],
                    recv_sem=small_recv.at[base + shift],
                    device_id={axis: lax.rem(me + shift, count)},
                )
            )
            copies[-1].start()
        got[me] = gains_ref[...]
        for copy in copies:
            copy.wait()
        total = got[0]
        for index in range(1, count):
            total = total + got[index]
        return total

    line.start(0)
    order = list(range(1, plane.chips)) + [0]
    for shift in order:
        to_pair(shift).start()
    for shift in order:
        to_pair(shift).wait_recv()
        if shift > 0:
            chip_sums[shift - 1] = both_cores(shift).astype(chip_sums.dtype)
            to_chip(shift).start()
    line.arrive(0)
    for step in range(1, tp_count - 1):
        line.start(step)
        line.arrive(step)
    line.collect()
    from_norm, gain_one = rms_back(
        grad_ref[...], emb_ref[...].astype(jnp.float32) * emb_scale, gain_ref[...]
    )
    gains_ref[...] = jnp.zeros_like(gains_ref)
    gains_ref[0:1, :] = gain_one
    gains_ref[1:2, :] = gain_two[...]
    grad_ref[...] = emb_scale * (mid_grad[...] + from_norm)
    total = both_cores(0)
    for shift in range(1, plane.chips):
        to_chip(shift).wait_recv()
        total = total + chip_got[shift - 1].astype(jnp.float32)
    w_sum[...] = total
    gains_ref[...] = exchange("tp", tp_me, tp_count, tp_got, 0)
    gains_ref[...] = exchange("fsdp", fsdp_me, fsdp_count, fsdp_got, tp_count)
    line.finish()
    for shift in order:
        to_pair(shift).wait_send()
        if shift > 0:
            to_chip(shift).wait_send()


def finish(dx_rows, weight_grads, emb, gain_row, mid_grad, gain_two, ident):
    tp_count, fsdp_count = lax.axis_size("tp"), lax.axis_size("fsdp")
    rows, width = emb.shape
    w_rows, w_width = weight_grads.shape[0] // fsdp_count, weight_grads.shape[1]
    chips = fsdp_count // 2
    return pl.pallas_call(
        functools.partial(finish_kernel, tp_count, fsdp_count),
        out_shape=[
            jax.ShapeDtypeStruct((rows, width), jnp.float32),
            jax.ShapeDtypeStruct((w_rows, w_width), jnp.float32),
            jax.ShapeDtypeStruct((8, width), jnp.float32),
        ],
        in_specs=[IN_VMEM] * 6,
        out_specs=[IN_VMEM] * 3,
        scratch_shapes=line_buffers(tp_count, rows, width)
        + [
            pltpu.VMEM((chips, w_rows, w_width), jnp.bfloat16),
            pltpu.VMEM((chips - 1, w_rows, w_width), jnp.bfloat16),
            pltpu.VMEM((chips - 1, w_rows, w_width), jnp.bfloat16),
            pltpu.SemaphoreType.DMA((chips,)),
            pltpu.SemaphoreType.DMA((chips,)),
            pltpu.SemaphoreType.DMA((chips - 1,)),
            pltpu.SemaphoreType.DMA((chips - 1,)),
            pltpu.VMEM((tp_count, 8, width), jnp.float32),
            pltpu.VMEM((fsdp_count, 8, width), jnp.float32),
            pltpu.SemaphoreType.DMA((tp_count + fsdp_count,)),
            pltpu.SemaphoreType.DMA((tp_count + fsdp_count,)),
        ],
        compiler_params=remote_params(ident),
        cost_estimate=TRANSFER,
    )(dx_rows, weight_grads, emb, gain_row, mid_grad, gain_two)


def pack_kernel(low, *refs):
    sources, target, held, in_sem, out_sem = refs[:-4], *refs[-4:]
    span = target.shape[0]
    gets = [
        pltpu.make_async_copy(source.at[pl.ds(low, span)], held.at[slot], in_sem.at[slot])
        for slot, source in enumerate(sources)
    ]
    puts = [
        pltpu.make_async_copy(held.at[slot], target.at[:, slot], out_sem.at[slot])
        for slot in range(len(sources))
    ]
    for get in gets:
        get.start()
    for get, put in zip(gets, puts):
        get.wait()
        put.start()
    for put in puts:
        put.wait()


def pack(stacks, low, high):
    _, rows, width = stacks[0].shape
    count, span = len(stacks), high - low
    return pl.pallas_call(
        functools.partial(pack_kernel, low),
        in_specs=[IN_PLACE] * count,
        out_specs=IN_PLACE,
        out_shape=jax.ShapeDtypeStruct((span, count, rows, width), jnp.bfloat16),
        scratch_shapes=[
            pltpu.VMEM((count, span, rows, width), jnp.bfloat16),
            pltpu.SemaphoreType.DMA((count,)),
            pltpu.SemaphoreType.DMA((count,)),
        ],
    )(*stacks)


def join_kernel(*refs):
    *sources, last, target = refs
    low = 0
    for source in sources:
        target[:, low : low + source.shape[1]] = source[...]
        low += source.shape[1]
    router = last[...].astype(jnp.float32).T.astype(jnp.bfloat16)
    target[:, low:] = jnp.zeros((target.shape[0], target.shape[1] - low), jnp.bfloat16)
    target[:, low : low + router.shape[1]] = router


def join(parts, last_turned, width):
    return pl.pallas_call(
        join_kernel,
        in_specs=[IN_VMEM] * (len(parts) + 1),
        out_specs=IN_VMEM,
        out_shape=jax.ShapeDtypeStruct((parts[0].shape[0], width), jnp.bfloat16),
    )(*parts, last_turned)


SLOTS = 256


def experts_kernel(
    first_expert,
    capacity,
    meta,
    place_rows,
    place_cols,
    gate_rows,
    x_ref,
    weights,
    *refs,
):
    g_blocks, (y_ref, dx_ref, grads, g_ref, g_sem) = refs[:-5], refs[-5:]
    step = pl.program_id(0)
    expert = step + first_expert
    group, width = x_ref.shape
    tail = dx_ref.shape[1] - width

    @pl.when(step == 0)
    def _():
        count, rows = len(g_blocks), g_blocks[0].shape[0]
        copies = []
        for shift, block in enumerate(g_blocks):
            home = lax.rem(meta[meta.shape[0] - 1] + count - shift, count)
            copies.append(pltpu.make_async_copy(block, rows_of(g_ref, home, rows), g_sem.at[shift]))
            copies[-1].start()
        y_ref[...] = jnp.zeros_like(y_ref)
        dx_ref[...] = jnp.zeros_like(dx_ref)
        for copy in copies:
            copy.wait()

    column = expert + meta[meta.shape[0] - 2]
    lanes = lax.broadcasted_iota(jnp.int32, place_cols.shape, 1)
    place_col = jnp.sum(jnp.where(lanes == column, place_cols[...], 0), axis=1, keepdims=True)
    place_row = place_rows[pl.ds(column, 1), :]
    gate_row = gate_rows[pl.ds(column, 1), :].astype(jnp.bfloat16).astype(jnp.float32)
    mark = jnp.where(lax.broadcasted_iota(jnp.int32, (1, tail), 1) == column, 1.0, 0.0)

    def run(base, span):
        slots = lax.broadcasted_iota(jnp.int32, (span, group), 0) + base
        hit = slots == place_row
        pick = jnp.where(hit, 1.0, 0.0).astype(jnp.bfloat16)
        scale = jnp.sum(jnp.where(hit, gate_row, 0.0), axis=1, keepdims=True)
        x_taken = jnp.dot(pick, x_ref[...], preferred_element_type=jnp.float32).astype(jnp.bfloat16)
        g_taken = jnp.dot(pick, g_ref[...], preferred_element_type=jnp.float32).astype(jnp.bfloat16)
        gate_pre = jnp.dot(x_taken, weights[0, 0], preferred_element_type=jnp.float32)
        up_pre = jnp.dot(x_taken, weights[0, 1], preferred_element_type=jnp.float32)
        raw = jnp.dot(g_taken, weights[0, 2], preferred_element_type=jnp.float32)
        sig = jax.nn.sigmoid(gate_pre)
        silu = gate_pre * sig
        act = (silu * up_pre).astype(jnp.bfloat16).astype(jnp.float32)
        slot_grad = jnp.sum(act * raw, axis=1, keepdims=True)
        act_grad = raw * scale
        act_scaled = (act * scale).astype(jnp.bfloat16)
        gate_grad = (act_grad * up_pre * sig * (1.0 + gate_pre * (1.0 - sig))).astype(jnp.bfloat16)
        up_grad = (act_grad * silu).astype(jnp.bfloat16)
        extra = (slot_grad * mark).astype(jnp.bfloat16)
        rows_out = contract_last(act_scaled, weights[0, 2]).astype(jnp.bfloat16)
        rows_in = (
            contract_last(gate_grad, weights[0, 0]) + contract_last(up_grad, weights[0, 1])
        ).astype(jnp.bfloat16)
        for slot, left_op, right_op in (
            (0, x_taken, gate_grad),
            (1, x_taken, up_grad),
            (2, g_taken, act_scaled),
        ):
            grad = contract_first(left_op, right_op)
            if base > 0:
                grad = grad + grads[0, slot].astype(jnp.float32)
            grads[0, slot] = grad.astype(jnp.bfloat16)
        block = min(256, group)
        for start in range(0, group, block):
            back = jnp.where(
                lax.broadcasted_iota(jnp.int32, (block, span), 1) + base
                == place_col[start : start + block],
                1.0,
                0.0,
            ).astype(jnp.bfloat16)
            for target, low_col, addend in (
                (y_ref, 0, rows_out),
                (dx_ref, 0, rows_in),
                (dx_ref, width, extra),
            ):
                area = (slice(start, start + block), slice(low_col, low_col + addend.shape[1]))
                target[area] = (
                    target[area].astype(jnp.float32)
                    + jnp.dot(back, addend, preferred_element_type=jnp.float32)
                ).astype(target.dtype)

    run(0, min(SLOTS, capacity))
    for base in range(SLOTS, capacity, SLOTS):
        span = min(SLOTS, -(-(capacity - base) // 16) * 16)

        @pl.when(meta[column] > base)
        def _():
            run(base, span)


def experts_step(meta, place_rows, place_cols, gate_rows, x_rows, g_blocks, weights, first, count, skip, capacity):
    group, width = x_rows.shape
    hidden = weights.shape[-1]
    tail = 128

    def whole(shape):
        return pl.BlockSpec(
            shape, lambda step, meta: (0,) * len(shape), pipeline_mode=pl.Buffered(1)
        )

    def big(offset):
        return pl.BlockSpec((1, 3, width, hidden), lambda step, meta: (step + offset, 0, 0, 0))

    return pl.pallas_call(
        functools.partial(experts_kernel, first, capacity),
        grid_spec=pltpu.PrefetchScalarGridSpec(
            num_scalar_prefetch=1,
            grid=(count,),
            in_specs=[
                whole(place_rows.shape),
                whole(place_cols.shape),
                whole(gate_rows.shape),
                whole(x_rows.shape),
                big(skip),
            ]
            + [IN_PLACE] * len(g_blocks),
            out_specs=[
                whole((group, width)),
                whole((group, width + tail)),
                big(0),
            ],
            scratch_shapes=[
                pltpu.VMEM((group, width), jnp.bfloat16),
                pltpu.SemaphoreType.DMA((len(g_blocks),)),
            ],
        ),
        out_shape=[
            jax.ShapeDtypeStruct((group, width), jnp.bfloat16),
            jax.ShapeDtypeStruct((group, width + tail), jnp.bfloat16),
            jax.ShapeDtypeStruct((count, 3, width, hidden), jnp.bfloat16),
        ],
        compiler_params=pltpu.CompilerParams(
            dimension_semantics=("arbitrary",), vmem_limit_bytes=63 << 20
        ),
        cost_estimate=pl.CostEstimate(
            flops=count * 17 * 2 * 408 * width * hidden,
            transcendentals=count * 408 * hidden,
            bytes_accessed=count * 12 * width * hidden,
        ),
    )(meta, place_rows, place_cols, gate_rows, x_rows, weights, *g_blocks)


def rotate_head(values, cosine, sine, sign):
    half = values.shape[-1] // 2
    other = jnp.concatenate([values[:, half:], values[:, :half]], axis=1)
    return values * cosine + other * (sine * sign)


def segment_bias(seg_row):
    length = seg_row.shape[1]
    shape = (length, length)
    seg_row = seg_row.astype(jnp.float32)
    seg_col = jnp.broadcast_to(seg_row, (128, length)).T[:, :1]
    keys = lax.broadcasted_iota(jnp.int32, shape, 0)
    queries = lax.broadcasted_iota(jnp.int32, shape, 1)
    return jnp.where((keys <= queries) & (seg_col == seg_row), 0.0, masked_value)


def attend_kernel(
    x_ref,
    w_ref,
    seg_row,
    cos_ref,
    sin_ref,
    q_ref,
    k_ref,
    v_ref,
    mixed_ref,
    logsum_ref,
    branch_ref,
    bias,
    v_turned,
    mixed_heads,
):
    heads, kv_heads = q_ref.shape[0], k_ref.shape[0]
    per_kv = heads // kv_heads
    block = SEQ // 2
    edge = (heads + 2 * kv_heads) * HEAD_DIM
    proj = jnp.dot(x_ref[...], w_ref[:, :edge], preferred_element_type=jnp.float32)
    cosine, sine = cos_ref[...], sin_ref[...]
    for head in range(heads + 2 * kv_heads):
        part = proj[:, head * HEAD_DIM : (head + 1) * HEAD_DIM]
        if head < heads:
            q_ref[head] = rotate_head(part, cosine, sine, 1.0).astype(jnp.bfloat16)
        elif head < heads + kv_heads:
            k_ref[head - heads] = rotate_head(part, cosine, sine, 1.0).astype(jnp.bfloat16)
        else:
            v_ref[head - heads - kv_heads] = part.astype(jnp.bfloat16)
            v_turned[head - heads - kv_heads] = part.T.astype(jnp.bfloat16)
    bias[...] = segment_bias(seg_row[0])

    def one_head(head, carry):
        kv = head // per_kv
        for part in range(2):
            span, low = block * (part + 1), block * part
            scores = contract_last(k_ref[kv, :span], q_ref[head, low : low + block]) * attn_scale
            scores = scores + bias[:span, low : low + block]
            top = jnp.max(scores, axis=0, keepdims=True)
            raised = jnp.exp(scores - top)
            total = jnp.sum(raised, axis=0, keepdims=True)
            probs = (raised * (1.0 / total)).astype(jnp.bfloat16)
            turned = jnp.dot(v_turned[kv, :, :span], probs, preferred_element_type=jnp.float32)
            mixed_heads[head, low : low + block, :] = turned.T.astype(jnp.bfloat16)
            logsum_ref[0, pl.ds(head, 1), low : low + block] = top + jnp.log(total)
        return carry

    lax.fori_loop(0, heads, one_head, 0)
    for head in range(heads):
        mixed_ref[:, head * HEAD_DIM : (head + 1) * HEAD_DIM] = mixed_heads[head]
    branch_ref[...] = contract_last(
        mixed_ref[...], w_ref[:, edge : edge + heads * HEAD_DIM]
    ).astype(jnp.bfloat16)


def attend_back_kernel(
    x_ref,
    w_ref,
    seg_row,
    cos_ref,
    sin_ref,
    q_ref,
    k_ref,
    v_ref,
    mixed_ref,
    logsum_ref,
    moe_rows,
    branch_grad,
    dx_ref,
    dw_ref,
    bias,
    k_turned,
    mixed_grads,
    q_grads,
    kv_grads,
    qkv_grad,
    dw_acc,
):
    heads, kv_heads = q_ref.shape[0], k_ref.shape[0]
    per_kv = heads // kv_heads
    block = SEQ // 2
    edge = (heads + 2 * kv_heads) * HEAD_DIM
    step = pl.program_id(0)
    out_edge = edge + heads * HEAD_DIM
    width = x_ref.shape[1]
    grad = jnp.dot(
        branch_grad[:, :width], w_ref[:, edge:out_edge], preferred_element_type=jnp.float32
    ).astype(jnp.bfloat16)
    for head in range(heads):
        mixed_grads[head] = grad[:, head * HEAD_DIM : (head + 1) * HEAD_DIM]
    for kv in range(kv_heads):
        k_turned[kv] = k_ref[kv].astype(jnp.float32).T.astype(jnp.bfloat16)
    bias[...] = segment_bias(seg_row[0])
    kv_grads[...] = jnp.zeros_like(kv_grads)

    def one_head(head, carry):
        kv = head // per_kv
        for part in range(2):
            span, low = block * (part + 1), block * part
            high = low + block
            scores = contract_last(k_ref[kv, :span], q_ref[head, low:high]) * attn_scale
            scores = scores + bias[:span, low:high]
            probs = jnp.exp(scores - logsum_ref[0, pl.ds(head, 1), low:high])
            probs_grad = contract_last(v_ref[kv, :span], mixed_grads[head, low:high])
            inner = jnp.sum(probs * probs_grad, axis=0, keepdims=True)
            score_grad = (probs * (probs_grad - inner)).astype(jnp.bfloat16)
            turned = jnp.dot(k_turned[kv, :, :span], score_grad, preferred_element_type=jnp.float32)
            q_grads[head, low:high, :] = turned.T * attn_scale
            kv_grads[0, kv, :span, :] += jnp.dot(
                score_grad, q_ref[head, low:high], preferred_element_type=jnp.float32
            )
            kv_grads[1, kv, :span, :] += jnp.dot(
                probs.astype(jnp.bfloat16), mixed_grads[head, low:high],
                preferred_element_type=jnp.float32,
            )
        return carry

    lax.fori_loop(0, heads, one_head, 0)
    cosine, sine = cos_ref[...], sin_ref[...]
    for head in range(heads + 2 * kv_heads):
        if head < heads:
            part = rotate_head(q_grads[head], cosine, sine, -1.0)
        elif head < heads + kv_heads:
            part = rotate_head(kv_grads[0, head - heads] * attn_scale, cosine, sine, -1.0)
        else:
            part = kv_grads[1, head - heads - kv_heads]
        qkv_grad[:, head * HEAD_DIM : (head + 1) * HEAD_DIM] = part.astype(jnp.bfloat16)
    dx_ref[...] = contract_last(qkv_grad[...], w_ref[:, :edge]).astype(jnp.bfloat16)
    for low, high, left_op, right_op in (
        (0, edge, x_ref[...], qkv_grad[...]),
        (edge, out_edge, branch_grad[:, :width], mixed_ref[...]),
        (out_edge, dw_acc.shape[1], moe_rows[...], branch_grad[:, width:]),
    ):
        part = contract_first(left_op, right_op)

        @pl.when(step == 0)
        def _():
            dw_acc[:, low:high] = part

        @pl.when(step > 0)
        def _():
            dw_acc[:, low:high] += part

    @pl.when(step == pl.num_programs(0) - 1)
    def _():
        dw_ref[...] = dw_acc[...].astype(jnp.bfloat16)


def fixed(shape):
    return pl.BlockSpec(shape, lambda seq: (0,) * len(shape), pipeline_mode=pl.Buffered(1))


def by_row(width):
    return pl.BlockSpec((SEQ, width), lambda seq: (seq, 0))


def by_head(heads):
    return pl.BlockSpec((heads, SEQ, HEAD_DIM), lambda seq: (0, seq, 0))


def attend_tables():
    half = HEAD_DIM // 2
    positions = jnp.arange(SEQ).astype(jnp.float32)
    frequency = rope_base ** (-jnp.arange(half).astype(jnp.float32) * 2.0 / HEAD_DIM)
    angles = positions[:, None] * frequency[None, :]
    cosine, sine = jnp.cos(angles), jnp.sin(angles)
    return (
        jnp.concatenate([cosine, cosine], axis=1),
        jnp.concatenate([-sine, sine], axis=1),
    )


def attend(rows, weights, segments, tables, heads, kv_heads):
    group, width = rows.shape
    seqs = group // SEQ
    return pl.pallas_call(
        attend_kernel,
        grid=(seqs,),
        in_specs=[
            by_row(width),
            fixed(weights.shape),
            pl.BlockSpec((1, 1, SEQ), lambda seq: (seq, 0, 0)),
            fixed(tables[0].shape),
            fixed(tables[1].shape),
        ],
        out_specs=[
            by_head(heads),
            by_head(kv_heads),
            by_head(kv_heads),
            by_row(heads * HEAD_DIM),
            pl.BlockSpec((1, heads, SEQ), lambda seq: (seq, 0, 0)),
            by_row(width),
        ],
        out_shape=[
            jax.ShapeDtypeStruct((heads, group, HEAD_DIM), jnp.bfloat16),
            jax.ShapeDtypeStruct((kv_heads, group, HEAD_DIM), jnp.bfloat16),
            jax.ShapeDtypeStruct((kv_heads, group, HEAD_DIM), jnp.bfloat16),
            jax.ShapeDtypeStruct((group, heads * HEAD_DIM), jnp.bfloat16),
            jax.ShapeDtypeStruct((seqs, heads, SEQ), jnp.float32),
            jax.ShapeDtypeStruct((group, width), jnp.bfloat16),
        ],
        scratch_shapes=[
            pltpu.VMEM((SEQ, SEQ), jnp.float32),
            pltpu.VMEM((kv_heads, HEAD_DIM, SEQ), jnp.bfloat16),
            pltpu.VMEM((heads, SEQ, HEAD_DIM), jnp.bfloat16),
        ],
        compiler_params=pltpu.CompilerParams(
            dimension_semantics=("arbitrary",), vmem_limit_bytes=56 << 20
        ),
        cost_estimate=pl.CostEstimate(
            flops=10_000_000_000, transcendentals=3_000_000, bytes_accessed=60_000_000
        ),
    )(rows, weights, segments[:, None, :], *tables)


def attend_back(rows, weights, segments, tables, kept, moe_rows, branch_grad):
    queries, keys, values, mixed, logsum = kept
    group, width = rows.shape
    heads, kv_heads = queries.shape[0], keys.shape[0]
    used = weights.shape[1]
    edge = (heads + 2 * kv_heads) * HEAD_DIM
    return pl.pallas_call(
        attend_back_kernel,
        grid=(group // SEQ,),
        in_specs=[
            by_row(width),
            fixed(weights.shape),
            pl.BlockSpec((1, 1, SEQ), lambda seq: (seq, 0, 0)),
            fixed(tables[0].shape),
            fixed(tables[1].shape),
            by_head(heads),
            by_head(kv_heads),
            by_head(kv_heads),
            by_row(heads * HEAD_DIM),
            pl.BlockSpec((1, heads, SEQ), lambda seq: (seq, 0, 0)),
            by_row(width),
            by_row(branch_grad.shape[1]),
        ],
        out_specs=[by_row(width), fixed((width, used))],
        out_shape=[
            jax.ShapeDtypeStruct((group, width), jnp.bfloat16),
            jax.ShapeDtypeStruct((width, used), jnp.bfloat16),
        ],
        scratch_shapes=[
            pltpu.VMEM((SEQ, SEQ), jnp.float32),
            pltpu.VMEM((kv_heads, HEAD_DIM, SEQ), jnp.bfloat16),
            pltpu.VMEM((heads, SEQ, HEAD_DIM), jnp.bfloat16),
            pltpu.VMEM((heads, SEQ, HEAD_DIM), jnp.float32),
            pltpu.VMEM((2, kv_heads, SEQ, HEAD_DIM), jnp.float32),
            pltpu.VMEM((SEQ, edge), jnp.bfloat16),
            pltpu.VMEM((width, used), jnp.float32),
        ],
        compiler_params=pltpu.CompilerParams(
            dimension_semantics=("arbitrary",), vmem_limit_bytes=60 << 20
        ),
        cost_estimate=pl.CostEstimate(
            flops=20_000_000_000, transcendentals=3_000_000, bytes_accessed=100_000_000
        ),
    )(rows, weights, segments[:, None, :], *tables,
      queries, keys, values, mixed, logsum, moe_rows, branch_grad)


def widen_kernel(edges, *refs):
    step = pl.program_id(0)
    packed, targets = refs[:-3], refs[-3:]
    for part, low, high in zip(packed, edges[:-1], edges[1:]):

        @pl.when((step >= low) & (step < high))
        def _():
            for slot, target in enumerate(targets):
                target[0] = part[0, slot].astype(jnp.float32)


def widen(packed, edges):
    _, _, rows, width = packed[0].shape

    def home(low, high):
        return pl.BlockSpec(
            (1, 3, rows, width),
            lambda step: (jnp.clip(step - low, 0, high - low - 1), 0, 0, 0),
        )

    return pl.pallas_call(
        functools.partial(widen_kernel, edges),
        grid=(edges[-1],),
        in_specs=[home(low, high) for low, high in zip(edges[:-1], edges[1:])],
        out_specs=[pl.BlockSpec((1, rows, width), lambda step: (step, 0, 0))] * 3,
        out_shape=[jax.ShapeDtypeStruct((edges[-1], rows, width), jnp.float32)] * 3,
    )(*packed)


def shifted_blocks(block, count):
    return [block] + [
        lax.ppermute(block, "tp", [(i, (i + shift) % count) for i in range(count)])
        for shift in range(1, count)
    ]


def shifted_scatter(partial_rows, count, me):
    rows = partial_rows.shape[0] // count
    total = lax.dynamic_slice_in_dim(partial_rows, me * rows, rows, 0).astype(jnp.float32)
    for shift in range(1, count):
        block = lax.dynamic_slice_in_dim(
            partial_rows, lax.rem(me + shift, count) * rows, rows, 0
        ).astype(jnp.bfloat16)
        got = lax.ppermute(block, "tp", [(i, (i + shift) % count) for i in range(count)])
        total = total + got.astype(jnp.float32)
    return total


RUNS = (0, 2, 5, 10)


def local(
    emb,
    segment_ids,
    routes,
    norm1_gain,
    w_query,
    w_key,
    w_value,
    w_out,
    norm2_gain,
    w_router,
    w_gate,
    w_up,
    w_down,
    cotangent,
):
    local_rows, _ = emb.shape
    tp_count, tp_index = lax.axis_size("tp"), lax.axis_index("tp")
    experts_here = w_gate.shape[0]
    expert_count = w_router.shape[1]
    q_width, kv_width = w_query.shape[1], w_key.shape[1]
    used = 2 * (q_width + kv_width)
    group_size = local_rows * tp_count
    gathers = 2 if group_size <= 1024 else 1

    attn_w = lax.all_gather(
        join([w_query, w_key, w_value, w_out], w_router.T, used + 128),
        "fsdp",
        axis=0,
        tiled=True,
    )
    gain_one = norm1_gain.astype(jnp.float32)[None, :]
    gain_two = norm2_gain.astype(jnp.float32)[None, :]
    group_rows, mask, place_cols, place_rows, counts = norm_gather(
        emb, gain_one, routes, tp_count, 0
    )
    edges = [experts_here * part // gathers for part in range(gathers + 1)]
    stacks = (w_gate, w_up, w_down)
    pieces = []
    for low, high in zip(edges[:-1], edges[1:]):
        pieces.append(lax.all_gather(pack(stacks, low, high), "fsdp", axis=2, tiled=True))
        stacks, _ = lax.optimization_barrier((stacks, counts))
    late_grad, _ = lax.optimization_barrier((cotangent, counts))
    moe_grad = (resid_scale * late_grad.astype(jnp.float32)).astype(jnp.bfloat16)
    moe_grad_blocks = shifted_blocks(moe_grad, tp_count)
    capacity = group_size * routes.shape[1] // expert_count * 2
    meta = jnp.concatenate([counts[0], jnp.stack([tp_index * experts_here, tp_index])])

    tables = attend_tables()
    heads_here, kv_here = q_width // HEAD_DIM, kv_width // HEAD_DIM
    *kept, branch_part = attend(group_rows, attn_w, segment_ids, tables, heads_here, kv_here)
    mid_x, moe_rows, gate_rows, own_gates = find_mid(
        branch_part, emb, gain_two, attn_w, used, mask, tp_count, 1
    )

    outs = []
    runs = edges
    if gathers > 1:
        runs = sorted({edge * experts_here // RUNS[-1] for edge in RUNS} | set(edges))
    for first, last in zip(runs[:-1], runs[1:]):
        home = max(index for index in range(gathers) if edges[index] <= first)
        outs.append(
            experts_step(
                meta,
                place_rows,
                place_cols,
                gate_rows,
                moe_rows,
                moe_grad_blocks,
                pieces[home],
                first,
                last - first,
                first - edges[home],
                capacity,
            )
        )
    grad_sums = [
        lax.psum_scatter(part[2], "fsdp", scatter_dimension=2, tiled=True) for part in outs
    ]
    y_part, mid_grad, gain_two_grad, sent = find_mid_grad(
        [part[1] for part in outs],
        [part[0] for part in outs],
        mid_x,
        cotangent,
        own_gates,
        gain_two,
        attn_w,
        used,
        tp_count,
        2,
    )
    moe_sum = shifted_scatter(y_part, tp_count, tp_index)
    out = (mid_x + resid_scale * moe_sum).astype(jnp.bfloat16)
    dx_one, attn_grads = attend_back(group_rows, attn_w, segment_ids, tables, kept, moe_rows, sent)
    grad_emb, attn_sum, gain_sums = finish(
        dx_one, attn_grads, emb, gain_one, mid_grad, gain_two_grad, 3
    )
    expert_sums = widen(grad_sums, runs)
    return (
        out,
        grad_emb,
        gain_sums[0],
        attn_sum[:, :q_width],
        attn_sum[:, q_width : q_width + kv_width],
        attn_sum[:, q_width + kv_width : q_width + 2 * kv_width],
        attn_sum[:, q_width + 2 * kv_width : used],
        gain_sums[1],
        attn_sum[:, used : used + expert_count],
        *expert_sums,
    )


def solution(mesh):
    return jax.shard_map(
        local,
        mesh=mesh,
        in_specs=(
            P(("fsdp", "tp"), None),
            P("fsdp", None),
            P("fsdp", None),
            P(),
            P("fsdp", "tp"),
            P("fsdp", "tp"),
            P("fsdp", "tp"),
            P("fsdp", "tp"),
            P(),
            P("fsdp", None),
            P("tp", "fsdp", None),
            P("tp", "fsdp", None),
            P("tp", "fsdp", None),
            P(("fsdp", "tp"), None),
        ),
        out_specs=(
            P(("fsdp", "tp"), None),
            P(("fsdp", "tp"), None),
            P(),
            P("fsdp", "tp"),
            P("fsdp", "tp"),
            P("fsdp", "tp"),
            P("fsdp", "tp"),
            P(),
            P("fsdp", None),
            P("tp", "fsdp", None),
            P("tp", "fsdp", None),
            P("tp", "fsdp", None),
        ),
        check_vma=False,
    )
```

```python
import functools

import jax
import jax.numpy as jnp
import numpy as np
from jax import lax
from jax.experimental import pallas as pl
from jax.experimental.pallas import tpu as pltpu
from jax.sharding import PartitionSpec as P

HEAD_DIM = 64
SEQ = 512


emb_scale = 12.0
resid_scale = 0.22
attn_scale = 0.015625
norm_eps = 1e-06
rope_base = 10000.0
masked_value = -1e30


def contract_last(left_op, right_op):
    return lax.dot_general(
        left_op, right_op, (((1,), (1,)), ((), ())), preferred_element_type=jnp.float32
    )


def contract_first(left_op, right_op):
    return lax.dot_general(
        left_op, right_op, (((0,), (0,)), ((), ())), preferred_element_type=jnp.float32
    )


def line_signal(barrier, me, count):
    @pl.when(me > 0)
    def _():
        pl.semaphore_signal(barrier, inc=1, device_id={"tp": me - 1})

    @pl.when(me < count - 1)
    def _():
        pl.semaphore_signal(barrier, inc=1, device_id={"tp": me + 1})

    return jnp.where((me > 0) & (me < count - 1), 2, 1)


class Plane:
    def __init__(self, count):
        self.me = lax.axis_index("fsdp")
        self.core = lax.rem(self.me, 2)
        self.chip = lax.div(self.me, 2)
        self.chips = count // 2
        self.partner = self.me + 1 - 2 * self.core

    def chip_at(self, shift):
        return lax.rem(self.chip + shift + self.chips, self.chips)

    def peer(self, shift):
        return self.chip_at(shift) * 2 + self.core

    def signal(self, barrier):
        for shift in range(1, self.chips):
            pl.semaphore_signal(barrier, inc=1, device_id={"fsdp": self.peer(shift)})
        pl.semaphore_signal(barrier, inc=1, device_id={"fsdp": self.partner})
        return self.chips


def rows_of(ref, index, rows):
    return ref.at[pl.ds(pl.multiple_of(index * rows, rows), rows)]


class LineGather:
    def __init__(self, count, o_ref, send_sem, recv_sem):
        self.count, self.o_ref = count, o_ref
        self.send_sem, self.recv_sem = send_sem, recv_sem
        self.rows = o_ref.shape[0] // count
        me = self.me = lax.axis_index("tp")
        steps = range(count - 1)
        self.sends = [
            [(me >= step) & (me < count - 1) for step in steps],
            [(me + step < count) & (me > 0) for step in steps],
        ]
        self.gets = [
            [me - 1 - step >= 0 for step in steps],
            [me + 1 + step < count for step in steps],
        ]

    def hop(self, way, step, chunk):
        part = rows_of(self.o_ref, chunk, self.rows)
        return pltpu.make_async_remote_copy(
            src_ref=part,
            dst_ref=part,
            send_sem=self.send_sem.at[way, step],
            recv_sem=self.recv_sem.at[way, step],
            device_id={"tp": self.me + 1 if way == 0 else self.me - 1},
        )

    def start(self, step):
        @pl.when(self.sends[0][step])
        def _():
            self.hop(0, step, self.me - step).start()

        @pl.when(self.sends[1][step])
        def _():
            self.hop(1, step, self.me + step).start()

    def arrive(self, step):
        @pl.when(self.gets[0][step])
        def _():
            self.hop(0, step, self.me - 1 - step).wait_recv()

        @pl.when(self.gets[1][step])
        def _():
            self.hop(1, step, self.me + 1 + step).wait_recv()

    def finish(self):
        for step in range(self.count - 1):

            @pl.when(self.sends[0][step])
            def _():
                self.hop(0, step, self.me - step).wait_send()

            @pl.when(self.sends[1][step])
            def _():
                self.hop(1, step, self.me + step).wait_send()


def line_sems(count):
    return [
        pltpu.SemaphoreType.DMA((2, count - 1)),
        pltpu.SemaphoreType.DMA((2, count - 1)),
    ]


class PlaneGather:
    def __init__(self, plane, w_ref, wo_ref, out_send, out_recv, on_send, on_recv, kept_sem):
        self.plane, self.w_ref, self.wo_ref = plane, w_ref, wo_ref
        self.out_send, self.out_recv = out_send, out_recv
        self.on_send, self.on_recv = on_send, on_recv
        self.rows = w_ref.shape[0]
        self.kept = pltpu.make_async_copy(w_ref, rows_of(wo_ref, plane.me, self.rows), kept_sem)

    def outward(self, shift, target, source_device):
        return pltpu.make_async_remote_copy(
            src_ref=self.w_ref,
            dst_ref=rows_of(self.wo_ref, source_device, self.rows),
            send_sem=self.out_send.at[shift],
            recv_sem=self.out_recv.at[shift],
            device_id={"fsdp": target},
        )

    def onward(self, shift, source_device):
        part = rows_of(self.wo_ref, source_device, self.rows)
        return pltpu.make_async_remote_copy(
            src_ref=part,
            dst_ref=part,
            send_sem=self.on_send.at[shift - 1],
            recv_sem=self.on_recv.at[shift - 1],
            device_id={"fsdp": self.plane.partner},
        )

    def start(self):
        plane = self.plane
        for shift in range(1, plane.chips):
            self.outward(shift, plane.peer(shift), plane.me).start()
        self.outward(0, plane.partner, plane.me).start()
        self.kept.start()

    def forward(self):
        plane = self.plane
        for shift in range(1, plane.chips):
            self.outward(shift, plane.peer(shift), plane.peer(-shift)).wait_recv()
            self.onward(shift, plane.peer(-shift)).start()

    def finish(self):
        plane = self.plane
        self.outward(0, plane.partner, plane.partner).wait_recv()
        for shift in range(1, plane.chips):
            self.onward(shift, plane.chip_at(-shift) * 2 + 1 - plane.core).wait_recv()
        for shift in range(1, plane.chips):
            self.outward(shift, plane.peer(shift), plane.me).wait_send()
            self.onward(shift, plane.peer(-shift)).wait_send()
        self.outward(0, plane.partner, plane.me).wait_send()
        self.kept.wait()


class ExpertSums:
    def __init__(self, plane, picks, grads_ref, out_ref, *refs):
        self.plane, self.picks, self.grads_ref, self.out_ref = plane, picks, grads_ref, out_ref
        (
            self.got, self.own, self.chip_got, self.held,
            self.pair_send, self.pair_recv, self.own_sem,
            self.chip_send, self.chip_recv, self.put_sem,
        ) = refs
        self.rows = out_ref.shape[2]

    def area(self, index, dest):
        low = pl.multiple_of(dest * self.rows, self.rows)
        return self.grads_ref.at[self.picks[index], :, pl.ds(low, self.rows)]

    def to_pair(self, index, shift):
        plane = self.plane
        return pltpu.make_async_remote_copy(
            src_ref=self.area(index, plane.chip_at(shift) * 2 + 1 - plane.core),
            dst_ref=self.got.at[index, shift],
            send_sem=self.pair_send.at[index, shift],
            recv_sem=self.pair_recv.at[index, shift],
            device_id={"fsdp": plane.partner},
        )

    def keep(self, index, shift):
        return pltpu.make_async_copy(
            self.area(index, self.plane.peer(shift)),
            self.own.at[index, shift],
            self.own_sem.at[index, shift],
        )

    def to_chip(self, index, shift):
        return pltpu.make_async_remote_copy(
            src_ref=self.own.at[index, shift],
            dst_ref=self.chip_got.at[index, shift - 1],
            send_sem=self.chip_send.at[index, shift - 1],
            recv_sem=self.chip_recv.at[index, shift - 1],
            device_id={"fsdp": self.plane.peer(shift)},
        )

    def put(self, index):
        return pltpu.make_async_copy(
            self.held.at[index], self.out_ref.at[index], self.put_sem.at[index]
        )

    def order(self):
        return list(range(1, self.plane.chips)) + [0]

    def begin(self, index):
        for shift in self.order():
            self.to_pair(index, shift).start()
            self.keep(index, shift).start()

    def pass_on(self, index):
        for shift in self.order():
            self.to_pair(index, shift).wait_recv()
            self.keep(index, shift).wait()
            for slot in range(self.own.shape[2]):
                both = self.own[index, shift, slot].astype(jnp.float32) + self.got[
                    index, shift, slot
                ].astype(jnp.float32)
                self.own[index, shift, slot] = both.astype(jnp.bfloat16)
            if shift > 0:
                self.to_chip(index, shift).start()

    def collect(self, index):
        chips = self.plane.chips
        for shift in range(1, chips):
            self.to_chip(index, shift).wait_recv()
        for slot in range(self.own.shape[2]):
            total = self.own[index, 0, slot].astype(jnp.float32)
            for shift in range(1, chips):
                total = total + self.chip_got[index, shift - 1, slot].astype(jnp.float32)
            self.held[index, slot] = total.astype(jnp.bfloat16)
        self.put(index).start()

    def finish(self):
        for index in range(len(self.picks)):
            self.put(index).wait()
            for shift in self.order():
                self.to_pair(index, shift).wait_send()
                if shift > 0:
                    self.to_chip(index, shift).wait_send()


def expert_buffers(count, chips, rows, width):
    if count == 0:
        return []
    return [
        pltpu.VMEM((count, chips, 3, rows, width), jnp.bfloat16),
        pltpu.VMEM((count, chips, 3, rows, width), jnp.bfloat16),
        pltpu.VMEM((count, chips - 1, 3, rows, width), jnp.bfloat16),
        pltpu.VMEM((count, 3, rows, width), jnp.bfloat16),
        pltpu.SemaphoreType.DMA((count, chips)),
        pltpu.SemaphoreType.DMA((count, chips)),
        pltpu.SemaphoreType.DMA((count, chips)),
        pltpu.SemaphoreType.DMA((count, chips - 1)),
        pltpu.SemaphoreType.DMA((count, chips - 1)),
        pltpu.SemaphoreType.DMA((count,)),
    ]


class LineScatter:
    def __init__(self, count, x_refs, o_ref, recv, send, send_sem, recv_sem):
        self.count, self.x_refs, self.o_ref = count, x_refs, o_ref
        self.recv, self.send = recv, send
        self.send_sem, self.recv_sem = send_sem, recv_sem
        self.rows = o_ref.shape[0]
        me = self.me = lax.axis_index("tp")
        self.behind = (me, count - 1 - me)
        self.has_next = (me < count - 1, me > 0)
        self.has_prev = (me > 0, me < count - 1)

    def block(self, dest):
        area = pl.ds(pl.multiple_of(dest * self.rows, self.rows), self.rows)
        total = self.x_refs[0][area, :].astype(jnp.float32)
        for x_ref in self.x_refs[1:]:
            total = total + x_ref[area, :].astype(jnp.float32)
        return total

    def hop(self, way, step):
        return pltpu.make_async_remote_copy(
            src_ref=self.send.at[way, step],
            dst_ref=self.recv.at[way, step],
            send_sem=self.send_sem.at[way, step],
            recv_sem=self.recv_sem.at[way, step],
            device_id={"tp": self.me + 1 if way == 0 else self.me - 1},
        )

    def start(self, step):
        count, me, send = self.count, self.me, self.send
        for way in range(2):
            dest = count - 1 - step + me if way == 0 else step - (count - 1 - me)
            active = self.has_next[way] & (step >= self.behind[way])

            @pl.when(active & (self.behind[way] == 0))
            def _():
                send[way, step] = self.block(dest).astype(send.dtype)
                self.hop(way, step).start()

            if step > 0:

                @pl.when(active & (self.behind[way] > 0))
                def _():
                    total = self.block(dest) + self.recv[way, step - 1].astype(jnp.float32)
                    send[way, step] = total.astype(send.dtype)
                    self.hop(way, step).start()

    def arrive(self, step):
        for way in range(2):

            @pl.when(self.has_prev[way] & (step >= self.behind[way] - 1))
            def _():
                self.hop(way, step).wait_recv()

    def collect(self):
        self.o_ref[...] = self.block(self.me)
        for way in range(2):

            @pl.when(self.has_prev[way])
            def _():
                self.o_ref[...] += self.recv[way, self.count - 2].astype(jnp.float32)

    def finish(self):
        for step in range(self.count - 1):
            for way in range(2):

                @pl.when(self.has_next[way] & (step >= self.behind[way]))
                def _():
                    self.hop(way, step).wait_send()


def line_buffers(count, rows, width):
    return [
        pltpu.VMEM((2, count - 1, rows, width), jnp.bfloat16),
        pltpu.VMEM((2, count - 1, rows, width), jnp.bfloat16),
    ] + line_sems(count)


def own_rows(rows):
    return pl.ds(pl.multiple_of(lax.axis_index("tp") * rows, rows), rows)


def inverse_norm(values):
    return lax.rsqrt(jnp.mean(values * values, axis=-1, keepdims=True) + norm_eps)


def rms_back(incoming, values, gain_row):
    inverse = inverse_norm(values)
    scaled = values * inverse
    gain_grad = jnp.sum(incoming * scaled, axis=0, keepdims=True)
    weighted = incoming * gain_row
    row_inner = jnp.mean(weighted * scaled, axis=-1, keepdims=True)
    return inverse * (weighted - scaled * row_inner), gain_grad


def enter_kernel(count, plane=None):
    barrier = pltpu.get_barrier_semaphore()
    waits = line_signal(barrier, lax.axis_index("tp"), count)
    if plane is not None:
        waits = waits + plane.signal(barrier)
    pl.semaphore_wait(barrier, waits)


def remote_params(ident, limit=60):
    return pltpu.CompilerParams(
        collective_id=ident, has_side_effects=True, vmem_limit_bytes=limit << 20
    )


IN_VMEM = pl.BlockSpec(memory_space=pltpu.VMEM)
IN_PLACE = pl.BlockSpec(memory_space=pl.ANY)
TRANSFER = pl.CostEstimate(flops=0, transcendentals=0, bytes_accessed=150_000_000)


def norm_gather_kernel(count, fsdp_count, low, *refs):
    emb_ref, gain_ref, routes_ref, w_ref, *refs = refs
    stacks, refs = (refs[:3], refs[3:]) if low else ((), refs)
    rows_ref, mask_ref, cols_ref, turned_ref, counts_ref, wo_ref, *refs = refs
    packed, refs = (refs[0], refs[1:]) if low else (None, refs)
    row_send, row_recv, *refs = refs
    plane = Plane(fsdp_count)
    if low:
        held, in_sem, out_sem = refs[5:]
        gets, puts = pack_copies(low, stacks, packed, held, in_sem, out_sem)
        for get in gets:
            get.start()
    enter_kernel(count, plane)
    line = LineGather(count, rows_ref, row_send, row_recv)
    weights = PlaneGather(plane, w_ref, wo_ref, *refs[:5])
    start_x = emb_ref[...].astype(jnp.float32) * emb_scale
    normed = start_x * inverse_norm(start_x) * gain_ref[...]
    rows_ref[own_rows(line.rows), :] = normed.astype(jnp.bfloat16)
    for step in range(count - 1):
        line.start(step)
        if step == 0:
            weights.start()
            place_routes(line.rows, routes_ref, mask_ref, cols_ref, turned_ref, counts_ref)
            if low:
                for get, put in zip(gets, puts):
                    get.wait()
                    put.start()
        if step == count - 2:
            weights.forward()
        line.arrive(step)
    if low:
        for put in puts:
            put.wait()
    weights.finish()
    line.finish()


def place_routes(rows, routes_ref, mask_ref, cols_ref, turned_ref, counts_ref):
    group, lanes = mask_ref.shape
    columns = lax.broadcasted_iota(jnp.int32, (rows, lanes), 1)
    for low in range(0, group, rows):
        area = slice(low, low + rows)
        mask = jnp.zeros((rows, lanes), jnp.float32)
        for choice in range(routes_ref.shape[1]):
            mask = jnp.where(routes_ref[area, choice : choice + 1] == columns, 1.0, mask)
        mask_ref[area, :] = mask
    counts_ref[...] = jnp.sum(mask_ref[...], axis=0, keepdims=True).astype(jnp.int32)
    member = mask_ref[...].astype(jnp.bfloat16)
    for low in range(0, group, rows):
        area = slice(low, low + rows)
        here = lax.broadcasted_iota(jnp.int32, (rows, group), 0) + low
        earlier = here > lax.broadcasted_iota(jnp.int32, (rows, group), 1)
        ranks = jnp.dot(
            jnp.where(earlier, 1.0, 0.0).astype(jnp.bfloat16),
            member,
            preferred_element_type=jnp.float32,
        )
        places = jnp.where(mask_ref[area, :] > 0.0, ranks, -1.0)
        cols_ref[area, :] = places.astype(jnp.int32)
        turned_ref[:, area] = places.T.astype(jnp.int32)


def norm_gather(emb, gain_row, routes, weights, stacks, low, count, fsdp_count, ident):
    rows, width = emb.shape
    group = rows * count
    chips = fsdp_count // 2
    experts, share, hidden = stacks[0].shape
    span = experts - low
    outs = [
        jax.ShapeDtypeStruct((group, width), jnp.bfloat16),
        jax.ShapeDtypeStruct((group, 128), jnp.float32),
        jax.ShapeDtypeStruct((group, 128), jnp.int32),
        jax.ShapeDtypeStruct((128, group), jnp.int32),
        jax.ShapeDtypeStruct((1, 128), jnp.int32),
        jax.ShapeDtypeStruct((weights.shape[0] * fsdp_count, weights.shape[1]), jnp.bfloat16),
    ]
    scratch = line_sems(count) + [
        pltpu.SemaphoreType.DMA((chips,)),
        pltpu.SemaphoreType.DMA((chips,)),
        pltpu.SemaphoreType.DMA((chips - 1,)),
        pltpu.SemaphoreType.DMA((chips - 1,)),
        pltpu.SemaphoreType.DMA,
    ]
    if low:
        outs.append(jax.ShapeDtypeStruct((span, 3, share, hidden), jnp.bfloat16))
        scratch += [
            pltpu.VMEM((3, span, share, hidden), jnp.bfloat16),
            pltpu.SemaphoreType.DMA((3,)),
            pltpu.SemaphoreType.DMA((3,)),
        ]
    return pl.pallas_call(
        functools.partial(norm_gather_kernel, count, fsdp_count, low),
        out_shape=outs,
        in_specs=[IN_VMEM] * 4 + [IN_PLACE] * (3 if low else 0),
        out_specs=[IN_VMEM] * 5 + [IN_PLACE] * (len(outs) - 5),
        scratch_shapes=scratch,
        compiler_params=remote_params(ident, 48),
        cost_estimate=TRANSFER,
    )(emb, gain_row, routes, weights, *(stacks if low else ()))


def mid_kernel(
    count, part_ref, emb_ref, gain_ref, router_ref, mask_ref,
    mid_ref, rows_ref, gates_ref, own_gates,
    recv, send, sum_send, sum_recv, row_send, row_recv,
):
    enter_kernel(count)
    total = LineScatter(count, [part_ref], mid_ref, recv, send, sum_send, sum_recv)
    line = LineGather(count, rows_ref, row_send, row_recv)
    rows = line.rows
    for step in range(count - 1):
        total.start(step)
        total.arrive(step)
    total.collect()
    mid = emb_ref[...].astype(jnp.float32) * emb_scale + resid_scale * mid_ref[...]
    mid_ref[...] = mid
    own = own_rows(rows)
    rows_ref[own, :] = (mid * inverse_norm(mid) * gain_ref[...]).astype(jnp.bfloat16)

    def find_gates(chunk):
        area = pl.ds(pl.multiple_of(chunk * rows, rows), rows)
        logits = jnp.dot(rows_ref[area, :], router_ref[...], preferred_element_type=jnp.float32)
        inside = mask_ref[area, :] > 0.0
        top = jnp.max(jnp.where(inside, logits, masked_value), axis=-1, keepdims=True)
        raised = jnp.where(inside, jnp.exp(jnp.where(inside, logits - top, 0.0)), 0.0)
        gates = raised / jnp.sum(raised, axis=-1, keepdims=True)
        gates_ref[:, area] = gates.T
        return gates

    for step in range(count - 1):
        line.start(step)
        if step == 0:
            own_gates[...] = find_gates(line.me)
        line.arrive(step)

        @pl.when(line.gets[0][step])
        def _():
            find_gates(line.me - 1 - step)

        @pl.when(line.gets[1][step])
        def _():
            find_gates(line.me + 1 + step)

    line.finish()
    total.finish()


def find_mid(part, emb, gain_row, weights, used, mask, count, ident):
    rows, width = emb.shape
    group = rows * count
    return pl.pallas_call(
        functools.partial(mid_kernel, count),
        grid=(1,),
        out_shape=[
            jax.ShapeDtypeStruct((rows, width), jnp.float32),
            jax.ShapeDtypeStruct((group, width), jnp.bfloat16),
            jax.ShapeDtypeStruct((128, group), jnp.float32),
            jax.ShapeDtypeStruct((rows, 128), jnp.float32),
        ],
        in_specs=[
            IN_VMEM,
            IN_VMEM,
            IN_VMEM,
            pl.BlockSpec((width, 128), lambda step: (0, used // 128)),
            IN_VMEM,
        ],
        out_specs=[IN_VMEM] * 4,
        scratch_shapes=line_buffers(count, rows, width) + line_sems(count),
        compiler_params=remote_params(ident),
        cost_estimate=TRANSFER,
    )(part, emb, gain_row, weights, mask)


def moe_back_kernel(count, fsdp_count, runs, picks, *refs):
    dx_refs, y_refs, refs = refs[:runs], refs[runs : 2 * runs], refs[2 * runs :]
    mid_ref, cotangent_ref, own_gates, gain_ref, router_ref, *refs = refs
    grads_ref, refs = (refs[0], refs[1:]) if picks else (None, refs)
    y_ref, mid_grad, gain_grad, sent_ref, *refs = refs
    sums_ref, refs = (refs[0], refs[1:]) if picks else (None, refs)
    (
        dx_parts, y_parts, load_sem, store_sem,
        sum_ref, recv, send, sum_send, sum_recv, row_send, row_recv, *refs,
    ) = refs
    loads = []
    for index, (source, parts) in enumerate(
        [(ref, dx_parts) for ref in dx_refs] + [(ref, y_parts) for ref in y_refs]
    ):
        loads.append(
            pltpu.make_async_copy(source, parts.at[index % runs], load_sem.at[index])
        )
        loads[-1].start()
    plane = Plane(fsdp_count) if picks else None
    enter_kernel(count, plane)
    total = LineScatter(
        count, [dx_parts.at[run] for run in range(runs)], sum_ref, recv, send, sum_send, sum_recv
    )
    line = LineGather(count, sent_ref, row_send, row_recv)
    experts = ExpertSums(plane, picks, grads_ref, sums_ref, *refs) if picks else None
    rows, width = mid_ref.shape
    store = pltpu.make_async_copy(y_parts.at[0], y_ref, store_sem)
    for index in range(len(picks)):
        experts.begin(index)
    for load in loads[:runs]:
        load.wait()
    for step in range(count - 1):
        total.start(step)
        if step == 0:
            for load in loads[runs:]:
                load.wait()
            for chunk in range(count if runs > 1 else 0):
                area = slice(chunk * rows, (chunk + 1) * rows)
                whole = y_parts[0, area, :].astype(jnp.float32)
                for run in range(1, runs):
                    whole = whole + y_parts[run, area, :].astype(jnp.float32)
                y_parts[0, area, :] = whole.astype(y_parts.dtype)
            store.start()
        if step < len(picks):
            experts.pass_on(step)
        total.arrive(step)
    total.collect()
    gates = own_gates[...]
    gates_grad = sum_ref[:, width:]
    gates_inner = jnp.sum(gates * gates_grad, axis=-1, keepdims=True)
    logits_grad = (gates * (gates_grad - gates_inner)).astype(jnp.bfloat16)
    incoming = sum_ref[:, :width] + contract_last(logits_grad, router_ref[...])
    from_norm, gain_part = rms_back(incoming, mid_ref[...], gain_ref[...])
    grad = cotangent_ref[...].astype(jnp.float32) + from_norm
    mid_grad[...] = grad
    gain_grad[...] = gain_part
    own = own_rows(rows)
    sent_ref[own, :width] = (resid_scale * grad).astype(jnp.bfloat16)
    sent_ref[own, width:] = logits_grad
    for step in range(count - 1):
        line.start(step)
        if 0 < step <= len(picks):
            experts.collect(step - 1)
        line.arrive(step)
    for index in range(count - 2, len(picks)):
        experts.collect(index)
    line.finish()
    total.finish()
    store.wait()
    if picks:
        experts.finish()


def find_mid_grad(
    dx_parts, y_parts, mid, cotangent, own_gates, gain_row, weights, used, grads, picks,
    count, fsdp_count, ident,
):
    rows, width = mid.shape
    runs, group = len(dx_parts), rows * count
    wide = dx_parts[0].shape[1]
    share = grads.shape[2] // fsdp_count
    sums = [jax.ShapeDtypeStruct((len(picks), 3, share, grads.shape[3]), jnp.bfloat16)]
    sums = sums if picks else []
    return pl.pallas_call(
        functools.partial(moe_back_kernel, count, fsdp_count, runs, picks),
        grid=(1,),
        out_shape=[
            jax.ShapeDtypeStruct((group, width), jnp.bfloat16),
            jax.ShapeDtypeStruct((rows, width), jnp.float32),
            jax.ShapeDtypeStruct((1, width), jnp.float32),
            jax.ShapeDtypeStruct((group, wide), jnp.bfloat16),
        ]
        + sums,
        in_specs=[IN_PLACE] * (2 * runs)
        + [IN_VMEM] * 4
        + [pl.BlockSpec((width, 128), lambda step: (0, used // 128))]
        + [IN_PLACE] * len(sums),
        out_specs=[IN_PLACE] + [IN_VMEM] * 3 + [IN_PLACE] * len(sums),
        scratch_shapes=[
            pltpu.VMEM((runs, group, wide), jnp.bfloat16),
            pltpu.VMEM((runs, group, width), jnp.bfloat16),
            pltpu.SemaphoreType.DMA((2 * runs,)),
            pltpu.SemaphoreType.DMA,
            pltpu.VMEM((rows, wide), jnp.float32),
        ]
        + line_buffers(count, rows, wide)
        + line_sems(count)
        + expert_buffers(len(picks), fsdp_count // 2, share, grads.shape[3]),
        compiler_params=remote_params(ident, 63),
        cost_estimate=TRANSFER,
    )(*dx_parts, *y_parts, mid, cotangent, own_gates, gain_row, weights, *([grads] if picks else []))


def finish_kernel(tp_count, fsdp_count, picks, *refs):
    x_ref, w_ref, emb_ref, gain_ref, mid_grad, gain_two, *refs = refs
    grads_ref, refs = (refs[0], refs[1:]) if picks else (None, refs)
    grad_ref, w_sum, gains_ref, *refs = refs
    sums_ref, refs = (refs[0], refs[1:]) if picks else (None, refs)
    (
        line_recv, line_send, line_send_sem, line_recv_sem,
        pair_got, chip_sums, chip_got, pair_send, pair_recv, chip_send, chip_recv,
        tp_got, fsdp_got, small_send, small_recv, *refs,
    ) = refs
    plane = Plane(fsdp_count)
    tp_me, fsdp_me = lax.axis_index("tp"), plane.me
    barrier = pltpu.get_barrier_semaphore()
    for shift in range(1, tp_count):
        pl.semaphore_signal(barrier, inc=1, device_id={"tp": lax.rem(tp_me + shift, tp_count)})
    for shift in range(1, fsdp_count):
        pl.semaphore_signal(
            barrier, inc=1, device_id={"fsdp": lax.rem(fsdp_me + shift, fsdp_count)}
        )
    pl.semaphore_wait(barrier, tp_count + fsdp_count - 2)
    line = LineScatter(
        tp_count, [x_ref], grad_ref, line_recv, line_send, line_send_sem, line_recv_sem
    )
    rows = w_sum.shape[0]

    def to_pair(shift):
        return pltpu.make_async_remote_copy(
            src_ref=rows_of(w_ref, plane.chip_at(shift) * 2 + 1 - plane.core, rows),
            dst_ref=pair_got.at[shift],
            send_sem=pair_send.at[shift],
            recv_sem=pair_recv.at[shift],
            device_id={"fsdp": plane.partner},
        )

    def to_chip(shift):
        return pltpu.make_async_remote_copy(
            src_ref=chip_sums.at[shift - 1],
            dst_ref=chip_got.at[shift - 1],
            send_sem=chip_send.at[shift - 1],
            recv_sem=chip_recv.at[shift - 1],
            device_id={"fsdp": plane.peer(shift)},
        )

    def both_cores(shift):
        own = pl.ds(pl.multiple_of(plane.peer(shift) * rows, rows), rows)
        return w_ref[own, :].astype(jnp.float32) + pair_got[shift].astype(jnp.float32)

    def exchange(axis, me, count, got, base):
        copies = []
        for shift in range(1, count):
            copies.append(
                pltpu.make_async_remote_copy(
                    src_ref=gains_ref,
                    dst_ref=got.at[me],
                    send_sem=small_send.at[base + shift],
                    recv_sem=small_recv.at[base + shift],
                    device_id={axis: lax.rem(me + shift, count)},
                )
            )
            copies[-1].start()
        got[me] = gains_ref[...]
        for copy in copies:
            copy.wait()
        total = got[0]
        for index in range(1, count):
            total = total + got[index]
        return total

    experts = ExpertSums(plane, picks, grads_ref, sums_ref, *refs) if picks else None
    line.start(0)
    order = list(range(1, plane.chips)) + [0]
    for shift in order:
        to_pair(shift).start()
    for index in range(len(picks)):
        experts.begin(index)
    for shift in order:
        to_pair(shift).wait_recv()
        if shift > 0:
            chip_sums[shift - 1] = both_cores(shift).astype(chip_sums.dtype)
            to_chip(shift).start()
    for index in range(len(picks)):
        experts.pass_on(index)
    line.arrive(0)
    for step in range(1, tp_count - 1):
        line.start(step)
        line.arrive(step)
    line.collect()
    from_norm, gain_one = rms_back(
        grad_ref[...], emb_ref[...].astype(jnp.float32) * emb_scale, gain_ref[...]
    )
    gains_ref[...] = jnp.zeros_like(gains_ref)
    gains_ref[0:1, :] = gain_one
    gains_ref[1:2, :] = gain_two[...]
    grad_ref[...] = emb_scale * (mid_grad[...] + from_norm)
    total = both_cores(0)
    for shift in range(1, plane.chips):
        to_chip(shift).wait_recv()
        total = total + chip_got[shift - 1].astype(jnp.float32)
    w_sum[...] = total
    for index in range(len(picks)):
        experts.collect(index)
    gains_ref[...] = exchange("tp", tp_me, tp_count, tp_got, 0)
    gains_ref[...] = exchange("fsdp", fsdp_me, fsdp_count, fsdp_got, tp_count)
    line.finish()
    for shift in order:
        to_pair(shift).wait_send()
        if shift > 0:
            to_chip(shift).wait_send()
    if picks:
        experts.finish()


def finish(dx_rows, weight_grads, emb, gain_row, mid_grad, gain_two, grads, picks, ident):
    tp_count, fsdp_count = lax.axis_size("tp"), lax.axis_size("fsdp")
    rows, width = emb.shape
    w_rows, w_width = weight_grads.shape[0] // fsdp_count, weight_grads.shape[1]
    chips = fsdp_count // 2
    share = grads.shape[2] // fsdp_count
    sums = [jax.ShapeDtypeStruct((len(picks), 3, share, grads.shape[3]), jnp.bfloat16)]
    sums = sums if picks else []
    return pl.pallas_call(
        functools.partial(finish_kernel, tp_count, fsdp_count, picks),
        out_shape=[
            jax.ShapeDtypeStruct((rows, width), jnp.float32),
            jax.ShapeDtypeStruct((w_rows, w_width), jnp.float32),
            jax.ShapeDtypeStruct((8, width), jnp.float32),
            *sums,
        ],
        in_specs=[IN_VMEM] * 6 + [IN_PLACE] * len(sums),
        out_specs=[IN_VMEM] * 3 + [IN_PLACE] * len(sums),
        scratch_shapes=line_buffers(tp_count, rows, width)
        + [
            pltpu.VMEM((chips, w_rows, w_width), jnp.bfloat16),
            pltpu.VMEM((chips - 1, w_rows, w_width), jnp.bfloat16),
            pltpu.VMEM((chips - 1, w_rows, w_width), jnp.bfloat16),
            pltpu.SemaphoreType.DMA((chips,)),
            pltpu.SemaphoreType.DMA((chips,)),
            pltpu.SemaphoreType.DMA((chips - 1,)),
            pltpu.SemaphoreType.DMA((chips - 1,)),
            pltpu.VMEM((tp_count, 8, width), jnp.float32),
            pltpu.VMEM((fsdp_count, 8, width), jnp.float32),
            pltpu.SemaphoreType.DMA((tp_count + fsdp_count,)),
            pltpu.SemaphoreType.DMA((tp_count + fsdp_count,)),
        ]
        + expert_buffers(len(picks), chips, share, grads.shape[3]),
        compiler_params=remote_params(ident),
        cost_estimate=TRANSFER,
    )(dx_rows, weight_grads, emb, gain_row, mid_grad, gain_two, *([grads] if picks else []))


def pack_copies(low, sources, target, held, in_sem, out_sem):
    span = target.shape[0]
    gets = [
        pltpu.make_async_copy(source.at[pl.ds(low, span)], held.at[slot], in_sem.at[slot])
        for slot, source in enumerate(sources)
    ]
    puts = [
        pltpu.make_async_copy(held.at[slot], target.at[:, slot], out_sem.at[slot])
        for slot in range(len(sources))
    ]
    return gets, puts


def pack_kernel(low, *refs):
    sources, target, held, in_sem, out_sem = refs[:-4], *refs[-4:]
    gets, puts = pack_copies(low, sources, target, held, in_sem, out_sem)
    for get in gets:
        get.start()
    for get, put in zip(gets, puts):
        get.wait()
        put.start()
    for put in puts:
        put.wait()


def pack(stacks, low, high):
    _, rows, width = stacks[0].shape
    count, span = len(stacks), high - low
    return pl.pallas_call(
        functools.partial(pack_kernel, low),
        in_specs=[IN_PLACE] * count,
        out_specs=IN_PLACE,
        out_shape=jax.ShapeDtypeStruct((span, count, rows, width), jnp.bfloat16),
        scratch_shapes=[
            pltpu.VMEM((count, span, rows, width), jnp.bfloat16),
            pltpu.SemaphoreType.DMA((count,)),
            pltpu.SemaphoreType.DMA((count,)),
        ],
    )(*stacks)


def join_kernel(*refs):
    *sources, last, target = refs
    low = 0
    for source in sources:
        target[:, low : low + source.shape[1]] = source[...]
        low += source.shape[1]
    router = last[...].astype(jnp.float32).T.astype(jnp.bfloat16)
    target[:, low:] = jnp.zeros((target.shape[0], target.shape[1] - low), jnp.bfloat16)
    target[:, low : low + router.shape[1]] = router


def join(parts, last_turned, width):
    return pl.pallas_call(
        join_kernel,
        in_specs=[IN_VMEM] * (len(parts) + 1),
        out_specs=IN_VMEM,
        out_shape=jax.ShapeDtypeStruct((parts[0].shape[0], width), jnp.bfloat16),
    )(*parts, last_turned)


SLOTS = 256


def experts_kernel(
    first_expert,
    capacity,
    meta,
    place_rows,
    place_cols,
    gate_rows,
    x_ref,
    weights,
    *refs,
):
    g_blocks, (y_ref, dx_ref, grads, g_ref, g_sem) = refs[:-5], refs[-5:]
    step = pl.program_id(0)
    expert = step + first_expert
    group, width = x_ref.shape
    tail = dx_ref.shape[1] - width

    @pl.when(step == 0)
    def _():
        count, rows = len(g_blocks), g_blocks[0].shape[0]
        copies = []
        for shift, block in enumerate(g_blocks):
            home = lax.rem(meta[meta.shape[0] - 1] + count - shift, count)
            copies.append(pltpu.make_async_copy(block, rows_of(g_ref, home, rows), g_sem.at[shift]))
            copies[-1].start()
        y_ref[...] = jnp.zeros_like(y_ref)
        dx_ref[...] = jnp.zeros_like(dx_ref)
        for copy in copies:
            copy.wait()

    column = expert + meta[meta.shape[0] - 2]
    lanes = lax.broadcasted_iota(jnp.int32, place_cols.shape, 1)
    place_col = jnp.sum(jnp.where(lanes == column, place_cols[...], 0), axis=1, keepdims=True)
    place_row = place_rows[pl.ds(column, 1), :]
    gate_row = gate_rows[pl.ds(column, 1), :].astype(jnp.bfloat16).astype(jnp.float32)
    mark = jnp.where(lax.broadcasted_iota(jnp.int32, (1, tail), 1) == column, 1.0, 0.0)

    def run(base, span):
        slots = lax.broadcasted_iota(jnp.int32, (span, group), 0) + base
        hit = slots == place_row
        pick = jnp.where(hit, 1.0, 0.0).astype(jnp.bfloat16)
        scale = jnp.sum(jnp.where(hit, gate_row, 0.0), axis=1, keepdims=True)
        x_taken = jnp.dot(pick, x_ref[...], preferred_element_type=jnp.float32).astype(jnp.bfloat16)
        g_taken = jnp.dot(pick, g_ref[...], preferred_element_type=jnp.float32).astype(jnp.bfloat16)
        gate_pre = jnp.dot(x_taken, weights[0, 0], preferred_element_type=jnp.float32)
        up_pre = jnp.dot(x_taken, weights[0, 1], preferred_element_type=jnp.float32)
        raw = jnp.dot(g_taken, weights[0, 2], preferred_element_type=jnp.float32)
        sig = jax.nn.sigmoid(gate_pre)
        silu = gate_pre * sig
        act = (silu * up_pre).astype(jnp.bfloat16).astype(jnp.float32)
        slot_grad = jnp.sum(act * raw, axis=1, keepdims=True)
        act_grad = raw * scale
        act_scaled = (act * scale).astype(jnp.bfloat16)
        gate_grad = (act_grad * up_pre * sig * (1.0 + gate_pre * (1.0 - sig))).astype(jnp.bfloat16)
        up_grad = (act_grad * silu).astype(jnp.bfloat16)
        extra = (slot_grad * mark).astype(jnp.bfloat16)
        rows_out = contract_last(act_scaled, weights[0, 2]).astype(jnp.bfloat16)
        rows_in = (
            contract_last(gate_grad, weights[0, 0]) + contract_last(up_grad, weights[0, 1])
        ).astype(jnp.bfloat16)
        for slot, left_op, right_op in (
            (0, x_taken, gate_grad),
            (1, x_taken, up_grad),
            (2, g_taken, act_scaled),
        ):
            grad = contract_first(left_op, right_op)
            if base > 0:
                grad = grad + grads[0, slot].astype(jnp.float32)
            grads[0, slot] = grad.astype(jnp.bfloat16)
        block = min(256, group)
        for start in range(0, group, block):
            back = jnp.where(
                lax.broadcasted_iota(jnp.int32, (block, span), 1) + base
                == place_col[start : start + block],
                1.0,
                0.0,
            ).astype(jnp.bfloat16)
            for target, low_col, addend in (
                (y_ref, 0, rows_out),
                (dx_ref, 0, rows_in),
                (dx_ref, width, extra),
            ):
                area = (slice(start, start + block), slice(low_col, low_col + addend.shape[1]))
                target[area] = (
                    target[area].astype(jnp.float32)
                    + jnp.dot(back, addend, preferred_element_type=jnp.float32)
                ).astype(target.dtype)

    run(0, min(SLOTS, capacity))
    for base in range(SLOTS, capacity, SLOTS):
        span = min(SLOTS, -(-(capacity - base) // 16) * 16)

        @pl.when(meta[column] > base)
        def _():
            run(base, span)


def experts_step(meta, place_rows, place_cols, gate_rows, x_rows, g_blocks, weights, first, count, skip, capacity):
    group, width = x_rows.shape
    hidden = weights.shape[-1]
    tail = 128

    def whole(shape):
        return pl.BlockSpec(
            shape, lambda step, meta: (0,) * len(shape), pipeline_mode=pl.Buffered(1)
        )

    def big(offset):
        return pl.BlockSpec((1, 3, width, hidden), lambda step, meta: (step + offset, 0, 0, 0))

    return pl.pallas_call(
        functools.partial(experts_kernel, first, capacity),
        grid_spec=pltpu.PrefetchScalarGridSpec(
            num_scalar_prefetch=1,
            grid=(count,),
            in_specs=[
                whole(place_rows.shape),
                whole(place_cols.shape),
                whole(gate_rows.shape),
                whole(x_rows.shape),
                big(skip),
            ]
            + [IN_PLACE] * len(g_blocks),
            out_specs=[
                whole((group, width)),
                whole((group, width + tail)),
                big(0),
            ],
            scratch_shapes=[
                pltpu.VMEM((group, width), jnp.bfloat16),
                pltpu.SemaphoreType.DMA((len(g_blocks),)),
            ],
        ),
        out_shape=[
            jax.ShapeDtypeStruct((group, width), jnp.bfloat16),
            jax.ShapeDtypeStruct((group, width + tail), jnp.bfloat16),
            jax.ShapeDtypeStruct((count, 3, width, hidden), jnp.bfloat16),
        ],
        compiler_params=pltpu.CompilerParams(
            dimension_semantics=("arbitrary",), vmem_limit_bytes=63 << 20
        ),
        cost_estimate=pl.CostEstimate(
            flops=count * 17 * 2 * 408 * width * hidden,
            transcendentals=count * 408 * hidden,
            bytes_accessed=count * 12 * width * hidden,
        ),
    )(meta, place_rows, place_cols, gate_rows, x_rows, weights, *g_blocks)


def rotate_head(values, cosine, sine, sign):
    half = values.shape[-1] // 2
    other = jnp.concatenate([values[:, half:], values[:, :half]], axis=1)
    return values * cosine + other * (sine * sign)


def segment_bias(seg_row):
    length = seg_row.shape[1]
    shape = (length, length)
    seg_row = seg_row.astype(jnp.float32)
    seg_col = jnp.broadcast_to(seg_row, (128, length)).T[:, :1]
    keys = lax.broadcasted_iota(jnp.int32, shape, 0)
    queries = lax.broadcasted_iota(jnp.int32, shape, 1)
    return jnp.where((keys <= queries) & (seg_col == seg_row), 0.0, masked_value)


def attend_kernel(
    x_ref,
    w_ref,
    seg_row,
    cos_ref,
    sin_ref,
    q_ref,
    k_ref,
    v_ref,
    mixed_ref,
    logsum_ref,
    branch_ref,
    bias,
    v_turned,
    mixed_heads,
):
    heads, kv_heads = q_ref.shape[0], k_ref.shape[0]
    per_kv = heads // kv_heads
    block = SEQ // 2
    edge = (heads + 2 * kv_heads) * HEAD_DIM
    proj = jnp.dot(x_ref[...], w_ref[:, :edge], preferred_element_type=jnp.float32)
    cosine, sine = cos_ref[...], sin_ref[...]
    for head in range(heads + 2 * kv_heads):
        part = proj[:, head * HEAD_DIM : (head + 1) * HEAD_DIM]
        if head < heads:
            q_ref[head] = rotate_head(part, cosine, sine, 1.0).astype(jnp.bfloat16)
        elif head < heads + kv_heads:
            k_ref[head - heads] = rotate_head(part, cosine, sine, 1.0).astype(jnp.bfloat16)
        else:
            v_ref[head - heads - kv_heads] = part.astype(jnp.bfloat16)
            v_turned[head - heads - kv_heads] = part.T.astype(jnp.bfloat16)
    bias[...] = segment_bias(seg_row[0])

    def one_head(head, carry):
        kv = head // per_kv
        for part in range(2):
            span, low = block * (part + 1), block * part
            scores = contract_last(k_ref[kv, :span], q_ref[head, low : low + block]) * attn_scale
            scores = scores + bias[:span, low : low + block]
            top = jnp.max(scores, axis=0, keepdims=True)
            raised = jnp.exp(scores - top)
            total = jnp.sum(raised, axis=0, keepdims=True)
            probs = (raised * (1.0 / total)).astype(jnp.bfloat16)
            turned = jnp.dot(v_turned[kv, :, :span], probs, preferred_element_type=jnp.float32)
            mixed_heads[head, low : low + block, :] = turned.T.astype(jnp.bfloat16)
            logsum_ref[0, pl.ds(head, 1), low : low + block] = top + jnp.log(total)
        return carry

    lax.fori_loop(0, heads, one_head, 0)
    for head in range(heads):
        mixed_ref[:, head * HEAD_DIM : (head + 1) * HEAD_DIM] = mixed_heads[head]
    branch_ref[...] = contract_last(
        mixed_ref[...], w_ref[:, edge : edge + heads * HEAD_DIM]
    ).astype(jnp.bfloat16)


def attend_back_kernel(
    x_ref,
    w_ref,
    seg_row,
    cos_ref,
    sin_ref,
    q_ref,
    k_ref,
    v_ref,
    mixed_ref,
    logsum_ref,
    moe_rows,
    branch_grad,
    dx_ref,
    dw_ref,
    bias,
    k_turned,
    mixed_grads,
    q_grads,
    kv_grads,
    qkv_grad,
    dw_acc,
):
    heads, kv_heads = q_ref.shape[0], k_ref.shape[0]
    per_kv = heads // kv_heads
    block = SEQ // 2
    edge = (heads + 2 * kv_heads) * HEAD_DIM
    step = pl.program_id(0)
    out_edge = edge + heads * HEAD_DIM
    width = x_ref.shape[1]
    grad = jnp.dot(
        branch_grad[:, :width], w_ref[:, edge:out_edge], preferred_element_type=jnp.float32
    ).astype(jnp.bfloat16)
    for head in range(heads):
        mixed_grads[head] = grad[:, head * HEAD_DIM : (head + 1) * HEAD_DIM]
    for kv in range(kv_heads):
        k_turned[kv] = k_ref[kv].astype(jnp.float32).T.astype(jnp.bfloat16)
    bias[...] = segment_bias(seg_row[0])
    kv_grads[...] = jnp.zeros_like(kv_grads)

    def one_head(head, carry):
        kv = head // per_kv
        for part in range(2):
            span, low = block * (part + 1), block * part
            high = low + block
            scores = contract_last(k_ref[kv, :span], q_ref[head, low:high]) * attn_scale
            scores = scores + bias[:span, low:high]
            probs = jnp.exp(scores - logsum_ref[0, pl.ds(head, 1), low:high])
            probs_grad = contract_last(v_ref[kv, :span], mixed_grads[head, low:high])
            inner = jnp.sum(probs * probs_grad, axis=0, keepdims=True)
            score_grad = (probs * (probs_grad - inner)).astype(jnp.bfloat16)
            turned = jnp.dot(k_turned[kv, :, :span], score_grad, preferred_element_type=jnp.float32)
            q_grads[head, low:high, :] = turned.T * attn_scale
            kv_grads[0, kv, :span, :] += jnp.dot(
                score_grad, q_ref[head, low:high], preferred_element_type=jnp.float32
            )
            kv_grads[1, kv, :span, :] += jnp.dot(
                probs.astype(jnp.bfloat16), mixed_grads[head, low:high],
                preferred_element_type=jnp.float32,
            )
        return carry

    lax.fori_loop(0, heads, one_head, 0)
    cosine, sine = cos_ref[...], sin_ref[...]
    for head in range(heads + 2 * kv_heads):
        if head < heads:
            part = rotate_head(q_grads[head], cosine, sine, -1.0)
        elif head < heads + kv_heads:
            part = rotate_head(kv_grads[0, head - heads] * attn_scale, cosine, sine, -1.0)
        else:
            part = kv_grads[1, head - heads - kv_heads]
        qkv_grad[:, head * HEAD_DIM : (head + 1) * HEAD_DIM] = part.astype(jnp.bfloat16)
    dx_ref[...] = contract_last(qkv_grad[...], w_ref[:, :edge]).astype(jnp.bfloat16)
    for low, high, left_op, right_op in (
        (0, edge, x_ref[...], qkv_grad[...]),
        (edge, out_edge, branch_grad[:, :width], mixed_ref[...]),
        (out_edge, dw_acc.shape[1], moe_rows[...], branch_grad[:, width:]),
    ):
        part = contract_first(left_op, right_op)

        @pl.when(step == 0)
        def _():
            dw_acc[:, low:high] = part

        @pl.when(step > 0)
        def _():
            dw_acc[:, low:high] += part

    @pl.when(step == pl.num_programs(0) - 1)
    def _():
        dw_ref[...] = dw_acc[...].astype(jnp.bfloat16)


def fixed(shape):
    return pl.BlockSpec(shape, lambda seq: (0,) * len(shape), pipeline_mode=pl.Buffered(1))


def by_row(width):
    return pl.BlockSpec((SEQ, width), lambda seq: (seq, 0))


def by_head(heads):
    return pl.BlockSpec((heads, SEQ, HEAD_DIM), lambda seq: (0, seq, 0))


def attend_tables():
    half = HEAD_DIM // 2
    positions = np.arange(SEQ, dtype=np.float32)
    frequency = np.float32(rope_base) ** (-np.arange(half, dtype=np.float32) * 2.0 / HEAD_DIM)
    angles = (positions[:, None] * frequency[None, :].astype(np.float32)).astype(np.float32)
    cosine, sine = np.cos(angles), np.sin(angles)
    return (
        jnp.asarray(np.concatenate([cosine, cosine], axis=1)),
        jnp.asarray(np.concatenate([-sine, sine], axis=1)),
    )


def attend(rows, weights, segments, tables, heads, kv_heads):
    group, width = rows.shape
    seqs = group // SEQ
    return pl.pallas_call(
        attend_kernel,
        grid=(seqs,),
        in_specs=[
            by_row(width),
            fixed(weights.shape),
            pl.BlockSpec((1, 1, SEQ), lambda seq: (seq, 0, 0)),
            fixed(tables[0].shape),
            fixed(tables[1].shape),
        ],
        out_specs=[
            by_head(heads),
            by_head(kv_heads),
            by_head(kv_heads),
            by_row(heads * HEAD_DIM),
            pl.BlockSpec((1, heads, SEQ), lambda seq: (seq, 0, 0)),
            by_row(width),
        ],
        out_shape=[
            jax.ShapeDtypeStruct((heads, group, HEAD_DIM), jnp.bfloat16),
            jax.ShapeDtypeStruct((kv_heads, group, HEAD_DIM), jnp.bfloat16),
            jax.ShapeDtypeStruct((kv_heads, group, HEAD_DIM), jnp.bfloat16),
            jax.ShapeDtypeStruct((group, heads * HEAD_DIM), jnp.bfloat16),
            jax.ShapeDtypeStruct((seqs, heads, SEQ), jnp.float32),
            jax.ShapeDtypeStruct((group, width), jnp.bfloat16),
        ],
        scratch_shapes=[
            pltpu.VMEM((SEQ, SEQ), jnp.float32),
            pltpu.VMEM((kv_heads, HEAD_DIM, SEQ), jnp.bfloat16),
            pltpu.VMEM((heads, SEQ, HEAD_DIM), jnp.bfloat16),
        ],
        compiler_params=pltpu.CompilerParams(
            dimension_semantics=("arbitrary",), vmem_limit_bytes=56 << 20
        ),
        cost_estimate=pl.CostEstimate(
            flops=10_000_000_000, transcendentals=3_000_000, bytes_accessed=60_000_000
        ),
    )(rows, weights, segments[:, None, :], *tables)


def attend_back(rows, weights, segments, tables, kept, moe_rows, branch_grad):
    queries, keys, values, mixed, logsum = kept
    group, width = rows.shape
    heads, kv_heads = queries.shape[0], keys.shape[0]
    used = weights.shape[1]
    edge = (heads + 2 * kv_heads) * HEAD_DIM
    return pl.pallas_call(
        attend_back_kernel,
        grid=(group // SEQ,),
        in_specs=[
            by_row(width),
            fixed(weights.shape),
            pl.BlockSpec((1, 1, SEQ), lambda seq: (seq, 0, 0)),
            fixed(tables[0].shape),
            fixed(tables[1].shape),
            by_head(heads),
            by_head(kv_heads),
            by_head(kv_heads),
            by_row(heads * HEAD_DIM),
            pl.BlockSpec((1, heads, SEQ), lambda seq: (seq, 0, 0)),
            by_row(width),
            by_row(branch_grad.shape[1]),
        ],
        out_specs=[by_row(width), fixed((width, used))],
        out_shape=[
            jax.ShapeDtypeStruct((group, width), jnp.bfloat16),
            jax.ShapeDtypeStruct((width, used), jnp.bfloat16),
        ],
        scratch_shapes=[
            pltpu.VMEM((SEQ, SEQ), jnp.float32),
            pltpu.VMEM((kv_heads, HEAD_DIM, SEQ), jnp.bfloat16),
            pltpu.VMEM((heads, SEQ, HEAD_DIM), jnp.bfloat16),
            pltpu.VMEM((heads, SEQ, HEAD_DIM), jnp.float32),
            pltpu.VMEM((2, kv_heads, SEQ, HEAD_DIM), jnp.float32),
            pltpu.VMEM((SEQ, edge), jnp.bfloat16),
            pltpu.VMEM((width, used), jnp.float32),
        ],
        compiler_params=pltpu.CompilerParams(
            dimension_semantics=("arbitrary",), vmem_limit_bytes=60 << 20
        ),
        cost_estimate=pl.CostEstimate(
            flops=20_000_000_000, transcendentals=3_000_000, bytes_accessed=100_000_000
        ),
    )(rows, weights, segments[:, None, :], *tables,
      queries, keys, values, mixed, logsum, moe_rows, branch_grad)


def widen_kernel(edges, *refs):
    step = pl.program_id(0)
    packed, targets = refs[:-3], refs[-3:]
    for part, low, high in zip(packed, edges[:-1], edges[1:]):

        @pl.when((step >= low) & (step < high))
        def _():
            for slot, target in enumerate(targets):
                target[0] = part[0, slot].astype(jnp.float32)


def widen(packed, edges):
    _, _, rows, width = packed[0].shape

    def home(low, high):
        return pl.BlockSpec(
            (1, 3, rows, width),
            lambda step: (jnp.clip(step - low, 0, high - low - 1), 0, 0, 0),
        )

    return pl.pallas_call(
        functools.partial(widen_kernel, edges),
        grid=(edges[-1],),
        in_specs=[home(low, high) for low, high in zip(edges[:-1], edges[1:])],
        out_specs=[pl.BlockSpec((1, rows, width), lambda step: (step, 0, 0))] * 3,
        out_shape=[jax.ShapeDtypeStruct((edges[-1], rows, width), jnp.float32)] * 3,
    )(*packed)


def shifted_blocks(block, count):
    return [block] + [
        lax.ppermute(block, "tp", [(i, (i + shift) % count) for i in range(count)])
        for shift in range(1, count)
    ]


def shifted_scatter(partial_rows, count, me):
    rows = partial_rows.shape[0] // count
    total = lax.dynamic_slice_in_dim(partial_rows, me * rows, rows, 0).astype(jnp.float32)
    for shift in range(1, count):
        block = lax.dynamic_slice_in_dim(
            partial_rows, lax.rem(me + shift, count) * rows, rows, 0
        ).astype(jnp.bfloat16)
        got = lax.ppermute(block, "tp", [(i, (i + shift) % count) for i in range(count)])
        total = total + got.astype(jnp.float32)
    return total


RUNS = (0, 6, 10)
DIRECT = (2, 2)


def local(
    emb,
    segment_ids,
    routes,
    norm1_gain,
    w_query,
    w_key,
    w_value,
    w_out,
    norm2_gain,
    w_router,
    w_gate,
    w_up,
    w_down,
    cotangent,
):
    local_rows, _ = emb.shape
    tp_count, tp_index = lax.axis_size("tp"), lax.axis_index("tp")
    experts_here = w_gate.shape[0]
    expert_count = w_router.shape[1]
    q_width, kv_width = w_query.shape[1], w_key.shape[1]
    used = 2 * (q_width + kv_width)
    group_size = local_rows * tp_count
    fsdp_count = lax.axis_size("fsdp")
    split = group_size <= 1024
    runs = [edge * experts_here // RUNS[-1] for edge in RUNS] if split else [0, experts_here]
    stacks = (w_gate, w_up, w_down)
    pieces = [lax.all_gather(pack(stacks, 0, runs[1]), "fsdp", axis=2, tiled=True)]
    gain_one = norm1_gain.astype(jnp.float32)[None, :]
    gain_two = norm2_gain.astype(jnp.float32)[None, :]
    group_rows, mask, place_cols, place_rows, counts, attn_w, *packed = norm_gather(
        emb,
        gain_one,
        routes,
        join([w_query, w_key, w_value, w_out], w_router.T, used + 128),
        stacks,
        runs[1] if split else 0,
        tp_count,
        fsdp_count,
        0,
    )
    if split:
        pieces.append(lax.all_gather(packed[0], "fsdp", axis=2, tiled=True))
    late_grad, _ = lax.optimization_barrier((cotangent, counts))
    moe_grad = (resid_scale * late_grad.astype(jnp.float32)).astype(jnp.bfloat16)
    moe_grad_blocks = shifted_blocks(moe_grad, tp_count)
    capacity = group_size * routes.shape[1] // expert_count * 2
    meta = jnp.concatenate([counts[0], jnp.stack([tp_index * experts_here, tp_index])])

    tables = attend_tables()
    heads_here, kv_here = q_width // HEAD_DIM, kv_width // HEAD_DIM
    *kept, branch_part = attend(group_rows, attn_w, segment_ids, tables, heads_here, kv_here)
    mid_x, moe_rows, gate_rows, own_gates = find_mid(
        branch_part, emb, gain_two, attn_w, used, mask, tp_count, 1
    )

    outs = []
    for first, last, piece in zip(runs[:-1], runs[1:], pieces):
        outs.append(
            experts_step(
                meta,
                place_rows,
                place_cols,
                gate_rows,
                moe_rows,
                moe_grad_blocks,
                piece,
                first,
                last - first,
                0,
                capacity,
            )
        )
    grad_sums = [lax.psum_scatter(outs[0][2], "fsdp", scatter_dimension=2, tiled=True)]
    last_grads = outs[-1][2]
    picks = (tuple(range(DIRECT[0])), tuple(range(DIRECT[0], sum(DIRECT)))) if split else ((), ())
    y_part, mid_grad, gain_two_grad, sent, *mid_sums = find_mid_grad(
        [part[1] for part in outs],
        [part[0] for part in outs],
        mid_x,
        cotangent,
        own_gates,
        gain_two,
        attn_w,
        used,
        last_grads,
        picks[0],
        tp_count,
        fsdp_count,
        2,
    )
    moe_sum = shifted_scatter(y_part, tp_count, tp_index)
    out = (mid_x + resid_scale * moe_sum).astype(jnp.bfloat16)
    dx_one, attn_grads = attend_back(group_rows, attn_w, segment_ids, tables, kept, moe_rows, sent)
    grad_emb, attn_sum, gain_sums, *end_sums = finish(
        dx_one, attn_grads, emb, gain_one, mid_grad, gain_two_grad, last_grads, picks[1], 3
    )
    grad_sums = grad_sums + mid_sums + end_sums
    ends = [0]
    for part in grad_sums:
        ends.append(ends[-1] + part.shape[0])
    expert_sums = widen(grad_sums, ends)
    return (
        out,
        grad_emb,
        gain_sums[0],
        attn_sum[:, :q_width],
        attn_sum[:, q_width : q_width + kv_width],
        attn_sum[:, q_width + kv_width : q_width + 2 * kv_width],
        attn_sum[:, q_width + 2 * kv_width : used],
        gain_sums[1],
        attn_sum[:, used : used + expert_count],
        *expert_sums,
    )


def solution(mesh):
    return jax.shard_map(
        local,
        mesh=mesh,
        in_specs=(
            P(("fsdp", "tp"), None),
            P("fsdp", None),
            P("fsdp", None),
            P(),
            P("fsdp", "tp"),
            P("fsdp", "tp"),
            P("fsdp", "tp"),
            P("fsdp", "tp"),
            P(),
            P("fsdp", None),
            P("tp", "fsdp", None),
            P("tp", "fsdp", None),
            P("tp", "fsdp", None),
            P(("fsdp", "tp"), None),
        ),
        out_specs=(
            P(("fsdp", "tp"), None),
            P(("fsdp", "tp"), None),
            P(),
            P("fsdp", "tp"),
            P("fsdp", "tp"),
            P("fsdp", "tp"),
            P("fsdp", "tp"),
            P(),
            P("fsdp", None),
            P("tp", "fsdp", None),
            P("tp", "fsdp", None),
            P("tp", "fsdp", None),
        ),
        check_vma=False,
    )
```

```python
import functools

import jax
import jax.numpy as jnp
import numpy as np
from jax import lax
from jax.experimental import pallas as pl
from jax.experimental.pallas import tpu as pltpu
from jax.sharding import PartitionSpec as P

HEAD_DIM = 64
SEQ = 512


emb_scale = 12.0
resid_scale = 0.22
attn_scale = 0.015625
norm_eps = 1e-06
rope_base = 10000.0
masked_value = -1e30


def contract_last(left_op, right_op):
    return lax.dot_general(
        left_op, right_op, (((1,), (1,)), ((), ())), preferred_element_type=jnp.float32
    )


def contract_first(left_op, right_op):
    return lax.dot_general(
        left_op, right_op, (((0,), (0,)), ((), ())), preferred_element_type=jnp.float32
    )


def line_signal(barrier, me, count):
    @pl.when(me > 0)
    def _():
        pl.semaphore_signal(barrier, inc=1, device_id={"tp": me - 1})

    @pl.when(me < count - 1)
    def _():
        pl.semaphore_signal(barrier, inc=1, device_id={"tp": me + 1})

    return jnp.where((me > 0) & (me < count - 1), 2, 1)


class Plane:
    def __init__(self, count):
        self.me = lax.axis_index("fsdp")
        self.core = lax.rem(self.me, 2)
        self.chip = lax.div(self.me, 2)
        self.chips = count // 2
        self.partner = self.me + 1 - 2 * self.core

    def chip_at(self, shift):
        return lax.rem(self.chip + shift + self.chips, self.chips)

    def peer(self, shift):
        return self.chip_at(shift) * 2 + self.core

    def signal(self, barrier):
        for shift in range(1, self.chips):
            pl.semaphore_signal(barrier, inc=1, device_id={"fsdp": self.peer(shift)})
        pl.semaphore_signal(barrier, inc=1, device_id={"fsdp": self.partner})
        return self.chips


def rows_of(ref, index, rows):
    return ref.at[pl.ds(pl.multiple_of(index * rows, rows), rows)]


class LineGather:
    def __init__(self, count, o_ref, send_sem, recv_sem):
        self.count, self.o_ref = count, o_ref
        self.send_sem, self.recv_sem = send_sem, recv_sem
        self.rows = o_ref.shape[0] // count
        me = self.me = lax.axis_index("tp")
        steps = range(count - 1)
        self.sends = [
            [(me >= step) & (me < count - 1) for step in steps],
            [(me + step < count) & (me > 0) for step in steps],
        ]
        self.gets = [
            [me - 1 - step >= 0 for step in steps],
            [me + 1 + step < count for step in steps],
        ]

    def hop(self, way, step, chunk):
        part = rows_of(self.o_ref, chunk, self.rows)
        return pltpu.make_async_remote_copy(
            src_ref=part,
            dst_ref=part,
            send_sem=self.send_sem.at[way, step],
            recv_sem=self.recv_sem.at[way, step],
            device_id={"tp": self.me + 1 if way == 0 else self.me - 1},
        )

    def start(self, step):
        @pl.when(self.sends[0][step])
        def _():
            self.hop(0, step, self.me - step).start()

        @pl.when(self.sends[1][step])
        def _():
            self.hop(1, step, self.me + step).start()

    def arrive(self, step):
        @pl.when(self.gets[0][step])
        def _():
            self.hop(0, step, self.me - 1 - step).wait_recv()

        @pl.when(self.gets[1][step])
        def _():
            self.hop(1, step, self.me + 1 + step).wait_recv()

    def finish(self):
        for step in range(self.count - 1):

            @pl.when(self.sends[0][step])
            def _():
                self.hop(0, step, self.me - step).wait_send()

            @pl.when(self.sends[1][step])
            def _():
                self.hop(1, step, self.me + step).wait_send()


def line_sems(count):
    return [
        pltpu.SemaphoreType.DMA((2, count - 1)),
        pltpu.SemaphoreType.DMA((2, count - 1)),
    ]


class PlaneGather:
    def __init__(self, plane, w_ref, wo_ref, out_send, out_recv, on_send, on_recv, kept_sem):
        self.plane, self.w_ref, self.wo_ref = plane, w_ref, wo_ref
        self.out_send, self.out_recv = out_send, out_recv
        self.on_send, self.on_recv = on_send, on_recv
        self.rows = w_ref.shape[0]
        self.kept = pltpu.make_async_copy(w_ref, rows_of(wo_ref, plane.me, self.rows), kept_sem)

    def outward(self, shift, target, source_device):
        return pltpu.make_async_remote_copy(
            src_ref=self.w_ref,
            dst_ref=rows_of(self.wo_ref, source_device, self.rows),
            send_sem=self.out_send.at[shift],
            recv_sem=self.out_recv.at[shift],
            device_id={"fsdp": target},
        )

    def onward(self, shift, source_device):
        part = rows_of(self.wo_ref, source_device, self.rows)
        return pltpu.make_async_remote_copy(
            src_ref=part,
            dst_ref=part,
            send_sem=self.on_send.at[shift - 1],
            recv_sem=self.on_recv.at[shift - 1],
            device_id={"fsdp": self.plane.partner},
        )

    def start(self):
        plane = self.plane
        for shift in range(1, plane.chips):
            self.outward(shift, plane.peer(shift), plane.me).start()
        self.outward(0, plane.partner, plane.me).start()
        self.kept.start()

    def forward(self):
        plane = self.plane
        for shift in range(1, plane.chips):
            self.outward(shift, plane.peer(shift), plane.peer(-shift)).wait_recv()
            self.onward(shift, plane.peer(-shift)).start()

    def finish(self):
        plane = self.plane
        self.outward(0, plane.partner, plane.partner).wait_recv()
        for shift in range(1, plane.chips):
            self.onward(shift, plane.chip_at(-shift) * 2 + 1 - plane.core).wait_recv()
        for shift in range(1, plane.chips):
            self.outward(shift, plane.peer(shift), plane.me).wait_send()
            self.onward(shift, plane.peer(-shift)).wait_send()
        self.outward(0, plane.partner, plane.me).wait_send()
        self.kept.wait()


class ExpertSums:
    def __init__(self, plane, picks, grads_ref, out_ref, *refs):
        self.plane, self.picks, self.grads_ref, self.out_ref = plane, picks, grads_ref, out_ref
        (
            self.got, self.own, self.chip_got, self.held,
            self.pair_send, self.pair_recv, self.own_sem,
            self.chip_send, self.chip_recv, self.put_sem,
        ) = refs
        self.rows = out_ref.shape[2]

    def area(self, index, dest):
        low = pl.multiple_of(dest * self.rows, self.rows)
        return self.grads_ref.at[self.picks[index], :, pl.ds(low, self.rows)]

    def to_pair(self, index, shift):
        plane = self.plane
        return pltpu.make_async_remote_copy(
            src_ref=self.area(index, plane.chip_at(shift) * 2 + 1 - plane.core),
            dst_ref=self.got.at[index, shift],
            send_sem=self.pair_send.at[index, shift],
            recv_sem=self.pair_recv.at[index, shift],
            device_id={"fsdp": plane.partner},
        )

    def keep(self, index, shift):
        return pltpu.make_async_copy(
            self.area(index, self.plane.peer(shift)),
            self.own.at[index, shift],
            self.own_sem.at[index, shift],
        )

    def to_chip(self, index, shift):
        return pltpu.make_async_remote_copy(
            src_ref=self.own.at[index, shift],
            dst_ref=self.chip_got.at[index, shift - 1],
            send_sem=self.chip_send.at[index, shift - 1],
            recv_sem=self.chip_recv.at[index, shift - 1],
            device_id={"fsdp": self.plane.peer(shift)},
        )

    def put(self, index):
        return pltpu.make_async_copy(
            self.held.at[index], self.out_ref.at[index], self.put_sem.at[index]
        )

    def order(self):
        return list(range(1, self.plane.chips)) + [0]

    def begin(self, index):
        for shift in self.order():
            self.to_pair(index, shift).start()
            self.keep(index, shift).start()

    def pass_on(self, index):
        for shift in self.order():
            self.to_pair(index, shift).wait_recv()
            self.keep(index, shift).wait()
            for slot in range(self.own.shape[2]):
                both = self.own[index, shift, slot].astype(jnp.float32) + self.got[
                    index, shift, slot
                ].astype(jnp.float32)
                self.own[index, shift, slot] = both.astype(jnp.bfloat16)
            if shift > 0:
                self.to_chip(index, shift).start()

    def collect(self, index):
        chips = self.plane.chips
        for shift in range(1, chips):
            self.to_chip(index, shift).wait_recv()
        for slot in range(self.own.shape[2]):
            total = self.own[index, 0, slot].astype(jnp.float32)
            for shift in range(1, chips):
                total = total + self.chip_got[index, shift - 1, slot].astype(jnp.float32)
            self.held[index, slot] = total.astype(jnp.bfloat16)
        self.put(index).start()

    def finish(self):
        for index in range(len(self.picks)):
            self.put(index).wait()
            for shift in self.order():
                self.to_pair(index, shift).wait_send()
                if shift > 0:
                    self.to_chip(index, shift).wait_send()


def expert_buffers(count, chips, rows, width):
    if count == 0:
        return []
    return [
        pltpu.VMEM((count, chips, 3, rows, width), jnp.bfloat16),
        pltpu.VMEM((count, chips, 3, rows, width), jnp.bfloat16),
        pltpu.VMEM((count, chips - 1, 3, rows, width), jnp.bfloat16),
        pltpu.VMEM((count, 3, rows, width), jnp.bfloat16),
        pltpu.SemaphoreType.DMA((count, chips)),
        pltpu.SemaphoreType.DMA((count, chips)),
        pltpu.SemaphoreType.DMA((count, chips)),
        pltpu.SemaphoreType.DMA((count, chips - 1)),
        pltpu.SemaphoreType.DMA((count, chips - 1)),
        pltpu.SemaphoreType.DMA((count,)),
    ]


class LineScatter:
    def __init__(self, count, x_refs, o_ref, recv, send_sem, recv_sem):
        self.count, self.x_refs, self.o_ref, self.recv = count, x_refs, o_ref, recv
        self.send_sem, self.recv_sem = send_sem, recv_sem
        self.rows = o_ref.shape[0]
        me = self.me = lax.axis_index("tp")
        self.behind = (me, count - 1 - me)
        self.has_next = (me < count - 1, me > 0)
        self.has_prev = (me > 0, me < count - 1)

    def block(self, dest):
        area = pl.ds(pl.multiple_of(dest * self.rows, self.rows), self.rows)
        total = self.x_refs[0][area, :].astype(jnp.float32)
        for x_ref in self.x_refs[1:]:
            total = total + x_ref[area, :].astype(jnp.float32)
        return total

    def hop(self, way, step, source):
        return pltpu.make_async_remote_copy(
            src_ref=source,
            dst_ref=self.recv.at[way, step],
            send_sem=self.send_sem.at[way, step],
            recv_sem=self.recv_sem.at[way, step],
            device_id={"tp": self.me + 1 if way == 0 else self.me - 1},
        )

    def start(self, step):
        count, me, recv = self.count, self.me, self.recv
        for way in range(2):
            dest = count - 1 - step + me if way == 0 else step - (count - 1 - me)
            active = self.has_next[way] & (step >= self.behind[way])

            @pl.when(active & (self.behind[way] == 0))
            def _():
                part = rows_of(self.x_refs[0], dest, self.rows)
                if len(self.x_refs) > 1:
                    part[...] = self.block(dest).astype(part.dtype)
                self.hop(way, step, part).start()

            if step > 0:

                @pl.when(active & (self.behind[way] > 0))
                def _():
                    total = self.block(dest) + recv[way, step - 1].astype(jnp.float32)
                    recv[way, step - 1] = total.astype(recv.dtype)
                    self.hop(way, step, recv.at[way, step - 1]).start()

    def arrive(self, step):
        for way in range(2):

            @pl.when(self.has_prev[way] & (step >= self.behind[way] - 1))
            def _():
                self.hop(way, step, self.recv.at[way, step]).wait_recv()

    def collect(self):
        self.o_ref[...] = self.block(self.me)
        for way in range(2):

            @pl.when(self.has_prev[way])
            def _():
                self.o_ref[...] += self.recv[way, self.count - 2].astype(jnp.float32)

    def finish(self):
        for step in range(self.count - 1):
            for way in range(2):

                @pl.when(self.has_next[way] & (step >= self.behind[way]))
                def _():
                    self.hop(way, step, self.recv.at[way, step]).wait_send()


def line_buffers(count, rows, width):
    return [pltpu.VMEM((2, count - 1, rows, width), jnp.bfloat16)] + line_sems(count)


def own_rows(ref, rows):
    return pl.ds(pl.multiple_of(lax.axis_index("tp") * rows, rows), rows)


def inverse_norm(values):
    return lax.rsqrt(jnp.mean(values * values, axis=-1, keepdims=True) + norm_eps)


def rms_back(incoming, values, gain_row):
    inverse = inverse_norm(values)
    scaled = values * inverse
    gain_grad = jnp.sum(incoming * scaled, axis=0, keepdims=True)
    weighted = incoming * gain_row
    row_inner = jnp.mean(weighted * scaled, axis=-1, keepdims=True)
    return inverse * (weighted - scaled * row_inner), gain_grad


def enter_kernel(count, plane=None):
    barrier = pltpu.get_barrier_semaphore()
    waits = line_signal(barrier, lax.axis_index("tp"), count)
    if plane is not None:
        waits = waits + plane.signal(barrier)
    pl.semaphore_wait(barrier, waits)


def remote_params(ident, limit=60):
    return pltpu.CompilerParams(
        collective_id=ident, has_side_effects=True, vmem_limit_bytes=limit << 20
    )


IN_VMEM = pl.BlockSpec(memory_space=pltpu.VMEM)
IN_PLACE = pl.BlockSpec(memory_space=pl.ANY)
TRANSFER = pl.CostEstimate(flops=0, transcendentals=0, bytes_accessed=150_000_000)


def norm_gather_kernel(count, fsdp_count, low, *refs):
    emb_ref, gain_ref, routes_ref, w_ref, *refs = refs
    stacks, refs = (refs[:3], refs[3:]) if low else ((), refs)
    rows_ref, mask_ref, cols_ref, turned_ref, counts_ref, wo_ref, *refs = refs
    packed, refs = (refs[0], refs[1:]) if low else (None, refs)
    row_send, row_recv, *refs = refs
    plane = Plane(fsdp_count)
    if low:
        held, in_sem, out_sem = refs[5:]
        gets, puts = pack_copies(low, stacks, packed, held, in_sem, out_sem)
        for get in gets:
            get.start()
    enter_kernel(count, plane)
    line = LineGather(count, rows_ref, row_send, row_recv)
    weights = PlaneGather(plane, w_ref, wo_ref, *refs[:5])
    start_x = emb_ref[...].astype(jnp.float32) * emb_scale
    normed = start_x * inverse_norm(start_x) * gain_ref[...]
    rows_ref[own_rows(rows_ref, line.rows), :] = normed.astype(jnp.bfloat16)
    for step in range(count - 1):
        line.start(step)
        if step == 0:
            weights.start()
            place_routes(line.rows, routes_ref, mask_ref, cols_ref, turned_ref, counts_ref)
            if low:
                for get, put in zip(gets, puts):
                    get.wait()
                    put.start()
        if step == count - 2:
            weights.forward()
        line.arrive(step)
    if low:
        for put in puts:
            put.wait()
    weights.finish()
    line.finish()


def place_routes(rows, routes_ref, mask_ref, cols_ref, turned_ref, counts_ref):
    group, lanes = mask_ref.shape
    columns = lax.broadcasted_iota(jnp.int32, (rows, lanes), 1)
    for low in range(0, group, rows):
        area = slice(low, low + rows)
        mask = jnp.zeros((rows, lanes), jnp.float32)
        for choice in range(routes_ref.shape[1]):
            mask = jnp.where(routes_ref[area, choice : choice + 1] == columns, 1.0, mask)
        mask_ref[area, :] = mask
    counts_ref[...] = jnp.sum(mask_ref[...], axis=0, keepdims=True).astype(jnp.int32)
    member = mask_ref[...].astype(jnp.bfloat16)
    for low in range(0, group, rows):
        area = slice(low, low + rows)
        here = lax.broadcasted_iota(jnp.int32, (rows, group), 0) + low
        earlier = here > lax.broadcasted_iota(jnp.int32, (rows, group), 1)
        ranks = jnp.dot(
            jnp.where(earlier, 1.0, 0.0).astype(jnp.bfloat16),
            member,
            preferred_element_type=jnp.float32,
        )
        places = jnp.where(mask_ref[area, :] > 0.0, ranks, -1.0)
        cols_ref[area, :] = places.astype(jnp.int32)
        turned_ref[:, area] = places.T.astype(jnp.int32)


def norm_gather(emb, gain_row, routes, weights, stacks, low, count, fsdp_count, ident):
    rows, width = emb.shape
    group = rows * count
    chips = fsdp_count // 2
    experts, share, hidden = stacks[0].shape
    span = experts - low
    outs = [
        jax.ShapeDtypeStruct((group, width), jnp.bfloat16),
        jax.ShapeDtypeStruct((group, 128), jnp.float32),
        jax.ShapeDtypeStruct((group, 128), jnp.int32),
        jax.ShapeDtypeStruct((128, group), jnp.int32),
        jax.ShapeDtypeStruct((1, 128), jnp.int32),
        jax.ShapeDtypeStruct((weights.shape[0] * fsdp_count, weights.shape[1]), jnp.bfloat16),
    ]
    scratch = line_sems(count) + [
        pltpu.SemaphoreType.DMA((chips,)),
        pltpu.SemaphoreType.DMA((chips,)),
        pltpu.SemaphoreType.DMA((chips - 1,)),
        pltpu.SemaphoreType.DMA((chips - 1,)),
        pltpu.SemaphoreType.DMA,
    ]
    if low:
        outs.append(jax.ShapeDtypeStruct((span, 3, share, hidden), jnp.bfloat16))
        scratch += [
            pltpu.VMEM((3, span, share, hidden), jnp.bfloat16),
            pltpu.SemaphoreType.DMA((3,)),
            pltpu.SemaphoreType.DMA((3,)),
        ]
    return pl.pallas_call(
        functools.partial(norm_gather_kernel, count, fsdp_count, low),
        out_shape=outs,
        in_specs=[IN_VMEM] * 4 + [IN_PLACE] * (3 if low else 0),
        out_specs=[IN_VMEM] * 5 + [IN_PLACE] * (len(outs) - 5),
        scratch_shapes=scratch,
        compiler_params=remote_params(ident, 48),
        cost_estimate=TRANSFER,
    )(emb, gain_row, routes, weights, *(stacks if low else ()))


def mid_kernel(
    count, part_ref, emb_ref, gain_ref, router_ref, mask_ref, cotangent_ref,
    mid_ref, rows_ref, gates_ref, own_gates, moe_grads,
    recv, sum_send, sum_recv, row_send, row_recv, grad_send, grad_recv,
):
    enter_kernel(count)
    total = LineScatter(count, [part_ref], mid_ref, recv, sum_send, sum_recv)
    line = LineGather(count, rows_ref, row_send, row_recv)
    others = LineGather(count, moe_grads, grad_send, grad_recv)
    rows = line.rows
    moe_grads[own_rows(moe_grads, rows), :] = (
        resid_scale * cotangent_ref[...].astype(jnp.float32)
    ).astype(jnp.bfloat16)
    for step in range(count - 1):
        total.start(step)
        others.start(step)
        total.arrive(step)
        others.arrive(step)
    total.collect()
    mid = emb_ref[...].astype(jnp.float32) * emb_scale + resid_scale * mid_ref[...]
    mid_ref[...] = mid
    own = own_rows(rows_ref, rows)
    rows_ref[own, :] = (mid * inverse_norm(mid) * gain_ref[...]).astype(jnp.bfloat16)

    def find_gates(chunk):
        area = pl.ds(pl.multiple_of(chunk * rows, rows), rows)
        logits = jnp.dot(rows_ref[area, :], router_ref[...], preferred_element_type=jnp.float32)
        inside = mask_ref[area, :] > 0.0
        top = jnp.max(jnp.where(inside, logits, masked_value), axis=-1, keepdims=True)
        raised = jnp.where(inside, jnp.exp(jnp.where(inside, logits - top, 0.0)), 0.0)
        gates = raised / jnp.sum(raised, axis=-1, keepdims=True)
        gates_ref[:, area] = gates.T
        return gates

    for step in range(count - 1):
        line.start(step)
        if step == 0:
            own_gates[...] = find_gates(line.me)
        line.arrive(step)

        @pl.when(line.gets[0][step])
        def _():
            find_gates(line.me - 1 - step)

        @pl.when(line.gets[1][step])
        def _():
            find_gates(line.me + 1 + step)

    line.finish()
    total.finish()
    others.finish()


def find_mid(part, emb, gain_row, weights, used, mask, cotangent, count, ident):
    rows, width = emb.shape
    group = rows * count
    return pl.pallas_call(
        functools.partial(mid_kernel, count),
        grid=(1,),
        out_shape=[
            jax.ShapeDtypeStruct((rows, width), jnp.float32),
            jax.ShapeDtypeStruct((group, width), jnp.bfloat16),
            jax.ShapeDtypeStruct((128, group), jnp.float32),
            jax.ShapeDtypeStruct((rows, 128), jnp.float32),
            jax.ShapeDtypeStruct((group, width), jnp.bfloat16),
        ],
        in_specs=[
            IN_VMEM,
            IN_VMEM,
            IN_VMEM,
            pl.BlockSpec((width, 128), lambda step: (0, used // 128)),
            IN_VMEM,
            IN_VMEM,
        ],
        out_specs=[IN_VMEM] * 5,
        scratch_shapes=line_buffers(count, rows, width) + line_sems(count) + line_sems(count),
        compiler_params=remote_params(ident),
        cost_estimate=TRANSFER,
    )(part, emb, gain_row, weights, mask, cotangent)


def moe_back_kernel(count, fsdp_count, runs, picks, *refs):
    dx_refs, y_refs, refs = refs[:runs], refs[runs : 2 * runs], refs[2 * runs :]
    mid_ref, cotangent_ref, own_gates, gain_ref, router_ref, *refs = refs
    grads_ref, refs = (refs[0], refs[1:]) if picks else (None, refs)
    out_ref, mid_grad, gain_grad, sent_ref, *refs = refs
    sums_ref, refs = (refs[0], refs[1:]) if picks else (None, refs)
    (
        dx_parts, y_parts, load_sem, sum_ref, moe_ref,
        recv, sum_send, sum_recv, moe_recv, moe_send, moe_recv_sem, row_send, row_recv, *refs,
    ) = refs
    loads = []
    for index, (source, parts) in enumerate(
        [(ref, dx_parts) for ref in dx_refs] + [(ref, y_parts) for ref in y_refs]
    ):
        loads.append(
            pltpu.make_async_copy(source, parts.at[index % runs], load_sem.at[index])
        )
        loads[-1].start()
    plane = Plane(fsdp_count) if picks else None
    enter_kernel(count, plane)
    total = LineScatter(
        count, [dx_parts.at[run] for run in range(runs)], sum_ref, recv, sum_send, sum_recv
    )
    moe = LineScatter(
        count, [y_parts.at[run] for run in range(runs)], moe_ref, moe_recv, moe_send, moe_recv_sem
    )
    line = LineGather(count, sent_ref, row_send, row_recv)
    experts = ExpertSums(plane, picks, grads_ref, sums_ref, *refs) if picks else None
    rows, width = mid_ref.shape
    for index in range(len(picks)):
        experts.begin(index)
    for load in loads[:runs]:
        load.wait()
    for step in range(count - 1):
        total.start(step)
        if step < len(picks):
            experts.pass_on(step)
        total.arrive(step)
    total.collect()
    gates = own_gates[...]
    gates_grad = sum_ref[:, width:]
    gates_inner = jnp.sum(gates * gates_grad, axis=-1, keepdims=True)
    logits_grad = (gates * (gates_grad - gates_inner)).astype(jnp.bfloat16)
    incoming = sum_ref[:, :width] + contract_last(logits_grad, router_ref[...])
    from_norm, gain_part = rms_back(incoming, mid_ref[...], gain_ref[...])
    grad = cotangent_ref[...].astype(jnp.float32) + from_norm
    mid_grad[...] = grad
    gain_grad[...] = gain_part
    own = own_rows(sent_ref, rows)
    sent_ref[own, :width] = (resid_scale * grad).astype(jnp.bfloat16)
    sent_ref[own, width:] = logits_grad
    for load in loads[runs:]:
        load.wait()
    for step in range(count - 1):
        line.start(step)
        moe.start(step)
        if 0 < step <= len(picks):
            experts.collect(step - 1)
        moe.arrive(step)
        line.arrive(step)
    moe.collect()
    out_ref[...] = (mid_ref[...] + resid_scale * moe_ref[...]).astype(out_ref.dtype)
    for index in range(count - 2, len(picks)):
        experts.collect(index)
    line.finish()
    total.finish()
    moe.finish()
    if picks:
        experts.finish()


def find_mid_grad(
    dx_parts, y_parts, mid, cotangent, own_gates, gain_row, weights, used, grads, picks,
    count, fsdp_count, ident,
):
    rows, width = mid.shape
    runs, group = len(dx_parts), rows * count
    wide = dx_parts[0].shape[1]
    share = grads.shape[2] // fsdp_count
    sums = [jax.ShapeDtypeStruct((len(picks), 3, share, grads.shape[3]), jnp.bfloat16)]
    sums = sums if picks else []
    return pl.pallas_call(
        functools.partial(moe_back_kernel, count, fsdp_count, runs, picks),
        grid=(1,),
        out_shape=[
            jax.ShapeDtypeStruct((rows, width), jnp.bfloat16),
            jax.ShapeDtypeStruct((rows, width), jnp.float32),
            jax.ShapeDtypeStruct((1, width), jnp.float32),
            jax.ShapeDtypeStruct((group, wide), jnp.bfloat16),
        ]
        + sums,
        in_specs=[IN_PLACE] * (2 * runs)
        + [IN_VMEM] * 4
        + [pl.BlockSpec((width, 128), lambda step: (0, used // 128))]
        + [IN_PLACE] * len(sums),
        out_specs=[IN_VMEM] * 4 + [IN_PLACE] * len(sums),
        scratch_shapes=[
            pltpu.VMEM((runs, group, wide), jnp.bfloat16),
            pltpu.VMEM((runs, group, width), jnp.bfloat16),
            pltpu.SemaphoreType.DMA((2 * runs,)),
            pltpu.VMEM((rows, wide), jnp.float32),
            pltpu.VMEM((rows, width), jnp.float32),
        ]
        + line_buffers(count, rows, wide)
        + line_buffers(count, rows, width)
        + line_sems(count)
        + expert_buffers(len(picks), fsdp_count // 2, share, grads.shape[3]),
        compiler_params=remote_params(ident, 63),
        cost_estimate=TRANSFER,
    )(*dx_parts, *y_parts, mid, cotangent, own_gates, gain_row, weights, *([grads] if picks else []))


def finish_kernel(tp_count, fsdp_count, picks, *refs):
    x_ref, w_ref, emb_ref, gain_ref, mid_grad, gain_two, *refs = refs
    grads_ref, refs = (refs[0], refs[1:]) if picks else (None, refs)
    grad_ref, w_sum, gains_ref, *refs = refs
    sums_ref, refs = (refs[0], refs[1:]) if picks else (None, refs)
    (
        line_recv, line_send_sem, line_recv_sem,
        pair_got, chip_sums, chip_got, pair_send, pair_recv, chip_send, chip_recv,
        tp_got, fsdp_got, small_send, small_recv, *refs,
    ) = refs
    plane = Plane(fsdp_count)
    tp_me, fsdp_me = lax.axis_index("tp"), plane.me
    barrier = pltpu.get_barrier_semaphore()
    for shift in range(1, tp_count):
        pl.semaphore_signal(barrier, inc=1, device_id={"tp": lax.rem(tp_me + shift, tp_count)})
    for shift in range(1, fsdp_count):
        pl.semaphore_signal(
            barrier, inc=1, device_id={"fsdp": lax.rem(fsdp_me + shift, fsdp_count)}
        )
    pl.semaphore_wait(barrier, tp_count + fsdp_count - 2)
    line = LineScatter(
        tp_count, [x_ref], grad_ref, line_recv, line_send_sem, line_recv_sem
    )
    rows = w_sum.shape[0]

    def to_pair(shift):
        return pltpu.make_async_remote_copy(
            src_ref=rows_of(w_ref, plane.chip_at(shift) * 2 + 1 - plane.core, rows),
            dst_ref=pair_got.at[shift],
            send_sem=pair_send.at[shift],
            recv_sem=pair_recv.at[shift],
            device_id={"fsdp": plane.partner},
        )

    def to_chip(shift):
        return pltpu.make_async_remote_copy(
            src_ref=chip_sums.at[shift - 1],
            dst_ref=chip_got.at[shift - 1],
            send_sem=chip_send.at[shift - 1],
            recv_sem=chip_recv.at[shift - 1],
            device_id={"fsdp": plane.peer(shift)},
        )

    def both_cores(shift):
        own = pl.ds(pl.multiple_of(plane.peer(shift) * rows, rows), rows)
        return w_ref[own, :].astype(jnp.float32) + pair_got[shift].astype(jnp.float32)

    def exchange(axis, me, count, got, base):
        copies = []
        for shift in range(1, count):
            copies.append(
                pltpu.make_async_remote_copy(
                    src_ref=gains_ref,
                    dst_ref=got.at[me],
                    send_sem=small_send.at[base + shift],
                    recv_sem=small_recv.at[base + shift],
                    device_id={axis: lax.rem(me + shift, count)},
                )
            )
            copies[-1].start()
        got[me] = gains_ref[...]
        for copy in copies:
            copy.wait()
        total = got[0]
        for index in range(1, count):
            total = total + got[index]
        return total

    experts = ExpertSums(plane, picks, grads_ref, sums_ref, *refs) if picks else None
    line.start(0)
    order = list(range(1, plane.chips)) + [0]
    for shift in order:
        to_pair(shift).start()
    for index in range(len(picks)):
        experts.begin(index)
    for shift in order:
        to_pair(shift).wait_recv()
        if shift > 0:
            chip_sums[shift - 1] = both_cores(shift).astype(chip_sums.dtype)
            to_chip(shift).start()
    for index in range(len(picks)):
        experts.pass_on(index)
    line.arrive(0)
    for step in range(1, tp_count - 1):
        line.start(step)
        line.arrive(step)
    line.collect()
    from_norm, gain_one = rms_back(
        grad_ref[...], emb_ref[...].astype(jnp.float32) * emb_scale, gain_ref[...]
    )
    gains_ref[...] = jnp.zeros_like(gains_ref)
    gains_ref[0:1, :] = gain_one
    gains_ref[1:2, :] = gain_two[...]
    grad_ref[...] = emb_scale * (mid_grad[...] + from_norm)
    total = both_cores(0)
    for shift in range(1, plane.chips):
        to_chip(shift).wait_recv()
        total = total + chip_got[shift - 1].astype(jnp.float32)
    w_sum[...] = total
    for index in range(len(picks)):
        experts.collect(index)
    gains_ref[...] = exchange("tp", tp_me, tp_count, tp_got, 0)
    gains_ref[...] = exchange("fsdp", fsdp_me, fsdp_count, fsdp_got, tp_count)
    line.finish()
    for shift in order:
        to_pair(shift).wait_send()
        if shift > 0:
            to_chip(shift).wait_send()
    if picks:
        experts.finish()


def finish(dx_rows, weight_grads, emb, gain_row, mid_grad, gain_two, grads, picks, ident):
    tp_count, fsdp_count = lax.axis_size("tp"), lax.axis_size("fsdp")
    rows, width = emb.shape
    w_rows, w_width = weight_grads.shape[0] // fsdp_count, weight_grads.shape[1]
    chips = fsdp_count // 2
    share = grads.shape[2] // fsdp_count
    sums = [jax.ShapeDtypeStruct((len(picks), 3, share, grads.shape[3]), jnp.bfloat16)]
    sums = sums if picks else []
    return pl.pallas_call(
        functools.partial(finish_kernel, tp_count, fsdp_count, picks),
        out_shape=[
            jax.ShapeDtypeStruct((rows, width), jnp.float32),
            jax.ShapeDtypeStruct((w_rows, w_width), jnp.float32),
            jax.ShapeDtypeStruct((8, width), jnp.float32),
            *sums,
        ],
        in_specs=[IN_VMEM] * 6 + [IN_PLACE] * len(sums),
        out_specs=[IN_VMEM] * 3 + [IN_PLACE] * len(sums),
        scratch_shapes=line_buffers(tp_count, rows, width)
        + [
            pltpu.VMEM((chips, w_rows, w_width), jnp.bfloat16),
            pltpu.VMEM((chips - 1, w_rows, w_width), jnp.bfloat16),
            pltpu.VMEM((chips - 1, w_rows, w_width), jnp.bfloat16),
            pltpu.SemaphoreType.DMA((chips,)),
            pltpu.SemaphoreType.DMA((chips,)),
            pltpu.SemaphoreType.DMA((chips - 1,)),
            pltpu.SemaphoreType.DMA((chips - 1,)),
            pltpu.VMEM((tp_count, 8, width), jnp.float32),
            pltpu.VMEM((fsdp_count, 8, width), jnp.float32),
            pltpu.SemaphoreType.DMA((tp_count + fsdp_count,)),
            pltpu.SemaphoreType.DMA((tp_count + fsdp_count,)),
        ]
        + expert_buffers(len(picks), chips, share, grads.shape[3]),
        compiler_params=remote_params(ident),
        cost_estimate=TRANSFER,
    )(dx_rows, weight_grads, emb, gain_row, mid_grad, gain_two, *([grads] if picks else []))


def pack_copies(low, sources, target, held, in_sem, out_sem):
    span = target.shape[0]
    gets = [
        pltpu.make_async_copy(source.at[pl.ds(low, span)], held.at[slot], in_sem.at[slot])
        for slot, source in enumerate(sources)
    ]
    puts = [
        pltpu.make_async_copy(held.at[slot], target.at[:, slot], out_sem.at[slot])
        for slot in range(len(sources))
    ]
    return gets, puts


def pack_kernel(low, *refs):
    sources, target, held, in_sem, out_sem = refs[:-4], *refs[-4:]
    gets, puts = pack_copies(low, sources, target, held, in_sem, out_sem)
    for get in gets:
        get.start()
    for get, put in zip(gets, puts):
        get.wait()
        put.start()
    for put in puts:
        put.wait()


def pack(stacks, low, high):
    _, rows, width = stacks[0].shape
    count, span = len(stacks), high - low
    return pl.pallas_call(
        functools.partial(pack_kernel, low),
        in_specs=[IN_PLACE] * count,
        out_specs=IN_PLACE,
        out_shape=jax.ShapeDtypeStruct((span, count, rows, width), jnp.bfloat16),
        scratch_shapes=[
            pltpu.VMEM((count, span, rows, width), jnp.bfloat16),
            pltpu.SemaphoreType.DMA((count,)),
            pltpu.SemaphoreType.DMA((count,)),
        ],
    )(*stacks)


def join_kernel(*refs):
    *sources, last, target = refs
    low = 0
    for source in sources:
        target[:, low : low + source.shape[1]] = source[...]
        low += source.shape[1]
    router = last[...].astype(jnp.float32).T.astype(jnp.bfloat16)
    target[:, low:] = jnp.zeros((target.shape[0], target.shape[1] - low), jnp.bfloat16)
    target[:, low : low + router.shape[1]] = router


def join(parts, last_turned, width):
    return pl.pallas_call(
        join_kernel,
        in_specs=[IN_VMEM] * (len(parts) + 1),
        out_specs=IN_VMEM,
        out_shape=jax.ShapeDtypeStruct((parts[0].shape[0], width), jnp.bfloat16),
    )(*parts, last_turned)


SLOTS = 256


def experts_kernel(
    first_expert,
    capacity,
    meta,
    place_rows,
    place_cols,
    gate_rows,
    x_ref,
    g_ref,
    weights,
    y_ref,
    dx_ref,
    grads,
):
    step = pl.program_id(0)
    expert = step + first_expert
    group, width = x_ref.shape
    tail = dx_ref.shape[1] - width

    @pl.when(step == 0)
    def _():
        y_ref[...] = jnp.zeros_like(y_ref)
        dx_ref[...] = jnp.zeros_like(dx_ref)

    column = expert + meta[meta.shape[0] - 1]
    lanes = lax.broadcasted_iota(jnp.int32, place_cols.shape, 1)
    place_col = jnp.sum(jnp.where(lanes == column, place_cols[...], 0), axis=1, keepdims=True)
    place_row = place_rows[pl.ds(column, 1), :]
    gate_row = gate_rows[pl.ds(column, 1), :].astype(jnp.bfloat16).astype(jnp.float32)
    mark = jnp.where(lax.broadcasted_iota(jnp.int32, (1, tail), 1) == column, 1.0, 0.0)

    def run(base, span):
        slots = lax.broadcasted_iota(jnp.int32, (span, group), 0) + base
        hit = slots == place_row
        pick = jnp.where(hit, 1.0, 0.0).astype(jnp.bfloat16)
        scale = jnp.sum(jnp.where(hit, gate_row, 0.0), axis=1, keepdims=True)
        x_taken = jnp.dot(pick, x_ref[...], preferred_element_type=jnp.float32).astype(jnp.bfloat16)
        g_taken = jnp.dot(pick, g_ref[...], preferred_element_type=jnp.float32).astype(jnp.bfloat16)
        gate_pre = jnp.dot(x_taken, weights[0, 0], preferred_element_type=jnp.float32)
        up_pre = jnp.dot(x_taken, weights[0, 1], preferred_element_type=jnp.float32)
        raw = jnp.dot(g_taken, weights[0, 2], preferred_element_type=jnp.float32)
        sig = jax.nn.sigmoid(gate_pre)
        silu = gate_pre * sig
        act = (silu * up_pre).astype(jnp.bfloat16).astype(jnp.float32)
        slot_grad = jnp.sum(act * raw, axis=1, keepdims=True)
        act_grad = raw * scale
        act_scaled = (act * scale).astype(jnp.bfloat16)
        gate_grad = (act_grad * up_pre * sig * (1.0 + gate_pre * (1.0 - sig))).astype(jnp.bfloat16)
        up_grad = (act_grad * silu).astype(jnp.bfloat16)
        extra = (slot_grad * mark).astype(jnp.bfloat16)
        rows_out = contract_last(act_scaled, weights[0, 2]).astype(jnp.bfloat16)
        rows_in = (
            contract_last(gate_grad, weights[0, 0]) + contract_last(up_grad, weights[0, 1])
        ).astype(jnp.bfloat16)
        for slot, left_op, right_op in (
            (0, x_taken, gate_grad),
            (1, x_taken, up_grad),
            (2, g_taken, act_scaled),
        ):
            grad = contract_first(left_op, right_op)
            if base > 0:
                grad = grad + grads[0, slot].astype(jnp.float32)
            grads[0, slot] = grad.astype(jnp.bfloat16)
        block = min(256, group)
        for start in range(0, group, block):
            back = jnp.where(
                lax.broadcasted_iota(jnp.int32, (block, span), 1) + base
                == place_col[start : start + block],
                1.0,
                0.0,
            ).astype(jnp.bfloat16)
            for target, low_col, addend in (
                (y_ref, 0, rows_out),
                (dx_ref, 0, rows_in),
                (dx_ref, width, extra),
            ):
                area = (slice(start, start + block), slice(low_col, low_col + addend.shape[1]))
                target[area] = (
                    target[area].astype(jnp.float32)
                    + jnp.dot(back, addend, preferred_element_type=jnp.float32)
                ).astype(target.dtype)

    run(0, min(SLOTS, capacity))
    for base in range(SLOTS, capacity, SLOTS):
        span = min(SLOTS, -(-(capacity - base) // 16) * 16)

        @pl.when(meta[column] > base)
        def _():
            run(base, span)


def experts_step(meta, place_rows, place_cols, gate_rows, x_rows, g_rows, weights, first, count, skip, capacity):
    group, width = x_rows.shape
    hidden = weights.shape[-1]
    tail = 128

    def whole(shape):
        return pl.BlockSpec(
            shape, lambda step, meta: (0,) * len(shape), pipeline_mode=pl.Buffered(1)
        )

    def big(offset):
        return pl.BlockSpec((1, 3, width, hidden), lambda step, meta: (step + offset, 0, 0, 0))

    return pl.pallas_call(
        functools.partial(experts_kernel, first, capacity),
        grid_spec=pltpu.PrefetchScalarGridSpec(
            num_scalar_prefetch=1,
            grid=(count,),
            in_specs=[
                whole(place_rows.shape),
                whole(place_cols.shape),
                whole(gate_rows.shape),
                whole(x_rows.shape),
                whole(g_rows.shape),
                big(skip),
            ],
            out_specs=[
                whole((group, width)),
                whole((group, width + tail)),
                big(0),
            ],
        ),
        out_shape=[
            jax.ShapeDtypeStruct((group, width), jnp.bfloat16),
            jax.ShapeDtypeStruct((group, width + tail), jnp.bfloat16),
            jax.ShapeDtypeStruct((count, 3, width, hidden), jnp.bfloat16),
        ],
        compiler_params=pltpu.CompilerParams(
            dimension_semantics=("arbitrary",), vmem_limit_bytes=63 << 20
        ),
        cost_estimate=pl.CostEstimate(
            flops=count * 17 * 2 * 408 * width * hidden,
            transcendentals=count * 408 * hidden,
            bytes_accessed=count * 12 * width * hidden,
        ),
    )(meta, place_rows, place_cols, gate_rows, x_rows, g_rows, weights)


def rotate_head(values, cosine, sine, sign):
    half = values.shape[-1] // 2
    other = jnp.concatenate([values[:, half:], values[:, :half]], axis=1)
    return values * cosine + other * (sine * sign)


def segment_bias(seg_row):
    length = seg_row.shape[1]
    shape = (length, length)
    seg_row = seg_row.astype(jnp.float32)
    seg_col = jnp.broadcast_to(seg_row, (128, length)).T[:, :1]
    keys = lax.broadcasted_iota(jnp.int32, shape, 0)
    queries = lax.broadcasted_iota(jnp.int32, shape, 1)
    return jnp.where((keys <= queries) & (seg_col == seg_row), 0.0, masked_value)


def attend_kernel(
    x_ref,
    w_ref,
    seg_row,
    cos_ref,
    sin_ref,
    q_ref,
    k_ref,
    v_ref,
    mixed_ref,
    logsum_ref,
    branch_ref,
    bias,
    v_turned,
    mixed_heads,
):
    heads, kv_heads = q_ref.shape[0], k_ref.shape[0]
    per_kv = heads // kv_heads
    block = SEQ // 2
    edge = (heads + 2 * kv_heads) * HEAD_DIM
    proj = jnp.dot(x_ref[...], w_ref[:, :edge], preferred_element_type=jnp.float32)
    cosine, sine = cos_ref[...], sin_ref[...]
    for head in range(heads + 2 * kv_heads):
        part = proj[:, head * HEAD_DIM : (head + 1) * HEAD_DIM]
        if head < heads:
            q_ref[head] = rotate_head(part, cosine, sine, 1.0).astype(jnp.bfloat16)
        elif head < heads + kv_heads:
            k_ref[head - heads] = rotate_head(part, cosine, sine, 1.0).astype(jnp.bfloat16)
        else:
            v_ref[head - heads - kv_heads] = part.astype(jnp.bfloat16)
            v_turned[head - heads - kv_heads] = part.T.astype(jnp.bfloat16)
    bias[...] = segment_bias(seg_row[0])

    def one_head(head, carry):
        kv = head // per_kv
        for part in range(2):
            span, low = block * (part + 1), block * part
            scores = contract_last(k_ref[kv, :span], q_ref[head, low : low + block]) * attn_scale
            scores = scores + bias[:span, low : low + block]
            top = jnp.max(scores, axis=0, keepdims=True)
            raised = jnp.exp(scores - top)
            total = jnp.sum(raised, axis=0, keepdims=True)
            probs = (raised * (1.0 / total)).astype(jnp.bfloat16)
            turned = jnp.dot(v_turned[kv, :, :span], probs, preferred_element_type=jnp.float32)
            mixed_heads[head, low : low + block, :] = turned.T.astype(jnp.bfloat16)
            logsum_ref[0, pl.ds(head, 1), low : low + block] = top + jnp.log(total)
        return carry

    lax.fori_loop(0, heads, one_head, 0)
    for head in range(heads):
        mixed_ref[:, head * HEAD_DIM : (head + 1) * HEAD_DIM] = mixed_heads[head]
    branch_ref[...] = contract_last(
        mixed_ref[...], w_ref[:, edge : edge + heads * HEAD_DIM]
    ).astype(jnp.bfloat16)


def attend_back_kernel(
    x_ref,
    w_ref,
    seg_row,
    cos_ref,
    sin_ref,
    q_ref,
    k_ref,
    v_ref,
    mixed_ref,
    logsum_ref,
    moe_rows,
    branch_grad,
    dx_ref,
    dw_ref,
    bias,
    k_turned,
    mixed_grads,
    q_grads,
    kv_grads,
    qkv_grad,
    dw_acc,
):
    heads, kv_heads = q_ref.shape[0], k_ref.shape[0]
    per_kv = heads // kv_heads
    block = SEQ // 2
    edge = (heads + 2 * kv_heads) * HEAD_DIM
    step = pl.program_id(0)
    out_edge = edge + heads * HEAD_DIM
    width = x_ref.shape[1]
    grad = jnp.dot(
        branch_grad[:, :width], w_ref[:, edge:out_edge], preferred_element_type=jnp.float32
    ).astype(jnp.bfloat16)
    for head in range(heads):
        mixed_grads[head] = grad[:, head * HEAD_DIM : (head + 1) * HEAD_DIM]
    for kv in range(kv_heads):
        k_turned[kv] = k_ref[kv].astype(jnp.float32).T.astype(jnp.bfloat16)
    bias[...] = segment_bias(seg_row[0])
    kv_grads[...] = jnp.zeros_like(kv_grads)

    def one_head(head, carry):
        kv = head // per_kv
        for part in range(2):
            span, low = block * (part + 1), block * part
            high = low + block
            scores = contract_last(k_ref[kv, :span], q_ref[head, low:high]) * attn_scale
            scores = scores + bias[:span, low:high]
            probs = jnp.exp(scores - logsum_ref[0, pl.ds(head, 1), low:high])
            probs_grad = contract_last(v_ref[kv, :span], mixed_grads[head, low:high])
            inner = jnp.sum(probs * probs_grad, axis=0, keepdims=True)
            score_grad = (probs * (probs_grad - inner)).astype(jnp.bfloat16)
            turned = jnp.dot(k_turned[kv, :, :span], score_grad, preferred_element_type=jnp.float32)
            q_grads[head, low:high, :] = turned.T * attn_scale
            kv_grads[0, kv, :span, :] += jnp.dot(
                score_grad, q_ref[head, low:high], preferred_element_type=jnp.float32
            )
            kv_grads[1, kv, :span, :] += jnp.dot(
                probs.astype(jnp.bfloat16), mixed_grads[head, low:high],
                preferred_element_type=jnp.float32,
            )
        return carry

    lax.fori_loop(0, heads, one_head, 0)
    cosine, sine = cos_ref[...], sin_ref[...]
    for head in range(heads + 2 * kv_heads):
        if head < heads:
            part = rotate_head(q_grads[head], cosine, sine, -1.0)
        elif head < heads + kv_heads:
            part = rotate_head(kv_grads[0, head - heads] * attn_scale, cosine, sine, -1.0)
        else:
            part = kv_grads[1, head - heads - kv_heads]
        qkv_grad[:, head * HEAD_DIM : (head + 1) * HEAD_DIM] = part.astype(jnp.bfloat16)
    dx_ref[...] = contract_last(qkv_grad[...], w_ref[:, :edge]).astype(jnp.bfloat16)
    for low, high, left_op, right_op in (
        (0, edge, x_ref[...], qkv_grad[...]),
        (edge, out_edge, branch_grad[:, :width], mixed_ref[...]),
        (out_edge, dw_acc.shape[1], moe_rows[...], branch_grad[:, width:]),
    ):
        part = contract_first(left_op, right_op)

        @pl.when(step == 0)
        def _():
            dw_acc[:, low:high] = part

        @pl.when(step > 0)
        def _():
            dw_acc[:, low:high] += part

    @pl.when(step == pl.num_programs(0) - 1)
    def _():
        dw_ref[...] = dw_acc[...].astype(jnp.bfloat16)


def fixed(shape):
    return pl.BlockSpec(shape, lambda seq: (0,) * len(shape), pipeline_mode=pl.Buffered(1))


def by_row(width):
    return pl.BlockSpec((SEQ, width), lambda seq: (seq, 0))


def by_head(heads):
    return pl.BlockSpec((heads, SEQ, HEAD_DIM), lambda seq: (0, seq, 0))


def attend_tables():
    half = HEAD_DIM // 2
    positions = np.arange(SEQ, dtype=np.float32)
    frequency = np.float32(rope_base) ** (-np.arange(half, dtype=np.float32) * 2.0 / HEAD_DIM)
    angles = (positions[:, None] * frequency[None, :].astype(np.float32)).astype(np.float32)
    cosine, sine = np.cos(angles), np.sin(angles)
    return (
        jnp.asarray(np.concatenate([cosine, cosine], axis=1)),
        jnp.asarray(np.concatenate([-sine, sine], axis=1)),
    )


def attend(rows, weights, segments, tables, heads, kv_heads):
    group, width = rows.shape
    seqs = group // SEQ
    return pl.pallas_call(
        attend_kernel,
        grid=(seqs,),
        in_specs=[
            by_row(width),
            fixed(weights.shape),
            pl.BlockSpec((1, 1, SEQ), lambda seq: (seq, 0, 0)),
            fixed(tables[0].shape),
            fixed(tables[1].shape),
        ],
        out_specs=[
            by_head(heads),
            by_head(kv_heads),
            by_head(kv_heads),
            by_row(heads * HEAD_DIM),
            pl.BlockSpec((1, heads, SEQ), lambda seq: (seq, 0, 0)),
            by_row(width),
        ],
        out_shape=[
            jax.ShapeDtypeStruct((heads, group, HEAD_DIM), jnp.bfloat16),
            jax.ShapeDtypeStruct((kv_heads, group, HEAD_DIM), jnp.bfloat16),
            jax.ShapeDtypeStruct((kv_heads, group, HEAD_DIM), jnp.bfloat16),
            jax.ShapeDtypeStruct((group, heads * HEAD_DIM), jnp.bfloat16),
            jax.ShapeDtypeStruct((seqs, heads, SEQ), jnp.float32),
            jax.ShapeDtypeStruct((group, width), jnp.bfloat16),
        ],
        scratch_shapes=[
            pltpu.VMEM((SEQ, SEQ), jnp.float32),
            pltpu.VMEM((kv_heads, HEAD_DIM, SEQ), jnp.bfloat16),
            pltpu.VMEM((heads, SEQ, HEAD_DIM), jnp.bfloat16),
        ],
        compiler_params=pltpu.CompilerParams(
            dimension_semantics=("arbitrary",), vmem_limit_bytes=56 << 20
        ),
        cost_estimate=pl.CostEstimate(
            flops=10_000_000_000, transcendentals=3_000_000, bytes_accessed=60_000_000
        ),
    )(rows, weights, segments[:, None, :], *tables)


def attend_back(rows, weights, segments, tables, kept, moe_rows, branch_grad):
    queries, keys, values, mixed, logsum = kept
    group, width = rows.shape
    heads, kv_heads = queries.shape[0], keys.shape[0]
    used = weights.shape[1]
    edge = (heads + 2 * kv_heads) * HEAD_DIM
    return pl.pallas_call(
        attend_back_kernel,
        grid=(group // SEQ,),
        in_specs=[
            by_row(width),
            fixed(weights.shape),
            pl.BlockSpec((1, 1, SEQ), lambda seq: (seq, 0, 0)),
            fixed(tables[0].shape),
            fixed(tables[1].shape),
            by_head(heads),
            by_head(kv_heads),
            by_head(kv_heads),
            by_row(heads * HEAD_DIM),
            pl.BlockSpec((1, heads, SEQ), lambda seq: (seq, 0, 0)),
            by_row(width),
            by_row(branch_grad.shape[1]),
        ],
        out_specs=[by_row(width), fixed((width, used))],
        out_shape=[
            jax.ShapeDtypeStruct((group, width), jnp.bfloat16),
            jax.ShapeDtypeStruct((width, used), jnp.bfloat16),
        ],
        scratch_shapes=[
            pltpu.VMEM((SEQ, SEQ), jnp.float32),
            pltpu.VMEM((kv_heads, HEAD_DIM, SEQ), jnp.bfloat16),
            pltpu.VMEM((heads, SEQ, HEAD_DIM), jnp.bfloat16),
            pltpu.VMEM((heads, SEQ, HEAD_DIM), jnp.float32),
            pltpu.VMEM((2, kv_heads, SEQ, HEAD_DIM), jnp.float32),
            pltpu.VMEM((SEQ, edge), jnp.bfloat16),
            pltpu.VMEM((width, used), jnp.float32),
        ],
        compiler_params=pltpu.CompilerParams(
            dimension_semantics=("arbitrary",), vmem_limit_bytes=60 << 20
        ),
        cost_estimate=pl.CostEstimate(
            flops=20_000_000_000, transcendentals=3_000_000, bytes_accessed=100_000_000
        ),
    )(rows, weights, segments[:, None, :], *tables,
      queries, keys, values, mixed, logsum, moe_rows, branch_grad)


def widen_kernel(edges, *refs):
    step = pl.program_id(0)
    packed, targets = refs[:-3], refs[-3:]
    for part, low, high in zip(packed, edges[:-1], edges[1:]):

        @pl.when((step >= low) & (step < high))
        def _():
            for slot, target in enumerate(targets):
                target[0] = part[0, slot].astype(jnp.float32)


def widen(packed, edges):
    _, _, rows, width = packed[0].shape

    def home(low, high):
        return pl.BlockSpec(
            (1, 3, rows, width),
            lambda step: (jnp.clip(step - low, 0, high - low - 1), 0, 0, 0),
        )

    return pl.pallas_call(
        functools.partial(widen_kernel, edges),
        grid=(edges[-1],),
        in_specs=[home(low, high) for low, high in zip(edges[:-1], edges[1:])],
        out_specs=[pl.BlockSpec((1, rows, width), lambda step: (step, 0, 0))] * 3,
        out_shape=[jax.ShapeDtypeStruct((edges[-1], rows, width), jnp.float32)] * 3,
    )(*packed)


RUNS = (0, 6, 10)
DIRECT = (2, 2)


def local(
    emb,
    segment_ids,
    routes,
    norm1_gain,
    w_query,
    w_key,
    w_value,
    w_out,
    norm2_gain,
    w_router,
    w_gate,
    w_up,
    w_down,
    cotangent,
):
    local_rows, width = emb.shape
    tp_count, tp_index = lax.axis_size("tp"), lax.axis_index("tp")
    experts_here = w_gate.shape[0]
    expert_count = w_router.shape[1]
    q_width, kv_width = w_query.shape[1], w_key.shape[1]
    used = 2 * (q_width + kv_width)
    group_size = local_rows * tp_count
    fsdp_count = lax.axis_size("fsdp")
    split = group_size <= 1024
    runs = [edge * experts_here // RUNS[-1] for edge in RUNS] if split else [0, experts_here]
    stacks = (w_gate, w_up, w_down)
    pieces = [lax.all_gather(pack(stacks, 0, runs[1]), "fsdp", axis=2, tiled=True)]
    gain_one = norm1_gain.astype(jnp.float32)[None, :]
    gain_two = norm2_gain.astype(jnp.float32)[None, :]
    group_rows, mask, place_cols, place_rows, counts, attn_w, *packed = norm_gather(
        emb,
        gain_one,
        routes,
        join([w_query, w_key, w_value, w_out], w_router.T, used + 128),
        stacks,
        runs[1] if split else 0,
        tp_count,
        fsdp_count,
        0,
    )
    if split:
        pieces.append(lax.all_gather(packed[0], "fsdp", axis=2, tiled=True))
    capacity = group_size * routes.shape[1] // expert_count * 2
    meta = jnp.concatenate([counts[0], (tp_index * experts_here)[None]])

    tables = attend_tables()
    heads_here, kv_here = q_width // HEAD_DIM, kv_width // HEAD_DIM
    *kept, branch_part = attend(group_rows, attn_w, segment_ids, tables, heads_here, kv_here)
    mid_x, moe_rows, gate_rows, own_gates, moe_grad_rows = find_mid(
        branch_part, emb, gain_two, attn_w, used, mask, cotangent, tp_count, 1
    )

    outs = []
    for first, last, piece in zip(runs[:-1], runs[1:], pieces):
        outs.append(
            experts_step(
                meta,
                place_rows,
                place_cols,
                gate_rows,
                moe_rows,
                moe_grad_rows,
                piece,
                first,
                last - first,
                0,
                capacity,
            )
        )
    grad_sums = [lax.psum_scatter(outs[0][2], "fsdp", scatter_dimension=2, tiled=True)]
    last_grads = outs[-1][2]
    picks = (tuple(range(DIRECT[0])), tuple(range(DIRECT[0], sum(DIRECT)))) if split else ((), ())
    out, mid_grad, gain_two_grad, sent, *mid_sums = find_mid_grad(
        [part[1] for part in outs],
        [part[0] for part in outs],
        mid_x,
        cotangent,
        own_gates,
        gain_two,
        attn_w,
        used,
        last_grads,
        picks[0],
        tp_count,
        fsdp_count,
        2,
    )
    dx_one, attn_grads = attend_back(
        group_rows, attn_w, segment_ids, tables, kept, moe_rows, sent
    )
    grad_emb, attn_sum, gain_sums, *end_sums = finish(
        dx_one, attn_grads, emb, gain_one, mid_grad, gain_two_grad, last_grads, picks[1], 3
    )
    grad_sums = grad_sums + mid_sums + end_sums
    ends = [0]
    for part in grad_sums:
        ends.append(ends[-1] + part.shape[0])
    expert_sums = widen(grad_sums, ends)
    return (
        out,
        grad_emb,
        gain_sums[0],
        attn_sum[:, :q_width],
        attn_sum[:, q_width : q_width + kv_width],
        attn_sum[:, q_width + kv_width : q_width + 2 * kv_width],
        attn_sum[:, q_width + 2 * kv_width : used],
        gain_sums[1],
        attn_sum[:, used : used + expert_count],
        *expert_sums,
    )


def solution(mesh):
    return jax.shard_map(
        local,
        mesh=mesh,
        in_specs=(
            P(("fsdp", "tp"), None),
            P("fsdp", None),
            P("fsdp", None),
            P(),
            P("fsdp", "tp"),
            P("fsdp", "tp"),
            P("fsdp", "tp"),
            P("fsdp", "tp"),
            P(),
            P("fsdp", None),
            P("tp", "fsdp", None),
            P("tp", "fsdp", None),
            P("tp", "fsdp", None),
            P(("fsdp", "tp"), None),
        ),
        out_specs=(
            P(("fsdp", "tp"), None),
            P(("fsdp", "tp"), None),
            P(),
            P("fsdp", "tp"),
            P("fsdp", "tp"),
            P("fsdp", "tp"),
            P("fsdp", "tp"),
            P(),
            P("fsdp", None),
            P("tp", "fsdp", None),
            P("tp", "fsdp", None),
            P("tp", "fsdp", None),
        ),
        check_vma=False,
    )
```

```python
import functools

import jax
import jax.numpy as jnp
import numpy as np
from jax import lax
from jax.experimental import pallas as pl
from jax.experimental.pallas import tpu as pltpu
from jax.sharding import PartitionSpec as P

HEAD_DIM = 64
SEQ = 512


emb_scale = 12.0
resid_scale = 0.22
attn_scale = 0.015625
norm_eps = 1e-06
rope_base = 10000.0
masked_value = -1e30


def contract_last(left_op, right_op):
    return lax.dot_general(
        left_op, right_op, (((1,), (1,)), ((), ())), preferred_element_type=jnp.float32
    )


def contract_first(left_op, right_op):
    return lax.dot_general(
        left_op, right_op, (((0,), (0,)), ((), ())), preferred_element_type=jnp.float32
    )


def line_signal(barrier, me, count):
    @pl.when(me > 0)
    def _():
        pl.semaphore_signal(barrier, inc=1, device_id={"tp": me - 1})

    @pl.when(me < count - 1)
    def _():
        pl.semaphore_signal(barrier, inc=1, device_id={"tp": me + 1})

    return jnp.where((me > 0) & (me < count - 1), 2, 1)


class Plane:
    def __init__(self, count):
        self.me = lax.axis_index("fsdp")
        self.core = lax.rem(self.me, 2)
        self.chip = lax.div(self.me, 2)
        self.chips = count // 2
        self.partner = self.me + 1 - 2 * self.core

    def chip_at(self, shift):
        return lax.rem(self.chip + shift + self.chips, self.chips)

    def peer(self, shift):
        return self.chip_at(shift) * 2 + self.core

    def signal(self, barrier):
        for shift in range(1, self.chips):
            pl.semaphore_signal(barrier, inc=1, device_id={"fsdp": self.peer(shift)})
        pl.semaphore_signal(barrier, inc=1, device_id={"fsdp": self.partner})
        return self.chips


def rows_of(ref, index, rows):
    return ref.at[pl.ds(pl.multiple_of(index * rows, rows), rows)]


class LineGather:
    def __init__(self, count, o_ref, send_sem, recv_sem):
        self.count, self.o_ref = count, o_ref
        self.send_sem, self.recv_sem = send_sem, recv_sem
        self.rows = o_ref.shape[0] // count
        me = self.me = lax.axis_index("tp")
        steps = range(count - 1)
        self.sends = [
            [(me >= step) & (me < count - 1) for step in steps],
            [(me + step < count) & (me > 0) for step in steps],
        ]
        self.gets = [
            [me - 1 - step >= 0 for step in steps],
            [me + 1 + step < count for step in steps],
        ]

    def hop(self, way, step, chunk):
        part = rows_of(self.o_ref, chunk, self.rows)
        return pltpu.make_async_remote_copy(
            src_ref=part,
            dst_ref=part,
            send_sem=self.send_sem.at[way, step],
            recv_sem=self.recv_sem.at[way, step],
            device_id={"tp": self.me + 1 if way == 0 else self.me - 1},
        )

    def start(self, step):
        @pl.when(self.sends[0][step])
        def _():
            self.hop(0, step, self.me - step).start()

        @pl.when(self.sends[1][step])
        def _():
            self.hop(1, step, self.me + step).start()

    def arrive(self, step):
        @pl.when(self.gets[0][step])
        def _():
            self.hop(0, step, self.me - 1 - step).wait_recv()

        @pl.when(self.gets[1][step])
        def _():
            self.hop(1, step, self.me + 1 + step).wait_recv()

    def finish(self):
        for step in range(self.count - 1):

            @pl.when(self.sends[0][step])
            def _():
                self.hop(0, step, self.me - step).wait_send()

            @pl.when(self.sends[1][step])
            def _():
                self.hop(1, step, self.me + step).wait_send()


def line_sems(count):
    return [
        pltpu.SemaphoreType.DMA((2, count - 1)),
        pltpu.SemaphoreType.DMA((2, count - 1)),
    ]


class PlaneGather:
    def __init__(self, plane, w_ref, wo_ref, out_send, out_recv, on_send, on_recv, kept_sem):
        self.plane, self.w_ref, self.wo_ref = plane, w_ref, wo_ref
        self.out_send, self.out_recv = out_send, out_recv
        self.on_send, self.on_recv = on_send, on_recv
        self.rows = w_ref.shape[0]
        self.kept = pltpu.make_async_copy(w_ref, rows_of(wo_ref, plane.me, self.rows), kept_sem)

    def outward(self, shift, target, source_device):
        return pltpu.make_async_remote_copy(
            src_ref=self.w_ref,
            dst_ref=rows_of(self.wo_ref, source_device, self.rows),
            send_sem=self.out_send.at[shift],
            recv_sem=self.out_recv.at[shift],
            device_id={"fsdp": target},
        )

    def onward(self, shift, source_device):
        part = rows_of(self.wo_ref, source_device, self.rows)
        return pltpu.make_async_remote_copy(
            src_ref=part,
            dst_ref=part,
            send_sem=self.on_send.at[shift - 1],
            recv_sem=self.on_recv.at[shift - 1],
            device_id={"fsdp": self.plane.partner},
        )

    def start(self):
        plane = self.plane
        for shift in range(1, plane.chips):
            self.outward(shift, plane.peer(shift), plane.me).start()
        self.outward(0, plane.partner, plane.me).start()
        self.kept.start()

    def forward(self):
        plane = self.plane
        for shift in range(1, plane.chips):
            self.outward(shift, plane.peer(shift), plane.peer(-shift)).wait_recv()
            self.onward(shift, plane.peer(-shift)).start()

    def finish(self):
        plane = self.plane
        self.outward(0, plane.partner, plane.partner).wait_recv()
        for shift in range(1, plane.chips):
            self.onward(shift, plane.chip_at(-shift) * 2 + 1 - plane.core).wait_recv()
        for shift in range(1, plane.chips):
            self.outward(shift, plane.peer(shift), plane.me).wait_send()
            self.onward(shift, plane.peer(-shift)).wait_send()
        self.outward(0, plane.partner, plane.me).wait_send()
        self.kept.wait()


class ExpertSums:
    def __init__(self, plane, picks, grads_ref, out_ref, *refs):
        self.plane, self.picks, self.grads_ref, self.out_ref = plane, picks, grads_ref, out_ref
        (
            self.got, self.own, self.chip_got, self.held,
            self.pair_send, self.pair_recv, self.own_sem,
            self.chip_send, self.chip_recv, self.put_sem,
        ) = refs
        self.rows = out_ref.shape[2]

    def area(self, index, dest):
        low = pl.multiple_of(dest * self.rows, self.rows)
        return self.grads_ref.at[self.picks[index], :, pl.ds(low, self.rows)]

    def to_pair(self, index, shift):
        plane = self.plane
        return pltpu.make_async_remote_copy(
            src_ref=self.area(index, plane.chip_at(shift) * 2 + 1 - plane.core),
            dst_ref=self.got.at[index, shift],
            send_sem=self.pair_send.at[index, shift],
            recv_sem=self.pair_recv.at[index, shift],
            device_id={"fsdp": plane.partner},
        )

    def keep(self, index, shift):
        return pltpu.make_async_copy(
            self.area(index, self.plane.peer(shift)),
            self.own.at[index, shift],
            self.own_sem.at[index, shift],
        )

    def to_chip(self, index, shift):
        return pltpu.make_async_remote_copy(
            src_ref=self.own.at[index, shift],
            dst_ref=self.chip_got.at[index, shift - 1],
            send_sem=self.chip_send.at[index, shift - 1],
            recv_sem=self.chip_recv.at[index, shift - 1],
            device_id={"fsdp": self.plane.peer(shift)},
        )

    def put(self, index):
        return pltpu.make_async_copy(
            self.held.at[index], self.out_ref.at[index], self.put_sem.at[index]
        )

    def order(self):
        return list(range(1, self.plane.chips)) + [0]

    def begin(self, index):
        for shift in self.order():
            self.to_pair(index, shift).start()
            self.keep(index, shift).start()

    def items(self):
        return [(index, shift) for index in range(len(self.picks)) for shift in self.order()]

    def pass_on(self, index, shift):
        self.to_pair(index, shift).wait_recv()
        self.keep(index, shift).wait()
        for slot in range(self.own.shape[2]):
            both = self.own[index, shift, slot].astype(jnp.float32) + self.got[
                index, shift, slot
            ].astype(jnp.float32)
            self.own[index, shift, slot] = both.astype(jnp.bfloat16)
        if shift > 0:
            self.to_chip(index, shift).start()

    def collect(self, index):
        chips = self.plane.chips
        for shift in range(1, chips):
            self.to_chip(index, shift).wait_recv()
        for slot in range(self.own.shape[2]):
            total = self.own[index, 0, slot].astype(jnp.float32)
            for shift in range(1, chips):
                total = total + self.chip_got[index, shift - 1, slot].astype(jnp.float32)
            self.held[index, slot] = total.astype(jnp.bfloat16)
        self.put(index).start()

    def finish(self):
        for index in range(len(self.picks)):
            self.put(index).wait()
            for shift in self.order():
                self.to_pair(index, shift).wait_send()
                if shift > 0:
                    self.to_chip(index, shift).wait_send()


def expert_buffers(count, chips, rows, width):
    if count == 0:
        return []
    return [
        pltpu.VMEM((count, chips, 3, rows, width), jnp.bfloat16),
        pltpu.VMEM((count, chips, 3, rows, width), jnp.bfloat16),
        pltpu.VMEM((count, chips - 1, 3, rows, width), jnp.bfloat16),
        pltpu.VMEM((count, 3, rows, width), jnp.bfloat16),
        pltpu.SemaphoreType.DMA((count, chips)),
        pltpu.SemaphoreType.DMA((count, chips)),
        pltpu.SemaphoreType.DMA((count, chips)),
        pltpu.SemaphoreType.DMA((count, chips - 1)),
        pltpu.SemaphoreType.DMA((count, chips - 1)),
        pltpu.SemaphoreType.DMA((count,)),
    ]


class LineScatter:
    def __init__(self, count, x_refs, o_ref, recv, send_sem, recv_sem):
        self.count, self.x_refs, self.o_ref, self.recv = count, x_refs, o_ref, recv
        self.send_sem, self.recv_sem = send_sem, recv_sem
        self.rows = o_ref.shape[0]
        me = self.me = lax.axis_index("tp")
        self.behind = (me, count - 1 - me)
        self.has_next = (me < count - 1, me > 0)
        self.has_prev = (me > 0, me < count - 1)

    def block(self, dest):
        area = pl.ds(pl.multiple_of(dest * self.rows, self.rows), self.rows)
        total = self.x_refs[0][area, :].astype(jnp.float32)
        for x_ref in self.x_refs[1:]:
            total = total + x_ref[area, :].astype(jnp.float32)
        return total

    def hop(self, way, step, source):
        return pltpu.make_async_remote_copy(
            src_ref=source,
            dst_ref=self.recv.at[way, step],
            send_sem=self.send_sem.at[way, step],
            recv_sem=self.recv_sem.at[way, step],
            device_id={"tp": self.me + 1 if way == 0 else self.me - 1},
        )

    def start(self, step):
        count, me, recv = self.count, self.me, self.recv
        for way in range(2):
            dest = count - 1 - step + me if way == 0 else step - (count - 1 - me)
            active = self.has_next[way] & (step >= self.behind[way])

            @pl.when(active & (self.behind[way] == 0))
            def _():
                part = rows_of(self.x_refs[0], dest, self.rows)
                if len(self.x_refs) > 1:
                    part[...] = self.block(dest).astype(part.dtype)
                self.hop(way, step, part).start()

            if step > 0:

                @pl.when(active & (self.behind[way] > 0))
                def _():
                    total = self.block(dest) + recv[way, step - 1].astype(jnp.float32)
                    recv[way, step - 1] = total.astype(recv.dtype)
                    self.hop(way, step, recv.at[way, step - 1]).start()

    def arrive(self, step):
        for way in range(2):

            @pl.when(self.has_prev[way] & (step >= self.behind[way] - 1))
            def _():
                self.hop(way, step, self.recv.at[way, step]).wait_recv()

    def collect(self):
        self.o_ref[...] = self.block(self.me)
        for way in range(2):

            @pl.when(self.has_prev[way])
            def _():
                self.o_ref[...] += self.recv[way, self.count - 2].astype(jnp.float32)

    def finish(self):
        for step in range(self.count - 1):
            for way in range(2):

                @pl.when(self.has_next[way] & (step >= self.behind[way]))
                def _():
                    self.hop(way, step, self.recv.at[way, step]).wait_send()


def line_buffers(count, rows, width):
    return [pltpu.VMEM((2, count - 1, rows, width), jnp.bfloat16)] + line_sems(count)


def own_rows(ref, rows):
    return pl.ds(pl.multiple_of(lax.axis_index("tp") * rows, rows), rows)


def inverse_norm(values):
    return lax.rsqrt(jnp.mean(values * values, axis=-1, keepdims=True) + norm_eps)


def rms_back(incoming, values, gain_row):
    inverse = inverse_norm(values)
    scaled = values * inverse
    gain_grad = jnp.sum(incoming * scaled, axis=0, keepdims=True)
    weighted = incoming * gain_row
    row_inner = jnp.mean(weighted * scaled, axis=-1, keepdims=True)
    return inverse * (weighted - scaled * row_inner), gain_grad


def enter_kernel(count, plane=None):
    barrier = pltpu.get_barrier_semaphore()
    waits = line_signal(barrier, lax.axis_index("tp"), count)
    if plane is not None:
        waits = waits + plane.signal(barrier)
    pl.semaphore_wait(barrier, waits)


def remote_params(ident, limit=60):
    return pltpu.CompilerParams(
        collective_id=ident, has_side_effects=True, vmem_limit_bytes=limit << 20
    )


IN_VMEM = pl.BlockSpec(memory_space=pltpu.VMEM)
IN_PLACE = pl.BlockSpec(memory_space=pl.ANY)
TRANSFER = pl.CostEstimate(flops=0, transcendentals=0, bytes_accessed=150_000_000)


def norm_gather_kernel(count, fsdp_count, low, *refs):
    emb_ref, gain_ref, routes_ref, w_ref, *refs = refs
    stacks, refs = (refs[:3], refs[3:]) if low else ((), refs)
    rows_ref, mask_ref, cols_ref, turned_ref, counts_ref, wo_ref, *refs = refs
    packed, refs = (refs[0], refs[1:]) if low else (None, refs)
    row_send, row_recv, *refs = refs
    plane = Plane(fsdp_count)
    if low:
        held, in_sem, out_sem = refs[5:]
        gets, puts = pack_copies(low, stacks, packed, held, in_sem, out_sem)
        for get in gets:
            get.start()
    enter_kernel(count, plane)
    line = LineGather(count, rows_ref, row_send, row_recv)
    weights = PlaneGather(plane, w_ref, wo_ref, *refs[:5])
    start_x = emb_ref[...].astype(jnp.float32) * emb_scale
    normed = start_x * inverse_norm(start_x) * gain_ref[...]
    rows_ref[own_rows(rows_ref, line.rows), :] = normed.astype(jnp.bfloat16)
    for step in range(count - 1):
        line.start(step)
        if step == 0:
            weights.start()
            place_routes(line.rows, routes_ref, mask_ref, cols_ref, turned_ref, counts_ref)
            if low:
                for get, put in zip(gets, puts):
                    get.wait()
                    put.start()
        if step == count - 2:
            weights.forward()
        line.arrive(step)
    if low:
        for put in puts:
            put.wait()
    weights.finish()
    line.finish()


def place_routes(rows, routes_ref, mask_ref, cols_ref, turned_ref, counts_ref):
    group, lanes = mask_ref.shape
    columns = lax.broadcasted_iota(jnp.int32, (rows, lanes), 1)
    for low in range(0, group, rows):
        area = slice(low, low + rows)
        mask = jnp.zeros((rows, lanes), jnp.float32)
        for choice in range(routes_ref.shape[1]):
            mask = jnp.where(routes_ref[area, choice : choice + 1] == columns, 1.0, mask)
        mask_ref[area, :] = mask
    counts_ref[...] = jnp.sum(mask_ref[...], axis=0, keepdims=True).astype(jnp.int32)
    member = mask_ref[...].astype(jnp.bfloat16)
    for low in range(0, group, rows):
        area = slice(low, low + rows)
        here = lax.broadcasted_iota(jnp.int32, (rows, group), 0) + low
        earlier = here > lax.broadcasted_iota(jnp.int32, (rows, group), 1)
        ranks = jnp.dot(
            jnp.where(earlier, 1.0, 0.0).astype(jnp.bfloat16),
            member,
            preferred_element_type=jnp.float32,
        )
        places = jnp.where(mask_ref[area, :] > 0.0, ranks, -1.0)
        cols_ref[area, :] = places.astype(jnp.int32)
        turned_ref[:, area] = places.T.astype(jnp.int32)


def norm_gather(emb, gain_row, routes, weights, stacks, low, count, fsdp_count, ident):
    rows, width = emb.shape
    group = rows * count
    chips = fsdp_count // 2
    experts, share, hidden = stacks[0].shape
    span = experts - low
    outs = [
        jax.ShapeDtypeStruct((group, width), jnp.bfloat16),
        jax.ShapeDtypeStruct((group, 128), jnp.float32),
        jax.ShapeDtypeStruct((group, 128), jnp.int32),
        jax.ShapeDtypeStruct((128, group), jnp.int32),
        jax.ShapeDtypeStruct((1, 128), jnp.int32),
        jax.ShapeDtypeStruct((weights.shape[0] * fsdp_count, weights.shape[1]), jnp.bfloat16),
    ]
    scratch = line_sems(count) + [
        pltpu.SemaphoreType.DMA((chips,)),
        pltpu.SemaphoreType.DMA((chips,)),
        pltpu.SemaphoreType.DMA((chips - 1,)),
        pltpu.SemaphoreType.DMA((chips - 1,)),
        pltpu.SemaphoreType.DMA,
    ]
    if low:
        outs.append(jax.ShapeDtypeStruct((span, 3, share, hidden), jnp.bfloat16))
        scratch += [
            pltpu.VMEM((3, span, share, hidden), jnp.bfloat16),
            pltpu.SemaphoreType.DMA((3,)),
            pltpu.SemaphoreType.DMA((3,)),
        ]
    return pl.pallas_call(
        functools.partial(norm_gather_kernel, count, fsdp_count, low),
        out_shape=outs,
        in_specs=[IN_VMEM] * 4 + [IN_PLACE] * (3 if low else 0),
        out_specs=[IN_VMEM] * 5 + [IN_PLACE] * (len(outs) - 5),
        scratch_shapes=scratch,
        compiler_params=remote_params(ident, 48),
        cost_estimate=TRANSFER,
    )(emb, gain_row, routes, weights, *(stacks if low else ()))


def mid_kernel(
    count, part_ref, emb_ref, gain_ref, router_ref, mask_ref, cotangent_ref,
    mid_ref, rows_ref, gates_ref, own_gates, moe_grads,
    recv, sum_send, sum_recv, row_send, row_recv, grad_send, grad_recv,
):
    enter_kernel(count)
    total = LineScatter(count, [part_ref], mid_ref, recv, sum_send, sum_recv)
    line = LineGather(count, rows_ref, row_send, row_recv)
    others = LineGather(count, moe_grads, grad_send, grad_recv)
    rows = line.rows
    moe_grads[own_rows(moe_grads, rows), :] = (
        resid_scale * cotangent_ref[...].astype(jnp.float32)
    ).astype(jnp.bfloat16)
    for step in range(count):
        if step < count - 1:
            others.start(step)
        if step > 0:
            total.start(step - 1)
        if step < count - 1:
            others.arrive(step)
        if step > 0:
            total.arrive(step - 1)
    total.collect()
    mid = emb_ref[...].astype(jnp.float32) * emb_scale + resid_scale * mid_ref[...]
    mid_ref[...] = mid
    own = own_rows(rows_ref, rows)
    rows_ref[own, :] = (mid * inverse_norm(mid) * gain_ref[...]).astype(jnp.bfloat16)

    def find_gates(chunk):
        area = pl.ds(pl.multiple_of(chunk * rows, rows), rows)
        logits = jnp.dot(rows_ref[area, :], router_ref[...], preferred_element_type=jnp.float32)
        inside = mask_ref[area, :] > 0.0
        top = jnp.max(jnp.where(inside, logits, masked_value), axis=-1, keepdims=True)
        raised = jnp.where(inside, jnp.exp(jnp.where(inside, logits - top, 0.0)), 0.0)
        gates = raised / jnp.sum(raised, axis=-1, keepdims=True)
        gates_ref[:, area] = gates.T
        return gates

    for step in range(count - 1):
        line.start(step)
        if step == 0:
            own_gates[...] = find_gates(line.me)
        line.arrive(step)

        @pl.when(line.gets[0][step])
        def _():
            find_gates(line.me - 1 - step)

        @pl.when(line.gets[1][step])
        def _():
            find_gates(line.me + 1 + step)

    line.finish()
    total.finish()
    others.finish()


def find_mid(part, emb, gain_row, weights, used, mask, cotangent, count, ident):
    rows, width = emb.shape
    group = rows * count
    return pl.pallas_call(
        functools.partial(mid_kernel, count),
        grid=(1,),
        out_shape=[
            jax.ShapeDtypeStruct((rows, width), jnp.float32),
            jax.ShapeDtypeStruct((group, width), jnp.bfloat16),
            jax.ShapeDtypeStruct((128, group), jnp.float32),
            jax.ShapeDtypeStruct((rows, 128), jnp.float32),
            jax.ShapeDtypeStruct((group, width), jnp.bfloat16),
        ],
        in_specs=[
            IN_VMEM,
            IN_VMEM,
            IN_VMEM,
            pl.BlockSpec((width, 128), lambda step: (0, used // 128)),
            IN_VMEM,
            IN_VMEM,
        ],
        out_specs=[IN_VMEM] * 5,
        scratch_shapes=line_buffers(count, rows, width) + line_sems(count) + line_sems(count),
        compiler_params=remote_params(ident),
        cost_estimate=TRANSFER,
    )(part, emb, gain_row, weights, mask, cotangent)


def moe_back_kernel(count, fsdp_count, runs, picks, *refs):
    dx_refs, y_refs, refs = refs[:runs], refs[runs : 2 * runs], refs[2 * runs :]
    mid_ref, cotangent_ref, own_gates, gain_ref, router_ref, *refs = refs
    grads_ref, refs = (refs[0], refs[1:]) if picks else (None, refs)
    out_ref, mid_grad, gain_grad, sent_ref, *refs = refs
    sums_ref, refs = (refs[0], refs[1:]) if picks else (None, refs)
    (
        dx_parts, y_parts, load_sem, sum_ref, moe_ref,
        recv, sum_send, sum_recv, moe_recv, moe_send, moe_recv_sem, row_send, row_recv, *refs,
    ) = refs
    loads = []
    for index, (source, parts) in enumerate(
        [(ref, dx_parts) for ref in dx_refs] + [(ref, y_parts) for ref in y_refs]
    ):
        loads.append(
            pltpu.make_async_copy(source, parts.at[index % runs], load_sem.at[index])
        )
        loads[-1].start()
    plane = Plane(fsdp_count) if picks else None
    enter_kernel(count, plane)
    total = LineScatter(
        count, [dx_parts.at[run] for run in range(runs)], sum_ref, recv, sum_send, sum_recv
    )
    moe = LineScatter(
        count, [y_parts.at[run] for run in range(runs)], moe_ref, moe_recv, moe_send, moe_recv_sem
    )
    line = LineGather(count, sent_ref, row_send, row_recv)
    experts = ExpertSums(plane, picks, grads_ref, sums_ref, *refs) if picks else None
    rows, width = mid_ref.shape
    for index in range(len(picks)):
        experts.begin(index)
    for load in loads[:runs]:
        load.wait()
    items = experts.items() if picks else []
    each = -(-len(items) // (2 * count - 2))
    for step in range(count - 1):
        total.start(step)
        for item in items[step * each : (step + 1) * each]:
            experts.pass_on(*item)
        total.arrive(step)
    items = items[(count - 1) * each :]
    total.collect()
    gates = own_gates[...]
    gates_grad = sum_ref[:, width:]
    gates_inner = jnp.sum(gates * gates_grad, axis=-1, keepdims=True)
    logits_grad = (gates * (gates_grad - gates_inner)).astype(jnp.bfloat16)
    incoming = sum_ref[:, :width] + contract_last(logits_grad, router_ref[...])
    from_norm, gain_part = rms_back(incoming, mid_ref[...], gain_ref[...])
    grad = cotangent_ref[...].astype(jnp.float32) + from_norm
    mid_grad[...] = grad
    gain_grad[...] = gain_part
    own = own_rows(sent_ref, rows)
    sent_ref[own, :width] = (resid_scale * grad).astype(jnp.bfloat16)
    sent_ref[own, width:] = logits_grad
    for load in loads[runs:]:
        load.wait()
    for step in range(count):
        if step < count - 1:
            line.start(step)
        if step > 0:
            moe.start(step - 1)
        for item in items[step * each : (step + 1) * each]:
            experts.pass_on(*item)
        if step < count - 1:
            line.arrive(step)
        if step > 0:
            moe.arrive(step - 1)
    moe.collect()
    out_ref[...] = (mid_ref[...] + resid_scale * moe_ref[...]).astype(out_ref.dtype)
    for index in range(len(picks)):
        experts.collect(index)
    line.finish()
    total.finish()
    moe.finish()
    if picks:
        experts.finish()


def find_mid_grad(
    dx_parts, y_parts, mid, cotangent, own_gates, gain_row, weights, used, grads, picks,
    count, fsdp_count, ident,
):
    rows, width = mid.shape
    runs, group = len(dx_parts), rows * count
    wide = dx_parts[0].shape[1]
    share = grads.shape[2] // fsdp_count
    sums = [jax.ShapeDtypeStruct((len(picks), 3, share, grads.shape[3]), jnp.bfloat16)]
    sums = sums if picks else []
    return pl.pallas_call(
        functools.partial(moe_back_kernel, count, fsdp_count, runs, picks),
        grid=(1,),
        out_shape=[
            jax.ShapeDtypeStruct((rows, width), jnp.bfloat16),
            jax.ShapeDtypeStruct((rows, width), jnp.float32),
            jax.ShapeDtypeStruct((1, width), jnp.float32),
            jax.ShapeDtypeStruct((group, wide), jnp.bfloat16),
        ]
        + sums,
        in_specs=[IN_PLACE] * (2 * runs)
        + [IN_VMEM] * 4
        + [pl.BlockSpec((width, 128), lambda step: (0, used // 128))]
        + [IN_PLACE] * len(sums),
        out_specs=[IN_VMEM] * 4 + [IN_PLACE] * len(sums),
        scratch_shapes=[
            pltpu.VMEM((runs, group, wide), jnp.bfloat16),
            pltpu.VMEM((runs, group, width), jnp.bfloat16),
            pltpu.SemaphoreType.DMA((2 * runs,)),
            pltpu.VMEM((rows, wide), jnp.float32),
            pltpu.VMEM((rows, width), jnp.float32),
        ]
        + line_buffers(count, rows, wide)
        + line_buffers(count, rows, width)
        + line_sems(count)
        + expert_buffers(len(picks), fsdp_count // 2, share, grads.shape[3]),
        compiler_params=remote_params(ident, 63),
        cost_estimate=TRANSFER,
    )(*dx_parts, *y_parts, mid, cotangent, own_gates, gain_row, weights, *([grads] if picks else []))


def finish_kernel(tp_count, fsdp_count, picks, *refs):
    x_ref, w_ref, emb_ref, gain_ref, mid_grad, gain_two, *refs = refs
    grads_ref, refs = (refs[0], refs[1:]) if picks else (None, refs)
    grad_ref, w_sum, gains_ref, *refs = refs
    sums_ref, refs = (refs[0], refs[1:]) if picks else (None, refs)
    (
        line_recv, line_send_sem, line_recv_sem,
        pair_got, chip_sums, chip_got, pair_send, pair_recv, chip_send, chip_recv,
        tp_got, fsdp_got, small_send, small_recv, *refs,
    ) = refs
    plane = Plane(fsdp_count)
    tp_me, fsdp_me = lax.axis_index("tp"), plane.me
    barrier = pltpu.get_barrier_semaphore()
    for shift in range(1, tp_count):
        pl.semaphore_signal(barrier, inc=1, device_id={"tp": lax.rem(tp_me + shift, tp_count)})
    for shift in range(1, fsdp_count):
        pl.semaphore_signal(
            barrier, inc=1, device_id={"fsdp": lax.rem(fsdp_me + shift, fsdp_count)}
        )
    pl.semaphore_wait(barrier, tp_count + fsdp_count - 2)
    line = LineScatter(
        tp_count, [x_ref], grad_ref, line_recv, line_send_sem, line_recv_sem
    )
    rows = w_sum.shape[0]

    def to_pair(shift):
        return pltpu.make_async_remote_copy(
            src_ref=rows_of(w_ref, plane.chip_at(shift) * 2 + 1 - plane.core, rows),
            dst_ref=pair_got.at[shift],
            send_sem=pair_send.at[shift],
            recv_sem=pair_recv.at[shift],
            device_id={"fsdp": plane.partner},
        )

    def to_chip(shift):
        return pltpu.make_async_remote_copy(
            src_ref=chip_sums.at[shift - 1],
            dst_ref=chip_got.at[shift - 1],
            send_sem=chip_send.at[shift - 1],
            recv_sem=chip_recv.at[shift - 1],
            device_id={"fsdp": plane.peer(shift)},
        )

    def both_cores(shift):
        own = pl.ds(pl.multiple_of(plane.peer(shift) * rows, rows), rows)
        return w_ref[own, :].astype(jnp.float32) + pair_got[shift].astype(jnp.float32)

    def exchange(axis, me, count, got, base):
        copies = []
        for shift in range(1, count):
            copies.append(
                pltpu.make_async_remote_copy(
                    src_ref=gains_ref,
                    dst_ref=got.at[me],
                    send_sem=small_send.at[base + shift],
                    recv_sem=small_recv.at[base + shift],
                    device_id={axis: lax.rem(me + shift, count)},
                )
            )
            copies[-1].start()
        got[me] = gains_ref[...]
        for copy in copies:
            copy.wait()
        total = got[0]
        for index in range(1, count):
            total = total + got[index]
        return total

    experts = ExpertSums(plane, picks, grads_ref, sums_ref, *refs) if picks else None
    line.start(0)
    order = list(range(1, plane.chips)) + [0]
    for shift in order:
        to_pair(shift).start()
    for index in range(len(picks)):
        experts.begin(index)
    for shift in order:
        to_pair(shift).wait_recv()
        if shift > 0:
            chip_sums[shift - 1] = both_cores(shift).astype(chip_sums.dtype)
            to_chip(shift).start()
    items = experts.items() if picks else []
    each = -(-len(items) // (tp_count - 2))
    line.arrive(0)
    for step in range(1, tp_count - 1):
        line.start(step)
        for item in items[(step - 1) * each : step * each]:
            experts.pass_on(*item)
        line.arrive(step)
    line.collect()
    from_norm, gain_one = rms_back(
        grad_ref[...], emb_ref[...].astype(jnp.float32) * emb_scale, gain_ref[...]
    )
    gains_ref[...] = jnp.zeros_like(gains_ref)
    gains_ref[0:1, :] = gain_one
    gains_ref[1:2, :] = gain_two[...]
    grad_ref[...] = emb_scale * (mid_grad[...] + from_norm)
    total = both_cores(0)
    for shift in range(1, plane.chips):
        to_chip(shift).wait_recv()
        total = total + chip_got[shift - 1].astype(jnp.float32)
    w_sum[...] = total
    for index in range(len(picks)):
        experts.collect(index)
    gains_ref[...] = exchange("tp", tp_me, tp_count, tp_got, 0)
    gains_ref[...] = exchange("fsdp", fsdp_me, fsdp_count, fsdp_got, tp_count)
    line.finish()
    for shift in order:
        to_pair(shift).wait_send()
        if shift > 0:
            to_chip(shift).wait_send()
    if picks:
        experts.finish()


def finish(dx_rows, weight_grads, emb, gain_row, mid_grad, gain_two, grads, picks, ident):
    tp_count, fsdp_count = lax.axis_size("tp"), lax.axis_size("fsdp")
    rows, width = emb.shape
    w_rows, w_width = weight_grads.shape[0] // fsdp_count, weight_grads.shape[1]
    chips = fsdp_count // 2
    share = grads.shape[2] // fsdp_count
    sums = [jax.ShapeDtypeStruct((len(picks), 3, share, grads.shape[3]), jnp.bfloat16)]
    sums = sums if picks else []
    return pl.pallas_call(
        functools.partial(finish_kernel, tp_count, fsdp_count, picks),
        out_shape=[
            jax.ShapeDtypeStruct((rows, width), jnp.float32),
            jax.ShapeDtypeStruct((w_rows, w_width), jnp.float32),
            jax.ShapeDtypeStruct((8, width), jnp.float32),
            *sums,
        ],
        in_specs=[IN_VMEM] * 6 + [IN_PLACE] * len(sums),
        out_specs=[IN_VMEM] * 3 + [IN_PLACE] * len(sums),
        scratch_shapes=line_buffers(tp_count, rows, width)
        + [
            pltpu.VMEM((chips, w_rows, w_width), jnp.bfloat16),
            pltpu.VMEM((chips - 1, w_rows, w_width), jnp.bfloat16),
            pltpu.VMEM((chips - 1, w_rows, w_width), jnp.bfloat16),
            pltpu.SemaphoreType.DMA((chips,)),
            pltpu.SemaphoreType.DMA((chips,)),
            pltpu.SemaphoreType.DMA((chips - 1,)),
            pltpu.SemaphoreType.DMA((chips - 1,)),
            pltpu.VMEM((tp_count, 8, width), jnp.float32),
            pltpu.VMEM((fsdp_count, 8, width), jnp.float32),
            pltpu.SemaphoreType.DMA((tp_count + fsdp_count,)),
            pltpu.SemaphoreType.DMA((tp_count + fsdp_count,)),
        ]
        + expert_buffers(len(picks), chips, share, grads.shape[3]),
        compiler_params=remote_params(ident),
        cost_estimate=TRANSFER,
    )(dx_rows, weight_grads, emb, gain_row, mid_grad, gain_two, *([grads] if picks else []))


def pack_copies(low, sources, target, held, in_sem, out_sem):
    span = target.shape[0]
    gets = [
        pltpu.make_async_copy(source.at[pl.ds(low, span)], held.at[slot], in_sem.at[slot])
        for slot, source in enumerate(sources)
    ]
    puts = [
        pltpu.make_async_copy(held.at[slot], target.at[:, slot], out_sem.at[slot])
        for slot in range(len(sources))
    ]
    return gets, puts


def pack_kernel(low, *refs):
    sources, target, held, in_sem, out_sem = refs[:-4], *refs[-4:]
    gets, puts = pack_copies(low, sources, target, held, in_sem, out_sem)
    for get in gets:
        get.start()
    for get, put in zip(gets, puts):
        get.wait()
        put.start()
    for put in puts:
        put.wait()


def pack(stacks, low, high):
    _, rows, width = stacks[0].shape
    count, span = len(stacks), high - low
    return pl.pallas_call(
        functools.partial(pack_kernel, low),
        in_specs=[IN_PLACE] * count,
        out_specs=IN_PLACE,
        out_shape=jax.ShapeDtypeStruct((span, count, rows, width), jnp.bfloat16),
        scratch_shapes=[
            pltpu.VMEM((count, span, rows, width), jnp.bfloat16),
            pltpu.SemaphoreType.DMA((count,)),
            pltpu.SemaphoreType.DMA((count,)),
        ],
    )(*stacks)


def join_kernel(*refs):
    *sources, last, target = refs
    low = 0
    for source in sources:
        target[:, low : low + source.shape[1]] = source[...]
        low += source.shape[1]
    router = last[...].astype(jnp.float32).T.astype(jnp.bfloat16)
    target[:, low:] = jnp.zeros((target.shape[0], target.shape[1] - low), jnp.bfloat16)
    target[:, low : low + router.shape[1]] = router


def join(parts, last_turned, width):
    return pl.pallas_call(
        join_kernel,
        in_specs=[IN_VMEM] * (len(parts) + 1),
        out_specs=IN_VMEM,
        out_shape=jax.ShapeDtypeStruct((parts[0].shape[0], width), jnp.bfloat16),
    )(*parts, last_turned)


SLOTS = 256


def experts_kernel(
    first_expert,
    capacity,
    meta,
    place_rows,
    place_cols,
    gate_rows,
    x_ref,
    g_ref,
    weights,
    y_ref,
    dx_ref,
    grads,
):
    step = pl.program_id(0)
    expert = step + first_expert
    group, width = x_ref.shape
    tail = dx_ref.shape[1] - width

    @pl.when(step == 0)
    def _():
        y_ref[...] = jnp.zeros_like(y_ref)
        dx_ref[...] = jnp.zeros_like(dx_ref)

    column = expert + meta[meta.shape[0] - 1]
    lanes = lax.broadcasted_iota(jnp.int32, place_cols.shape, 1)
    place_col = jnp.sum(jnp.where(lanes == column, place_cols[...], 0), axis=1, keepdims=True)
    place_row = place_rows[pl.ds(column, 1), :]
    gate_row = gate_rows[pl.ds(column, 1), :].astype(jnp.bfloat16).astype(jnp.float32)
    mark = jnp.where(lax.broadcasted_iota(jnp.int32, (1, tail), 1) == column, 1.0, 0.0)

    def run(base, span):
        slots = lax.broadcasted_iota(jnp.int32, (span, group), 0) + base
        hit = slots == place_row
        pick = jnp.where(hit, 1.0, 0.0).astype(jnp.bfloat16)
        scale = jnp.sum(jnp.where(hit, gate_row, 0.0), axis=1, keepdims=True)
        x_taken = jnp.dot(pick, x_ref[...], preferred_element_type=jnp.float32).astype(jnp.bfloat16)
        g_taken = jnp.dot(pick, g_ref[...], preferred_element_type=jnp.float32).astype(jnp.bfloat16)
        gate_pre = jnp.dot(x_taken, weights[0, 0], preferred_element_type=jnp.float32)
        up_pre = jnp.dot(x_taken, weights[0, 1], preferred_element_type=jnp.float32)
        raw = jnp.dot(g_taken, weights[0, 2], preferred_element_type=jnp.float32)
        sig = jax.nn.sigmoid(gate_pre)
        silu = gate_pre * sig
        act = (silu * up_pre).astype(jnp.bfloat16).astype(jnp.float32)
        slot_grad = jnp.sum(act * raw, axis=1, keepdims=True)
        act_grad = raw * scale
        act_scaled = (act * scale).astype(jnp.bfloat16)
        gate_grad = (act_grad * up_pre * sig * (1.0 + gate_pre * (1.0 - sig))).astype(jnp.bfloat16)
        up_grad = (act_grad * silu).astype(jnp.bfloat16)
        extra = (slot_grad * mark).astype(jnp.bfloat16)
        rows_out = contract_last(act_scaled, weights[0, 2]).astype(jnp.bfloat16)
        rows_in = (
            contract_last(gate_grad, weights[0, 0]) + contract_last(up_grad, weights[0, 1])
        ).astype(jnp.bfloat16)
        for slot, left_op, right_op in (
            (0, x_taken, gate_grad),
            (1, x_taken, up_grad),
            (2, g_taken, act_scaled),
        ):
            grad = contract_first(left_op, right_op)
            if base > 0:
                grad = grad + grads[0, slot].astype(jnp.float32)
            grads[0, slot] = grad.astype(jnp.bfloat16)
        block = min(256, group)
        for start in range(0, group, block):
            back = jnp.where(
                lax.broadcasted_iota(jnp.int32, (block, span), 1) + base
                == place_col[start : start + block],
                1.0,
                0.0,
            ).astype(jnp.bfloat16)
            for target, low_col, addend in (
                (y_ref, 0, rows_out),
                (dx_ref, 0, rows_in),
                (dx_ref, width, extra),
            ):
                area = (slice(start, start + block), slice(low_col, low_col + addend.shape[1]))
                target[area] = (
                    target[area].astype(jnp.float32)
                    + jnp.dot(back, addend, preferred_element_type=jnp.float32)
                ).astype(target.dtype)

    run(0, min(SLOTS, capacity))
    for base in range(SLOTS, capacity, SLOTS):
        span = min(SLOTS, -(-(capacity - base) // 16) * 16)

        @pl.when(meta[column] > base)
        def _():
            run(base, span)


def experts_step(meta, place_rows, place_cols, gate_rows, x_rows, g_rows, weights, first, count, skip, capacity):
    group, width = x_rows.shape
    hidden = weights.shape[-1]
    tail = 128

    def whole(shape):
        return pl.BlockSpec(
            shape, lambda step, meta: (0,) * len(shape), pipeline_mode=pl.Buffered(1)
        )

    def big(offset):
        return pl.BlockSpec((1, 3, width, hidden), lambda step, meta: (step + offset, 0, 0, 0))

    return pl.pallas_call(
        functools.partial(experts_kernel, first, capacity),
        grid_spec=pltpu.PrefetchScalarGridSpec(
            num_scalar_prefetch=1,
            grid=(count,),
            in_specs=[
                whole(place_rows.shape),
                whole(place_cols.shape),
                whole(gate_rows.shape),
                whole(x_rows.shape),
                whole(g_rows.shape),
                big(skip),
            ],
            out_specs=[
                whole((group, width)),
                whole((group, width + tail)),
                big(0),
            ],
        ),
        out_shape=[
            jax.ShapeDtypeStruct((group, width), jnp.bfloat16),
            jax.ShapeDtypeStruct((group, width + tail), jnp.bfloat16),
            jax.ShapeDtypeStruct((count, 3, width, hidden), jnp.bfloat16),
        ],
        compiler_params=pltpu.CompilerParams(
            dimension_semantics=("arbitrary",), vmem_limit_bytes=63 << 20
        ),
        cost_estimate=pl.CostEstimate(
            flops=count * 17 * 2 * 408 * width * hidden,
            transcendentals=count * 408 * hidden,
            bytes_accessed=count * 12 * width * hidden,
        ),
    )(meta, place_rows, place_cols, gate_rows, x_rows, g_rows, weights)


def rotate_head(values, cosine, sine, sign):
    half = values.shape[-1] // 2
    other = jnp.concatenate([values[:, half:], values[:, :half]], axis=1)
    return values * cosine + other * (sine * sign)


def segment_bias(seg_row):
    length = seg_row.shape[1]
    shape = (length, length)
    seg_row = seg_row.astype(jnp.float32)
    seg_col = jnp.broadcast_to(seg_row, (128, length)).T[:, :1]
    keys = lax.broadcasted_iota(jnp.int32, shape, 0)
    queries = lax.broadcasted_iota(jnp.int32, shape, 1)
    return jnp.where((keys <= queries) & (seg_col == seg_row), 0.0, masked_value)


def attend_kernel(
    x_ref,
    w_ref,
    seg_row,
    cos_ref,
    sin_ref,
    q_ref,
    k_ref,
    v_ref,
    mixed_ref,
    logsum_ref,
    branch_ref,
    bias,
    v_turned,
    mixed_heads,
):
    heads, kv_heads = q_ref.shape[0], k_ref.shape[0]
    per_kv = heads // kv_heads
    block = SEQ // 2
    edge = (heads + 2 * kv_heads) * HEAD_DIM
    proj = jnp.dot(x_ref[...], w_ref[:, :edge], preferred_element_type=jnp.float32)
    cosine, sine = cos_ref[...], sin_ref[...]
    for head in range(heads + 2 * kv_heads):
        part = proj[:, head * HEAD_DIM : (head + 1) * HEAD_DIM]
        if head < heads:
            q_ref[head] = rotate_head(part, cosine, sine, 1.0).astype(jnp.bfloat16)
        elif head < heads + kv_heads:
            k_ref[head - heads] = rotate_head(part, cosine, sine, 1.0).astype(jnp.bfloat16)
        else:
            v_ref[head - heads - kv_heads] = part.astype(jnp.bfloat16)
            v_turned[head - heads - kv_heads] = part.T.astype(jnp.bfloat16)
    bias[...] = segment_bias(seg_row[0])

    def one_head(head, carry):
        kv = head // per_kv
        for part in range(2):
            span, low = block * (part + 1), block * part
            scores = contract_last(k_ref[kv, :span], q_ref[head, low : low + block]) * attn_scale
            scores = scores + bias[:span, low : low + block]
            top = jnp.max(scores, axis=0, keepdims=True)
            raised = jnp.exp(scores - top)
            total = jnp.sum(raised, axis=0, keepdims=True)
            probs = (raised * (1.0 / total)).astype(jnp.bfloat16)
            turned = jnp.dot(v_turned[kv, :, :span], probs, preferred_element_type=jnp.float32)
            mixed_heads[head, low : low + block, :] = turned.T.astype(jnp.bfloat16)
            logsum_ref[0, pl.ds(head, 1), low : low + block] = top + jnp.log(total)
        return carry

    lax.fori_loop(0, heads, one_head, 0)
    for head in range(heads):
        mixed_ref[:, head * HEAD_DIM : (head + 1) * HEAD_DIM] = mixed_heads[head]
    branch_ref[...] = contract_last(
        mixed_ref[...], w_ref[:, edge : edge + heads * HEAD_DIM]
    ).astype(jnp.bfloat16)


def attend_back_kernel(
    x_ref,
    w_ref,
    seg_row,
    cos_ref,
    sin_ref,
    q_ref,
    k_ref,
    v_ref,
    mixed_ref,
    logsum_ref,
    moe_rows,
    branch_grad,
    dx_ref,
    dw_ref,
    bias,
    k_turned,
    mixed_grads,
    q_grads,
    kv_grads,
    qkv_grad,
    dw_acc,
):
    heads, kv_heads = q_ref.shape[0], k_ref.shape[0]
    per_kv = heads // kv_heads
    block = SEQ // 2
    edge = (heads + 2 * kv_heads) * HEAD_DIM
    step = pl.program_id(0)
    out_edge = edge + heads * HEAD_DIM
    width = x_ref.shape[1]
    grad = jnp.dot(
        branch_grad[:, :width], w_ref[:, edge:out_edge], preferred_element_type=jnp.float32
    ).astype(jnp.bfloat16)
    for head in range(heads):
        mixed_grads[head] = grad[:, head * HEAD_DIM : (head + 1) * HEAD_DIM]
    for kv in range(kv_heads):
        k_turned[kv] = k_ref[kv].astype(jnp.float32).T.astype(jnp.bfloat16)
    bias[...] = segment_bias(seg_row[0])
    kv_grads[...] = jnp.zeros_like(kv_grads)

    def one_head(head, carry):
        kv = head // per_kv
        for part in range(2):
            span, low = block * (part + 1), block * part
            high = low + block
            scores = contract_last(k_ref[kv, :span], q_ref[head, low:high]) * attn_scale
            scores = scores + bias[:span, low:high]
            probs = jnp.exp(scores - logsum_ref[0, pl.ds(head, 1), low:high])
            probs_grad = contract_last(v_ref[kv, :span], mixed_grads[head, low:high])
            inner = jnp.sum(probs * probs_grad, axis=0, keepdims=True)
            score_grad = (probs * (probs_grad - inner)).astype(jnp.bfloat16)
            turned = jnp.dot(k_turned[kv, :, :span], score_grad, preferred_element_type=jnp.float32)
            q_grads[head, low:high, :] = turned.T * attn_scale
            kv_grads[0, kv, :span, :] += jnp.dot(
                score_grad, q_ref[head, low:high], preferred_element_type=jnp.float32
            )
            kv_grads[1, kv, :span, :] += jnp.dot(
                probs.astype(jnp.bfloat16), mixed_grads[head, low:high],
                preferred_element_type=jnp.float32,
            )
        return carry

    lax.fori_loop(0, heads, one_head, 0)
    cosine, sine = cos_ref[...], sin_ref[...]
    for head in range(heads + 2 * kv_heads):
        if head < heads:
            part = rotate_head(q_grads[head], cosine, sine, -1.0)
        elif head < heads + kv_heads:
            part = rotate_head(kv_grads[0, head - heads] * attn_scale, cosine, sine, -1.0)
        else:
            part = kv_grads[1, head - heads - kv_heads]
        qkv_grad[:, head * HEAD_DIM : (head + 1) * HEAD_DIM] = part.astype(jnp.bfloat16)
    dx_ref[...] = contract_last(qkv_grad[...], w_ref[:, :edge]).astype(jnp.bfloat16)
    for low, high, left_op, right_op in (
        (0, edge, x_ref[...], qkv_grad[...]),
        (edge, out_edge, branch_grad[:, :width], mixed_ref[...]),
        (out_edge, dw_acc.shape[1], moe_rows[...], branch_grad[:, width:]),
    ):
        part = contract_first(left_op, right_op)

        @pl.when(step == 0)
        def _():
            dw_acc[:, low:high] = part

        @pl.when(step > 0)
        def _():
            dw_acc[:, low:high] += part

    @pl.when(step == pl.num_programs(0) - 1)
    def _():
        dw_ref[...] = dw_acc[...].astype(jnp.bfloat16)


def fixed(shape):
    return pl.BlockSpec(shape, lambda seq: (0,) * len(shape), pipeline_mode=pl.Buffered(1))


def by_row(width):
    return pl.BlockSpec((SEQ, width), lambda seq: (seq, 0))


def by_head(heads):
    return pl.BlockSpec((heads, SEQ, HEAD_DIM), lambda seq: (0, seq, 0))


def attend_tables():
    half = HEAD_DIM // 2
    positions = np.arange(SEQ, dtype=np.float32)
    frequency = np.float32(rope_base) ** (-np.arange(half, dtype=np.float32) * 2.0 / HEAD_DIM)
    angles = (positions[:, None] * frequency[None, :].astype(np.float32)).astype(np.float32)
    cosine, sine = np.cos(angles), np.sin(angles)
    return (
        jnp.asarray(np.concatenate([cosine, cosine], axis=1)),
        jnp.asarray(np.concatenate([-sine, sine], axis=1)),
    )


def attend(rows, weights, segments, tables, heads, kv_heads):
    group, width = rows.shape
    seqs = group // SEQ
    return pl.pallas_call(
        attend_kernel,
        grid=(seqs,),
        in_specs=[
            by_row(width),
            fixed(weights.shape),
            pl.BlockSpec((1, 1, SEQ), lambda seq: (seq, 0, 0)),
            fixed(tables[0].shape),
            fixed(tables[1].shape),
        ],
        out_specs=[
            by_head(heads),
            by_head(kv_heads),
            by_head(kv_heads),
            by_row(heads * HEAD_DIM),
            pl.BlockSpec((1, heads, SEQ), lambda seq: (seq, 0, 0)),
            by_row(width),
        ],
        out_shape=[
            jax.ShapeDtypeStruct((heads, group, HEAD_DIM), jnp.bfloat16),
            jax.ShapeDtypeStruct((kv_heads, group, HEAD_DIM), jnp.bfloat16),
            jax.ShapeDtypeStruct((kv_heads, group, HEAD_DIM), jnp.bfloat16),
            jax.ShapeDtypeStruct((group, heads * HEAD_DIM), jnp.bfloat16),
            jax.ShapeDtypeStruct((seqs, heads, SEQ), jnp.float32),
            jax.ShapeDtypeStruct((group, width), jnp.bfloat16),
        ],
        scratch_shapes=[
            pltpu.VMEM((SEQ, SEQ), jnp.float32),
            pltpu.VMEM((kv_heads, HEAD_DIM, SEQ), jnp.bfloat16),
            pltpu.VMEM((heads, SEQ, HEAD_DIM), jnp.bfloat16),
        ],
        compiler_params=pltpu.CompilerParams(
            dimension_semantics=("arbitrary",), vmem_limit_bytes=56 << 20
        ),
        cost_estimate=pl.CostEstimate(
            flops=10_000_000_000, transcendentals=3_000_000, bytes_accessed=60_000_000
        ),
    )(rows, weights, segments[:, None, :], *tables)


def attend_back(rows, weights, segments, tables, kept, moe_rows, branch_grad):
    queries, keys, values, mixed, logsum = kept
    group, width = rows.shape
    heads, kv_heads = queries.shape[0], keys.shape[0]
    used = weights.shape[1]
    edge = (heads + 2 * kv_heads) * HEAD_DIM
    return pl.pallas_call(
        attend_back_kernel,
        grid=(group // SEQ,),
        in_specs=[
            by_row(width),
            fixed(weights.shape),
            pl.BlockSpec((1, 1, SEQ), lambda seq: (seq, 0, 0)),
            fixed(tables[0].shape),
            fixed(tables[1].shape),
            by_head(heads),
            by_head(kv_heads),
            by_head(kv_heads),
            by_row(heads * HEAD_DIM),
            pl.BlockSpec((1, heads, SEQ), lambda seq: (seq, 0, 0)),
            by_row(width),
            by_row(branch_grad.shape[1]),
        ],
        out_specs=[by_row(width), fixed((width, used))],
        out_shape=[
            jax.ShapeDtypeStruct((group, width), jnp.bfloat16),
            jax.ShapeDtypeStruct((width, used), jnp.bfloat16),
        ],
        scratch_shapes=[
            pltpu.VMEM((SEQ, SEQ), jnp.float32),
            pltpu.VMEM((kv_heads, HEAD_DIM, SEQ), jnp.bfloat16),
            pltpu.VMEM((heads, SEQ, HEAD_DIM), jnp.bfloat16),
            pltpu.VMEM((heads, SEQ, HEAD_DIM), jnp.float32),
            pltpu.VMEM((2, kv_heads, SEQ, HEAD_DIM), jnp.float32),
            pltpu.VMEM((SEQ, edge), jnp.bfloat16),
            pltpu.VMEM((width, used), jnp.float32),
        ],
        compiler_params=pltpu.CompilerParams(
            dimension_semantics=("arbitrary",), vmem_limit_bytes=60 << 20
        ),
        cost_estimate=pl.CostEstimate(
            flops=20_000_000_000, transcendentals=3_000_000, bytes_accessed=100_000_000
        ),
    )(rows, weights, segments[:, None, :], *tables,
      queries, keys, values, mixed, logsum, moe_rows, branch_grad)


def widen_kernel(edges, *refs):
    step = pl.program_id(0)
    packed, targets = refs[:-3], refs[-3:]
    for part, low, high in zip(packed, edges[:-1], edges[1:]):

        @pl.when((step >= low) & (step < high))
        def _():
            for slot, target in enumerate(targets):
                target[0] = part[0, slot].astype(jnp.float32)


def widen(packed, edges):
    _, _, rows, width = packed[0].shape

    def home(low, high):
        return pl.BlockSpec(
            (1, 3, rows, width),
            lambda step: (jnp.clip(step - low, 0, high - low - 1), 0, 0, 0),
        )

    return pl.pallas_call(
        functools.partial(widen_kernel, edges),
        grid=(edges[-1],),
        in_specs=[home(low, high) for low, high in zip(edges[:-1], edges[1:])],
        out_specs=[pl.BlockSpec((1, rows, width), lambda step: (step, 0, 0))] * 3,
        out_shape=[jax.ShapeDtypeStruct((edges[-1], rows, width), jnp.float32)] * 3,
    )(*packed)


RUNS = (0, 7, 10)
DIRECT = (2, 1)


def local(
    emb,
    segment_ids,
    routes,
    norm1_gain,
    w_query,
    w_key,
    w_value,
    w_out,
    norm2_gain,
    w_router,
    w_gate,
    w_up,
    w_down,
    cotangent,
):
    local_rows, width = emb.shape
    tp_count, tp_index = lax.axis_size("tp"), lax.axis_index("tp")
    experts_here = w_gate.shape[0]
    expert_count = w_router.shape[1]
    q_width, kv_width = w_query.shape[1], w_key.shape[1]
    used = 2 * (q_width + kv_width)
    group_size = local_rows * tp_count
    fsdp_count = lax.axis_size("fsdp")
    split = group_size <= 1024
    runs = [edge * experts_here // RUNS[-1] for edge in RUNS] if split else [0, experts_here]
    stacks = (w_gate, w_up, w_down)
    pieces = [lax.all_gather(pack(stacks, 0, runs[1]), "fsdp", axis=2, tiled=True)]
    gain_one = norm1_gain.astype(jnp.float32)[None, :]
    gain_two = norm2_gain.astype(jnp.float32)[None, :]
    group_rows, mask, place_cols, place_rows, counts, attn_w, *packed = norm_gather(
        emb,
        gain_one,
        routes,
        join([w_query, w_key, w_value, w_out], w_router.T, used + 128),
        stacks,
        runs[1] if split else 0,
        tp_count,
        fsdp_count,
        0,
    )
    if split:
        pieces.append(lax.all_gather(packed[0], "fsdp", axis=2, tiled=True))
    capacity = group_size * routes.shape[1] // expert_count * 2
    meta = jnp.concatenate([counts[0], (tp_index * experts_here)[None]])

    tables = attend_tables()
    heads_here, kv_here = q_width // HEAD_DIM, kv_width // HEAD_DIM
    *kept, branch_part = attend(group_rows, attn_w, segment_ids, tables, heads_here, kv_here)
    mid_x, moe_rows, gate_rows, own_gates, moe_grad_rows = find_mid(
        branch_part, emb, gain_two, attn_w, used, mask, cotangent, tp_count, 1
    )

    outs = []
    for first, last, piece in zip(runs[:-1], runs[1:], pieces):
        outs.append(
            experts_step(
                meta,
                place_rows,
                place_cols,
                gate_rows,
                moe_rows,
                moe_grad_rows,
                piece,
                first,
                last - first,
                0,
                capacity,
            )
        )
    grad_sums = [lax.psum_scatter(outs[0][2], "fsdp", scatter_dimension=2, tiled=True)]
    last_grads = outs[-1][2]
    picks = (tuple(range(DIRECT[0])), tuple(range(DIRECT[0], sum(DIRECT)))) if split else ((), ())
    out, mid_grad, gain_two_grad, sent, *mid_sums = find_mid_grad(
        [part[1] for part in outs],
        [part[0] for part in outs],
        mid_x,
        cotangent,
        own_gates,
        gain_two,
        attn_w,
        used,
        last_grads,
        picks[0],
        tp_count,
        fsdp_count,
        2,
    )
    dx_one, attn_grads = attend_back(
        group_rows, attn_w, segment_ids, tables, kept, moe_rows, sent
    )
    grad_emb, attn_sum, gain_sums, *end_sums = finish(
        dx_one, attn_grads, emb, gain_one, mid_grad, gain_two_grad, last_grads, picks[1], 3
    )
    grad_sums = grad_sums + mid_sums + end_sums
    ends = [0]
    for part in grad_sums:
        ends.append(ends[-1] + part.shape[0])
    expert_sums = widen(grad_sums, ends)
    return (
        out,
        grad_emb,
        gain_sums[0],
        attn_sum[:, :q_width],
        attn_sum[:, q_width : q_width + kv_width],
        attn_sum[:, q_width + kv_width : q_width + 2 * kv_width],
        attn_sum[:, q_width + 2 * kv_width : used],
        gain_sums[1],
        attn_sum[:, used : used + expert_count],
        *expert_sums,
    )


def solution(mesh):
    return jax.shard_map(
        local,
        mesh=mesh,
        in_specs=(
            P(("fsdp", "tp"), None),
            P("fsdp", None),
            P("fsdp", None),
            P(),
            P("fsdp", "tp"),
            P("fsdp", "tp"),
            P("fsdp", "tp"),
            P("fsdp", "tp"),
            P(),
            P("fsdp", None),
            P("tp", "fsdp", None),
            P("tp", "fsdp", None),
            P("tp", "fsdp", None),
            P(("fsdp", "tp"), None),
        ),
        out_specs=(
            P(("fsdp", "tp"), None),
            P(("fsdp", "tp"), None),
            P(),
            P("fsdp", "tp"),
            P("fsdp", "tp"),
            P("fsdp", "tp"),
            P("fsdp", "tp"),
            P(),
            P("fsdp", None),
            P("tp", "fsdp", None),
            P("tp", "fsdp", None),
            P("tp", "fsdp", None),
        ),
        check_vma=False,
    )
```

```python
import functools

import jax
import jax.numpy as jnp
import numpy as np
from jax import lax
from jax.experimental import pallas as pl
from jax.experimental.pallas import tpu as pltpu
from jax.sharding import PartitionSpec as P

HEAD_DIM = 64
SEQ = 512


emb_scale = 12.0
resid_scale = 0.22
attn_scale = 0.015625
norm_eps = 1e-06
rope_base = 10000.0
masked_value = -1e30


def contract_last(left_op, right_op):
    return lax.dot_general(
        left_op, right_op, (((1,), (1,)), ((), ())), preferred_element_type=jnp.float32
    )


def contract_first(left_op, right_op):
    return lax.dot_general(
        left_op, right_op, (((0,), (0,)), ((), ())), preferred_element_type=jnp.float32
    )


def line_signal(barrier, me, count):
    @pl.when(me > 0)
    def _():
        pl.semaphore_signal(barrier, inc=1, device_id={"tp": me - 1})

    @pl.when(me < count - 1)
    def _():
        pl.semaphore_signal(barrier, inc=1, device_id={"tp": me + 1})

    return jnp.where((me > 0) & (me < count - 1), 2, 1)


class Plane:
    def __init__(self, count):
        self.me = lax.axis_index("fsdp")
        self.core = lax.rem(self.me, 2)
        self.chip = lax.div(self.me, 2)
        self.chips = count // 2
        self.partner = self.me + 1 - 2 * self.core

    def chip_at(self, shift):
        return lax.rem(self.chip + shift + self.chips, self.chips)

    def peer(self, shift):
        return self.chip_at(shift) * 2 + self.core

    def signal(self, barrier):
        for shift in range(1, self.chips):
            pl.semaphore_signal(barrier, inc=1, device_id={"fsdp": self.peer(shift)})
        pl.semaphore_signal(barrier, inc=1, device_id={"fsdp": self.partner})
        return self.chips


def rows_of(ref, index, rows):
    return ref.at[pl.ds(pl.multiple_of(index * rows, rows), rows)]


class LineGather:
    def __init__(self, count, o_ref, send_sem, recv_sem):
        self.count, self.o_ref = count, o_ref
        self.send_sem, self.recv_sem = send_sem, recv_sem
        self.rows = o_ref.shape[0] // count
        me = self.me = lax.axis_index("tp")
        steps = range(count - 1)
        self.sends = [
            [(me >= step) & (me < count - 1) for step in steps],
            [(me + step < count) & (me > 0) for step in steps],
        ]
        self.gets = [
            [me - 1 - step >= 0 for step in steps],
            [me + 1 + step < count for step in steps],
        ]

    def hop(self, way, step, chunk):
        part = rows_of(self.o_ref, chunk, self.rows)
        return pltpu.make_async_remote_copy(
            src_ref=part,
            dst_ref=part,
            send_sem=self.send_sem.at[way, step],
            recv_sem=self.recv_sem.at[way, step],
            device_id={"tp": self.me + 1 if way == 0 else self.me - 1},
        )

    def start(self, step):
        @pl.when(self.sends[0][step])
        def _():
            self.hop(0, step, self.me - step).start()

        @pl.when(self.sends[1][step])
        def _():
            self.hop(1, step, self.me + step).start()

    def arrive(self, step):
        @pl.when(self.gets[0][step])
        def _():
            self.hop(0, step, self.me - 1 - step).wait_recv()

        @pl.when(self.gets[1][step])
        def _():
            self.hop(1, step, self.me + 1 + step).wait_recv()

    def finish(self):
        for step in range(self.count - 1):

            @pl.when(self.sends[0][step])
            def _():
                self.hop(0, step, self.me - step).wait_send()

            @pl.when(self.sends[1][step])
            def _():
                self.hop(1, step, self.me + step).wait_send()


def line_sems(count):
    return [
        pltpu.SemaphoreType.DMA((2, count - 1)),
        pltpu.SemaphoreType.DMA((2, count - 1)),
    ]


class PlaneGather:
    def __init__(self, plane, w_ref, wo_ref, out_send, out_recv, on_send, on_recv, kept_sem):
        self.plane, self.w_ref, self.wo_ref = plane, w_ref, wo_ref
        self.out_send, self.out_recv = out_send, out_recv
        self.on_send, self.on_recv = on_send, on_recv
        self.rows = w_ref.shape[0]
        self.kept = pltpu.make_async_copy(w_ref, rows_of(wo_ref, plane.me, self.rows), kept_sem)

    def outward(self, shift, target, source_device):
        return pltpu.make_async_remote_copy(
            src_ref=self.w_ref,
            dst_ref=rows_of(self.wo_ref, source_device, self.rows),
            send_sem=self.out_send.at[shift],
            recv_sem=self.out_recv.at[shift],
            device_id={"fsdp": target},
        )

    def onward(self, shift, source_device):
        part = rows_of(self.wo_ref, source_device, self.rows)
        return pltpu.make_async_remote_copy(
            src_ref=part,
            dst_ref=part,
            send_sem=self.on_send.at[shift - 1],
            recv_sem=self.on_recv.at[shift - 1],
            device_id={"fsdp": self.plane.partner},
        )

    def start(self):
        plane = self.plane
        for shift in range(1, plane.chips):
            self.outward(shift, plane.peer(shift), plane.me).start()
        self.outward(0, plane.partner, plane.me).start()
        self.kept.start()

    def forward(self):
        plane = self.plane
        for shift in range(1, plane.chips):
            self.outward(shift, plane.peer(shift), plane.peer(-shift)).wait_recv()
            self.onward(shift, plane.peer(-shift)).start()

    def finish(self):
        plane = self.plane
        self.outward(0, plane.partner, plane.partner).wait_recv()
        for shift in range(1, plane.chips):
            self.onward(shift, plane.chip_at(-shift) * 2 + 1 - plane.core).wait_recv()
        for shift in range(1, plane.chips):
            self.outward(shift, plane.peer(shift), plane.me).wait_send()
            self.onward(shift, plane.peer(-shift)).wait_send()
        self.outward(0, plane.partner, plane.me).wait_send()
        self.kept.wait()


class ExpertSums:
    NEAR = {0: (1, 0), 1: (3, 0), 2: (2, 1), 3: (3, 1), 4: (2, 0), 5: (1, 1)}

    def __init__(self, plane, picks, grads_ref, out_ref, *refs):
        self.plane, self.picks, self.grads_ref, self.out_ref = plane, picks, grads_ref, out_ref
        (
            self.got, self.own, self.hop_got, self.held,
            self.pair_send, self.pair_recv, self.own_sem,
            self.hop_send, self.hop_recv, self.put_sem,
        ) = refs
        self.rows = out_ref.shape[2]
        self.half = self.rows // 2

    def chip_by(self, way):
        chip = self.plane.chip
        low, high = lax.rem(chip, 2), lax.div(chip, 2)
        if way % 2:
            low = 1 - low
        if way >= 2:
            high = 1 - high
        return high * 2 + low

    def area(self, index, dest):
        low = pl.multiple_of(dest * self.rows, self.rows)
        return self.grads_ref.at[self.picks[index], :, pl.ds(low, self.rows)]

    def part(self, index, way, half):
        return self.own.at[index, way, :, pl.ds(half * self.half, self.half)]

    def to_pair(self, index, way):
        return pltpu.make_async_remote_copy(
            src_ref=self.area(index, self.chip_by(way) * 2 + 1 - self.plane.core),
            dst_ref=self.got.at[index, way],
            send_sem=self.pair_send.at[index, way],
            recv_sem=self.pair_recv.at[index, way],
            device_id={"fsdp": self.plane.partner},
        )

    def keep(self, index, way):
        return pltpu.make_async_copy(
            self.area(index, self.chip_by(way) * 2 + self.plane.core),
            self.own.at[index, way],
            self.own_sem.at[index, way],
        )

    def hop(self, index, slot):
        way, half = self.NEAR[slot]
        source = self.part(index, way, half) if slot < 4 else self.hop_got.at[index, 2 * slot - 7]
        target = (1, 1, 2, 2, 2, 1)[slot]
        return pltpu.make_async_remote_copy(
            src_ref=source,
            dst_ref=self.hop_got.at[index, slot],
            send_sem=self.hop_send.at[index, slot],
            recv_sem=self.hop_recv.at[index, slot],
            device_id={"fsdp": self.chip_by(target) * 2 + self.plane.core},
        )

    def put(self, index):
        return pltpu.make_async_copy(
            self.held.at[index], self.out_ref.at[index], self.put_sem.at[index]
        )

    def begin(self, index):
        for way in (3, 1, 2, 0):
            self.to_pair(index, way).start()
            self.keep(index, way).start()

    def both_cores(self, index, way):
        self.to_pair(index, way).wait_recv()
        self.keep(index, way).wait()
        for slot in range(self.own.shape[2]):
            both = self.own[index, way, slot].astype(jnp.float32) + self.got[
                index, way, slot
            ].astype(jnp.float32)
            self.own[index, way, slot] = both.astype(jnp.bfloat16)

    def items(self):
        count = len(self.picks)
        order = []
        for index in range(count + 1):
            if index < count:
                order += [(index, 0), (index, 1)]
            if index > 0:
                order += [(index - 1, 2), (index - 1, 3)]
        return order

    def do(self, index, stage):
        if stage == 0:
            self.both_cores(index, 3)
            self.hop(index, 1).start()
            self.hop(index, 3).start()
        elif stage == 1:
            self.both_cores(index, 1)
            self.hop(index, 0).start()
            self.both_cores(index, 2)
            self.hop(index, 2).start()
        elif stage == 2:
            for slot in (4, 5):
                behind = 2 * slot - 7
                way, half = self.NEAR[slot]
                self.hop(index, behind).wait_recv()
                for layer in range(self.own.shape[2]):
                    mine = self.own[
                        index, way, layer, half * self.half : (half + 1) * self.half, :
                    ].astype(jnp.float32)
                    total = mine + self.hop_got[index, behind, layer].astype(jnp.float32)
                    self.hop_got[index, behind, layer] = total.astype(jnp.bfloat16)
                self.hop(index, slot).start()
        else:
            self.both_cores(index, 0)

    def collect(self, index):
        for half, slots in ((0, (0, 4)), (1, (2, 5))):
            area = slice(half * self.half, (half + 1) * self.half)
            for slot in slots:
                self.hop(index, slot).wait_recv()
            for layer in range(self.own.shape[2]):
                total = self.own[index, 0, layer, area, :].astype(jnp.float32)
                for slot in slots:
                    total = total + self.hop_got[index, slot, layer].astype(jnp.float32)
                self.held[index, layer, area, :] = total.astype(jnp.bfloat16)
        self.put(index).start()

    def finish(self):
        for index in range(len(self.picks)):
            self.put(index).wait()
            for way in range(4):
                self.to_pair(index, way).wait_send()
            for slot in range(6):
                self.hop(index, slot).wait_send()


def expert_buffers(count, rows, width):
    if count == 0:
        return []
    return [
        pltpu.VMEM((count, 4, 3, rows, width), jnp.bfloat16),
        pltpu.VMEM((count, 4, 3, rows, width), jnp.bfloat16),
        pltpu.VMEM((count, 6, 3, rows // 2, width), jnp.bfloat16),
        pltpu.VMEM((count, 3, rows, width), jnp.bfloat16),
        pltpu.SemaphoreType.DMA((count, 4)),
        pltpu.SemaphoreType.DMA((count, 4)),
        pltpu.SemaphoreType.DMA((count, 4)),
        pltpu.SemaphoreType.DMA((count, 6)),
        pltpu.SemaphoreType.DMA((count, 6)),
        pltpu.SemaphoreType.DMA((count,)),
    ]


class LineScatter:
    def __init__(self, count, x_refs, o_ref, recv, send_sem, recv_sem):
        self.count, self.x_refs, self.o_ref, self.recv = count, x_refs, o_ref, recv
        self.send_sem, self.recv_sem = send_sem, recv_sem
        self.rows = o_ref.shape[0]
        me = self.me = lax.axis_index("tp")
        self.behind = (me, count - 1 - me)
        self.has_next = (me < count - 1, me > 0)
        self.has_prev = (me > 0, me < count - 1)

    def block(self, dest):
        area = pl.ds(pl.multiple_of(dest * self.rows, self.rows), self.rows)
        total = self.x_refs[0][area, :].astype(jnp.float32)
        for x_ref in self.x_refs[1:]:
            total = total + x_ref[area, :].astype(jnp.float32)
        return total

    def hop(self, way, step, source):
        return pltpu.make_async_remote_copy(
            src_ref=source,
            dst_ref=self.recv.at[way, step],
            send_sem=self.send_sem.at[way, step],
            recv_sem=self.recv_sem.at[way, step],
            device_id={"tp": self.me + 1 if way == 0 else self.me - 1},
        )

    def start(self, step):
        count, me, recv = self.count, self.me, self.recv
        for way in range(2):
            dest = count - 1 - step + me if way == 0 else step - (count - 1 - me)
            active = self.has_next[way] & (step >= self.behind[way])

            @pl.when(active & (self.behind[way] == 0))
            def _():
                part = rows_of(self.x_refs[0], dest, self.rows)
                if len(self.x_refs) > 1:
                    part[...] = self.block(dest).astype(part.dtype)
                self.hop(way, step, part).start()

            if step > 0:

                @pl.when(active & (self.behind[way] > 0))
                def _():
                    total = self.block(dest) + recv[way, step - 1].astype(jnp.float32)
                    recv[way, step - 1] = total.astype(recv.dtype)
                    self.hop(way, step, recv.at[way, step - 1]).start()

    def arrive(self, step):
        for way in range(2):

            @pl.when(self.has_prev[way] & (step >= self.behind[way] - 1))
            def _():
                self.hop(way, step, self.recv.at[way, step]).wait_recv()

    def collect(self):
        self.o_ref[...] = self.block(self.me)
        for way in range(2):

            @pl.when(self.has_prev[way])
            def _():
                self.o_ref[...] += self.recv[way, self.count - 2].astype(jnp.float32)

    def finish(self):
        for step in range(self.count - 1):
            for way in range(2):

                @pl.when(self.has_next[way] & (step >= self.behind[way]))
                def _():
                    self.hop(way, step, self.recv.at[way, step]).wait_send()


def line_buffers(count, rows, width):
    return [pltpu.VMEM((2, count - 1, rows, width), jnp.bfloat16)] + line_sems(count)


def own_rows(ref, rows):
    return pl.ds(pl.multiple_of(lax.axis_index("tp") * rows, rows), rows)


def inverse_norm(values):
    return lax.rsqrt(jnp.mean(values * values, axis=-1, keepdims=True) + norm_eps)


def rms_back(incoming, values, gain_row):
    inverse = inverse_norm(values)
    scaled = values * inverse
    gain_grad = jnp.sum(incoming * scaled, axis=0, keepdims=True)
    weighted = incoming * gain_row
    row_inner = jnp.mean(weighted * scaled, axis=-1, keepdims=True)
    return inverse * (weighted - scaled * row_inner), gain_grad


def enter_kernel(count, plane=None):
    barrier = pltpu.get_barrier_semaphore()
    waits = line_signal(barrier, lax.axis_index("tp"), count)
    if plane is not None:
        waits = waits + plane.signal(barrier)
    pl.semaphore_wait(barrier, waits)


def remote_params(ident, limit=60):
    return pltpu.CompilerParams(
        collective_id=ident, has_side_effects=True, vmem_limit_bytes=limit << 20
    )


IN_VMEM = pl.BlockSpec(memory_space=pltpu.VMEM)
IN_PLACE = pl.BlockSpec(memory_space=pl.ANY)
TRANSFER = pl.CostEstimate(flops=0, transcendentals=0, bytes_accessed=150_000_000)


def norm_gather_kernel(count, fsdp_count, low, *refs):
    emb_ref, gain_ref, routes_ref, w_ref, *refs = refs
    stacks, refs = (refs[:3], refs[3:]) if low else ((), refs)
    rows_ref, mask_ref, cols_ref, turned_ref, counts_ref, wo_ref, *refs = refs
    packed, refs = (refs[0], refs[1:]) if low else (None, refs)
    row_send, row_recv, *refs = refs
    plane = Plane(fsdp_count)
    if low:
        held, in_sem, out_sem = refs[5:]
        gets, puts = pack_copies(low, stacks, packed, held, in_sem, out_sem)
        for get in gets:
            get.start()
    enter_kernel(count, plane)
    line = LineGather(count, rows_ref, row_send, row_recv)
    weights = PlaneGather(plane, w_ref, wo_ref, *refs[:5])
    start_x = emb_ref[...].astype(jnp.float32) * emb_scale
    normed = start_x * inverse_norm(start_x) * gain_ref[...]
    rows_ref[own_rows(rows_ref, line.rows), :] = normed.astype(jnp.bfloat16)
    for step in range(count - 1):
        line.start(step)
        if step == 0:
            weights.start()
            place_routes(line.rows, routes_ref, mask_ref, cols_ref, turned_ref, counts_ref)
            if low:
                for get, put in zip(gets, puts):
                    get.wait()
                    put.start()
        if step == count - 2:
            weights.forward()
        line.arrive(step)
    if low:
        for put in puts:
            put.wait()
    weights.finish()
    line.finish()


def place_routes(rows, routes_ref, mask_ref, cols_ref, turned_ref, counts_ref):
    group, lanes = mask_ref.shape
    columns = lax.broadcasted_iota(jnp.int32, (rows, lanes), 1)
    for low in range(0, group, rows):
        area = slice(low, low + rows)
        mask = jnp.zeros((rows, lanes), jnp.float32)
        for choice in range(routes_ref.shape[1]):
            mask = jnp.where(routes_ref[area, choice : choice + 1] == columns, 1.0, mask)
        mask_ref[area, :] = mask
    counts_ref[...] = jnp.sum(mask_ref[...], axis=0, keepdims=True).astype(jnp.int32)
    member = mask_ref[...].astype(jnp.bfloat16)
    for low in range(0, group, rows):
        area = slice(low, low + rows)
        here = lax.broadcasted_iota(jnp.int32, (rows, group), 0) + low
        earlier = here > lax.broadcasted_iota(jnp.int32, (rows, group), 1)
        ranks = jnp.dot(
            jnp.where(earlier, 1.0, 0.0).astype(jnp.bfloat16),
            member,
            preferred_element_type=jnp.float32,
        )
        places = jnp.where(mask_ref[area, :] > 0.0, ranks, -1.0)
        cols_ref[area, :] = places.astype(jnp.int32)
        turned_ref[:, area] = places.T.astype(jnp.int32)


def norm_gather(emb, gain_row, routes, weights, stacks, low, count, fsdp_count, ident):
    rows, width = emb.shape
    group = rows * count
    chips = fsdp_count // 2
    experts, share, hidden = stacks[0].shape
    span = experts - low
    outs = [
        jax.ShapeDtypeStruct((group, width), jnp.bfloat16),
        jax.ShapeDtypeStruct((group, 128), jnp.float32),
        jax.ShapeDtypeStruct((group, 128), jnp.int32),
        jax.ShapeDtypeStruct((128, group), jnp.int32),
        jax.ShapeDtypeStruct((1, 128), jnp.int32),
        jax.ShapeDtypeStruct((weights.shape[0] * fsdp_count, weights.shape[1]), jnp.bfloat16),
    ]
    scratch = line_sems(count) + [
        pltpu.SemaphoreType.DMA((chips,)),
        pltpu.SemaphoreType.DMA((chips,)),
        pltpu.SemaphoreType.DMA((chips - 1,)),
        pltpu.SemaphoreType.DMA((chips - 1,)),
        pltpu.SemaphoreType.DMA,
    ]
    if low:
        outs.append(jax.ShapeDtypeStruct((span, 3, share, hidden), jnp.bfloat16))
        scratch += [
            pltpu.VMEM((3, span, share, hidden), jnp.bfloat16),
            pltpu.SemaphoreType.DMA((3,)),
            pltpu.SemaphoreType.DMA((3,)),
        ]
    return pl.pallas_call(
        functools.partial(norm_gather_kernel, count, fsdp_count, low),
        out_shape=outs,
        in_specs=[IN_VMEM] * 4 + [IN_PLACE] * (3 if low else 0),
        out_specs=[IN_VMEM] * 5 + [IN_PLACE] * (len(outs) - 5),
        scratch_shapes=scratch,
        compiler_params=remote_params(ident, 48),
        cost_estimate=TRANSFER,
    )(emb, gain_row, routes, weights, *(stacks if low else ()))


def mid_kernel(
    count, part_ref, emb_ref, gain_ref, router_ref, mask_ref, cotangent_ref,
    mid_ref, rows_ref, gates_ref, own_gates, moe_grads,
    recv, sum_send, sum_recv, row_send, row_recv, grad_send, grad_recv,
):
    enter_kernel(count)
    total = LineScatter(count, [part_ref], mid_ref, recv, sum_send, sum_recv)
    line = LineGather(count, rows_ref, row_send, row_recv)
    others = LineGather(count, moe_grads, grad_send, grad_recv)
    rows = line.rows
    moe_grads[own_rows(moe_grads, rows), :] = (
        resid_scale * cotangent_ref[...].astype(jnp.float32)
    ).astype(jnp.bfloat16)
    for step in range(count):
        if step < count - 1:
            others.start(step)
        if step > 0:
            total.start(step - 1)
        if step < count - 1:
            others.arrive(step)
        if step > 0:
            total.arrive(step - 1)
    total.collect()
    mid = emb_ref[...].astype(jnp.float32) * emb_scale + resid_scale * mid_ref[...]
    mid_ref[...] = mid
    own = own_rows(rows_ref, rows)
    rows_ref[own, :] = (mid * inverse_norm(mid) * gain_ref[...]).astype(jnp.bfloat16)

    def find_gates(chunk):
        area = pl.ds(pl.multiple_of(chunk * rows, rows), rows)
        logits = jnp.dot(rows_ref[area, :], router_ref[...], preferred_element_type=jnp.float32)
        inside = mask_ref[area, :] > 0.0
        top = jnp.max(jnp.where(inside, logits, masked_value), axis=-1, keepdims=True)
        raised = jnp.where(inside, jnp.exp(jnp.where(inside, logits - top, 0.0)), 0.0)
        gates = raised / jnp.sum(raised, axis=-1, keepdims=True)
        gates_ref[:, area] = gates.T
        return gates

    for step in range(count - 1):
        line.start(step)
        if step == 0:
            own_gates[...] = find_gates(line.me)
        line.arrive(step)

        @pl.when(line.gets[0][step])
        def _():
            find_gates(line.me - 1 - step)

        @pl.when(line.gets[1][step])
        def _():
            find_gates(line.me + 1 + step)

    line.finish()
    total.finish()
    others.finish()


def find_mid(part, emb, gain_row, weights, used, mask, cotangent, count, ident):
    rows, width = emb.shape
    group = rows * count
    return pl.pallas_call(
        functools.partial(mid_kernel, count),
        grid=(1,),
        out_shape=[
            jax.ShapeDtypeStruct((rows, width), jnp.float32),
            jax.ShapeDtypeStruct((group, width), jnp.bfloat16),
            jax.ShapeDtypeStruct((128, group), jnp.float32),
            jax.ShapeDtypeStruct((rows, 128), jnp.float32),
            jax.ShapeDtypeStruct((group, width), jnp.bfloat16),
        ],
        in_specs=[
            IN_VMEM,
            IN_VMEM,
            IN_VMEM,
            pl.BlockSpec((width, 128), lambda step: (0, used // 128)),
            IN_VMEM,
            IN_VMEM,
        ],
        out_specs=[IN_VMEM] * 5,
        scratch_shapes=line_buffers(count, rows, width) + line_sems(count) + line_sems(count),
        compiler_params=remote_params(ident),
        cost_estimate=TRANSFER,
    )(part, emb, gain_row, weights, mask, cotangent)


def moe_back_kernel(count, fsdp_count, runs, picks, *refs):
    dx_refs, y_refs, refs = refs[:runs], refs[runs : 2 * runs], refs[2 * runs :]
    mid_ref, cotangent_ref, own_gates, gain_ref, router_ref, *refs = refs
    grads_ref, refs = (refs[0], refs[1:]) if picks else (None, refs)
    out_ref, mid_grad, gain_grad, sent_ref, *refs = refs
    sums_ref, refs = (refs[0], refs[1:]) if picks else (None, refs)
    (
        dx_parts, y_parts, load_sem, sum_ref, moe_ref,
        recv, sum_send, sum_recv, moe_recv, moe_send, moe_recv_sem, row_send, row_recv, *refs,
    ) = refs
    loads = []
    for index, (source, parts) in enumerate(
        [(ref, dx_parts) for ref in dx_refs] + [(ref, y_parts) for ref in y_refs]
    ):
        loads.append(
            pltpu.make_async_copy(source, parts.at[index % runs], load_sem.at[index])
        )
        loads[-1].start()
    plane = Plane(fsdp_count) if picks else None
    enter_kernel(count, plane)
    total = LineScatter(
        count, [dx_parts.at[run] for run in range(runs)], sum_ref, recv, sum_send, sum_recv
    )
    moe = LineScatter(
        count, [y_parts.at[run] for run in range(runs)], moe_ref, moe_recv, moe_send, moe_recv_sem
    )
    line = LineGather(count, sent_ref, row_send, row_recv)
    experts = ExpertSums(plane, picks, grads_ref, sums_ref, *refs) if picks else None
    rows, width = mid_ref.shape
    for index in range(len(picks)):
        experts.begin(index)
    for load in loads[:runs]:
        load.wait()
    items = experts.items() if picks else []
    each = -(-len(items) // (2 * count - 2))
    for step in range(count - 1):
        total.start(step)
        for item in items[step * each : (step + 1) * each]:
            experts.do(*item)
        total.arrive(step)
    items = items[(count - 1) * each :]
    total.collect()
    gates = own_gates[...]
    gates_grad = sum_ref[:, width:]
    gates_inner = jnp.sum(gates * gates_grad, axis=-1, keepdims=True)
    logits_grad = (gates * (gates_grad - gates_inner)).astype(jnp.bfloat16)
    incoming = sum_ref[:, :width] + contract_last(logits_grad, router_ref[...])
    from_norm, gain_part = rms_back(incoming, mid_ref[...], gain_ref[...])
    grad = cotangent_ref[...].astype(jnp.float32) + from_norm
    mid_grad[...] = grad
    gain_grad[...] = gain_part
    own = own_rows(sent_ref, rows)
    sent_ref[own, :width] = (resid_scale * grad).astype(jnp.bfloat16)
    sent_ref[own, width:] = logits_grad
    for load in loads[runs:]:
        load.wait()
    for step in range(count):
        if step < count - 1:
            line.start(step)
        if step > 0:
            moe.start(step - 1)
        for item in items[step * each : (step + 1) * each]:
            experts.do(*item)
        if step < count - 1:
            line.arrive(step)
        if step > 0:
            moe.arrive(step - 1)
    moe.collect()
    out_ref[...] = (mid_ref[...] + resid_scale * moe_ref[...]).astype(out_ref.dtype)
    for index in range(len(picks)):
        experts.collect(index)
    line.finish()
    total.finish()
    moe.finish()
    if picks:
        experts.finish()


def find_mid_grad(
    dx_parts, y_parts, mid, cotangent, own_gates, gain_row, weights, used, grads, picks,
    count, fsdp_count, ident,
):
    rows, width = mid.shape
    runs, group = len(dx_parts), rows * count
    wide = dx_parts[0].shape[1]
    share = grads.shape[2] // fsdp_count
    sums = [jax.ShapeDtypeStruct((len(picks), 3, share, grads.shape[3]), jnp.bfloat16)]
    sums = sums if picks else []
    return pl.pallas_call(
        functools.partial(moe_back_kernel, count, fsdp_count, runs, picks),
        grid=(1,),
        out_shape=[
            jax.ShapeDtypeStruct((rows, width), jnp.bfloat16),
            jax.ShapeDtypeStruct((rows, width), jnp.float32),
            jax.ShapeDtypeStruct((1, width), jnp.float32),
            jax.ShapeDtypeStruct((group, wide), jnp.bfloat16),
        ]
        + sums,
        in_specs=[IN_PLACE] * (2 * runs)
        + [IN_VMEM] * 4
        + [pl.BlockSpec((width, 128), lambda step: (0, used // 128))]
        + [IN_PLACE] * len(sums),
        out_specs=[IN_VMEM] * 4 + [IN_PLACE] * len(sums),
        scratch_shapes=[
            pltpu.VMEM((runs, group, wide), jnp.bfloat16),
            pltpu.VMEM((runs, group, width), jnp.bfloat16),
            pltpu.SemaphoreType.DMA((2 * runs,)),
            pltpu.VMEM((rows, wide), jnp.float32),
            pltpu.VMEM((rows, width), jnp.float32),
        ]
        + line_buffers(count, rows, wide)
        + line_buffers(count, rows, width)
        + line_sems(count)
        + expert_buffers(len(picks), share, grads.shape[3]),
        compiler_params=remote_params(ident, 63),
        cost_estimate=TRANSFER,
    )(*dx_parts, *y_parts, mid, cotangent, own_gates, gain_row, weights, *([grads] if picks else []))


def finish_kernel(tp_count, fsdp_count, picks, *refs):
    x_ref, w_ref, emb_ref, gain_ref, mid_grad, gain_two, *refs = refs
    grads_ref, refs = (refs[0], refs[1:]) if picks else (None, refs)
    grad_ref, w_sum, gains_ref, *refs = refs
    sums_ref, refs = (refs[0], refs[1:]) if picks else (None, refs)
    (
        line_recv, line_send_sem, line_recv_sem,
        pair_got, chip_sums, chip_got, pair_send, pair_recv, chip_send, chip_recv,
        tp_got, fsdp_got, small_send, small_recv, *refs,
    ) = refs
    plane = Plane(fsdp_count)
    tp_me, fsdp_me = lax.axis_index("tp"), plane.me
    barrier = pltpu.get_barrier_semaphore()
    for shift in range(1, tp_count):
        pl.semaphore_signal(barrier, inc=1, device_id={"tp": lax.rem(tp_me + shift, tp_count)})
    for shift in range(1, fsdp_count):
        pl.semaphore_signal(
            barrier, inc=1, device_id={"fsdp": lax.rem(fsdp_me + shift, fsdp_count)}
        )
    pl.semaphore_wait(barrier, tp_count + fsdp_count - 2)
    line = LineScatter(
        tp_count, [x_ref], grad_ref, line_recv, line_send_sem, line_recv_sem
    )
    rows = w_sum.shape[0]

    def to_pair(shift):
        return pltpu.make_async_remote_copy(
            src_ref=rows_of(w_ref, plane.chip_at(shift) * 2 + 1 - plane.core, rows),
            dst_ref=pair_got.at[shift],
            send_sem=pair_send.at[shift],
            recv_sem=pair_recv.at[shift],
            device_id={"fsdp": plane.partner},
        )

    def to_chip(shift):
        return pltpu.make_async_remote_copy(
            src_ref=chip_sums.at[shift - 1],
            dst_ref=chip_got.at[shift - 1],
            send_sem=chip_send.at[shift - 1],
            recv_sem=chip_recv.at[shift - 1],
            device_id={"fsdp": plane.peer(shift)},
        )

    def both_cores(shift):
        own = pl.ds(pl.multiple_of(plane.peer(shift) * rows, rows), rows)
        return w_ref[own, :].astype(jnp.float32) + pair_got[shift].astype(jnp.float32)

    def exchange(axis, me, count, got, base):
        copies = []
        for shift in range(1, count):
            copies.append(
                pltpu.make_async_remote_copy(
                    src_ref=gains_ref,
                    dst_ref=got.at[me],
                    send_sem=small_send.at[base + shift],
                    recv_sem=small_recv.at[base + shift],
                    device_id={axis: lax.rem(me + shift, count)},
                )
            )
            copies[-1].start()
        got[me] = gains_ref[...]
        for copy in copies:
            copy.wait()
        total = got[0]
        for index in range(1, count):
            total = total + got[index]
        return total

    experts = ExpertSums(plane, picks, grads_ref, sums_ref, *refs) if picks else None
    line.start(0)
    order = list(range(1, plane.chips)) + [0]
    for shift in order:
        to_pair(shift).start()
    for index in range(len(picks)):
        experts.begin(index)
    for shift in order:
        to_pair(shift).wait_recv()
        if shift > 0:
            chip_sums[shift - 1] = both_cores(shift).astype(chip_sums.dtype)
            to_chip(shift).start()
    items = experts.items() if picks else []
    each = -(-len(items) // (tp_count - 2))
    line.arrive(0)
    for step in range(1, tp_count - 1):
        line.start(step)
        for item in items[(step - 1) * each : step * each]:
            experts.do(*item)
        line.arrive(step)
    line.collect()
    from_norm, gain_one = rms_back(
        grad_ref[...], emb_ref[...].astype(jnp.float32) * emb_scale, gain_ref[...]
    )
    gains_ref[...] = jnp.zeros_like(gains_ref)
    gains_ref[0:1, :] = gain_one
    gains_ref[1:2, :] = gain_two[...]
    grad_ref[...] = emb_scale * (mid_grad[...] + from_norm)
    total = both_cores(0)
    for shift in range(1, plane.chips):
        to_chip(shift).wait_recv()
        total = total + chip_got[shift - 1].astype(jnp.float32)
    w_sum[...] = total
    for index in range(len(picks)):
        experts.collect(index)
    gains_ref[...] = exchange("tp", tp_me, tp_count, tp_got, 0)
    gains_ref[...] = exchange("fsdp", fsdp_me, fsdp_count, fsdp_got, tp_count)
    line.finish()
    for shift in order:
        to_pair(shift).wait_send()
        if shift > 0:
            to_chip(shift).wait_send()
    if picks:
        experts.finish()


def finish(dx_rows, weight_grads, emb, gain_row, mid_grad, gain_two, grads, picks, ident):
    tp_count, fsdp_count = lax.axis_size("tp"), lax.axis_size("fsdp")
    rows, width = emb.shape
    w_rows, w_width = weight_grads.shape[0] // fsdp_count, weight_grads.shape[1]
    chips = fsdp_count // 2
    share = grads.shape[2] // fsdp_count
    sums = [jax.ShapeDtypeStruct((len(picks), 3, share, grads.shape[3]), jnp.bfloat16)]
    sums = sums if picks else []
    return pl.pallas_call(
        functools.partial(finish_kernel, tp_count, fsdp_count, picks),
        out_shape=[
            jax.ShapeDtypeStruct((rows, width), jnp.float32),
            jax.ShapeDtypeStruct((w_rows, w_width), jnp.float32),
            jax.ShapeDtypeStruct((8, width), jnp.float32),
            *sums,
        ],
        in_specs=[IN_VMEM] * 6 + [IN_PLACE] * len(sums),
        out_specs=[IN_VMEM] * 3 + [IN_PLACE] * len(sums),
        scratch_shapes=line_buffers(tp_count, rows, width)
        + [
            pltpu.VMEM((chips, w_rows, w_width), jnp.bfloat16),
            pltpu.VMEM((chips - 1, w_rows, w_width), jnp.bfloat16),
            pltpu.VMEM((chips - 1, w_rows, w_width), jnp.bfloat16),
            pltpu.SemaphoreType.DMA((chips,)),
            pltpu.SemaphoreType.DMA((chips,)),
            pltpu.SemaphoreType.DMA((chips - 1,)),
            pltpu.SemaphoreType.DMA((chips - 1,)),
            pltpu.VMEM((tp_count, 8, width), jnp.float32),
            pltpu.VMEM((fsdp_count, 8, width), jnp.float32),
            pltpu.SemaphoreType.DMA((tp_count + fsdp_count,)),
            pltpu.SemaphoreType.DMA((tp_count + fsdp_count,)),
        ]
        + expert_buffers(len(picks), share, grads.shape[3]),
        compiler_params=remote_params(ident),
        cost_estimate=TRANSFER,
    )(dx_rows, weight_grads, emb, gain_row, mid_grad, gain_two, *([grads] if picks else []))


def pack_copies(low, sources, target, held, in_sem, out_sem):
    span = target.shape[0]
    gets = [
        pltpu.make_async_copy(source.at[pl.ds(low, span)], held.at[slot], in_sem.at[slot])
        for slot, source in enumerate(sources)
    ]
    puts = [
        pltpu.make_async_copy(held.at[slot], target.at[:, slot], out_sem.at[slot])
        for slot in range(len(sources))
    ]
    return gets, puts


def pack_kernel(low, *refs):
    sources, target, held, in_sem, out_sem = refs[:-4], *refs[-4:]
    gets, puts = pack_copies(low, sources, target, held, in_sem, out_sem)
    for get in gets:
        get.start()
    for get, put in zip(gets, puts):
        get.wait()
        put.start()
    for put in puts:
        put.wait()


def pack(stacks, low, high):
    _, rows, width = stacks[0].shape
    count, span = len(stacks), high - low
    return pl.pallas_call(
        functools.partial(pack_kernel, low),
        in_specs=[IN_PLACE] * count,
        out_specs=IN_PLACE,
        out_shape=jax.ShapeDtypeStruct((span, count, rows, width), jnp.bfloat16),
        scratch_shapes=[
            pltpu.VMEM((count, span, rows, width), jnp.bfloat16),
            pltpu.SemaphoreType.DMA((count,)),
            pltpu.SemaphoreType.DMA((count,)),
        ],
    )(*stacks)


def join_kernel(*refs):
    *sources, last, target = refs
    low = 0
    for source in sources:
        target[:, low : low + source.shape[1]] = source[...]
        low += source.shape[1]
    router = last[...].astype(jnp.float32).T.astype(jnp.bfloat16)
    target[:, low:] = jnp.zeros((target.shape[0], target.shape[1] - low), jnp.bfloat16)
    target[:, low : low + router.shape[1]] = router


def join(parts, last_turned, width):
    return pl.pallas_call(
        join_kernel,
        in_specs=[IN_VMEM] * (len(parts) + 1),
        out_specs=IN_VMEM,
        out_shape=jax.ShapeDtypeStruct((parts[0].shape[0], width), jnp.bfloat16),
    )(*parts, last_turned)


SLOTS = 256


def experts_kernel(
    first_expert,
    capacity,
    meta,
    place_rows,
    place_cols,
    gate_rows,
    x_ref,
    g_ref,
    weights,
    *refs,
):
    *held, y_ref, dx_ref, grads, load_sem = refs
    step = pl.program_id(0)
    expert = step + first_expert
    group, width = x_ref.shape
    tail = dx_ref.shape[1] - width

    @pl.when(step == 0)
    def _():
        if held:
            loads = [
                pltpu.make_async_copy(source, target, load_sem.at[index])
                for index, (source, target) in enumerate(zip(held, (y_ref, dx_ref)))
            ]
            for load in loads:
                load.start()
            for load in loads:
                load.wait()
        else:
            y_ref[...] = jnp.zeros_like(y_ref)
            dx_ref[...] = jnp.zeros_like(dx_ref)

    column = expert + meta[meta.shape[0] - 1]
    lanes = lax.broadcasted_iota(jnp.int32, place_cols.shape, 1)
    place_col = jnp.sum(jnp.where(lanes == column, place_cols[...], 0), axis=1, keepdims=True)
    place_row = place_rows[pl.ds(column, 1), :]
    gate_row = gate_rows[pl.ds(column, 1), :].astype(jnp.bfloat16).astype(jnp.float32)
    mark = jnp.where(lax.broadcasted_iota(jnp.int32, (1, tail), 1) == column, 1.0, 0.0)

    def run(base, span):
        slots = lax.broadcasted_iota(jnp.int32, (span, group), 0) + base
        hit = slots == place_row
        pick = jnp.where(hit, 1.0, 0.0).astype(jnp.bfloat16)
        scale = jnp.sum(jnp.where(hit, gate_row, 0.0), axis=1, keepdims=True)
        x_taken = jnp.dot(pick, x_ref[...], preferred_element_type=jnp.float32).astype(jnp.bfloat16)
        g_taken = jnp.dot(pick, g_ref[...], preferred_element_type=jnp.float32).astype(jnp.bfloat16)
        gate_pre = jnp.dot(x_taken, weights[0, 0], preferred_element_type=jnp.float32)
        up_pre = jnp.dot(x_taken, weights[0, 1], preferred_element_type=jnp.float32)
        raw = jnp.dot(g_taken, weights[0, 2], preferred_element_type=jnp.float32)
        sig = jax.nn.sigmoid(gate_pre)
        silu = gate_pre * sig
        act = (silu * up_pre).astype(jnp.bfloat16).astype(jnp.float32)
        slot_grad = jnp.sum(act * raw, axis=1, keepdims=True)
        act_grad = raw * scale
        act_scaled = (act * scale).astype(jnp.bfloat16)
        gate_grad = (act_grad * up_pre * sig * (1.0 + gate_pre * (1.0 - sig))).astype(jnp.bfloat16)
        up_grad = (act_grad * silu).astype(jnp.bfloat16)
        extra = (slot_grad * mark).astype(jnp.bfloat16)
        rows_out = contract_last(act_scaled, weights[0, 2]).astype(jnp.bfloat16)
        rows_in = (
            contract_last(gate_grad, weights[0, 0]) + contract_last(up_grad, weights[0, 1])
        ).astype(jnp.bfloat16)
        for slot, left_op, right_op in (
            (0, x_taken, gate_grad),
            (1, x_taken, up_grad),
            (2, g_taken, act_scaled),
        ):
            grad = contract_first(left_op, right_op)
            if base > 0:
                grad = grad + grads[0, slot].astype(jnp.float32)
            grads[0, slot] = grad.astype(jnp.bfloat16)
        block = min(256, group)
        for start in range(0, group, block):
            back = jnp.where(
                lax.broadcasted_iota(jnp.int32, (block, span), 1) + base
                == place_col[start : start + block],
                1.0,
                0.0,
            ).astype(jnp.bfloat16)
            for target, low_col, addend in (
                (y_ref, 0, rows_out),
                (dx_ref, 0, rows_in),
                (dx_ref, width, extra),
            ):
                area = (slice(start, start + block), slice(low_col, low_col + addend.shape[1]))
                target[area] = (
                    target[area].astype(jnp.float32)
                    + jnp.dot(back, addend, preferred_element_type=jnp.float32)
                ).astype(target.dtype)

    run(0, min(SLOTS, capacity))
    for base in range(SLOTS, capacity, SLOTS):
        span = min(SLOTS, -(-(capacity - base) // 16) * 16)

        @pl.when(meta[column] > base)
        def _():
            run(base, span)


def experts_step(meta, place_rows, place_cols, gate_rows, x_rows, g_rows, weights, held, first, count, skip, capacity):
    group, width = x_rows.shape
    hidden = weights.shape[-1]
    tail = 128

    def whole(shape):
        return pl.BlockSpec(
            shape, lambda step, meta: (0,) * len(shape), pipeline_mode=pl.Buffered(1)
        )

    def big(offset):
        return pl.BlockSpec((1, 3, width, hidden), lambda step, meta: (step + offset, 0, 0, 0))

    return pl.pallas_call(
        functools.partial(experts_kernel, first, capacity),
        grid_spec=pltpu.PrefetchScalarGridSpec(
            num_scalar_prefetch=1,
            grid=(count,),
            in_specs=[
                whole(place_rows.shape),
                whole(place_cols.shape),
                whole(gate_rows.shape),
                whole(x_rows.shape),
                whole(g_rows.shape),
                big(skip),
            ]
            + [IN_PLACE] * len(held),
            out_specs=[
                whole((group, width)),
                whole((group, width + tail)),
                big(0),
            ],
            scratch_shapes=[pltpu.SemaphoreType.DMA((2,))],
        ),
        out_shape=[
            jax.ShapeDtypeStruct((group, width), jnp.bfloat16),
            jax.ShapeDtypeStruct((group, width + tail), jnp.bfloat16),
            jax.ShapeDtypeStruct((count, 3, width, hidden), jnp.bfloat16),
        ],
        compiler_params=pltpu.CompilerParams(
            dimension_semantics=("arbitrary",), vmem_limit_bytes=63 << 20
        ),
        cost_estimate=pl.CostEstimate(
            flops=count * 17 * 2 * 408 * width * hidden,
            transcendentals=count * 408 * hidden,
            bytes_accessed=count * 12 * width * hidden,
        ),
    )(meta, place_rows, place_cols, gate_rows, x_rows, g_rows, weights, *held)


def rotate_head(values, cosine, sine, sign):
    half = values.shape[-1] // 2
    other = jnp.concatenate([values[:, half:], values[:, :half]], axis=1)
    return values * cosine + other * (sine * sign)


def segment_bias(seg_row):
    length = seg_row.shape[1]
    shape = (length, length)
    seg_row = seg_row.astype(jnp.float32)
    seg_col = jnp.broadcast_to(seg_row, (128, length)).T[:, :1]
    keys = lax.broadcasted_iota(jnp.int32, shape, 0)
    queries = lax.broadcasted_iota(jnp.int32, shape, 1)
    return jnp.where((keys <= queries) & (seg_col == seg_row), 0.0, masked_value)


def attend_kernel(
    x_ref,
    w_ref,
    seg_row,
    cos_ref,
    sin_ref,
    q_ref,
    k_ref,
    v_ref,
    mixed_ref,
    logsum_ref,
    branch_ref,
    bias,
    v_turned,
    mixed_heads,
):
    heads, kv_heads = q_ref.shape[0], k_ref.shape[0]
    per_kv = heads // kv_heads
    block = SEQ // 2
    edge = (heads + 2 * kv_heads) * HEAD_DIM
    proj = jnp.dot(x_ref[...], w_ref[:, :edge], preferred_element_type=jnp.float32)
    cosine, sine = cos_ref[...], sin_ref[...]
    for head in range(heads + 2 * kv_heads):
        part = proj[:, head * HEAD_DIM : (head + 1) * HEAD_DIM]
        if head < heads:
            q_ref[head] = rotate_head(part, cosine, sine, 1.0).astype(jnp.bfloat16)
        elif head < heads + kv_heads:
            k_ref[head - heads] = rotate_head(part, cosine, sine, 1.0).astype(jnp.bfloat16)
        else:
            v_ref[head - heads - kv_heads] = part.astype(jnp.bfloat16)
            v_turned[head - heads - kv_heads] = part.T.astype(jnp.bfloat16)
    bias[...] = segment_bias(seg_row[0])

    def one_head(head, carry):
        kv = head // per_kv
        for part in range(2):
            span, low = block * (part + 1), block * part
            scores = contract_last(k_ref[kv, :span], q_ref[head, low : low + block]) * attn_scale
            scores = scores + bias[:span, low : low + block]
            top = jnp.max(scores, axis=0, keepdims=True)
            raised = jnp.exp(scores - top)
            total = jnp.sum(raised, axis=0, keepdims=True)
            probs = (raised * (1.0 / total)).astype(jnp.bfloat16)
            turned = jnp.dot(v_turned[kv, :, :span], probs, preferred_element_type=jnp.float32)
            mixed_heads[head, low : low + block, :] = turned.T.astype(jnp.bfloat16)
            logsum_ref[0, pl.ds(head, 1), low : low + block] = top + jnp.log(total)
        return carry

    lax.fori_loop(0, heads, one_head, 0)
    for head in range(heads):
        mixed_ref[:, head * HEAD_DIM : (head + 1) * HEAD_DIM] = mixed_heads[head]
    branch_ref[...] = contract_last(
        mixed_ref[...], w_ref[:, edge : edge + heads * HEAD_DIM]
    ).astype(jnp.bfloat16)


def attend_back_kernel(
    x_ref,
    w_ref,
    seg_row,
    cos_ref,
    sin_ref,
    q_ref,
    k_ref,
    v_ref,
    mixed_ref,
    logsum_ref,
    moe_rows,
    branch_grad,
    dx_ref,
    dw_ref,
    bias,
    k_turned,
    mixed_grads,
    q_grads,
    kv_grads,
    qkv_grad,
    dw_acc,
):
    heads, kv_heads = q_ref.shape[0], k_ref.shape[0]
    per_kv = heads // kv_heads
    block = SEQ // 2
    edge = (heads + 2 * kv_heads) * HEAD_DIM
    step = pl.program_id(0)
    out_edge = edge + heads * HEAD_DIM
    width = x_ref.shape[1]
    grad = jnp.dot(
        branch_grad[:, :width], w_ref[:, edge:out_edge], preferred_element_type=jnp.float32
    ).astype(jnp.bfloat16)
    for head in range(heads):
        mixed_grads[head] = grad[:, head * HEAD_DIM : (head + 1) * HEAD_DIM]
    for kv in range(kv_heads):
        k_turned[kv] = k_ref[kv].astype(jnp.float32).T.astype(jnp.bfloat16)
    bias[...] = segment_bias(seg_row[0])
    kv_grads[...] = jnp.zeros_like(kv_grads)

    def one_head(head, carry):
        kv = head // per_kv
        for part in range(2):
            span, low = block * (part + 1), block * part
            high = low + block
            scores = contract_last(k_ref[kv, :span], q_ref[head, low:high]) * attn_scale
            scores = scores + bias[:span, low:high]
            probs = jnp.exp(scores - logsum_ref[0, pl.ds(head, 1), low:high])
            probs_grad = contract_last(v_ref[kv, :span], mixed_grads[head, low:high])
            inner = jnp.sum(probs * probs_grad, axis=0, keepdims=True)
            score_grad = (probs * (probs_grad - inner)).astype(jnp.bfloat16)
            turned = jnp.dot(k_turned[kv, :, :span], score_grad, preferred_element_type=jnp.float32)
            q_grads[head, low:high, :] = turned.T * attn_scale
            kv_grads[0, kv, :span, :] += jnp.dot(
                score_grad, q_ref[head, low:high], preferred_element_type=jnp.float32
            )
            kv_grads[1, kv, :span, :] += jnp.dot(
                probs.astype(jnp.bfloat16), mixed_grads[head, low:high],
                preferred_element_type=jnp.float32,
            )
        return carry

    lax.fori_loop(0, heads, one_head, 0)
    cosine, sine = cos_ref[...], sin_ref[...]
    for head in range(heads + 2 * kv_heads):
        if head < heads:
            part = rotate_head(q_grads[head], cosine, sine, -1.0)
        elif head < heads + kv_heads:
            part = rotate_head(kv_grads[0, head - heads] * attn_scale, cosine, sine, -1.0)
        else:
            part = kv_grads[1, head - heads - kv_heads]
        qkv_grad[:, head * HEAD_DIM : (head + 1) * HEAD_DIM] = part.astype(jnp.bfloat16)
    dx_ref[...] = contract_last(qkv_grad[...], w_ref[:, :edge]).astype(jnp.bfloat16)
    for low, high, left_op, right_op in (
        (0, edge, x_ref[...], qkv_grad[...]),
        (edge, out_edge, branch_grad[:, :width], mixed_ref[...]),
        (out_edge, dw_acc.shape[1], moe_rows[...], branch_grad[:, width:]),
    ):
        part = contract_first(left_op, right_op)

        @pl.when(step == 0)
        def _():
            dw_acc[:, low:high] = part

        @pl.when(step > 0)
        def _():
            dw_acc[:, low:high] += part

    @pl.when(step == pl.num_programs(0) - 1)
    def _():
        dw_ref[...] = dw_acc[...].astype(jnp.bfloat16)


def fixed(shape):
    return pl.BlockSpec(shape, lambda seq: (0,) * len(shape), pipeline_mode=pl.Buffered(1))


def by_row(width):
    return pl.BlockSpec((SEQ, width), lambda seq: (seq, 0))


def by_head(heads):
    return pl.BlockSpec((heads, SEQ, HEAD_DIM), lambda seq: (0, seq, 0))


def attend_tables():
    half = HEAD_DIM // 2
    positions = np.arange(SEQ, dtype=np.float32)
    frequency = np.float32(rope_base) ** (-np.arange(half, dtype=np.float32) * 2.0 / HEAD_DIM)
    angles = (positions[:, None] * frequency[None, :].astype(np.float32)).astype(np.float32)
    cosine, sine = np.cos(angles), np.sin(angles)
    return (
        jnp.asarray(np.concatenate([cosine, cosine], axis=1)),
        jnp.asarray(np.concatenate([-sine, sine], axis=1)),
    )


def attend(rows, weights, segments, tables, heads, kv_heads):
    group, width = rows.shape
    seqs = group // SEQ
    return pl.pallas_call(
        attend_kernel,
        grid=(seqs,),
        in_specs=[
            by_row(width),
            fixed(weights.shape),
            pl.BlockSpec((1, 1, SEQ), lambda seq: (seq, 0, 0)),
            fixed(tables[0].shape),
            fixed(tables[1].shape),
        ],
        out_specs=[
            by_head(heads),
            by_head(kv_heads),
            by_head(kv_heads),
            by_row(heads * HEAD_DIM),
            pl.BlockSpec((1, heads, SEQ), lambda seq: (seq, 0, 0)),
            by_row(width),
        ],
        out_shape=[
            jax.ShapeDtypeStruct((heads, group, HEAD_DIM), jnp.bfloat16),
            jax.ShapeDtypeStruct((kv_heads, group, HEAD_DIM), jnp.bfloat16),
            jax.ShapeDtypeStruct((kv_heads, group, HEAD_DIM), jnp.bfloat16),
            jax.ShapeDtypeStruct((group, heads * HEAD_DIM), jnp.bfloat16),
            jax.ShapeDtypeStruct((seqs, heads, SEQ), jnp.float32),
            jax.ShapeDtypeStruct((group, width), jnp.bfloat16),
        ],
        scratch_shapes=[
            pltpu.VMEM((SEQ, SEQ), jnp.float32),
            pltpu.VMEM((kv_heads, HEAD_DIM, SEQ), jnp.bfloat16),
            pltpu.VMEM((heads, SEQ, HEAD_DIM), jnp.bfloat16),
        ],
        compiler_params=pltpu.CompilerParams(
            dimension_semantics=("arbitrary",), vmem_limit_bytes=56 << 20
        ),
        cost_estimate=pl.CostEstimate(
            flops=10_000_000_000, transcendentals=3_000_000, bytes_accessed=60_000_000
        ),
    )(rows, weights, segments[:, None, :], *tables)


def attend_back(rows, weights, segments, tables, kept, moe_rows, branch_grad):
    queries, keys, values, mixed, logsum = kept
    group, width = rows.shape
    heads, kv_heads = queries.shape[0], keys.shape[0]
    used = weights.shape[1]
    edge = (heads + 2 * kv_heads) * HEAD_DIM
    return pl.pallas_call(
        attend_back_kernel,
        grid=(group // SEQ,),
        in_specs=[
            by_row(width),
            fixed(weights.shape),
            pl.BlockSpec((1, 1, SEQ), lambda seq: (seq, 0, 0)),
            fixed(tables[0].shape),
            fixed(tables[1].shape),
            by_head(heads),
            by_head(kv_heads),
            by_head(kv_heads),
            by_row(heads * HEAD_DIM),
            pl.BlockSpec((1, heads, SEQ), lambda seq: (seq, 0, 0)),
            by_row(width),
            by_row(branch_grad.shape[1]),
        ],
        out_specs=[by_row(width), fixed((width, used))],
        out_shape=[
            jax.ShapeDtypeStruct((group, width), jnp.bfloat16),
            jax.ShapeDtypeStruct((width, used), jnp.bfloat16),
        ],
        scratch_shapes=[
            pltpu.VMEM((SEQ, SEQ), jnp.float32),
            pltpu.VMEM((kv_heads, HEAD_DIM, SEQ), jnp.bfloat16),
            pltpu.VMEM((heads, SEQ, HEAD_DIM), jnp.bfloat16),
            pltpu.VMEM((heads, SEQ, HEAD_DIM), jnp.float32),
            pltpu.VMEM((2, kv_heads, SEQ, HEAD_DIM), jnp.float32),
            pltpu.VMEM((SEQ, edge), jnp.bfloat16),
            pltpu.VMEM((width, used), jnp.float32),
        ],
        compiler_params=pltpu.CompilerParams(
            dimension_semantics=("arbitrary",), vmem_limit_bytes=60 << 20
        ),
        cost_estimate=pl.CostEstimate(
            flops=20_000_000_000, transcendentals=3_000_000, bytes_accessed=100_000_000
        ),
    )(rows, weights, segments[:, None, :], *tables,
      queries, keys, values, mixed, logsum, moe_rows, branch_grad)


def widen_kernel(edges, *refs):
    step = pl.program_id(0)
    packed, targets = refs[:-3], refs[-3:]
    for part, low, high in zip(packed, edges[:-1], edges[1:]):

        @pl.when((step >= low) & (step < high))
        def _():
            for slot, target in enumerate(targets):
                target[0] = part[0, slot].astype(jnp.float32)


def widen(packed, edges):
    _, _, rows, width = packed[0].shape

    def home(low, high):
        return pl.BlockSpec(
            (1, 3, rows, width),
            lambda step: (jnp.clip(step - low, 0, high - low - 1), 0, 0, 0),
        )

    return pl.pallas_call(
        functools.partial(widen_kernel, edges),
        grid=(edges[-1],),
        in_specs=[home(low, high) for low, high in zip(edges[:-1], edges[1:])],
        out_specs=[pl.BlockSpec((1, rows, width), lambda step: (step, 0, 0))] * 3,
        out_shape=[jax.ShapeDtypeStruct((edges[-1], rows, width), jnp.float32)] * 3,
    )(*packed)


RUNS = (0, 5, 10)
DIRECT = (3, 2)


def local(
    emb,
    segment_ids,
    routes,
    norm1_gain,
    w_query,
    w_key,
    w_value,
    w_out,
    norm2_gain,
    w_router,
    w_gate,
    w_up,
    w_down,
    cotangent,
):
    local_rows, width = emb.shape
    tp_count, tp_index = lax.axis_size("tp"), lax.axis_index("tp")
    experts_here = w_gate.shape[0]
    expert_count = w_router.shape[1]
    q_width, kv_width = w_query.shape[1], w_key.shape[1]
    used = 2 * (q_width + kv_width)
    group_size = local_rows * tp_count
    fsdp_count = lax.axis_size("fsdp")
    split = group_size <= 1024
    runs = [edge * experts_here // RUNS[-1] for edge in RUNS] if split else [0, experts_here]
    stacks = (w_gate, w_up, w_down)
    pieces = [lax.all_gather(pack(stacks, 0, runs[1]), "fsdp", axis=2, tiled=True)]
    gain_one = norm1_gain.astype(jnp.float32)[None, :]
    gain_two = norm2_gain.astype(jnp.float32)[None, :]
    group_rows, mask, place_cols, place_rows, counts, attn_w, *packed = norm_gather(
        emb,
        gain_one,
        routes,
        join([w_query, w_key, w_value, w_out], w_router.T, used + 128),
        stacks,
        runs[1] if split else 0,
        tp_count,
        fsdp_count,
        0,
    )
    if split:
        pieces.append(lax.all_gather(packed[0], "fsdp", axis=2, tiled=True))
    capacity = group_size * routes.shape[1] // expert_count * 2
    meta = jnp.concatenate([counts[0], (tp_index * experts_here)[None]])

    tables = attend_tables()
    heads_here, kv_here = q_width // HEAD_DIM, kv_width // HEAD_DIM
    *kept, branch_part = attend(group_rows, attn_w, segment_ids, tables, heads_here, kv_here)
    mid_x, moe_rows, gate_rows, own_gates, moe_grad_rows = find_mid(
        branch_part, emb, gain_two, attn_w, used, mask, cotangent, tp_count, 1
    )

    outs = []
    for first, last, piece in zip(runs[:-1], runs[1:], pieces):
        outs.append(
            experts_step(
                meta,
                place_rows,
                place_cols,
                gate_rows,
                moe_rows,
                moe_grad_rows,
                piece,
                outs[-1][:2] if outs else (),
                first,
                last - first,
                0,
                capacity,
            )
        )
    grad_sums = [lax.psum_scatter(outs[0][2], "fsdp", scatter_dimension=2, tiled=True)]
    last_grads = outs[-1][2]
    picks = (tuple(range(DIRECT[0])), tuple(range(DIRECT[0], sum(DIRECT)))) if split else ((), ())
    out, mid_grad, gain_two_grad, sent, *mid_sums = find_mid_grad(
        outs[-1][1:2],
        outs[-1][0:1],
        mid_x,
        cotangent,
        own_gates,
        gain_two,
        attn_w,
        used,
        last_grads,
        picks[0],
        tp_count,
        fsdp_count,
        2,
    )
    dx_one, attn_grads = attend_back(
        group_rows, attn_w, segment_ids, tables, kept, moe_rows, sent
    )
    grad_emb, attn_sum, gain_sums, *end_sums = finish(
        dx_one, attn_grads, emb, gain_one, mid_grad, gain_two_grad, last_grads, picks[1], 3
    )
    grad_sums = grad_sums + mid_sums + end_sums
    ends = [0]
    for part in grad_sums:
        ends.append(ends[-1] + part.shape[0])
    expert_sums = widen(grad_sums, ends)
    return (
        out,
        grad_emb,
        gain_sums[0],
        attn_sum[:, :q_width],
        attn_sum[:, q_width : q_width + kv_width],
        attn_sum[:, q_width + kv_width : q_width + 2 * kv_width],
        attn_sum[:, q_width + 2 * kv_width : used],
        gain_sums[1],
        attn_sum[:, used : used + expert_count],
        *expert_sums,
    )


def solution(mesh):
    return jax.shard_map(
        local,
        mesh=mesh,
        in_specs=(
            P(("fsdp", "tp"), None),
            P("fsdp", None),
            P("fsdp", None),
            P(),
            P("fsdp", "tp"),
            P("fsdp", "tp"),
            P("fsdp", "tp"),
            P("fsdp", "tp"),
            P(),
            P("fsdp", None),
            P("tp", "fsdp", None),
            P("tp", "fsdp", None),
            P("tp", "fsdp", None),
            P(("fsdp", "tp"), None),
        ),
        out_specs=(
            P(("fsdp", "tp"), None),
            P(("fsdp", "tp"), None),
            P(),
            P("fsdp", "tp"),
            P("fsdp", "tp"),
            P("fsdp", "tp"),
            P("fsdp", "tp"),
            P(),
            P("fsdp", None),
            P("tp", "fsdp", None),
            P("tp", "fsdp", None),
            P("tp", "fsdp", None),
        ),
        check_vma=False,
    )
```

```python
import functools

import jax
import jax.numpy as jnp
import numpy as np
from jax import lax
from jax.experimental import pallas as pl
from jax.experimental.pallas import tpu as pltpu
from jax.sharding import PartitionSpec as P

HEAD_DIM = 64
SEQ = 512


emb_scale = 12.0
resid_scale = 0.22
attn_scale = 0.015625
norm_eps = 1e-06
rope_base = 10000.0
masked_value = -1e30


def contract_last(left_op, right_op):
    return lax.dot_general(
        left_op, right_op, (((1,), (1,)), ((), ())), preferred_element_type=jnp.float32
    )


def contract_first(left_op, right_op):
    return lax.dot_general(
        left_op, right_op, (((0,), (0,)), ((), ())), preferred_element_type=jnp.float32
    )


def line_signal(barrier, me, count):
    @pl.when(me > 0)
    def _():
        pl.semaphore_signal(barrier, inc=1, device_id={"tp": me - 1})

    @pl.when(me < count - 1)
    def _():
        pl.semaphore_signal(barrier, inc=1, device_id={"tp": me + 1})

    return jnp.where((me > 0) & (me < count - 1), 2, 1)


class Plane:
    def __init__(self, count):
        self.me = lax.axis_index("fsdp")
        self.core = lax.rem(self.me, 2)
        self.chip = lax.div(self.me, 2)
        self.chips = count // 2
        self.partner = self.me + 1 - 2 * self.core

    def chip_at(self, shift):
        return lax.rem(self.chip + shift + self.chips, self.chips)

    def peer(self, shift):
        return self.chip_at(shift) * 2 + self.core

    def signal(self, barrier):
        for shift in range(1, self.chips):
            pl.semaphore_signal(barrier, inc=1, device_id={"fsdp": self.peer(shift)})
        pl.semaphore_signal(barrier, inc=1, device_id={"fsdp": self.partner})
        return self.chips


def rows_of(ref, index, rows):
    return ref.at[pl.ds(pl.multiple_of(index * rows, rows), rows)]


class LineGather:
    def __init__(self, count, o_ref, send_sem, recv_sem):
        self.count, self.o_ref = count, o_ref
        self.send_sem, self.recv_sem = send_sem, recv_sem
        self.rows = o_ref.shape[0] // count
        me = self.me = lax.axis_index("tp")
        steps = range(count - 1)
        self.sends = [
            [(me >= step) & (me < count - 1) for step in steps],
            [(me + step < count) & (me > 0) for step in steps],
        ]
        self.gets = [
            [me - 1 - step >= 0 for step in steps],
            [me + 1 + step < count for step in steps],
        ]

    def hop(self, way, step, chunk):
        part = rows_of(self.o_ref, chunk, self.rows)
        return pltpu.make_async_remote_copy(
            src_ref=part,
            dst_ref=part,
            send_sem=self.send_sem.at[way, step],
            recv_sem=self.recv_sem.at[way, step],
            device_id={"tp": self.me + 1 if way == 0 else self.me - 1},
        )

    def start(self, step):
        @pl.when(self.sends[0][step])
        def _():
            self.hop(0, step, self.me - step).start()

        @pl.when(self.sends[1][step])
        def _():
            self.hop(1, step, self.me + step).start()

    def arrive(self, step):
        @pl.when(self.gets[0][step])
        def _():
            self.hop(0, step, self.me - 1 - step).wait_recv()

        @pl.when(self.gets[1][step])
        def _():
            self.hop(1, step, self.me + 1 + step).wait_recv()

    def finish(self):
        for step in range(self.count - 1):

            @pl.when(self.sends[0][step])
            def _():
                self.hop(0, step, self.me - step).wait_send()

            @pl.when(self.sends[1][step])
            def _():
                self.hop(1, step, self.me + step).wait_send()


def line_sems(count):
    return [
        pltpu.SemaphoreType.DMA((2, count - 1)),
        pltpu.SemaphoreType.DMA((2, count - 1)),
    ]


class PlaneGather:
    def __init__(self, plane, w_ref, wo_ref, out_send, out_recv, on_send, on_recv, kept_sem):
        self.plane, self.w_ref, self.wo_ref = plane, w_ref, wo_ref
        self.out_send, self.out_recv = out_send, out_recv
        self.on_send, self.on_recv = on_send, on_recv
        self.rows = w_ref.shape[0]
        self.kept = pltpu.make_async_copy(w_ref, rows_of(wo_ref, plane.me, self.rows), kept_sem)

    def outward(self, shift, target, source_device):
        return pltpu.make_async_remote_copy(
            src_ref=self.w_ref,
            dst_ref=rows_of(self.wo_ref, source_device, self.rows),
            send_sem=self.out_send.at[shift],
            recv_sem=self.out_recv.at[shift],
            device_id={"fsdp": target},
        )

    def onward(self, shift, source_device):
        part = rows_of(self.wo_ref, source_device, self.rows)
        return pltpu.make_async_remote_copy(
            src_ref=part,
            dst_ref=part,
            send_sem=self.on_send.at[shift - 1],
            recv_sem=self.on_recv.at[shift - 1],
            device_id={"fsdp": self.plane.partner},
        )

    def start(self):
        plane = self.plane
        for shift in range(1, plane.chips):
            self.outward(shift, plane.peer(shift), plane.me).start()
        self.outward(0, plane.partner, plane.me).start()
        self.kept.start()

    def forward(self):
        plane = self.plane
        for shift in range(1, plane.chips):
            self.outward(shift, plane.peer(shift), plane.peer(-shift)).wait_recv()
            self.onward(shift, plane.peer(-shift)).start()

    def finish(self):
        plane = self.plane
        self.outward(0, plane.partner, plane.partner).wait_recv()
        for shift in range(1, plane.chips):
            self.onward(shift, plane.chip_at(-shift) * 2 + 1 - plane.core).wait_recv()
        for shift in range(1, plane.chips):
            self.outward(shift, plane.peer(shift), plane.me).wait_send()
            self.onward(shift, plane.peer(-shift)).wait_send()
        self.outward(0, plane.partner, plane.me).wait_send()
        self.kept.wait()


class ExpertSums:
    NEAR = {0: (1, 0), 1: (3, 0), 2: (2, 1), 3: (3, 1), 4: (2, 0), 5: (1, 1)}

    def __init__(self, plane, picks, grads_ref, out_ref, *refs):
        self.plane, self.picks, self.grads_ref, self.out_ref = plane, picks, grads_ref, out_ref
        (
            self.got, self.own, self.hop_got, self.held,
            self.pair_send, self.pair_recv, self.own_sem,
            self.hop_send, self.hop_recv, self.put_sem,
        ) = refs
        self.rows = out_ref.shape[2]
        self.half = self.rows // 2

    def chip_by(self, way):
        chip = self.plane.chip
        low, high = lax.rem(chip, 2), lax.div(chip, 2)
        if way % 2:
            low = 1 - low
        if way >= 2:
            high = 1 - high
        return high * 2 + low

    def area(self, index, dest):
        low = pl.multiple_of(dest * self.rows, self.rows)
        return self.grads_ref.at[self.picks[index], :, pl.ds(low, self.rows)]

    def part(self, index, way, half):
        return self.own.at[index, way, :, pl.ds(half * self.half, self.half)]

    def to_pair(self, index, way):
        return pltpu.make_async_remote_copy(
            src_ref=self.area(index, self.chip_by(way) * 2 + 1 - self.plane.core),
            dst_ref=self.got.at[index, way],
            send_sem=self.pair_send.at[index, way],
            recv_sem=self.pair_recv.at[index, way],
            device_id={"fsdp": self.plane.partner},
        )

    def keep(self, index, way):
        return pltpu.make_async_copy(
            self.area(index, self.chip_by(way) * 2 + self.plane.core),
            self.own.at[index, way],
            self.own_sem.at[index, way],
        )

    def hop(self, index, slot):
        way, half = self.NEAR[slot]
        source = self.part(index, way, half) if slot < 4 else self.hop_got.at[index, 2 * slot - 7]
        target = (1, 1, 2, 2, 2, 1)[slot]
        return pltpu.make_async_remote_copy(
            src_ref=source,
            dst_ref=self.hop_got.at[index, slot],
            send_sem=self.hop_send.at[index, slot],
            recv_sem=self.hop_recv.at[index, slot],
            device_id={"fsdp": self.chip_by(target) * 2 + self.plane.core},
        )

    def put(self, index):
        return pltpu.make_async_copy(
            self.held.at[index], self.out_ref.at[index], self.put_sem.at[index]
        )

    def begin(self, index):
        for way in (3, 1, 2, 0):
            self.to_pair(index, way).start()
            self.keep(index, way).start()

    def both_cores(self, index, way):
        self.to_pair(index, way).wait_recv()
        self.keep(index, way).wait()
        for slot in range(self.own.shape[2]):
            both = self.own[index, way, slot].astype(jnp.float32) + self.got[
                index, way, slot
            ].astype(jnp.float32)
            self.own[index, way, slot] = both.astype(jnp.bfloat16)

    def items(self):
        count = len(self.picks)
        order = []
        for index in range(count + 1):
            if index < count:
                order += [(index, 0), (index, 1)]
            if index > 0:
                order += [(index - 1, 2), (index - 1, 3)]
        return order

    def do(self, index, stage):
        if stage == 0:
            self.both_cores(index, 3)
            self.hop(index, 1).start()
            self.hop(index, 3).start()
        elif stage == 1:
            self.both_cores(index, 1)
            self.hop(index, 0).start()
            self.both_cores(index, 2)
            self.hop(index, 2).start()
        elif stage == 2:
            for slot in (4, 5):
                behind = 2 * slot - 7
                way, half = self.NEAR[slot]
                self.hop(index, behind).wait_recv()
                for layer in range(self.own.shape[2]):
                    mine = self.own[
                        index, way, layer, half * self.half : (half + 1) * self.half, :
                    ].astype(jnp.float32)
                    total = mine + self.hop_got[index, behind, layer].astype(jnp.float32)
                    self.hop_got[index, behind, layer] = total.astype(jnp.bfloat16)
                self.hop(index, slot).start()
        else:
            self.both_cores(index, 0)

    def collect(self, index):
        for half, slots in ((0, (0, 4)), (1, (2, 5))):
            area = slice(half * self.half, (half + 1) * self.half)
            for slot in slots:
                self.hop(index, slot).wait_recv()
            for layer in range(self.own.shape[2]):
                total = self.own[index, 0, layer, area, :].astype(jnp.float32)
                for slot in slots:
                    total = total + self.hop_got[index, slot, layer].astype(jnp.float32)
                self.held[index, layer, area, :] = total.astype(jnp.bfloat16)
        self.put(index).start()

    def finish(self):
        for index in range(len(self.picks)):
            self.put(index).wait()
            for way in range(4):
                self.to_pair(index, way).wait_send()
            for slot in range(6):
                self.hop(index, slot).wait_send()


def expert_buffers(count, rows, width):
    if count == 0:
        return []
    return [
        pltpu.VMEM((count, 4, 3, rows, width), jnp.bfloat16),
        pltpu.VMEM((count, 4, 3, rows, width), jnp.bfloat16),
        pltpu.VMEM((count, 6, 3, rows // 2, width), jnp.bfloat16),
        pltpu.VMEM((count, 3, rows, width), jnp.bfloat16),
        pltpu.SemaphoreType.DMA((count, 4)),
        pltpu.SemaphoreType.DMA((count, 4)),
        pltpu.SemaphoreType.DMA((count, 4)),
        pltpu.SemaphoreType.DMA((count, 6)),
        pltpu.SemaphoreType.DMA((count, 6)),
        pltpu.SemaphoreType.DMA((count,)),
    ]


class LineScatter:
    def __init__(self, count, x_refs, o_ref, recv, send_sem, recv_sem):
        self.count, self.x_refs, self.o_ref, self.recv = count, x_refs, o_ref, recv
        self.send_sem, self.recv_sem = send_sem, recv_sem
        self.rows = o_ref.shape[0]
        me = self.me = lax.axis_index("tp")
        self.behind = (me, count - 1 - me)
        self.has_next = (me < count - 1, me > 0)
        self.has_prev = (me > 0, me < count - 1)

    def block(self, dest):
        area = pl.ds(pl.multiple_of(dest * self.rows, self.rows), self.rows)
        total = self.x_refs[0][area, :].astype(jnp.float32)
        for x_ref in self.x_refs[1:]:
            total = total + x_ref[area, :].astype(jnp.float32)
        return total

    def hop(self, way, step, source):
        return pltpu.make_async_remote_copy(
            src_ref=source,
            dst_ref=self.recv.at[way, step],
            send_sem=self.send_sem.at[way, step],
            recv_sem=self.recv_sem.at[way, step],
            device_id={"tp": self.me + 1 if way == 0 else self.me - 1},
        )

    def start(self, step):
        count, me, recv = self.count, self.me, self.recv
        for way in range(2):
            dest = count - 1 - step + me if way == 0 else step - (count - 1 - me)
            active = self.has_next[way] & (step >= self.behind[way])

            @pl.when(active & (self.behind[way] == 0))
            def _():
                part = rows_of(self.x_refs[0], dest, self.rows)
                if len(self.x_refs) > 1:
                    part[...] = self.block(dest).astype(part.dtype)
                self.hop(way, step, part).start()

            if step > 0:

                @pl.when(active & (self.behind[way] > 0))
                def _():
                    total = self.block(dest) + recv[way, step - 1].astype(jnp.float32)
                    recv[way, step - 1] = total.astype(recv.dtype)
                    self.hop(way, step, recv.at[way, step - 1]).start()

    def arrive(self, step):
        for way in range(2):

            @pl.when(self.has_prev[way] & (step >= self.behind[way] - 1))
            def _():
                self.hop(way, step, self.recv.at[way, step]).wait_recv()

    def collect(self):
        self.o_ref[...] = self.block(self.me)
        for way in range(2):

            @pl.when(self.has_prev[way])
            def _():
                self.o_ref[...] += self.recv[way, self.count - 2].astype(jnp.float32)

    def finish(self):
        for step in range(self.count - 1):
            for way in range(2):

                @pl.when(self.has_next[way] & (step >= self.behind[way]))
                def _():
                    self.hop(way, step, self.recv.at[way, step]).wait_send()


def line_buffers(count, rows, width):
    return [pltpu.VMEM((2, count - 1, rows, width), jnp.bfloat16)] + line_sems(count)


def own_rows(ref, rows):
    return pl.ds(pl.multiple_of(lax.axis_index("tp") * rows, rows), rows)


def inverse_norm(values):
    return lax.rsqrt(jnp.mean(values * values, axis=-1, keepdims=True) + norm_eps)


def rms_back(incoming, values, gain_row):
    inverse = inverse_norm(values)
    scaled = values * inverse
    gain_grad = jnp.sum(incoming * scaled, axis=0, keepdims=True)
    weighted = incoming * gain_row
    row_inner = jnp.mean(weighted * scaled, axis=-1, keepdims=True)
    return inverse * (weighted - scaled * row_inner), gain_grad


def enter_kernel(count, plane=None):
    barrier = pltpu.get_barrier_semaphore()
    waits = line_signal(barrier, lax.axis_index("tp"), count)
    if plane is not None:
        waits = waits + plane.signal(barrier)
    pl.semaphore_wait(barrier, waits)


def remote_params(ident, limit=60):
    return pltpu.CompilerParams(
        collective_id=ident, has_side_effects=True, vmem_limit_bytes=limit << 20
    )


IN_VMEM = pl.BlockSpec(memory_space=pltpu.VMEM)
IN_PLACE = pl.BlockSpec(memory_space=pl.ANY)
TRANSFER = pl.CostEstimate(flops=0, transcendentals=0, bytes_accessed=150_000_000)


def norm_gather_kernel(count, fsdp_count, low, *refs):
    emb_ref, gain_ref, routes_ref, *refs = refs
    parts, refs = refs[:5], refs[5:]
    stacks, refs = (refs[:3], refs[3:]) if low else ((), refs)
    rows_ref, mask_ref, cols_ref, turned_ref, counts_ref, wo_ref, *refs = refs
    packed, refs = (refs[0], refs[1:]) if low else (None, refs)
    w_ref, row_send, row_recv, *refs = refs
    plane = Plane(fsdp_count)
    join(parts, w_ref)
    if low:
        held, in_sem, out_sem = refs[5:]
        gets, puts = pack_copies(low, stacks, packed, held, in_sem, out_sem)
        for get in gets:
            get.start()
    enter_kernel(count, plane)
    line = LineGather(count, rows_ref, row_send, row_recv)
    weights = PlaneGather(plane, w_ref, wo_ref, *refs[:5])
    start_x = emb_ref[...].astype(jnp.float32) * emb_scale
    normed = start_x * inverse_norm(start_x) * gain_ref[...]
    rows_ref[own_rows(rows_ref, line.rows), :] = normed.astype(jnp.bfloat16)
    for step in range(count - 1):
        line.start(step)
        if step == 0:
            weights.start()
            place_routes(line.rows, routes_ref, mask_ref, cols_ref, turned_ref, counts_ref)
            if low:
                for get, put in zip(gets, puts):
                    get.wait()
                    put.start()
        if step == count - 2:
            weights.forward()
        line.arrive(step)
    if low:
        for put in puts:
            put.wait()
    weights.finish()
    line.finish()


def place_routes(rows, routes_ref, mask_ref, cols_ref, turned_ref, counts_ref):
    group, lanes = mask_ref.shape
    columns = lax.broadcasted_iota(jnp.int32, (rows, lanes), 1)
    for low in range(0, group, rows):
        area = slice(low, low + rows)
        mask = jnp.zeros((rows, lanes), jnp.float32)
        for choice in range(routes_ref.shape[1]):
            mask = jnp.where(routes_ref[area, choice : choice + 1] == columns, 1.0, mask)
        mask_ref[area, :] = mask
    counts_ref[...] = jnp.sum(mask_ref[...], axis=0, keepdims=True).astype(jnp.int32)
    member = mask_ref[...].astype(jnp.bfloat16)
    for low in range(0, group, rows):
        area = slice(low, low + rows)
        here = lax.broadcasted_iota(jnp.int32, (rows, group), 0) + low
        earlier = here > lax.broadcasted_iota(jnp.int32, (rows, group), 1)
        ranks = jnp.dot(
            jnp.where(earlier, 1.0, 0.0).astype(jnp.bfloat16),
            member,
            preferred_element_type=jnp.float32,
        )
        places = jnp.where(mask_ref[area, :] > 0.0, ranks, -1.0)
        cols_ref[area, :] = places.astype(jnp.int32)
        turned_ref[:, area] = places.T.astype(jnp.int32)


def norm_gather(emb, gain_row, routes, parts, w_width, stacks, low, count, fsdp_count, ident):
    rows, width = emb.shape
    group = rows * count
    chips = fsdp_count // 2
    experts, share, hidden = stacks[0].shape
    span = experts - low
    w_rows = parts[0].shape[0]
    outs = [
        jax.ShapeDtypeStruct((group, width), jnp.bfloat16),
        jax.ShapeDtypeStruct((group, 128), jnp.float32),
        jax.ShapeDtypeStruct((group, 128), jnp.int32),
        jax.ShapeDtypeStruct((128, group), jnp.int32),
        jax.ShapeDtypeStruct((1, 128), jnp.int32),
        jax.ShapeDtypeStruct((w_rows * fsdp_count, w_width), jnp.bfloat16),
    ]
    scratch = [pltpu.VMEM((w_rows, w_width), jnp.bfloat16)] + line_sems(count) + [
        pltpu.SemaphoreType.DMA((chips,)),
        pltpu.SemaphoreType.DMA((chips,)),
        pltpu.SemaphoreType.DMA((chips - 1,)),
        pltpu.SemaphoreType.DMA((chips - 1,)),
        pltpu.SemaphoreType.DMA,
    ]
    if low:
        outs.append(jax.ShapeDtypeStruct((span, 3, share, hidden), jnp.bfloat16))
        scratch += [
            pltpu.VMEM((3, span, share, hidden), jnp.bfloat16),
            pltpu.SemaphoreType.DMA((3,)),
            pltpu.SemaphoreType.DMA((3,)),
        ]
    return pl.pallas_call(
        functools.partial(norm_gather_kernel, count, fsdp_count, low),
        out_shape=outs,
        in_specs=[IN_VMEM] * (3 + len(parts)) + [IN_PLACE] * (3 if low else 0),
        out_specs=[IN_VMEM] * 5 + [IN_PLACE] * (len(outs) - 5),
        scratch_shapes=scratch,
        compiler_params=remote_params(ident, 48),
        cost_estimate=TRANSFER,
    )(emb, gain_row, routes, *parts, *(stacks if low else ()))


def mid_kernel(
    count, part_ref, emb_ref, gain_ref, router_ref, mask_ref, cotangent_ref,
    mid_ref, rows_ref, gates_ref, own_gates, moe_grads,
    recv, sum_send, sum_recv, row_send, row_recv, grad_send, grad_recv,
):
    enter_kernel(count)
    total = LineScatter(count, [part_ref], mid_ref, recv, sum_send, sum_recv)
    line = LineGather(count, rows_ref, row_send, row_recv)
    others = LineGather(count, moe_grads, grad_send, grad_recv)
    rows = line.rows
    moe_grads[own_rows(moe_grads, rows), :] = (
        resid_scale * cotangent_ref[...].astype(jnp.float32)
    ).astype(jnp.bfloat16)
    for step in range(count):
        if step < count - 1:
            others.start(step)
        if step > 0:
            total.start(step - 1)
        if step < count - 1:
            others.arrive(step)
        if step > 0:
            total.arrive(step - 1)
    total.collect()
    mid = emb_ref[...].astype(jnp.float32) * emb_scale + resid_scale * mid_ref[...]
    mid_ref[...] = mid
    own = own_rows(rows_ref, rows)
    rows_ref[own, :] = (mid * inverse_norm(mid) * gain_ref[...]).astype(jnp.bfloat16)

    def find_gates(chunk):
        area = pl.ds(pl.multiple_of(chunk * rows, rows), rows)
        logits = jnp.dot(rows_ref[area, :], router_ref[...], preferred_element_type=jnp.float32)
        inside = mask_ref[area, :] > 0.0
        top = jnp.max(jnp.where(inside, logits, masked_value), axis=-1, keepdims=True)
        raised = jnp.where(inside, jnp.exp(jnp.where(inside, logits - top, 0.0)), 0.0)
        gates = raised / jnp.sum(raised, axis=-1, keepdims=True)
        gates_ref[:, area] = gates.T
        return gates

    for step in range(count - 1):
        line.start(step)
        if step == 0:
            own_gates[...] = find_gates(line.me)
        line.arrive(step)

        @pl.when(line.gets[0][step])
        def _():
            find_gates(line.me - 1 - step)

        @pl.when(line.gets[1][step])
        def _():
            find_gates(line.me + 1 + step)

    line.finish()
    total.finish()
    others.finish()


def find_mid(part, emb, gain_row, weights, used, mask, cotangent, count, ident):
    rows, width = emb.shape
    group = rows * count
    return pl.pallas_call(
        functools.partial(mid_kernel, count),
        grid=(1,),
        out_shape=[
            jax.ShapeDtypeStruct((rows, width), jnp.float32),
            jax.ShapeDtypeStruct((group, width), jnp.bfloat16),
            jax.ShapeDtypeStruct((128, group), jnp.float32),
            jax.ShapeDtypeStruct((rows, 128), jnp.float32),
            jax.ShapeDtypeStruct((group, width), jnp.bfloat16),
        ],
        in_specs=[
            IN_VMEM,
            IN_VMEM,
            IN_VMEM,
            pl.BlockSpec((width, 128), lambda step: (0, used // 128)),
            IN_VMEM,
            IN_VMEM,
        ],
        out_specs=[IN_VMEM] * 5,
        scratch_shapes=line_buffers(count, rows, width) + line_sems(count) + line_sems(count),
        compiler_params=remote_params(ident),
        cost_estimate=TRANSFER,
    )(part, emb, gain_row, weights, mask, cotangent)


def moe_back_kernel(count, fsdp_count, runs, picks, *refs):
    dx_refs, y_refs, refs = refs[:runs], refs[runs : 2 * runs], refs[2 * runs :]
    mid_ref, cotangent_ref, own_gates, gain_ref, router_ref, *refs = refs
    grads_ref, refs = (refs[0], refs[1:]) if picks else (None, refs)
    out_ref, mid_grad, gain_grad, sent_ref, *refs = refs
    sums_ref, refs = (refs[0], refs[1:]) if picks else (None, refs)
    (
        dx_parts, y_parts, load_sem, sum_ref, moe_ref,
        recv, sum_send, sum_recv, moe_recv, moe_send, moe_recv_sem, row_send, row_recv, *refs,
    ) = refs
    loads = []
    for index, (source, parts) in enumerate(
        [(ref, dx_parts) for ref in dx_refs] + [(ref, y_parts) for ref in y_refs]
    ):
        loads.append(
            pltpu.make_async_copy(source, parts.at[index % runs], load_sem.at[index])
        )
        loads[-1].start()
    plane = Plane(fsdp_count) if picks else None
    enter_kernel(count, plane)
    total = LineScatter(
        count, [dx_parts.at[run] for run in range(runs)], sum_ref, recv, sum_send, sum_recv
    )
    moe = LineScatter(
        count, [y_parts.at[run] for run in range(runs)], moe_ref, moe_recv, moe_send, moe_recv_sem
    )
    line = LineGather(count, sent_ref, row_send, row_recv)
    experts = ExpertSums(plane, picks, grads_ref, sums_ref, *refs) if picks else None
    rows, width = mid_ref.shape
    for index in range(len(picks)):
        experts.begin(index)
    for load in loads[:runs]:
        load.wait()
    items = experts.items() if picks else []
    each = -(-len(items) // (2 * count - 2))
    for step in range(count - 1):
        total.start(step)
        for item in items[step * each : (step + 1) * each]:
            experts.do(*item)
        total.arrive(step)
    items = items[(count - 1) * each :]
    total.collect()
    gates = own_gates[...]
    gates_grad = sum_ref[:, width:]
    gates_inner = jnp.sum(gates * gates_grad, axis=-1, keepdims=True)
    logits_grad = (gates * (gates_grad - gates_inner)).astype(jnp.bfloat16)
    incoming = sum_ref[:, :width] + contract_last(logits_grad, router_ref[...])
    from_norm, gain_part = rms_back(incoming, mid_ref[...], gain_ref[...])
    grad = cotangent_ref[...].astype(jnp.float32) + from_norm
    mid_grad[...] = grad
    gain_grad[...] = gain_part
    own = own_rows(sent_ref, rows)
    sent_ref[own, :width] = (resid_scale * grad).astype(jnp.bfloat16)
    sent_ref[own, width:] = logits_grad
    for load in loads[runs:]:
        load.wait()
    for step in range(count):
        if step < count - 1:
            line.start(step)
        if step > 0:
            moe.start(step - 1)
        for item in items[step * each : (step + 1) * each]:
            experts.do(*item)
        if step < count - 1:
            line.arrive(step)
        if step > 0:
            moe.arrive(step - 1)
    moe.collect()
    out_ref[...] = (mid_ref[...] + resid_scale * moe_ref[...]).astype(out_ref.dtype)
    for index in range(len(picks)):
        experts.collect(index)
    line.finish()
    total.finish()
    moe.finish()
    if picks:
        experts.finish()


def find_mid_grad(
    dx_parts, y_parts, mid, cotangent, own_gates, gain_row, weights, used, grads, picks,
    count, fsdp_count, ident,
):
    rows, width = mid.shape
    runs, group = len(dx_parts), rows * count
    wide = dx_parts[0].shape[1]
    share = grads.shape[2] // fsdp_count
    sums = [jax.ShapeDtypeStruct((len(picks), 3, share, grads.shape[3]), jnp.bfloat16)]
    sums = sums if picks else []
    return pl.pallas_call(
        functools.partial(moe_back_kernel, count, fsdp_count, runs, picks),
        grid=(1,),
        out_shape=[
            jax.ShapeDtypeStruct((rows, width), jnp.bfloat16),
            jax.ShapeDtypeStruct((rows, width), jnp.float32),
            jax.ShapeDtypeStruct((1, width), jnp.float32),
            jax.ShapeDtypeStruct((group, wide), jnp.bfloat16),
        ]
        + sums,
        in_specs=[IN_PLACE] * (2 * runs)
        + [IN_VMEM] * 4
        + [pl.BlockSpec((width, 128), lambda step: (0, used // 128))]
        + [IN_PLACE] * len(sums),
        out_specs=[IN_VMEM] * 4 + [IN_PLACE] * len(sums),
        scratch_shapes=[
            pltpu.VMEM((runs, group, wide), jnp.bfloat16),
            pltpu.VMEM((runs, group, width), jnp.bfloat16),
            pltpu.SemaphoreType.DMA((2 * runs,)),
            pltpu.VMEM((rows, wide), jnp.float32),
            pltpu.VMEM((rows, width), jnp.float32),
        ]
        + line_buffers(count, rows, wide)
        + line_buffers(count, rows, width)
        + line_sems(count)
        + expert_buffers(len(picks), share, grads.shape[3]),
        compiler_params=remote_params(ident, 63),
        cost_estimate=TRANSFER,
    )(*dx_parts, *y_parts, mid, cotangent, own_gates, gain_row, weights, *([grads] if picks else []))


def finish_kernel(tp_count, fsdp_count, picks, *refs):
    x_ref, w_ref, emb_ref, gain_ref, mid_grad, gain_two, *refs = refs
    grads_ref, refs = (refs[0], refs[1:]) if picks else (None, refs)
    grad_ref, w_sum, gains_ref, *refs = refs
    sums_ref, refs = (refs[0], refs[1:]) if picks else (None, refs)
    (
        line_recv, line_send_sem, line_recv_sem,
        pair_got, chip_sums, chip_got, pair_send, pair_recv, chip_send, chip_recv,
        tp_got, fsdp_got, small_send, small_recv, *refs,
    ) = refs
    plane = Plane(fsdp_count)
    tp_me, fsdp_me = lax.axis_index("tp"), plane.me
    barrier = pltpu.get_barrier_semaphore()
    for shift in range(1, tp_count):
        pl.semaphore_signal(barrier, inc=1, device_id={"tp": lax.rem(tp_me + shift, tp_count)})
    for shift in range(1, fsdp_count):
        pl.semaphore_signal(
            barrier, inc=1, device_id={"fsdp": lax.rem(fsdp_me + shift, fsdp_count)}
        )
    pl.semaphore_wait(barrier, tp_count + fsdp_count - 2)
    line = LineScatter(
        tp_count, [x_ref], grad_ref, line_recv, line_send_sem, line_recv_sem
    )
    rows = w_sum.shape[0]

    def to_pair(shift):
        return pltpu.make_async_remote_copy(
            src_ref=rows_of(w_ref, plane.chip_at(shift) * 2 + 1 - plane.core, rows),
            dst_ref=pair_got.at[shift],
            send_sem=pair_send.at[shift],
            recv_sem=pair_recv.at[shift],
            device_id={"fsdp": plane.partner},
        )

    def to_chip(shift):
        return pltpu.make_async_remote_copy(
            src_ref=chip_sums.at[shift - 1],
            dst_ref=chip_got.at[shift - 1],
            send_sem=chip_send.at[shift - 1],
            recv_sem=chip_recv.at[shift - 1],
            device_id={"fsdp": plane.peer(shift)},
        )

    def both_cores(shift):
        own = pl.ds(pl.multiple_of(plane.peer(shift) * rows, rows), rows)
        return w_ref[own, :].astype(jnp.float32) + pair_got[shift].astype(jnp.float32)

    def exchange(axis, me, count, got, base):
        copies = []
        for shift in range(1, count):
            copies.append(
                pltpu.make_async_remote_copy(
                    src_ref=gains_ref,
                    dst_ref=got.at[me],
                    send_sem=small_send.at[base + shift],
                    recv_sem=small_recv.at[base + shift],
                    device_id={axis: lax.rem(me + shift, count)},
                )
            )
            copies[-1].start()
        got[me] = gains_ref[...]
        for copy in copies:
            copy.wait()
        total = got[0]
        for index in range(1, count):
            total = total + got[index]
        return total

    experts = ExpertSums(plane, picks, grads_ref, sums_ref, *refs) if picks else None
    line.start(0)
    order = list(range(1, plane.chips)) + [0]
    for shift in order:
        to_pair(shift).start()
    for index in range(len(picks)):
        experts.begin(index)
    for shift in order:
        to_pair(shift).wait_recv()
        if shift > 0:
            chip_sums[shift - 1] = both_cores(shift).astype(chip_sums.dtype)
            to_chip(shift).start()
    items = experts.items() if picks else []
    each = -(-len(items) // (tp_count - 2))
    line.arrive(0)
    for step in range(1, tp_count - 1):
        line.start(step)
        for item in items[(step - 1) * each : step * each]:
            experts.do(*item)
        line.arrive(step)
    line.collect()
    from_norm, gain_one = rms_back(
        grad_ref[...], emb_ref[...].astype(jnp.float32) * emb_scale, gain_ref[...]
    )
    gains_ref[...] = jnp.zeros_like(gains_ref)
    gains_ref[0:1, :] = gain_one
    gains_ref[1:2, :] = gain_two[...]
    grad_ref[...] = emb_scale * (mid_grad[...] + from_norm)
    total = both_cores(0)
    for shift in range(1, plane.chips):
        to_chip(shift).wait_recv()
        total = total + chip_got[shift - 1].astype(jnp.float32)
    w_sum[...] = total
    for index in range(len(picks)):
        experts.collect(index)
    gains_ref[...] = exchange("tp", tp_me, tp_count, tp_got, 0)
    gains_ref[...] = exchange("fsdp", fsdp_me, fsdp_count, fsdp_got, tp_count)
    line.finish()
    for shift in order:
        to_pair(shift).wait_send()
        if shift > 0:
            to_chip(shift).wait_send()
    if picks:
        experts.finish()


def finish(dx_rows, weight_grads, emb, gain_row, mid_grad, gain_two, grads, picks, ident):
    tp_count, fsdp_count = lax.axis_size("tp"), lax.axis_size("fsdp")
    rows, width = emb.shape
    w_rows, w_width = weight_grads.shape[0] // fsdp_count, weight_grads.shape[1]
    chips = fsdp_count // 2
    share = grads.shape[2] // fsdp_count
    sums = [jax.ShapeDtypeStruct((len(picks), 3, share, grads.shape[3]), jnp.bfloat16)]
    sums = sums if picks else []
    return pl.pallas_call(
        functools.partial(finish_kernel, tp_count, fsdp_count, picks),
        out_shape=[
            jax.ShapeDtypeStruct((rows, width), jnp.float32),
            jax.ShapeDtypeStruct((w_rows, w_width), jnp.float32),
            jax.ShapeDtypeStruct((8, width), jnp.float32),
            *sums,
        ],
        in_specs=[IN_VMEM] * 6 + [IN_PLACE] * len(sums),
        out_specs=[IN_VMEM] * 3 + [IN_PLACE] * len(sums),
        scratch_shapes=line_buffers(tp_count, rows, width)
        + [
            pltpu.VMEM((chips, w_rows, w_width), jnp.bfloat16),
            pltpu.VMEM((chips - 1, w_rows, w_width), jnp.bfloat16),
            pltpu.VMEM((chips - 1, w_rows, w_width), jnp.bfloat16),
            pltpu.SemaphoreType.DMA((chips,)),
            pltpu.SemaphoreType.DMA((chips,)),
            pltpu.SemaphoreType.DMA((chips - 1,)),
            pltpu.SemaphoreType.DMA((chips - 1,)),
            pltpu.VMEM((tp_count, 8, width), jnp.float32),
            pltpu.VMEM((fsdp_count, 8, width), jnp.float32),
            pltpu.SemaphoreType.DMA((tp_count + fsdp_count,)),
            pltpu.SemaphoreType.DMA((tp_count + fsdp_count,)),
        ]
        + expert_buffers(len(picks), share, grads.shape[3]),
        compiler_params=remote_params(ident),
        cost_estimate=TRANSFER,
    )(dx_rows, weight_grads, emb, gain_row, mid_grad, gain_two, *([grads] if picks else []))


def pack_copies(low, sources, target, held, in_sem, out_sem):
    span = target.shape[0]
    gets = [
        pltpu.make_async_copy(source.at[pl.ds(low, span)], held.at[slot], in_sem.at[slot])
        for slot, source in enumerate(sources)
    ]
    puts = [
        pltpu.make_async_copy(held.at[slot], target.at[:, slot], out_sem.at[slot])
        for slot in range(len(sources))
    ]
    return gets, puts


def pack_kernel(low, *refs):
    sources, target, held, in_sem, out_sem = refs[:-4], *refs[-4:]
    gets, puts = pack_copies(low, sources, target, held, in_sem, out_sem)
    for get in gets:
        get.start()
    for get, put in zip(gets, puts):
        get.wait()
        put.start()
    for put in puts:
        put.wait()


def pack(stacks, low, high):
    _, rows, width = stacks[0].shape
    count, span = len(stacks), high - low
    return pl.pallas_call(
        functools.partial(pack_kernel, low),
        in_specs=[IN_PLACE] * count,
        out_specs=IN_PLACE,
        out_shape=jax.ShapeDtypeStruct((span, count, rows, width), jnp.bfloat16),
        scratch_shapes=[
            pltpu.VMEM((count, span, rows, width), jnp.bfloat16),
            pltpu.SemaphoreType.DMA((count,)),
            pltpu.SemaphoreType.DMA((count,)),
        ],
    )(*stacks)


def join(parts, target):
    *sources, last = parts
    low = 0
    for source in sources:
        target[:, low : low + source.shape[1]] = source[...]
        low += source.shape[1]
    router = last[...].astype(jnp.float32).T.astype(jnp.bfloat16)
    target[:, low:] = jnp.zeros((target.shape[0], target.shape[1] - low), jnp.bfloat16)
    target[:, low : low + router.shape[1]] = router


SLOTS = 256


def experts_kernel(
    first_expert,
    capacity,
    meta,
    place_rows,
    place_cols,
    gate_rows,
    x_ref,
    g_ref,
    weights,
    *refs,
):
    *held, y_ref, dx_ref, grads, load_sem = refs
    step = pl.program_id(0)
    expert = step + first_expert
    group, width = x_ref.shape
    tail = dx_ref.shape[1] - width

    @pl.when(step == 0)
    def _():
        if held:
            loads = [
                pltpu.make_async_copy(source, target, load_sem.at[index])
                for index, (source, target) in enumerate(zip(held, (y_ref, dx_ref)))
            ]
            for load in loads:
                load.start()
            for load in loads:
                load.wait()
        else:
            y_ref[...] = jnp.zeros_like(y_ref)
            dx_ref[...] = jnp.zeros_like(dx_ref)

    column = expert + meta[meta.shape[0] - 1]
    lanes = lax.broadcasted_iota(jnp.int32, place_cols.shape, 1)
    place_col = jnp.sum(jnp.where(lanes == column, place_cols[...], 0), axis=1, keepdims=True)
    place_row = place_rows[pl.ds(column, 1), :]
    gate_row = gate_rows[pl.ds(column, 1), :].astype(jnp.bfloat16).astype(jnp.float32)
    mark = jnp.where(lax.broadcasted_iota(jnp.int32, (1, tail), 1) == column, 1.0, 0.0)

    def run(base, span):
        slots = lax.broadcasted_iota(jnp.int32, (span, group), 0) + base
        hit = slots == place_row
        pick = jnp.where(hit, 1.0, 0.0).astype(jnp.bfloat16)
        scale = jnp.sum(jnp.where(hit, gate_row, 0.0), axis=1, keepdims=True)
        x_taken = jnp.dot(pick, x_ref[...], preferred_element_type=jnp.float32).astype(jnp.bfloat16)
        g_taken = jnp.dot(pick, g_ref[...], preferred_element_type=jnp.float32).astype(jnp.bfloat16)
        gate_pre = jnp.dot(x_taken, weights[0, 0], preferred_element_type=jnp.float32)
        up_pre = jnp.dot(x_taken, weights[0, 1], preferred_element_type=jnp.float32)
        raw = jnp.dot(g_taken, weights[0, 2], preferred_element_type=jnp.float32)
        sig = jax.nn.sigmoid(gate_pre)
        silu = gate_pre * sig
        act = (silu * up_pre).astype(jnp.bfloat16).astype(jnp.float32)
        slot_grad = jnp.sum(act * raw, axis=1, keepdims=True)
        act_grad = raw * scale
        act_scaled = (act * scale).astype(jnp.bfloat16)
        gate_grad = (act_grad * up_pre * sig * (1.0 + gate_pre * (1.0 - sig))).astype(jnp.bfloat16)
        up_grad = (act_grad * silu).astype(jnp.bfloat16)
        extra = (slot_grad * mark).astype(jnp.bfloat16)
        rows_out = contract_last(act_scaled, weights[0, 2]).astype(jnp.bfloat16)
        rows_in = (
            contract_last(gate_grad, weights[0, 0]) + contract_last(up_grad, weights[0, 1])
        ).astype(jnp.bfloat16)
        for slot, left_op, right_op in (
            (0, x_taken, gate_grad),
            (1, x_taken, up_grad),
            (2, g_taken, act_scaled),
        ):
            grad = contract_first(left_op, right_op)
            if base > 0:
                grad = grad + grads[0, slot].astype(jnp.float32)
            grads[0, slot] = grad.astype(jnp.bfloat16)
        block = min(256, group)
        for start in range(0, group, block):
            back = jnp.where(
                lax.broadcasted_iota(jnp.int32, (block, span), 1) + base
                == place_col[start : start + block],
                1.0,
                0.0,
            ).astype(jnp.bfloat16)
            for target, low_col, addend in (
                (y_ref, 0, rows_out),
                (dx_ref, 0, rows_in),
                (dx_ref, width, extra),
            ):
                area = (slice(start, start + block), slice(low_col, low_col + addend.shape[1]))
                target[area] = (
                    target[area].astype(jnp.float32)
                    + jnp.dot(back, addend, preferred_element_type=jnp.float32)
                ).astype(target.dtype)

    run(0, min(SLOTS, capacity))
    for base in range(SLOTS, capacity, SLOTS):
        span = min(SLOTS, -(-(capacity - base) // 16) * 16)

        @pl.when(meta[column] > base)
        def _():
            run(base, span)


def experts_step(meta, place_rows, place_cols, gate_rows, x_rows, g_rows, weights, held, first, count, skip, capacity):
    group, width = x_rows.shape
    hidden = weights.shape[-1]
    tail = 128

    def whole(shape):
        return pl.BlockSpec(
            shape, lambda step, meta: (0,) * len(shape), pipeline_mode=pl.Buffered(1)
        )

    def big(offset):
        return pl.BlockSpec((1, 3, width, hidden), lambda step, meta: (step + offset, 0, 0, 0))

    return pl.pallas_call(
        functools.partial(experts_kernel, first, capacity),
        grid_spec=pltpu.PrefetchScalarGridSpec(
            num_scalar_prefetch=1,
            grid=(count,),
            in_specs=[
                whole(place_rows.shape),
                whole(place_cols.shape),
                whole(gate_rows.shape),
                whole(x_rows.shape),
                whole(g_rows.shape),
                big(skip),
            ]
            + [IN_PLACE] * len(held),
            out_specs=[
                whole((group, width)),
                whole((group, width + tail)),
                big(0),
            ],
            scratch_shapes=[pltpu.SemaphoreType.DMA((2,))],
        ),
        out_shape=[
            jax.ShapeDtypeStruct((group, width), jnp.bfloat16),
            jax.ShapeDtypeStruct((group, width + tail), jnp.bfloat16),
            jax.ShapeDtypeStruct((count, 3, width, hidden), jnp.bfloat16),
        ],
        compiler_params=pltpu.CompilerParams(
            dimension_semantics=("arbitrary",), vmem_limit_bytes=63 << 20
        ),
        cost_estimate=pl.CostEstimate(
            flops=count * 17 * 2 * 408 * width * hidden,
            transcendentals=count * 408 * hidden,
            bytes_accessed=count * 12 * width * hidden,
        ),
    )(meta, place_rows, place_cols, gate_rows, x_rows, g_rows, weights, *held)


def rotate_head(values, cosine, sine, sign):
    half = values.shape[-1] // 2
    other = jnp.concatenate([values[:, half:], values[:, :half]], axis=1)
    return values * cosine + other * (sine * sign)


def segment_bias(seg_row):
    length = seg_row.shape[1]
    shape = (length, length)
    seg_row = seg_row.astype(jnp.float32)
    seg_col = jnp.broadcast_to(seg_row, (128, length)).T[:, :1]
    keys = lax.broadcasted_iota(jnp.int32, shape, 0)
    queries = lax.broadcasted_iota(jnp.int32, shape, 1)
    return jnp.where((keys <= queries) & (seg_col == seg_row), 0.0, masked_value)


def attend_kernel(
    x_ref,
    w_ref,
    seg_row,
    cos_ref,
    sin_ref,
    q_ref,
    k_ref,
    v_ref,
    mixed_ref,
    logsum_ref,
    branch_ref,
    bias,
    v_turned,
    mixed_heads,
):
    heads, kv_heads = q_ref.shape[0], k_ref.shape[0]
    per_kv = heads // kv_heads
    block = SEQ // 2
    edge = (heads + 2 * kv_heads) * HEAD_DIM
    proj = jnp.dot(x_ref[...], w_ref[:, :edge], preferred_element_type=jnp.float32)
    cosine, sine = cos_ref[...], sin_ref[...]
    for head in range(heads + 2 * kv_heads):
        part = proj[:, head * HEAD_DIM : (head + 1) * HEAD_DIM]
        if head < heads:
            q_ref[head] = rotate_head(part, cosine, sine, 1.0).astype(jnp.bfloat16)
        elif head < heads + kv_heads:
            k_ref[head - heads] = rotate_head(part, cosine, sine, 1.0).astype(jnp.bfloat16)
        else:
            v_ref[head - heads - kv_heads] = part.astype(jnp.bfloat16)
            v_turned[head - heads - kv_heads] = part.T.astype(jnp.bfloat16)
    bias[...] = segment_bias(seg_row[0])

    def one_head(head, carry):
        kv = head // per_kv
        for part in range(2):
            span, low = block * (part + 1), block * part
            scores = contract_last(k_ref[kv, :span], q_ref[head, low : low + block]) * attn_scale
            scores = scores + bias[:span, low : low + block]
            top = jnp.max(scores, axis=0, keepdims=True)
            raised = jnp.exp(scores - top)
            total = jnp.sum(raised, axis=0, keepdims=True)
            probs = (raised * (1.0 / total)).astype(jnp.bfloat16)
            turned = jnp.dot(v_turned[kv, :, :span], probs, preferred_element_type=jnp.float32)
            mixed_heads[head, low : low + block, :] = turned.T.astype(jnp.bfloat16)
            logsum_ref[0, pl.ds(head, 1), low : low + block] = top + jnp.log(total)
        return carry

    lax.fori_loop(0, heads, one_head, 0)
    for head in range(heads):
        mixed_ref[:, head * HEAD_DIM : (head + 1) * HEAD_DIM] = mixed_heads[head]
    branch_ref[...] = contract_last(
        mixed_ref[...], w_ref[:, edge : edge + heads * HEAD_DIM]
    ).astype(jnp.bfloat16)


def attend_back_kernel(
    x_ref,
    w_ref,
    seg_row,
    cos_ref,
    sin_ref,
    q_ref,
    k_ref,
    v_ref,
    mixed_ref,
    logsum_ref,
    moe_rows,
    branch_grad,
    dx_ref,
    dw_ref,
    bias,
    k_turned,
    mixed_grads,
    q_grads,
    kv_grads,
    qkv_grad,
    dw_acc,
):
    heads, kv_heads = q_ref.shape[0], k_ref.shape[0]
    per_kv = heads // kv_heads
    block = SEQ // 2
    edge = (heads + 2 * kv_heads) * HEAD_DIM
    step = pl.program_id(0)
    out_edge = edge + heads * HEAD_DIM
    width = x_ref.shape[1]
    grad = jnp.dot(
        branch_grad[:, :width], w_ref[:, edge:out_edge], preferred_element_type=jnp.float32
    ).astype(jnp.bfloat16)
    for head in range(heads):
        mixed_grads[head] = grad[:, head * HEAD_DIM : (head + 1) * HEAD_DIM]
    for kv in range(kv_heads):
        k_turned[kv] = k_ref[kv].astype(jnp.float32).T.astype(jnp.bfloat16)
    bias[...] = segment_bias(seg_row[0])
    kv_grads[...] = jnp.zeros_like(kv_grads)

    def one_head(head, carry):
        kv = head // per_kv
        for part in range(2):
            span, low = block * (part + 1), block * part
            high = low + block
            scores = contract_last(k_ref[kv, :span], q_ref[head, low:high]) * attn_scale
            scores = scores + bias[:span, low:high]
            probs = jnp.exp(scores - logsum_ref[0, pl.ds(head, 1), low:high])
            probs_grad = contract_last(v_ref[kv, :span], mixed_grads[head, low:high])
            inner = jnp.sum(probs * probs_grad, axis=0, keepdims=True)
            score_grad = (probs * (probs_grad - inner)).astype(jnp.bfloat16)
            turned = jnp.dot(k_turned[kv, :, :span], score_grad, preferred_element_type=jnp.float32)
            q_grads[head, low:high, :] = turned.T * attn_scale
            kv_grads[0, kv, :span, :] += jnp.dot(
                score_grad, q_ref[head, low:high], preferred_element_type=jnp.float32
            )
            kv_grads[1, kv, :span, :] += jnp.dot(
                probs.astype(jnp.bfloat16), mixed_grads[head, low:high],
                preferred_element_type=jnp.float32,
            )
        return carry

    lax.fori_loop(0, heads, one_head, 0)
    cosine, sine = cos_ref[...], sin_ref[...]
    for head in range(heads + 2 * kv_heads):
        if head < heads:
            part = rotate_head(q_grads[head], cosine, sine, -1.0)
        elif head < heads + kv_heads:
            part = rotate_head(kv_grads[0, head - heads] * attn_scale, cosine, sine, -1.0)
        else:
            part = kv_grads[1, head - heads - kv_heads]
        qkv_grad[:, head * HEAD_DIM : (head + 1) * HEAD_DIM] = part.astype(jnp.bfloat16)
    dx_ref[...] = contract_last(qkv_grad[...], w_ref[:, :edge]).astype(jnp.bfloat16)
    for low, high, left_op, right_op in (
        (0, edge, x_ref[...], qkv_grad[...]),
        (edge, out_edge, branch_grad[:, :width], mixed_ref[...]),
        (out_edge, dw_acc.shape[1], moe_rows[...], branch_grad[:, width:]),
    ):
        part = contract_first(left_op, right_op)

        @pl.when(step == 0)
        def _():
            dw_acc[:, low:high] = part

        @pl.when(step > 0)
        def _():
            dw_acc[:, low:high] += part

    @pl.when(step == pl.num_programs(0) - 1)
    def _():
        dw_ref[...] = dw_acc[...].astype(jnp.bfloat16)


def fixed(shape):
    return pl.BlockSpec(shape, lambda seq: (0,) * len(shape), pipeline_mode=pl.Buffered(1))


def by_row(width):
    return pl.BlockSpec((SEQ, width), lambda seq: (seq, 0))


def by_head(heads):
    return pl.BlockSpec((heads, SEQ, HEAD_DIM), lambda seq: (0, seq, 0))


def attend_tables():
    half = HEAD_DIM // 2
    positions = np.arange(SEQ, dtype=np.float32)
    frequency = np.float32(rope_base) ** (-np.arange(half, dtype=np.float32) * 2.0 / HEAD_DIM)
    angles = (positions[:, None] * frequency[None, :].astype(np.float32)).astype(np.float32)
    cosine, sine = np.cos(angles), np.sin(angles)
    return (
        jnp.asarray(np.concatenate([cosine, cosine], axis=1)),
        jnp.asarray(np.concatenate([-sine, sine], axis=1)),
    )


def attend(rows, weights, segments, tables, heads, kv_heads):
    group, width = rows.shape
    seqs = group // SEQ
    return pl.pallas_call(
        attend_kernel,
        grid=(seqs,),
        in_specs=[
            by_row(width),
            fixed(weights.shape),
            pl.BlockSpec((1, 1, SEQ), lambda seq: (seq, 0, 0)),
            fixed(tables[0].shape),
            fixed(tables[1].shape),
        ],
        out_specs=[
            by_head(heads),
            by_head(kv_heads),
            by_head(kv_heads),
            by_row(heads * HEAD_DIM),
            pl.BlockSpec((1, heads, SEQ), lambda seq: (seq, 0, 0)),
            by_row(width),
        ],
        out_shape=[
            jax.ShapeDtypeStruct((heads, group, HEAD_DIM), jnp.bfloat16),
            jax.ShapeDtypeStruct((kv_heads, group, HEAD_DIM), jnp.bfloat16),
            jax.ShapeDtypeStruct((kv_heads, group, HEAD_DIM), jnp.bfloat16),
            jax.ShapeDtypeStruct((group, heads * HEAD_DIM), jnp.bfloat16),
            jax.ShapeDtypeStruct((seqs, heads, SEQ), jnp.float32),
            jax.ShapeDtypeStruct((group, width), jnp.bfloat16),
        ],
        scratch_shapes=[
            pltpu.VMEM((SEQ, SEQ), jnp.float32),
            pltpu.VMEM((kv_heads, HEAD_DIM, SEQ), jnp.bfloat16),
            pltpu.VMEM((heads, SEQ, HEAD_DIM), jnp.bfloat16),
        ],
        compiler_params=pltpu.CompilerParams(
            dimension_semantics=("arbitrary",), vmem_limit_bytes=56 << 20
        ),
        cost_estimate=pl.CostEstimate(
            flops=10_000_000_000, transcendentals=3_000_000, bytes_accessed=60_000_000
        ),
    )(rows, weights, segments[:, None, :], *tables)


def attend_back(rows, weights, segments, tables, kept, moe_rows, branch_grad):
    queries, keys, values, mixed, logsum = kept
    group, width = rows.shape
    heads, kv_heads = queries.shape[0], keys.shape[0]
    used = weights.shape[1]
    edge = (heads + 2 * kv_heads) * HEAD_DIM
    return pl.pallas_call(
        attend_back_kernel,
        grid=(group // SEQ,),
        in_specs=[
            by_row(width),
            fixed(weights.shape),
            pl.BlockSpec((1, 1, SEQ), lambda seq: (seq, 0, 0)),
            fixed(tables[0].shape),
            fixed(tables[1].shape),
            by_head(heads),
            by_head(kv_heads),
            by_head(kv_heads),
            by_row(heads * HEAD_DIM),
            pl.BlockSpec((1, heads, SEQ), lambda seq: (seq, 0, 0)),
            by_row(width),
            by_row(branch_grad.shape[1]),
        ],
        out_specs=[by_row(width), fixed((width, used))],
        out_shape=[
            jax.ShapeDtypeStruct((group, width), jnp.bfloat16),
            jax.ShapeDtypeStruct((width, used), jnp.bfloat16),
        ],
        scratch_shapes=[
            pltpu.VMEM((SEQ, SEQ), jnp.float32),
            pltpu.VMEM((kv_heads, HEAD_DIM, SEQ), jnp.bfloat16),
            pltpu.VMEM((heads, SEQ, HEAD_DIM), jnp.bfloat16),
            pltpu.VMEM((heads, SEQ, HEAD_DIM), jnp.float32),
            pltpu.VMEM((2, kv_heads, SEQ, HEAD_DIM), jnp.float32),
            pltpu.VMEM((SEQ, edge), jnp.bfloat16),
            pltpu.VMEM((width, used), jnp.float32),
        ],
        compiler_params=pltpu.CompilerParams(
            dimension_semantics=("arbitrary",), vmem_limit_bytes=60 << 20
        ),
        cost_estimate=pl.CostEstimate(
            flops=20_000_000_000, transcendentals=3_000_000, bytes_accessed=100_000_000
        ),
    )(rows, weights, segments[:, None, :], *tables,
      queries, keys, values, mixed, logsum, moe_rows, branch_grad)


def outputs_kernel(edges, attn_ref, gains_ref, *refs):
    step = pl.program_id(0)
    packed, refs = refs[: len(edges) - 1], refs[len(edges) - 1 :]
    *small, router_ref, gain_one, gain_two = refs[:7]
    targets = refs[7:]

    @pl.when(step == 0)
    def _():
        low = 0
        for target in small:
            target[...] = attn_ref[:, low : low + target.shape[1]]
            low += target.shape[1]
        router_ref[...] = attn_ref[:, low:].T[: router_ref.shape[0], :]
        gain_one[...] = gains_ref[0:1, :]
        gain_two[...] = gains_ref[1:2, :]

    for part, low, high in zip(packed, edges[:-1], edges[1:]):

        @pl.when((step >= low) & (step < high))
        def _():
            for slot, target in enumerate(targets):
                target[0] = part[0, slot].astype(jnp.float32)


def outputs(attn_sum, gains, packed, edges, widths, expert_count):
    _, _, rows, width = packed[0].shape
    shapes = [(rows, span) for span in widths] + [(expert_count, rows)] + [(1, gains.shape[1])] * 2

    def home(low, high):
        return pl.BlockSpec(
            (1, 3, rows, width),
            lambda step: (jnp.clip(step - low, 0, high - low - 1), 0, 0, 0),
        )

    def still(shape):
        return pl.BlockSpec(shape, lambda step: (0,) * len(shape))

    return pl.pallas_call(
        functools.partial(outputs_kernel, edges),
        grid=(edges[-1],),
        in_specs=[still(attn_sum.shape), still(gains.shape)]
        + [home(low, high) for low, high in zip(edges[:-1], edges[1:])],
        out_specs=[still(shape) for shape in shapes]
        + [pl.BlockSpec((1, rows, width), lambda step: (step, 0, 0))] * 3,
        out_shape=[jax.ShapeDtypeStruct(shape, jnp.float32) for shape in shapes]
        + [jax.ShapeDtypeStruct((edges[-1], rows, width), jnp.float32)] * 3,
    )(attn_sum, gains, *packed)


RUNS = (0, 6, 10)
DIRECT = (3, 1)


def local(
    emb,
    segment_ids,
    routes,
    norm1_gain,
    w_query,
    w_key,
    w_value,
    w_out,
    norm2_gain,
    w_router,
    w_gate,
    w_up,
    w_down,
    cotangent,
):
    local_rows, width = emb.shape
    tp_count, tp_index = lax.axis_size("tp"), lax.axis_index("tp")
    experts_here = w_gate.shape[0]
    expert_count = w_router.shape[1]
    q_width, kv_width = w_query.shape[1], w_key.shape[1]
    used = 2 * (q_width + kv_width)
    group_size = local_rows * tp_count
    fsdp_count = lax.axis_size("fsdp")
    split = group_size <= 1024
    runs = [edge * experts_here // RUNS[-1] for edge in RUNS] if split else [0, experts_here]
    stacks = (w_gate, w_up, w_down)
    pieces = [lax.all_gather(pack(stacks, 0, runs[1]), "fsdp", axis=2, tiled=True)]
    gain_one = norm1_gain.astype(jnp.float32)[None, :]
    gain_two = norm2_gain.astype(jnp.float32)[None, :]
    group_rows, mask, place_cols, place_rows, counts, attn_w, *packed = norm_gather(
        emb,
        gain_one,
        routes,
        [w_query, w_key, w_value, w_out, w_router.T],
        used + 128,
        stacks,
        runs[1] if split else 0,
        tp_count,
        fsdp_count,
        0,
    )
    if split:
        pieces.append(lax.all_gather(packed[0], "fsdp", axis=2, tiled=True))
    capacity = group_size * routes.shape[1] // expert_count * 2
    meta = jnp.concatenate([counts[0], (tp_index * experts_here)[None]])

    tables = attend_tables()
    heads_here, kv_here = q_width // HEAD_DIM, kv_width // HEAD_DIM
    *kept, branch_part = attend(group_rows, attn_w, segment_ids, tables, heads_here, kv_here)
    mid_x, moe_rows, gate_rows, own_gates, moe_grad_rows = find_mid(
        branch_part, emb, gain_two, attn_w, used, mask, cotangent, tp_count, 1
    )

    outs = []
    for first, last, piece in zip(runs[:-1], runs[1:], pieces):
        outs.append(
            experts_step(
                meta,
                place_rows,
                place_cols,
                gate_rows,
                moe_rows,
                moe_grad_rows,
                piece,
                outs[-1][:2] if outs else (),
                first,
                last - first,
                0,
                capacity,
            )
        )
    grad_sums = [lax.psum_scatter(outs[0][2], "fsdp", scatter_dimension=2, tiled=True)]
    last_grads = outs[-1][2]
    picks = (tuple(range(DIRECT[0])), tuple(range(DIRECT[0], sum(DIRECT)))) if split else ((), ())
    out, mid_grad, gain_two_grad, sent, *mid_sums = find_mid_grad(
        outs[-1][1:2],
        outs[-1][0:1],
        mid_x,
        cotangent,
        own_gates,
        gain_two,
        attn_w,
        used,
        last_grads,
        picks[0],
        tp_count,
        fsdp_count,
        2,
    )
    dx_one, attn_grads = attend_back(
        group_rows, attn_w, segment_ids, tables, kept, moe_rows, sent
    )
    grad_emb, attn_sum, gain_sums, *end_sums = finish(
        dx_one, attn_grads, emb, gain_one, mid_grad, gain_two_grad, last_grads, picks[1], 3
    )
    grad_sums = grad_sums + mid_sums + end_sums
    ends = [0]
    for part in grad_sums:
        ends.append(ends[-1] + part.shape[0])
    widths = [q_width, kv_width, kv_width, q_width]
    *attn_outs, router_turned, gain_one_sum, gain_two_sum, gate_sum, up_sum, down_sum = outputs(
        attn_sum, gain_sums, grad_sums, ends, widths, expert_count
    )
    return (
        out,
        grad_emb,
        gain_one_sum[0],
        *attn_outs,
        gain_two_sum[0],
        router_turned.T,
        gate_sum,
        up_sum,
        down_sum,
    )


def solution(mesh):
    return jax.shard_map(
        local,
        mesh=mesh,
        in_specs=(
            P(("fsdp", "tp"), None),
            P("fsdp", None),
            P("fsdp", None),
            P(),
            P("fsdp", "tp"),
            P("fsdp", "tp"),
            P("fsdp", "tp"),
            P("fsdp", "tp"),
            P(),
            P("fsdp", None),
            P("tp", "fsdp", None),
            P("tp", "fsdp", None),
            P("tp", "fsdp", None),
            P(("fsdp", "tp"), None),
        ),
        out_specs=(
            P(("fsdp", "tp"), None),
            P(("fsdp", "tp"), None),
            P(),
            P("fsdp", "tp"),
            P("fsdp", "tp"),
            P("fsdp", "tp"),
            P("fsdp", "tp"),
            P(),
            P("fsdp", None),
            P("tp", "fsdp", None),
            P("tp", "fsdp", None),
            P("tp", "fsdp", None),
        ),
        check_vma=False,
    )
```

```python
import functools

import jax
import jax.numpy as jnp
import numpy as np
from jax import lax
from jax.experimental import pallas as pl
from jax.experimental.pallas import tpu as pltpu
from jax.sharding import PartitionSpec as P

HEAD_DIM = 64
SEQ = 512


emb_scale = 12.0
resid_scale = 0.22
attn_scale = 0.015625
norm_eps = 1e-06
rope_base = 10000.0
masked_value = -1e30


def contract_last(left_op, right_op):
    return lax.dot_general(
        left_op, right_op, (((1,), (1,)), ((), ())), preferred_element_type=jnp.float32
    )


def contract_first(left_op, right_op):
    return lax.dot_general(
        left_op, right_op, (((0,), (0,)), ((), ())), preferred_element_type=jnp.float32
    )


def line_signal(barrier, me, count):
    @pl.when(me > 0)
    def _():
        pl.semaphore_signal(barrier, inc=1, device_id={"tp": me - 1})

    @pl.when(me < count - 1)
    def _():
        pl.semaphore_signal(barrier, inc=1, device_id={"tp": me + 1})

    return jnp.where((me > 0) & (me < count - 1), 2, 1)


class Plane:
    def __init__(self, count):
        self.me = lax.axis_index("fsdp")
        self.core = lax.rem(self.me, 2)
        self.chip = lax.div(self.me, 2)
        self.chips = count // 2
        self.partner = self.me + 1 - 2 * self.core

    def chip_at(self, shift):
        return lax.rem(self.chip + shift + self.chips, self.chips)

    def peer(self, shift):
        return self.chip_at(shift) * 2 + self.core

    def signal(self, barrier):
        for shift in range(1, self.chips):
            pl.semaphore_signal(barrier, inc=1, device_id={"fsdp": self.peer(shift)})
        pl.semaphore_signal(barrier, inc=1, device_id={"fsdp": self.partner})
        return self.chips


def rows_of(ref, index, rows):
    return ref.at[pl.ds(pl.multiple_of(index * rows, rows), rows)]


class LineGather:
    def __init__(self, count, o_ref, send_sem, recv_sem):
        self.count, self.o_ref = count, o_ref
        self.send_sem, self.recv_sem = send_sem, recv_sem
        self.rows = o_ref.shape[0] // count
        me = self.me = lax.axis_index("tp")
        steps = range(count - 1)
        self.sends = [
            [(me >= step) & (me < count - 1) for step in steps],
            [(me + step < count) & (me > 0) for step in steps],
        ]
        self.gets = [
            [me - 1 - step >= 0 for step in steps],
            [me + 1 + step < count for step in steps],
        ]

    def hop(self, way, step, chunk):
        part = rows_of(self.o_ref, chunk, self.rows)
        return pltpu.make_async_remote_copy(
            src_ref=part,
            dst_ref=part,
            send_sem=self.send_sem.at[way, step],
            recv_sem=self.recv_sem.at[way, step],
            device_id={"tp": self.me + 1 if way == 0 else self.me - 1},
        )

    def start(self, step):
        @pl.when(self.sends[0][step])
        def _():
            self.hop(0, step, self.me - step).start()

        @pl.when(self.sends[1][step])
        def _():
            self.hop(1, step, self.me + step).start()

    def arrive(self, step):
        @pl.when(self.gets[0][step])
        def _():
            self.hop(0, step, self.me - 1 - step).wait_recv()

        @pl.when(self.gets[1][step])
        def _():
            self.hop(1, step, self.me + 1 + step).wait_recv()

    def finish(self):
        for step in range(self.count - 1):

            @pl.when(self.sends[0][step])
            def _():
                self.hop(0, step, self.me - step).wait_send()

            @pl.when(self.sends[1][step])
            def _():
                self.hop(1, step, self.me + step).wait_send()


def line_sems(count):
    return [
        pltpu.SemaphoreType.DMA((2, count - 1)),
        pltpu.SemaphoreType.DMA((2, count - 1)),
    ]


class PlaneGather:
    def __init__(self, plane, w_ref, wo_ref, out_send, out_recv, on_send, on_recv, kept_sem):
        self.plane, self.w_ref, self.wo_ref = plane, w_ref, wo_ref
        self.out_send, self.out_recv = out_send, out_recv
        self.on_send, self.on_recv = on_send, on_recv
        self.rows = w_ref.shape[0]
        self.kept = pltpu.make_async_copy(w_ref, rows_of(wo_ref, plane.me, self.rows), kept_sem)

    def outward(self, shift, target, source_device):
        return pltpu.make_async_remote_copy(
            src_ref=self.w_ref,
            dst_ref=rows_of(self.wo_ref, source_device, self.rows),
            send_sem=self.out_send.at[shift],
            recv_sem=self.out_recv.at[shift],
            device_id={"fsdp": target},
        )

    def onward(self, shift, source_device):
        part = rows_of(self.wo_ref, source_device, self.rows)
        return pltpu.make_async_remote_copy(
            src_ref=part,
            dst_ref=part,
            send_sem=self.on_send.at[shift - 1],
            recv_sem=self.on_recv.at[shift - 1],
            device_id={"fsdp": self.plane.partner},
        )

    def start(self):
        plane = self.plane
        for shift in range(1, plane.chips):
            self.outward(shift, plane.peer(shift), plane.me).start()
        self.outward(0, plane.partner, plane.me).start()
        self.kept.start()

    def forward(self):
        plane = self.plane
        for shift in range(1, plane.chips):
            self.outward(shift, plane.peer(shift), plane.peer(-shift)).wait_recv()
            self.onward(shift, plane.peer(-shift)).start()

    def finish(self):
        plane = self.plane
        self.outward(0, plane.partner, plane.partner).wait_recv()
        for shift in range(1, plane.chips):
            self.onward(shift, plane.chip_at(-shift) * 2 + 1 - plane.core).wait_recv()
        for shift in range(1, plane.chips):
            self.outward(shift, plane.peer(shift), plane.me).wait_send()
            self.onward(shift, plane.peer(-shift)).wait_send()
        self.outward(0, plane.partner, plane.me).wait_send()
        self.kept.wait()


class ExpertSums:
    NEAR = {0: (1, 0), 1: (3, 0), 2: (2, 1), 3: (3, 1), 4: (2, 0), 5: (1, 1)}

    def __init__(self, plane, picks, grads_ref, out_ref, *refs):
        self.plane, self.picks, self.grads_ref, self.out_ref = plane, picks, grads_ref, out_ref
        (
            self.got, self.own, self.hop_got, self.held,
            self.pair_send, self.pair_recv, self.own_sem,
            self.hop_send, self.hop_recv, self.put_sem,
        ) = refs
        self.rows = out_ref.shape[2]
        self.half = self.rows // 2

    def chip_by(self, way):
        chip = self.plane.chip
        low, high = lax.rem(chip, 2), lax.div(chip, 2)
        if way % 2:
            low = 1 - low
        if way >= 2:
            high = 1 - high
        return high * 2 + low

    def area(self, index, dest):
        low = pl.multiple_of(dest * self.rows, self.rows)
        return self.grads_ref.at[self.picks[index], :, pl.ds(low, self.rows)]

    def part(self, index, way, half):
        return self.own.at[index, way, :, pl.ds(half * self.half, self.half)]

    def to_pair(self, index, way):
        return pltpu.make_async_remote_copy(
            src_ref=self.area(index, self.chip_by(way) * 2 + 1 - self.plane.core),
            dst_ref=self.got.at[index, way],
            send_sem=self.pair_send.at[index, way],
            recv_sem=self.pair_recv.at[index, way],
            device_id={"fsdp": self.plane.partner},
        )

    def keep(self, index, way):
        return pltpu.make_async_copy(
            self.area(index, self.chip_by(way) * 2 + self.plane.core),
            self.own.at[index, way],
            self.own_sem.at[index, way],
        )

    def hop(self, index, slot):
        way, half = self.NEAR[slot]
        source = self.part(index, way, half) if slot < 4 else self.hop_got.at[index, 2 * slot - 7]
        target = (1, 1, 2, 2, 2, 1)[slot]
        return pltpu.make_async_remote_copy(
            src_ref=source,
            dst_ref=self.hop_got.at[index, slot],
            send_sem=self.hop_send.at[index, slot],
            recv_sem=self.hop_recv.at[index, slot],
            device_id={"fsdp": self.chip_by(target) * 2 + self.plane.core},
        )

    def put(self, index):
        return pltpu.make_async_copy(
            self.held.at[index], self.out_ref.at[index], self.put_sem.at[index]
        )

    def begin(self, index):
        for way in (3, 1, 2, 0):
            self.to_pair(index, way).start()
            self.keep(index, way).start()

    def both_cores(self, index, way):
        self.to_pair(index, way).wait_recv()
        self.keep(index, way).wait()
        for slot in range(self.own.shape[2]):
            both = self.own[index, way, slot].astype(jnp.float32) + self.got[
                index, way, slot
            ].astype(jnp.float32)
            self.own[index, way, slot] = both.astype(jnp.bfloat16)

    def items(self):
        count = len(self.picks)
        order = []
        for index in range(count + 1):
            if index < count:
                order += [(index, 0), (index, 1)]
            if index > 0:
                order += [(index - 1, 2), (index - 1, 3)]
        return order

    def do(self, index, stage):
        if stage == 0:
            self.both_cores(index, 3)
            self.hop(index, 1).start()
            self.hop(index, 3).start()
        elif stage == 1:
            self.both_cores(index, 1)
            self.hop(index, 0).start()
            self.both_cores(index, 2)
            self.hop(index, 2).start()
        elif stage == 2:
            for slot in (4, 5):
                behind = 2 * slot - 7
                way, half = self.NEAR[slot]
                self.hop(index, behind).wait_recv()
                for layer in range(self.own.shape[2]):
                    mine = self.own[
                        index, way, layer, half * self.half : (half + 1) * self.half, :
                    ].astype(jnp.float32)
                    total = mine + self.hop_got[index, behind, layer].astype(jnp.float32)
                    self.hop_got[index, behind, layer] = total.astype(jnp.bfloat16)
                self.hop(index, slot).start()
        else:
            self.both_cores(index, 0)

    def collect(self, index):
        for half, slots in ((0, (0, 4)), (1, (2, 5))):
            area = slice(half * self.half, (half + 1) * self.half)
            for slot in slots:
                self.hop(index, slot).wait_recv()
            for layer in range(self.own.shape[2]):
                total = self.own[index, 0, layer, area, :].astype(jnp.float32)
                for slot in slots:
                    total = total + self.hop_got[index, slot, layer].astype(jnp.float32)
                self.held[index, layer, area, :] = total.astype(jnp.bfloat16)
        self.put(index).start()

    def finish(self):
        for index in range(len(self.picks)):
            self.put(index).wait()
            for way in range(4):
                self.to_pair(index, way).wait_send()
            for slot in range(6):
                self.hop(index, slot).wait_send()


def expert_buffers(count, rows, width):
    if count == 0:
        return []
    return [
        pltpu.VMEM((count, 4, 3, rows, width), jnp.bfloat16),
        pltpu.VMEM((count, 4, 3, rows, width), jnp.bfloat16),
        pltpu.VMEM((count, 6, 3, rows // 2, width), jnp.bfloat16),
        pltpu.VMEM((count, 3, rows, width), jnp.bfloat16),
        pltpu.SemaphoreType.DMA((count, 4)),
        pltpu.SemaphoreType.DMA((count, 4)),
        pltpu.SemaphoreType.DMA((count, 4)),
        pltpu.SemaphoreType.DMA((count, 6)),
        pltpu.SemaphoreType.DMA((count, 6)),
        pltpu.SemaphoreType.DMA((count,)),
    ]


class LineScatter:
    def __init__(self, count, x_refs, o_ref, recv, send_sem, recv_sem):
        self.count, self.x_refs, self.o_ref, self.recv = count, x_refs, o_ref, recv
        self.send_sem, self.recv_sem = send_sem, recv_sem
        self.rows = o_ref.shape[0]
        me = self.me = lax.axis_index("tp")
        self.behind = (me, count - 1 - me)
        self.has_next = (me < count - 1, me > 0)
        self.has_prev = (me > 0, me < count - 1)

    def block(self, dest):
        area = pl.ds(pl.multiple_of(dest * self.rows, self.rows), self.rows)
        total = self.x_refs[0][area, :].astype(jnp.float32)
        for x_ref in self.x_refs[1:]:
            total = total + x_ref[area, :].astype(jnp.float32)
        return total

    def hop(self, way, step, source):
        return pltpu.make_async_remote_copy(
            src_ref=source,
            dst_ref=self.recv.at[way, step],
            send_sem=self.send_sem.at[way, step],
            recv_sem=self.recv_sem.at[way, step],
            device_id={"tp": self.me + 1 if way == 0 else self.me - 1},
        )

    def start(self, step):
        count, me, recv = self.count, self.me, self.recv
        for way in range(2):
            dest = count - 1 - step + me if way == 0 else step - (count - 1 - me)
            active = self.has_next[way] & (step >= self.behind[way])

            @pl.when(active & (self.behind[way] == 0))
            def _():
                part = rows_of(self.x_refs[0], dest, self.rows)
                if len(self.x_refs) > 1:
                    part[...] = self.block(dest).astype(part.dtype)
                self.hop(way, step, part).start()

            if step > 0:

                @pl.when(active & (self.behind[way] > 0))
                def _():
                    total = self.block(dest) + recv[way, step - 1].astype(jnp.float32)
                    recv[way, step - 1] = total.astype(recv.dtype)
                    self.hop(way, step, recv.at[way, step - 1]).start()

    def arrive(self, step):
        for way in range(2):

            @pl.when(self.has_prev[way] & (step >= self.behind[way] - 1))
            def _():
                self.hop(way, step, self.recv.at[way, step]).wait_recv()

    def collect(self):
        self.o_ref[...] = self.block(self.me)
        for way in range(2):

            @pl.when(self.has_prev[way])
            def _():
                self.o_ref[...] += self.recv[way, self.count - 2].astype(jnp.float32)

    def finish(self):
        for step in range(self.count - 1):
            for way in range(2):

                @pl.when(self.has_next[way] & (step >= self.behind[way]))
                def _():
                    self.hop(way, step, self.recv.at[way, step]).wait_send()


def line_buffers(count, rows, width):
    return [pltpu.VMEM((2, count - 1, rows, width), jnp.bfloat16)] + line_sems(count)


def own_rows(ref, rows):
    return pl.ds(pl.multiple_of(lax.axis_index("tp") * rows, rows), rows)


def inverse_norm(values):
    return lax.rsqrt(jnp.mean(values * values, axis=-1, keepdims=True) + norm_eps)


def rms_back(incoming, values, gain_row):
    inverse = inverse_norm(values)
    scaled = values * inverse
    gain_grad = jnp.sum(incoming * scaled, axis=0, keepdims=True)
    weighted = incoming * gain_row
    row_inner = jnp.mean(weighted * scaled, axis=-1, keepdims=True)
    return inverse * (weighted - scaled * row_inner), gain_grad


def enter_kernel(count, plane=None):
    barrier = pltpu.get_barrier_semaphore()
    waits = line_signal(barrier, lax.axis_index("tp"), count)
    if plane is not None:
        waits = waits + plane.signal(barrier)
    pl.semaphore_wait(barrier, waits)


def remote_params(ident, limit=60):
    return pltpu.CompilerParams(
        collective_id=ident, has_side_effects=True, vmem_limit_bytes=limit << 20
    )


IN_VMEM = pl.BlockSpec(memory_space=pltpu.VMEM)
IN_PLACE = pl.BlockSpec(memory_space=pl.ANY)
TRANSFER = pl.CostEstimate(flops=0, transcendentals=0, bytes_accessed=150_000_000)


def norm_gather_kernel(count, fsdp_count, low, *refs):
    emb_ref, gain_ref, routes_ref, *refs = refs
    parts, refs = refs[:5], refs[5:]
    stacks, refs = (refs[:3], refs[3:]) if low else ((), refs)
    rows_ref, mask_ref, cols_ref, turned_ref, counts_ref, wo_ref, *refs = refs
    packed, refs = (refs[0], refs[1:]) if low else (None, refs)
    w_ref, row_send, row_recv, *refs = refs
    plane = Plane(fsdp_count)
    join(parts, w_ref)
    if low:
        held, in_sem, out_sem = refs[5:]
        gets, puts = pack_copies(low, stacks, packed, held, in_sem, out_sem)
        for get in gets:
            get.start()
    enter_kernel(count, plane)
    line = LineGather(count, rows_ref, row_send, row_recv)
    weights = PlaneGather(plane, w_ref, wo_ref, *refs[:5])
    start_x = emb_ref[...].astype(jnp.float32) * emb_scale
    normed = start_x * inverse_norm(start_x) * gain_ref[...]
    rows_ref[own_rows(rows_ref, line.rows), :] = normed.astype(jnp.bfloat16)
    for step in range(count - 1):
        line.start(step)
        if step == 0:
            weights.start()
            place_routes(line.rows, routes_ref, mask_ref, cols_ref, turned_ref, counts_ref)
            if low:
                for get, put in zip(gets, puts):
                    get.wait()
                    put.start()
        if step == count - 2:
            weights.forward()
        line.arrive(step)
    if low:
        for put in puts:
            put.wait()
    weights.finish()
    line.finish()


def place_routes(rows, routes_ref, mask_ref, cols_ref, turned_ref, counts_ref):
    group, lanes = mask_ref.shape
    columns = lax.broadcasted_iota(jnp.int32, (rows, lanes), 1)
    for low in range(0, group, rows):
        area = slice(low, low + rows)
        mask = jnp.zeros((rows, lanes), jnp.float32)
        named = routes_ref[:, area].astype(jnp.float32).T.astype(jnp.int32)
        for choice in range(routes_ref.shape[0]):
            mask = jnp.where(named[:, choice : choice + 1] == columns, 1.0, mask)
        mask_ref[area, :] = mask
    counts_ref[...] = jnp.sum(mask_ref[...], axis=0, keepdims=True).astype(jnp.int32)
    member = mask_ref[...].astype(jnp.bfloat16)
    for low in range(0, group, rows):
        area = slice(low, low + rows)
        here = lax.broadcasted_iota(jnp.int32, (rows, group), 0) + low
        earlier = here > lax.broadcasted_iota(jnp.int32, (rows, group), 1)
        ranks = jnp.dot(
            jnp.where(earlier, 1.0, 0.0).astype(jnp.bfloat16),
            member,
            preferred_element_type=jnp.float32,
        )
        places = jnp.where(mask_ref[area, :] > 0.0, ranks, -1.0)
        cols_ref[area, :] = places.astype(jnp.int32)
        turned_ref[:, area] = places.T.astype(jnp.int32)


def norm_gather(emb, gain_row, routes, parts, w_width, stacks, low, count, fsdp_count, ident):
    rows, width = emb.shape
    group = rows * count
    chips = fsdp_count // 2
    experts, share, hidden = stacks[0].shape
    span = experts - low
    w_rows = parts[0].shape[0]
    outs = [
        jax.ShapeDtypeStruct((group, width), jnp.bfloat16),
        jax.ShapeDtypeStruct((group, 128), jnp.float32),
        jax.ShapeDtypeStruct((group, 128), jnp.int32),
        jax.ShapeDtypeStruct((128, group), jnp.int32),
        jax.ShapeDtypeStruct((1, 128), jnp.int32),
        jax.ShapeDtypeStruct((w_rows * fsdp_count, w_width), jnp.bfloat16),
    ]
    scratch = [pltpu.VMEM((w_rows, w_width), jnp.bfloat16)] + line_sems(count) + [
        pltpu.SemaphoreType.DMA((chips,)),
        pltpu.SemaphoreType.DMA((chips,)),
        pltpu.SemaphoreType.DMA((chips - 1,)),
        pltpu.SemaphoreType.DMA((chips - 1,)),
        pltpu.SemaphoreType.DMA,
    ]
    if low:
        outs.append(jax.ShapeDtypeStruct((span, 3, share, hidden), jnp.bfloat16))
        scratch += [
            pltpu.VMEM((3, span, share, hidden), jnp.bfloat16),
            pltpu.SemaphoreType.DMA((3,)),
            pltpu.SemaphoreType.DMA((3,)),
        ]
    return pl.pallas_call(
        functools.partial(norm_gather_kernel, count, fsdp_count, low),
        out_shape=outs,
        in_specs=[IN_VMEM] * (3 + len(parts)) + [IN_PLACE] * (3 if low else 0),
        out_specs=[IN_VMEM] * 5 + [IN_PLACE] * (len(outs) - 5),
        scratch_shapes=scratch,
        compiler_params=remote_params(ident, 48),
        cost_estimate=TRANSFER,
    )(emb, gain_row, routes, *parts, *(stacks if low else ()))


def mid_kernel(
    count, part_ref, emb_ref, gain_ref, router_ref, mask_ref, cotangent_ref,
    mid_ref, rows_ref, gates_ref, own_gates, moe_grads,
    recv, sum_send, sum_recv, row_send, row_recv, grad_send, grad_recv,
):
    enter_kernel(count)
    total = LineScatter(count, [part_ref], mid_ref, recv, sum_send, sum_recv)
    line = LineGather(count, rows_ref, row_send, row_recv)
    others = LineGather(count, moe_grads, grad_send, grad_recv)
    rows = line.rows
    moe_grads[own_rows(moe_grads, rows), :] = (
        resid_scale * cotangent_ref[...].astype(jnp.float32)
    ).astype(jnp.bfloat16)
    for step in range(count):
        if step < count - 1:
            others.start(step)
        if step > 0:
            total.start(step - 1)
        if step < count - 1:
            others.arrive(step)
        if step > 0:
            total.arrive(step - 1)
    total.collect()
    mid = emb_ref[...].astype(jnp.float32) * emb_scale + resid_scale * mid_ref[...]
    mid_ref[...] = mid
    own = own_rows(rows_ref, rows)
    rows_ref[own, :] = (mid * inverse_norm(mid) * gain_ref[...]).astype(jnp.bfloat16)

    def find_gates(chunk):
        area = pl.ds(pl.multiple_of(chunk * rows, rows), rows)
        logits = jnp.dot(rows_ref[area, :], router_ref[...], preferred_element_type=jnp.float32)
        inside = mask_ref[area, :] > 0.0
        top = jnp.max(jnp.where(inside, logits, masked_value), axis=-1, keepdims=True)
        raised = jnp.where(inside, jnp.exp(jnp.where(inside, logits - top, 0.0)), 0.0)
        gates = raised / jnp.sum(raised, axis=-1, keepdims=True)
        gates_ref[:, area] = gates.T
        return gates

    for step in range(count - 1):
        line.start(step)
        if step == 0:
            own_gates[...] = find_gates(line.me)
        line.arrive(step)

        @pl.when(line.gets[0][step])
        def _():
            find_gates(line.me - 1 - step)

        @pl.when(line.gets[1][step])
        def _():
            find_gates(line.me + 1 + step)

    line.finish()
    total.finish()
    others.finish()


def find_mid(part, emb, gain_row, weights, used, mask, cotangent, count, ident):
    rows, width = emb.shape
    group = rows * count
    return pl.pallas_call(
        functools.partial(mid_kernel, count),
        grid=(1,),
        out_shape=[
            jax.ShapeDtypeStruct((rows, width), jnp.float32),
            jax.ShapeDtypeStruct((group, width), jnp.bfloat16),
            jax.ShapeDtypeStruct((128, group), jnp.float32),
            jax.ShapeDtypeStruct((rows, 128), jnp.float32),
            jax.ShapeDtypeStruct((group, width), jnp.bfloat16),
        ],
        in_specs=[
            IN_VMEM,
            IN_VMEM,
            IN_VMEM,
            pl.BlockSpec((width, 128), lambda step: (0, used // 128)),
            IN_VMEM,
            IN_VMEM,
        ],
        out_specs=[IN_VMEM] * 5,
        scratch_shapes=line_buffers(count, rows, width) + line_sems(count) + line_sems(count),
        compiler_params=remote_params(ident),
        cost_estimate=TRANSFER,
    )(part, emb, gain_row, weights, mask, cotangent)


def moe_back_kernel(count, fsdp_count, runs, picks, *refs):
    dx_refs, y_refs, refs = refs[:runs], refs[runs : 2 * runs], refs[2 * runs :]
    mid_ref, cotangent_ref, own_gates, gain_ref, router_ref, *refs = refs
    grads_ref, refs = (refs[0], refs[1:]) if picks else (None, refs)
    out_ref, mid_grad, gain_grad, sent_ref, *refs = refs
    sums_ref, refs = (refs[0], refs[1:]) if picks else (None, refs)
    (
        dx_parts, y_parts, load_sem, sum_ref, moe_ref,
        recv, sum_send, sum_recv, moe_recv, moe_send, moe_recv_sem, row_send, row_recv, *refs,
    ) = refs
    loads = []
    for index, (source, parts) in enumerate(
        [(ref, dx_parts) for ref in dx_refs] + [(ref, y_parts) for ref in y_refs]
    ):
        loads.append(
            pltpu.make_async_copy(source, parts.at[index % runs], load_sem.at[index])
        )
        loads[-1].start()
    plane = Plane(fsdp_count) if picks else None
    enter_kernel(count, plane)
    total = LineScatter(
        count, [dx_parts.at[run] for run in range(runs)], sum_ref, recv, sum_send, sum_recv
    )
    moe = LineScatter(
        count, [y_parts.at[run] for run in range(runs)], moe_ref, moe_recv, moe_send, moe_recv_sem
    )
    line = LineGather(count, sent_ref, row_send, row_recv)
    experts = ExpertSums(plane, picks, grads_ref, sums_ref, *refs) if picks else None
    rows, width = mid_ref.shape
    for index in range(len(picks)):
        experts.begin(index)
    for load in loads[:runs]:
        load.wait()
    items = experts.items() if picks else []
    each = -(-len(items) // (2 * count - 2))
    for step in range(count - 1):
        total.start(step)
        for item in items[step * each : (step + 1) * each]:
            experts.do(*item)
        total.arrive(step)
    items = items[(count - 1) * each :]
    total.collect()
    gates = own_gates[...]
    gates_grad = sum_ref[:, width:]
    gates_inner = jnp.sum(gates * gates_grad, axis=-1, keepdims=True)
    logits_grad = (gates * (gates_grad - gates_inner)).astype(jnp.bfloat16)
    incoming = sum_ref[:, :width] + contract_last(logits_grad, router_ref[...])
    from_norm, gain_part = rms_back(incoming, mid_ref[...], gain_ref[...])
    grad = cotangent_ref[...].astype(jnp.float32) + from_norm
    mid_grad[...] = grad
    gain_grad[...] = gain_part
    own = own_rows(sent_ref, rows)
    sent_ref[own, :width] = (resid_scale * grad).astype(jnp.bfloat16)
    sent_ref[own, width:] = logits_grad
    for load in loads[runs:]:
        load.wait()
    for step in range(count):
        if step < count - 1:
            line.start(step)
        if step > 0:
            moe.start(step - 1)
        for item in items[step * each : (step + 1) * each]:
            experts.do(*item)
        if step < count - 1:
            line.arrive(step)
        if step > 0:
            moe.arrive(step - 1)
    moe.collect()
    out_ref[...] = (mid_ref[...] + resid_scale * moe_ref[...]).astype(out_ref.dtype)
    for index in range(len(picks)):
        experts.collect(index)
    line.finish()
    total.finish()
    moe.finish()
    if picks:
        experts.finish()


def find_mid_grad(
    dx_parts, y_parts, mid, cotangent, own_gates, gain_row, weights, used, grads, picks,
    count, fsdp_count, ident,
):
    rows, width = mid.shape
    runs, group = len(dx_parts), rows * count
    wide = dx_parts[0].shape[1]
    share = grads.shape[2] // fsdp_count
    sums = [jax.ShapeDtypeStruct((len(picks), 3, share, grads.shape[3]), jnp.bfloat16)]
    sums = sums if picks else []
    return pl.pallas_call(
        functools.partial(moe_back_kernel, count, fsdp_count, runs, picks),
        grid=(1,),
        out_shape=[
            jax.ShapeDtypeStruct((rows, width), jnp.bfloat16),
            jax.ShapeDtypeStruct((rows, width), jnp.float32),
            jax.ShapeDtypeStruct((1, width), jnp.float32),
            jax.ShapeDtypeStruct((group, wide), jnp.bfloat16),
        ]
        + sums,
        in_specs=[IN_PLACE] * (2 * runs)
        + [IN_VMEM] * 4
        + [pl.BlockSpec((width, 128), lambda step: (0, used // 128))]
        + [IN_PLACE] * len(sums),
        out_specs=[IN_VMEM] * 4 + [IN_PLACE] * len(sums),
        scratch_shapes=[
            pltpu.VMEM((runs, group, wide), jnp.bfloat16),
            pltpu.VMEM((runs, group, width), jnp.bfloat16),
            pltpu.SemaphoreType.DMA((2 * runs,)),
            pltpu.VMEM((rows, wide), jnp.float32),
            pltpu.VMEM((rows, width), jnp.float32),
        ]
        + line_buffers(count, rows, wide)
        + line_buffers(count, rows, width)
        + line_sems(count)
        + expert_buffers(len(picks), share, grads.shape[3]),
        compiler_params=remote_params(ident, 63),
        cost_estimate=TRANSFER,
    )(*dx_parts, *y_parts, mid, cotangent, own_gates, gain_row, weights, *([grads] if picks else []))


def finish_kernel(tp_count, fsdp_count, picks, *refs):
    x_ref, w_ref, emb_ref, gain_ref, mid_grad, gain_two, *refs = refs
    grads_ref, refs = (refs[0], refs[1:]) if picks else (None, refs)
    grad_ref, w_sum, gains_ref, *refs = refs
    sums_ref, refs = (refs[0], refs[1:]) if picks else (None, refs)
    (
        line_recv, line_send_sem, line_recv_sem,
        pair_got, chip_sums, chip_got, pair_send, pair_recv, chip_send, chip_recv,
        tp_got, fsdp_got, small_send, small_recv, *refs,
    ) = refs
    plane = Plane(fsdp_count)
    tp_me, fsdp_me = lax.axis_index("tp"), plane.me
    barrier = pltpu.get_barrier_semaphore()
    for shift in range(1, tp_count):
        pl.semaphore_signal(barrier, inc=1, device_id={"tp": lax.rem(tp_me + shift, tp_count)})
    for shift in range(1, fsdp_count):
        pl.semaphore_signal(
            barrier, inc=1, device_id={"fsdp": lax.rem(fsdp_me + shift, fsdp_count)}
        )
    pl.semaphore_wait(barrier, tp_count + fsdp_count - 2)
    line = LineScatter(
        tp_count, [x_ref], grad_ref, line_recv, line_send_sem, line_recv_sem
    )
    rows = w_sum.shape[0]

    def to_pair(shift):
        return pltpu.make_async_remote_copy(
            src_ref=rows_of(w_ref, plane.chip_at(shift) * 2 + 1 - plane.core, rows),
            dst_ref=pair_got.at[shift],
            send_sem=pair_send.at[shift],
            recv_sem=pair_recv.at[shift],
            device_id={"fsdp": plane.partner},
        )

    def to_chip(shift):
        return pltpu.make_async_remote_copy(
            src_ref=chip_sums.at[shift - 1],
            dst_ref=chip_got.at[shift - 1],
            send_sem=chip_send.at[shift - 1],
            recv_sem=chip_recv.at[shift - 1],
            device_id={"fsdp": plane.peer(shift)},
        )

    def both_cores(shift):
        own = pl.ds(pl.multiple_of(plane.peer(shift) * rows, rows), rows)
        return w_ref[own, :].astype(jnp.float32) + pair_got[shift].astype(jnp.float32)

    def send_gains(axis, me, count, got, base):
        copies = []
        for shift in range(1, count):
            copies.append(
                pltpu.make_async_remote_copy(
                    src_ref=gains_ref,
                    dst_ref=got.at[me],
                    send_sem=small_send.at[base + shift],
                    recv_sem=small_recv.at[base + shift],
                    device_id={axis: lax.rem(me + shift, count)},
                )
            )
            copies[-1].start()
        got[me] = gains_ref[...]
        return copies

    def add_gains(copies, got):
        for copy in copies:
            copy.wait()
        total = got[0]
        for index in range(1, len(copies) + 1):
            total = total + got[index]
        gains_ref[...] = total

    experts = ExpertSums(plane, picks, grads_ref, sums_ref, *refs) if picks else None
    line.start(0)
    order = list(range(1, plane.chips)) + [0]
    for shift in order:
        to_pair(shift).start()
    for index in range(len(picks)):
        experts.begin(index)
    for shift in order:
        to_pair(shift).wait_recv()
        if shift > 0:
            chip_sums[shift - 1] = both_cores(shift).astype(chip_sums.dtype)
            to_chip(shift).start()
    items = experts.items() if picks else []
    each = -(-len(items) // (tp_count - 2))
    line.arrive(0)
    for step in range(1, tp_count - 1):
        line.start(step)
        for item in items[(step - 1) * each : step * each]:
            experts.do(*item)
        line.arrive(step)
    line.collect()
    from_norm, gain_one = rms_back(
        grad_ref[...], emb_ref[...].astype(jnp.float32) * emb_scale, gain_ref[...]
    )
    gains_ref[0:1, :] = gain_one
    gains_ref[1:2, :] = gain_two[...]
    copies = send_gains("tp", tp_me, tp_count, tp_got, 0)
    grad_ref[...] = emb_scale * (mid_grad[...] + from_norm)
    add_gains(copies, tp_got)
    copies = send_gains("fsdp", fsdp_me, fsdp_count, fsdp_got, tp_count)
    total = both_cores(0)
    for shift in range(1, plane.chips):
        to_chip(shift).wait_recv()
        total = total + chip_got[shift - 1].astype(jnp.float32)
    w_sum[...] = total
    for index in range(len(picks)):
        experts.collect(index)
    add_gains(copies, fsdp_got)
    line.finish()
    for shift in order:
        to_pair(shift).wait_send()
        if shift > 0:
            to_chip(shift).wait_send()
    if picks:
        experts.finish()


def finish(dx_rows, weight_grads, emb, gain_row, mid_grad, gain_two, grads, picks, ident):
    tp_count, fsdp_count = lax.axis_size("tp"), lax.axis_size("fsdp")
    rows, width = emb.shape
    w_rows, w_width = weight_grads.shape[0] // fsdp_count, weight_grads.shape[1]
    chips = fsdp_count // 2
    share = grads.shape[2] // fsdp_count
    sums = [jax.ShapeDtypeStruct((len(picks), 3, share, grads.shape[3]), jnp.bfloat16)]
    sums = sums if picks else []
    return pl.pallas_call(
        functools.partial(finish_kernel, tp_count, fsdp_count, picks),
        out_shape=[
            jax.ShapeDtypeStruct((rows, width), jnp.float32),
            jax.ShapeDtypeStruct((w_rows, w_width), jnp.float32),
            jax.ShapeDtypeStruct((2, width), jnp.float32),
            *sums,
        ],
        in_specs=[IN_VMEM] * 6 + [IN_PLACE] * len(sums),
        out_specs=[IN_VMEM] * 3 + [IN_PLACE] * len(sums),
        scratch_shapes=line_buffers(tp_count, rows, width)
        + [
            pltpu.VMEM((chips, w_rows, w_width), jnp.bfloat16),
            pltpu.VMEM((chips - 1, w_rows, w_width), jnp.bfloat16),
            pltpu.VMEM((chips - 1, w_rows, w_width), jnp.bfloat16),
            pltpu.SemaphoreType.DMA((chips,)),
            pltpu.SemaphoreType.DMA((chips,)),
            pltpu.SemaphoreType.DMA((chips - 1,)),
            pltpu.SemaphoreType.DMA((chips - 1,)),
            pltpu.VMEM((tp_count, 2, width), jnp.float32),
            pltpu.VMEM((fsdp_count, 2, width), jnp.float32),
            pltpu.SemaphoreType.DMA((tp_count + fsdp_count,)),
            pltpu.SemaphoreType.DMA((tp_count + fsdp_count,)),
        ]
        + expert_buffers(len(picks), share, grads.shape[3]),
        compiler_params=remote_params(ident),
        cost_estimate=TRANSFER,
    )(dx_rows, weight_grads, emb, gain_row, mid_grad, gain_two, *([grads] if picks else []))


def pack_copies(low, sources, target, held, in_sem, out_sem):
    span = target.shape[0]
    gets = [
        pltpu.make_async_copy(source.at[pl.ds(low, span)], held.at[slot], in_sem.at[slot])
        for slot, source in enumerate(sources)
    ]
    puts = [
        pltpu.make_async_copy(held.at[slot], target.at[:, slot], out_sem.at[slot])
        for slot in range(len(sources))
    ]
    return gets, puts


def pack_kernel(low, *refs):
    sources, target, held, in_sem, out_sem = refs[:-4], *refs[-4:]
    gets, puts = pack_copies(low, sources, target, held, in_sem, out_sem)
    for get in gets:
        get.start()
    for get, put in zip(gets, puts):
        get.wait()
        put.start()
    for put in puts:
        put.wait()


def pack(stacks, low, high):
    _, rows, width = stacks[0].shape
    count, span = len(stacks), high - low
    return pl.pallas_call(
        functools.partial(pack_kernel, low),
        in_specs=[IN_PLACE] * count,
        out_specs=IN_PLACE,
        out_shape=jax.ShapeDtypeStruct((span, count, rows, width), jnp.bfloat16),
        scratch_shapes=[
            pltpu.VMEM((count, span, rows, width), jnp.bfloat16),
            pltpu.SemaphoreType.DMA((count,)),
            pltpu.SemaphoreType.DMA((count,)),
        ],
    )(*stacks)


def join(parts, target):
    *sources, last = parts
    low = 0
    for source in sources:
        target[:, low : low + source.shape[1]] = source[...]
        low += source.shape[1]
    router = last[...].astype(jnp.float32).T.astype(jnp.bfloat16)
    target[:, low:] = jnp.zeros((target.shape[0], target.shape[1] - low), jnp.bfloat16)
    target[:, low : low + router.shape[1]] = router


SLOTS = 256


def experts_kernel(
    first_expert,
    capacity,
    meta,
    place_rows,
    place_cols,
    gate_rows,
    x_ref,
    g_ref,
    weights,
    *refs,
):
    *held, y_ref, dx_ref, grads, load_sem = refs
    step = pl.program_id(0)
    expert = step + first_expert
    group, width = x_ref.shape
    tail = dx_ref.shape[1] - width

    @pl.when(step == 0)
    def _():
        if held:
            loads = [
                pltpu.make_async_copy(source, target, load_sem.at[index])
                for index, (source, target) in enumerate(zip(held, (y_ref, dx_ref)))
            ]
            for load in loads:
                load.start()
            for load in loads:
                load.wait()
        else:
            y_ref[...] = jnp.zeros_like(y_ref)
            dx_ref[...] = jnp.zeros_like(dx_ref)

    column = expert + meta[meta.shape[0] - 1]
    lanes = lax.broadcasted_iota(jnp.int32, place_cols.shape, 1)
    place_col = jnp.sum(jnp.where(lanes == column, place_cols[...], 0), axis=1, keepdims=True)
    place_row = place_rows[pl.ds(column, 1), :]
    gate_row = gate_rows[pl.ds(column, 1), :].astype(jnp.bfloat16).astype(jnp.float32)
    mark = jnp.where(lax.broadcasted_iota(jnp.int32, (1, tail), 1) == column, 1.0, 0.0)

    def run(base, span):
        slots = lax.broadcasted_iota(jnp.int32, (span, group), 0) + base
        hit = slots == place_row
        pick = jnp.where(hit, 1.0, 0.0).astype(jnp.bfloat16)
        scale = jnp.sum(jnp.where(hit, gate_row, 0.0), axis=1, keepdims=True)
        x_taken = jnp.dot(pick, x_ref[...], preferred_element_type=jnp.float32).astype(jnp.bfloat16)
        g_taken = jnp.dot(pick, g_ref[...], preferred_element_type=jnp.float32).astype(jnp.bfloat16)
        gate_pre = jnp.dot(x_taken, weights[0, 0], preferred_element_type=jnp.float32)
        up_pre = jnp.dot(x_taken, weights[0, 1], preferred_element_type=jnp.float32)
        raw = jnp.dot(g_taken, weights[0, 2], preferred_element_type=jnp.float32)
        sig = jax.nn.sigmoid(gate_pre)
        silu = gate_pre * sig
        act = (silu * up_pre).astype(jnp.bfloat16).astype(jnp.float32)
        slot_grad = jnp.sum(act * raw, axis=1, keepdims=True)
        act_grad = raw * scale
        act_scaled = (act * scale).astype(jnp.bfloat16)
        gate_grad = (act_grad * up_pre * sig * (1.0 + gate_pre * (1.0 - sig))).astype(jnp.bfloat16)
        up_grad = (act_grad * silu).astype(jnp.bfloat16)
        extra = (slot_grad * mark).astype(jnp.bfloat16)
        rows_out = contract_last(act_scaled, weights[0, 2]).astype(jnp.bfloat16)
        rows_in = (
            contract_last(gate_grad, weights[0, 0]) + contract_last(up_grad, weights[0, 1])
        ).astype(jnp.bfloat16)
        for slot, left_op, right_op in (
            (0, x_taken, gate_grad),
            (1, x_taken, up_grad),
            (2, g_taken, act_scaled),
        ):
            grad = contract_first(left_op, right_op)
            if base > 0:
                grad = grad + grads[0, slot].astype(jnp.float32)
            grads[0, slot] = grad.astype(jnp.bfloat16)
        block = min(256, group)
        for start in range(0, group, block):
            back = jnp.where(
                lax.broadcasted_iota(jnp.int32, (block, span), 1) + base
                == place_col[start : start + block],
                1.0,
                0.0,
            ).astype(jnp.bfloat16)
            for target, low_col, addend in (
                (y_ref, 0, rows_out),
                (dx_ref, 0, rows_in),
                (dx_ref, width, extra),
            ):
                area = (slice(start, start + block), slice(low_col, low_col + addend.shape[1]))
                target[area] = (
                    target[area].astype(jnp.float32)
                    + jnp.dot(back, addend, preferred_element_type=jnp.float32)
                ).astype(target.dtype)

    run(0, min(SLOTS, capacity))
    for base in range(SLOTS, capacity, SLOTS):
        span = min(SLOTS, -(-(capacity - base) // 16) * 16)

        @pl.when(meta[column] > base)
        def _():
            run(base, span)


def experts_step(meta, place_rows, place_cols, gate_rows, x_rows, g_rows, weights, held, first, count, skip, capacity):
    group, width = x_rows.shape
    hidden = weights.shape[-1]
    tail = 128

    def whole(shape):
        return pl.BlockSpec(
            shape, lambda step, meta: (0,) * len(shape), pipeline_mode=pl.Buffered(1)
        )

    def big(offset):
        return pl.BlockSpec((1, 3, width, hidden), lambda step, meta: (step + offset, 0, 0, 0))

    return pl.pallas_call(
        functools.partial(experts_kernel, first, capacity),
        grid_spec=pltpu.PrefetchScalarGridSpec(
            num_scalar_prefetch=1,
            grid=(count,),
            in_specs=[
                whole(place_rows.shape),
                whole(place_cols.shape),
                whole(gate_rows.shape),
                whole(x_rows.shape),
                whole(g_rows.shape),
                big(skip),
            ]
            + [IN_PLACE] * len(held),
            out_specs=[
                whole((group, width)),
                whole((group, width + tail)),
                big(0),
            ],
            scratch_shapes=[pltpu.SemaphoreType.DMA((2,))],
        ),
        out_shape=[
            jax.ShapeDtypeStruct((group, width), jnp.bfloat16),
            jax.ShapeDtypeStruct((group, width + tail), jnp.bfloat16),
            jax.ShapeDtypeStruct((count, 3, width, hidden), jnp.bfloat16),
        ],
        compiler_params=pltpu.CompilerParams(
            dimension_semantics=("arbitrary",), vmem_limit_bytes=63 << 20
        ),
        cost_estimate=pl.CostEstimate(
            flops=count * 17 * 2 * 408 * width * hidden,
            transcendentals=count * 408 * hidden,
            bytes_accessed=count * 12 * width * hidden,
        ),
    )(meta, place_rows, place_cols, gate_rows, x_rows, g_rows, weights, *held)


def rotate_head(values, cosine, sine, sign):
    half = values.shape[-1] // 2
    other = jnp.concatenate([values[:, half:], values[:, :half]], axis=1)
    return values * cosine + other * (sine * sign)


def segment_bias(seg_row):
    length = seg_row.shape[1]
    shape = (length, length)
    seg_row = seg_row.astype(jnp.float32)
    seg_col = jnp.broadcast_to(seg_row, (128, length)).T[:, :1]
    keys = lax.broadcasted_iota(jnp.int32, shape, 0)
    queries = lax.broadcasted_iota(jnp.int32, shape, 1)
    return jnp.where((keys <= queries) & (seg_col == seg_row), 0.0, masked_value)


def attend_kernel(
    x_ref,
    w_ref,
    seg_row,
    cos_ref,
    sin_ref,
    q_ref,
    k_ref,
    v_ref,
    mixed_ref,
    logsum_ref,
    branch_ref,
    bias,
    v_turned,
    mixed_heads,
):
    heads, kv_heads = q_ref.shape[0], k_ref.shape[0]
    per_kv = heads // kv_heads
    block = SEQ // 2
    edge = (heads + 2 * kv_heads) * HEAD_DIM
    proj = jnp.dot(x_ref[...], w_ref[:, :edge], preferred_element_type=jnp.float32)
    cosine, sine = cos_ref[...], sin_ref[...]
    for head in range(heads + 2 * kv_heads):
        part = proj[:, head * HEAD_DIM : (head + 1) * HEAD_DIM]
        if head < heads:
            q_ref[head] = rotate_head(part, cosine, sine, 1.0).astype(jnp.bfloat16)
        elif head < heads + kv_heads:
            k_ref[head - heads] = rotate_head(part, cosine, sine, 1.0).astype(jnp.bfloat16)
        else:
            v_ref[head - heads - kv_heads] = part.astype(jnp.bfloat16)
            v_turned[head - heads - kv_heads] = part.T.astype(jnp.bfloat16)
    bias[...] = segment_bias(seg_row[pl.ds(pl.program_id(0), 1), :])

    def one_head(head, carry):
        kv = head // per_kv
        for part in range(2):
            span, low = block * (part + 1), block * part
            scores = contract_last(k_ref[kv, :span], q_ref[head, low : low + block]) * attn_scale
            scores = scores + bias[:span, low : low + block]
            top = jnp.max(scores, axis=0, keepdims=True)
            raised = jnp.exp(scores - top)
            total = jnp.sum(raised, axis=0, keepdims=True)
            probs = (raised * (1.0 / total)).astype(jnp.bfloat16)
            turned = jnp.dot(v_turned[kv, :, :span], probs, preferred_element_type=jnp.float32)
            mixed_heads[head, low : low + block, :] = turned.T.astype(jnp.bfloat16)
            logsum_ref[0, pl.ds(head, 1), low : low + block] = top + jnp.log(total)
        return carry

    lax.fori_loop(0, heads, one_head, 0)
    for head in range(heads):
        mixed_ref[:, head * HEAD_DIM : (head + 1) * HEAD_DIM] = mixed_heads[head]
    branch_ref[...] = contract_last(
        mixed_ref[...], w_ref[:, edge : edge + heads * HEAD_DIM]
    ).astype(jnp.bfloat16)


def attend_back_kernel(
    x_ref,
    w_ref,
    seg_row,
    cos_ref,
    sin_ref,
    q_ref,
    k_ref,
    v_ref,
    mixed_ref,
    logsum_ref,
    moe_rows,
    branch_grad,
    dx_ref,
    dw_ref,
    bias,
    k_turned,
    mixed_grads,
    q_grads,
    kv_grads,
    qkv_grad,
    dw_acc,
):
    heads, kv_heads = q_ref.shape[0], k_ref.shape[0]
    per_kv = heads // kv_heads
    block = SEQ // 2
    edge = (heads + 2 * kv_heads) * HEAD_DIM
    step = pl.program_id(0)
    out_edge = edge + heads * HEAD_DIM
    width = x_ref.shape[1]
    grad = jnp.dot(
        branch_grad[:, :width], w_ref[:, edge:out_edge], preferred_element_type=jnp.float32
    ).astype(jnp.bfloat16)
    for head in range(heads):
        mixed_grads[head] = grad[:, head * HEAD_DIM : (head + 1) * HEAD_DIM]
    for kv in range(kv_heads):
        k_turned[kv] = k_ref[kv].astype(jnp.float32).T.astype(jnp.bfloat16)
    bias[...] = segment_bias(seg_row[pl.ds(pl.program_id(0), 1), :])
    kv_grads[...] = jnp.zeros_like(kv_grads)

    def one_head(head, carry):
        kv = head // per_kv
        for part in range(2):
            span, low = block * (part + 1), block * part
            high = low + block
            scores = contract_last(k_ref[kv, :span], q_ref[head, low:high]) * attn_scale
            scores = scores + bias[:span, low:high]
            probs = jnp.exp(scores - logsum_ref[0, pl.ds(head, 1), low:high])
            probs_grad = contract_last(v_ref[kv, :span], mixed_grads[head, low:high])
            inner = jnp.sum(probs * probs_grad, axis=0, keepdims=True)
            score_grad = (probs * (probs_grad - inner)).astype(jnp.bfloat16)
            turned = jnp.dot(k_turned[kv, :, :span], score_grad, preferred_element_type=jnp.float32)
            q_grads[head, low:high, :] = turned.T * attn_scale
            kv_grads[0, kv, :span, :] += jnp.dot(
                score_grad, q_ref[head, low:high], preferred_element_type=jnp.float32
            )
            kv_grads[1, kv, :span, :] += jnp.dot(
                probs.astype(jnp.bfloat16), mixed_grads[head, low:high],
                preferred_element_type=jnp.float32,
            )
        return carry

    lax.fori_loop(0, heads, one_head, 0)
    cosine, sine = cos_ref[...], sin_ref[...]
    for head in range(heads + 2 * kv_heads):
        if head < heads:
            part = rotate_head(q_grads[head], cosine, sine, -1.0)
        elif head < heads + kv_heads:
            part = rotate_head(kv_grads[0, head - heads] * attn_scale, cosine, sine, -1.0)
        else:
            part = kv_grads[1, head - heads - kv_heads]
        qkv_grad[:, head * HEAD_DIM : (head + 1) * HEAD_DIM] = part.astype(jnp.bfloat16)
    dx_ref[...] = contract_last(qkv_grad[...], w_ref[:, :edge]).astype(jnp.bfloat16)
    for low, high, left_op, right_op in (
        (0, edge, x_ref[...], qkv_grad[...]),
        (edge, out_edge, branch_grad[:, :width], mixed_ref[...]),
        (out_edge, dw_acc.shape[1], moe_rows[...], branch_grad[:, width:]),
    ):
        part = contract_first(left_op, right_op)

        @pl.when(step == 0)
        def _():
            dw_acc[:, low:high] = part

        @pl.when(step > 0)
        def _():
            dw_acc[:, low:high] += part

    @pl.when(step == pl.num_programs(0) - 1)
    def _():
        dw_ref[...] = dw_acc[...].astype(jnp.bfloat16)


def fixed(shape):
    return pl.BlockSpec(shape, lambda seq: (0,) * len(shape), pipeline_mode=pl.Buffered(1))


def by_row(width):
    return pl.BlockSpec((SEQ, width), lambda seq: (seq, 0))


def by_head(heads):
    return pl.BlockSpec((heads, SEQ, HEAD_DIM), lambda seq: (0, seq, 0))


def attend_tables():
    half = HEAD_DIM // 2
    positions = np.arange(SEQ, dtype=np.float32)
    frequency = np.float32(rope_base) ** (-np.arange(half, dtype=np.float32) * 2.0 / HEAD_DIM)
    angles = (positions[:, None] * frequency[None, :].astype(np.float32)).astype(np.float32)
    cosine, sine = np.cos(angles), np.sin(angles)
    return (
        jnp.asarray(np.concatenate([cosine, cosine], axis=1)),
        jnp.asarray(np.concatenate([-sine, sine], axis=1)),
    )


def attend(rows, weights, segments, tables, heads, kv_heads):
    group, width = rows.shape
    seqs = group // SEQ
    return pl.pallas_call(
        attend_kernel,
        grid=(seqs,),
        in_specs=[
            by_row(width),
            fixed(weights.shape),
            fixed(segments.shape),
            fixed(tables[0].shape),
            fixed(tables[1].shape),
        ],
        out_specs=[
            by_head(heads),
            by_head(kv_heads),
            by_head(kv_heads),
            by_row(heads * HEAD_DIM),
            pl.BlockSpec((1, heads, SEQ), lambda seq: (seq, 0, 0)),
            by_row(width),
        ],
        out_shape=[
            jax.ShapeDtypeStruct((heads, group, HEAD_DIM), jnp.bfloat16),
            jax.ShapeDtypeStruct((kv_heads, group, HEAD_DIM), jnp.bfloat16),
            jax.ShapeDtypeStruct((kv_heads, group, HEAD_DIM), jnp.bfloat16),
            jax.ShapeDtypeStruct((group, heads * HEAD_DIM), jnp.bfloat16),
            jax.ShapeDtypeStruct((seqs, heads, SEQ), jnp.float32),
            jax.ShapeDtypeStruct((group, width), jnp.bfloat16),
        ],
        scratch_shapes=[
            pltpu.VMEM((SEQ, SEQ), jnp.float32),
            pltpu.VMEM((kv_heads, HEAD_DIM, SEQ), jnp.bfloat16),
            pltpu.VMEM((heads, SEQ, HEAD_DIM), jnp.bfloat16),
        ],
        compiler_params=pltpu.CompilerParams(
            dimension_semantics=("arbitrary",), vmem_limit_bytes=56 << 20
        ),
        cost_estimate=pl.CostEstimate(
            flops=10_000_000_000, transcendentals=3_000_000, bytes_accessed=60_000_000
        ),
    )(rows, weights, segments, *tables)


def attend_back(rows, weights, segments, tables, kept, moe_rows, branch_grad):
    queries, keys, values, mixed, logsum = kept
    group, width = rows.shape
    heads, kv_heads = queries.shape[0], keys.shape[0]
    used = weights.shape[1]
    edge = (heads + 2 * kv_heads) * HEAD_DIM
    return pl.pallas_call(
        attend_back_kernel,
        grid=(group // SEQ,),
        in_specs=[
            by_row(width),
            fixed(weights.shape),
            fixed(segments.shape),
            fixed(tables[0].shape),
            fixed(tables[1].shape),
            by_head(heads),
            by_head(kv_heads),
            by_head(kv_heads),
            by_row(heads * HEAD_DIM),
            pl.BlockSpec((1, heads, SEQ), lambda seq: (seq, 0, 0)),
            by_row(width),
            by_row(branch_grad.shape[1]),
        ],
        out_specs=[by_row(width), fixed((width, used))],
        out_shape=[
            jax.ShapeDtypeStruct((group, width), jnp.bfloat16),
            jax.ShapeDtypeStruct((width, used), jnp.bfloat16),
        ],
        scratch_shapes=[
            pltpu.VMEM((SEQ, SEQ), jnp.float32),
            pltpu.VMEM((kv_heads, HEAD_DIM, SEQ), jnp.bfloat16),
            pltpu.VMEM((heads, SEQ, HEAD_DIM), jnp.bfloat16),
            pltpu.VMEM((heads, SEQ, HEAD_DIM), jnp.float32),
            pltpu.VMEM((2, kv_heads, SEQ, HEAD_DIM), jnp.float32),
            pltpu.VMEM((SEQ, edge), jnp.bfloat16),
            pltpu.VMEM((width, used), jnp.float32),
        ],
        compiler_params=pltpu.CompilerParams(
            dimension_semantics=("arbitrary",), vmem_limit_bytes=60 << 20
        ),
        cost_estimate=pl.CostEstimate(
            flops=20_000_000_000, transcendentals=3_000_000, bytes_accessed=100_000_000
        ),
    )(rows, weights, segments, *tables,
      queries, keys, values, mixed, logsum, moe_rows, branch_grad)


def outputs_kernel(edges, attn_ref, gains_ref, *refs):
    step = pl.program_id(0)
    packed, refs = refs[: len(edges) - 1], refs[len(edges) - 1 :]
    *small, router_ref, gain_one, gain_two = refs[:7]
    targets = refs[7:]

    @pl.when(step == 0)
    def _():
        low = 0
        for target in small:
            target[...] = attn_ref[:, low : low + target.shape[1]]
            low += target.shape[1]
        router_ref[...] = attn_ref[:, low:].T[: router_ref.shape[0], :]
        gain_one[...] = gains_ref[0, :]
        gain_two[...] = gains_ref[1, :]

    for part, low, high in zip(packed, edges[:-1], edges[1:]):

        @pl.when((step >= low) & (step < high))
        def _():
            for slot, target in enumerate(targets):
                target[0] = part[0, slot].astype(jnp.float32)


def outputs(attn_sum, gains, packed, edges, widths, expert_count):
    _, _, rows, width = packed[0].shape
    shapes = [(rows, span) for span in widths] + [(expert_count, rows)] + [(gains.shape[1],)] * 2

    def home(low, high):
        return pl.BlockSpec(
            (1, 3, rows, width),
            lambda step: (jnp.clip(step - low, 0, high - low - 1), 0, 0, 0),
        )

    def still(shape):
        return pl.BlockSpec(shape, lambda step: (0,) * len(shape))

    return pl.pallas_call(
        functools.partial(outputs_kernel, edges),
        grid=(edges[-1],),
        in_specs=[still(attn_sum.shape), still(gains.shape)]
        + [home(low, high) for low, high in zip(edges[:-1], edges[1:])],
        out_specs=[still(shape) for shape in shapes]
        + [pl.BlockSpec((1, rows, width), lambda step: (step, 0, 0))] * 3,
        out_shape=[jax.ShapeDtypeStruct(shape, jnp.float32) for shape in shapes]
        + [jax.ShapeDtypeStruct((edges[-1], rows, width), jnp.float32)] * 3,
    )(attn_sum, gains, *packed)


RUNS = (0, 6, 10)
DIRECT = (3, 1)


def local(
    emb,
    segment_ids,
    routes,
    norm1_gain,
    w_query,
    w_key,
    w_value,
    w_out,
    norm2_gain,
    w_router,
    w_gate,
    w_up,
    w_down,
    cotangent,
):
    local_rows, width = emb.shape
    tp_count, tp_index = lax.axis_size("tp"), lax.axis_index("tp")
    experts_here = w_gate.shape[0]
    expert_count = w_router.shape[1]
    q_width, kv_width = w_query.shape[1], w_key.shape[1]
    used = 2 * (q_width + kv_width)
    group_size = local_rows * tp_count
    fsdp_count = lax.axis_size("fsdp")
    split = group_size <= 1024
    runs = [edge * experts_here // RUNS[-1] for edge in RUNS] if split else [0, experts_here]
    stacks = (w_gate, w_up, w_down)
    pieces = [lax.all_gather(pack(stacks, 0, runs[1]), "fsdp", axis=2, tiled=True)]
    gain_one = norm1_gain.astype(jnp.float32)[None, :]
    gain_two = norm2_gain.astype(jnp.float32)[None, :]
    group_rows, mask, place_cols, place_rows, counts, attn_w, *packed = norm_gather(
        emb,
        gain_one,
        routes.T,
        [w_query, w_key, w_value, w_out, w_router.T],
        used + 128,
        stacks,
        runs[1] if split else 0,
        tp_count,
        fsdp_count,
        0,
    )
    if split:
        pieces.append(lax.all_gather(packed[0], "fsdp", axis=2, tiled=True))
    capacity = group_size * routes.shape[1] // expert_count * 2
    meta = jnp.concatenate([counts[0], (tp_index * experts_here)[None]])

    tables = attend_tables()
    heads_here, kv_here = q_width // HEAD_DIM, kv_width // HEAD_DIM
    *kept, branch_part = attend(group_rows, attn_w, segment_ids, tables, heads_here, kv_here)
    mid_x, moe_rows, gate_rows, own_gates, moe_grad_rows = find_mid(
        branch_part, emb, gain_two, attn_w, used, mask, cotangent, tp_count, 1
    )

    outs = []
    for first, last, piece in zip(runs[:-1], runs[1:], pieces):
        outs.append(
            experts_step(
                meta,
                place_rows,
                place_cols,
                gate_rows,
                moe_rows,
                moe_grad_rows,
                piece,
                outs[-1][:2] if outs else (),
                first,
                last - first,
                0,
                capacity,
            )
        )
    grad_sums = [lax.psum_scatter(outs[0][2], "fsdp", scatter_dimension=2, tiled=True)]
    last_grads = outs[-1][2]
    picks = (tuple(range(DIRECT[0])), tuple(range(DIRECT[0], sum(DIRECT)))) if split else ((), ())
    out, mid_grad, gain_two_grad, sent, *mid_sums = find_mid_grad(
        outs[-1][1:2],
        outs[-1][0:1],
        mid_x,
        cotangent,
        own_gates,
        gain_two,
        attn_w,
        used,
        last_grads,
        picks[0],
        tp_count,
        fsdp_count,
        2,
    )
    dx_one, attn_grads = attend_back(
        group_rows, attn_w, segment_ids, tables, kept, moe_rows, sent
    )
    grad_emb, attn_sum, gain_sums, *end_sums = finish(
        dx_one, attn_grads, emb, gain_one, mid_grad, gain_two_grad, last_grads, picks[1], 3
    )
    grad_sums = grad_sums + mid_sums + end_sums
    ends = [0]
    for part in grad_sums:
        ends.append(ends[-1] + part.shape[0])
    widths = [q_width, kv_width, kv_width, q_width]
    *attn_outs, router_turned, gain_one_sum, gain_two_sum, gate_sum, up_sum, down_sum = outputs(
        attn_sum, gain_sums, grad_sums, ends, widths, expert_count
    )
    return (
        out,
        grad_emb,
        gain_one_sum,
        *attn_outs,
        gain_two_sum,
        router_turned.T,
        gate_sum,
        up_sum,
        down_sum,
    )


def solution(mesh):
    return jax.shard_map(
        local,
        mesh=mesh,
        in_specs=(
            P(("fsdp", "tp"), None),
            P("fsdp", None),
            P("fsdp", None),
            P(),
            P("fsdp", "tp"),
            P("fsdp", "tp"),
            P("fsdp", "tp"),
            P("fsdp", "tp"),
            P(),
            P("fsdp", None),
            P("tp", "fsdp", None),
            P("tp", "fsdp", None),
            P("tp", "fsdp", None),
            P(("fsdp", "tp"), None),
        ),
        out_specs=(
            P(("fsdp", "tp"), None),
            P(("fsdp", "tp"), None),
            P(),
            P("fsdp", "tp"),
            P("fsdp", "tp"),
            P("fsdp", "tp"),
            P("fsdp", "tp"),
            P(),
            P("fsdp", None),
            P("tp", "fsdp", None),
            P("tp", "fsdp", None),
            P("tp", "fsdp", None),
        ),
        check_vma=False,
    )
```
